8 devices in a mesh: dp: 2 (over z, y), sp: 4 (over x, core).
Axes of the slice: x: 2, y: 2, z: 1, core: 2. Of those that a mesh axis runs over, the one named last changes fastest.
Arguments:
- tokens: bfloat16 [128, 2048], P('dp'), parts along dimension 0
- positions: int32 [128], P('dp'), parts along dimension 0
- k_cache: bfloat16 [128, 1024, 4, 128], P('dp', 'sp'), parts along dimension 0
- v_cache: bfloat16 [128, 1024, 4, 128], P('dp', 'sp'), parts along dimension 0
- w_q: bfloat16 [2048, 4096], replicated
- w_k: bfloat16 [2048, 512], replicated
- w_v: bfloat16 [2048, 512], replicated
- w_o: bfloat16 [4096, 2048], replicated
- attn_norm: bfloat16 [2048], replicated
- q_norm: bfloat16 [128], replicated
- k_norm: bfloat16 [128], replicated
Outputs:
- output 1: bfloat16 [128, 2048], P('dp'), parts along dimension 0
- output 2: bfloat16 [128, 1024, 4, 128], P('dp', 'sp'), parts along dimension 0
- output 3: bfloat16 [128, 1024, 4, 128], P('dp', 'sp'), parts along dimension 0
- output 4: bfloat16 [128, 2, 4, 128], P('dp'), parts along dimension 0
There are 2 independent parts. The reference program is written for one: setup_inputs(seed, part) draws one part's arguments, and reference() takes and returns one part's arrays. A program takes and returns all parts, laid end to end along the dimension named above; an argument that names none is the same for every part.
All inputs are finite; a program needn't handle non-finite values.
Results may differ from the reference program's by a relative error of at most 0.00658002.
Values sent between devices are 32-bit elements.
A program may use at most 1 GiB of HBM per device.

```python
import jax
import jax.numpy as jnp
from jax import lax

NUM_SEQS = 64
MODEL_DIM = 2048
Q_HEADS = 32
KV_HEADS = 4
HEAD_DIM = 128
CACHE_LEN = 1024

Q_PER_KV = Q_HEADS // KV_HEADS
NORM_EPS = 1e-6
ROPE_THETA = 1000000.0
NEG_FILL = -1e30


def setup_inputs(seed: int = 0, part: int = 0) -> dict:
    part_keys = jax.random.split(jax.random.fold_in(jax.random.key(seed), part), 5)
    shared = jax.random.split(jax.random.key(seed + 1), 7)
    cache_shape = (NUM_SEQS, CACHE_LEN, KV_HEADS, HEAD_DIM)
    tokens = jax.random.normal(part_keys[0], (NUM_SEQS, MODEL_DIM), jnp.float32)
    pos_draw = jax.random.randint(part_keys[1], (NUM_SEQS,), CACHE_LEN // 4, CACHE_LEN, dtype=jnp.int32)
    positions = pos_draw.at[0].set(CACHE_LEN - 1).at[1].set(CACHE_LEN // 4)
    k_cache = jax.random.normal(part_keys[2], cache_shape, jnp.float32)
    coarse = jax.random.normal(part_keys[3], (NUM_SEQS, 16, KV_HEADS, HEAD_DIM), jnp.float32)
    v_noise = jax.random.normal(part_keys[4], cache_shape, jnp.float32)
    v_cache = 1.5 * jnp.repeat(coarse, CACHE_LEN // 16, axis=1) + 0.5 * v_noise
    w_q = jax.random.normal(shared[0], (MODEL_DIM, Q_HEADS * HEAD_DIM), jnp.float32) * MODEL_DIM ** -0.5
    w_k = jax.random.normal(shared[1], (MODEL_DIM, KV_HEADS * HEAD_DIM), jnp.float32) * MODEL_DIM ** -0.5
    w_v = jax.random.normal(shared[2], (MODEL_DIM, KV_HEADS * HEAD_DIM), jnp.float32) * MODEL_DIM ** -0.5
    w_o = jax.random.normal(shared[3], (Q_HEADS * HEAD_DIM, MODEL_DIM), jnp.float32) * (Q_HEADS * HEAD_DIM) ** -0.5
    attn_norm = jax.random.uniform(shared[4], (MODEL_DIM,), jnp.float32, 0.5, 1.5)
    q_norm = jax.random.uniform(shared[5], (HEAD_DIM,), jnp.float32, 0.5, 2.0)
    k_norm = jax.random.uniform(shared[6], (HEAD_DIM,), jnp.float32, 0.5, 2.0)
    return {
        'tokens': tokens.astype(jnp.bfloat16),
        'positions': positions,
        'k_cache': k_cache.astype(jnp.bfloat16),
        'v_cache': v_cache.astype(jnp.bfloat16),
        'w_q': w_q.astype(jnp.bfloat16),
        'w_k': w_k.astype(jnp.bfloat16),
        'w_v': w_v.astype(jnp.bfloat16),
        'w_o': w_o.astype(jnp.bfloat16),
        'attn_norm': attn_norm.astype(jnp.bfloat16),
        'q_norm': q_norm.astype(jnp.bfloat16),
        'k_norm': k_norm.astype(jnp.bfloat16),
    }


def rms_scale(values, gain):
    return values * lax.rsqrt(jnp.mean(values * values, axis=-1, keepdims=True) + NORM_EPS) * gain.astype(jnp.float32)


def rope_table(positions):
    inv_freq = ROPE_THETA ** (-jnp.arange(HEAD_DIM // 2, dtype=jnp.float32) * 2.0 / HEAD_DIM)
    angles = positions.astype(jnp.float32)[:, None] * inv_freq[None, :]
    return jnp.cos(angles)[:, None, :], jnp.sin(angles)[:, None, :]


def norm_rope(proj, gain, cos_table, sin_table):
    normed = rms_scale(proj.astype(jnp.float32), gain)
    first_half = normed[..., :HEAD_DIM // 2]
    second_half = normed[..., HEAD_DIM // 2:]
    rotated = jnp.concatenate([first_half * cos_table - second_half * sin_table, second_half * cos_table + first_half * sin_table], axis=-1)
    return rotated.astype(jnp.bfloat16)


def reference(tokens, positions, k_cache, v_cache, w_q, w_k, w_v, w_o, attn_norm, q_norm, k_norm):
    tokens_f = tokens.astype(jnp.float32)
    hidden = rms_scale(tokens_f, attn_norm).astype(jnp.bfloat16)
    q_proj = jnp.dot(hidden, w_q, preferred_element_type=jnp.float32).astype(jnp.bfloat16).reshape(NUM_SEQS, Q_HEADS, HEAD_DIM)
    k_proj = jnp.dot(hidden, w_k, preferred_element_type=jnp.float32).astype(jnp.bfloat16).reshape(NUM_SEQS, KV_HEADS, HEAD_DIM)
    v_new = jnp.dot(hidden, w_v, preferred_element_type=jnp.float32).astype(jnp.bfloat16).reshape(NUM_SEQS, KV_HEADS, HEAD_DIM)
    cos_table, sin_table = rope_table(positions)
    q_rot = norm_rope(q_proj, q_norm, cos_table, sin_table)
    k_rot = norm_rope(k_proj, k_norm, cos_table, sin_table)
    slot_ids = jnp.arange(CACHE_LEN)
    write_mask = (slot_ids[None, :] == positions[:, None])[:, :, None, None]
    k_out = jnp.where(write_mask, k_rot[:, None], k_cache)
    v_out = jnp.where(write_mask, v_new[:, None], v_cache)
    score_scale = HEAD_DIM ** -0.5

    def one_seq(items):
        q_one, k_one, v_one, pos_one = items
        q_grp = q_one.reshape(KV_HEADS, Q_PER_KV, HEAD_DIM).astype(jnp.float32)
        scores = jnp.einsum('kgd,tkd->kgt', q_grp, k_one.astype(jnp.float32)) * score_scale
        live_mask = (slot_ids <= pos_one)[None, None, :]
        global_peak = jnp.max(jnp.where(live_mask, scores, NEG_FILL), axis=-1, keepdims=True)
        weights = jnp.where(live_mask, jnp.exp(scores - global_peak), 0.0)
        total_sum = jnp.sum(weights, axis=-1, keepdims=True)
        mixed = jnp.einsum('kgt,tkd->kgd', weights.astype(jnp.bfloat16).astype(jnp.float32), v_one.astype(jnp.float32))
        return (mixed / total_sum).astype(jnp.bfloat16).reshape(Q_HEADS * HEAD_DIM)

    attn_out = lax.map(one_seq, (q_rot, k_out, v_out, positions))
    block_out = (tokens_f + jnp.dot(attn_out, w_o, preferred_element_type=jnp.float32)).astype(jnp.bfloat16)
    new_kv = jnp.stack([k_rot, v_new], axis=1)
    return (block_out, k_out, v_out, new_kv)
```

```python
import functools

import jax
import jax.numpy as jnp
import numpy as np
from jax import lax
from jax.experimental import pallas as pl
from jax.experimental.pallas import tpu as pltpu
from jax.sharding import PartitionSpec as P

NORM_EPS = 1e-6
ROPE_THETA = 1000000.0
MESH = pl.DeviceIdType.MESH
BF16 = jnp.bfloat16
F32 = jnp.float32

SEQS = 64
DIM = 2048
HD = 128
KVH = 4
HALF = 16
SLOTS = 256
ROWS = SLOTS * KVH
BLK = 8
NBLK = SEQS // BLK
WCH = 512
PIECE = (HALF + 1) * BLK
VMEM_LIMIT = 26 * 2**20
EXP_SCALE = HD ** -0.5 * 1.4426950408889634
NEG = -jnp.inf


def bcast_col(tile, col):
    return jnp.broadcast_to(tile[:, col:col + 1], (tile.shape[0], HD))


def attend_kernel(pos_s, tok, aux, wq, wk, wv, wo, kc, vc,
                  kv, vv, rep, bout,
                  w_s, hid, ang, cosr, sinr, qmine, qmate, colslot, opart, drx, comb, xrx, ofin, pbuf, prx,
                  wsem, ksem, vsem, wosem, qs, qr, ds_, dr, xs, xr, ps, pr):
    me = lax.axis_index('sp')
    core = lax.rem(me, 2)
    chip = me // 2
    mate = {'sp': me + 1 - 2 * core}
    peer = {'sp': me + 2 - 4 * chip}

    def w_copy(n):
        if n < 4:
            src = wq.at[:, pl.ds(pl.multiple_of(core * (HALF * HD) + n * WCH, WCH), WCH)]
        else:
            src = (wk, wv)[n - 4]
        return pltpu.make_async_copy(src, w_s.at[n], wsem.at[n])

    def wo_copy(n):
        src = wo.at[pl.ds(pl.multiple_of(core * (HALF * HD), HD), HALF * HD), pl.ds(n * WCH, WCH)]
        return pltpu.make_async_copy(src, w_s.at[n], wosem.at[n])

    def k_copy(i):
        return pltpu.make_async_copy(kc.at[pl.ds(i * BLK, BLK)], kv.at[pl.ds(i * BLK, BLK)], ksem.at[i])

    def v_copy(i):
        return pltpu.make_async_copy(vc.at[pl.ds(i * BLK, BLK)], vv.at[pl.ds(i * BLK, BLK)], vsem.at[i])

    def q_send():
        return pltpu.make_async_remote_copy(qmine, qmate, qs, qr, device_id=mate, device_id_type=MESH)

    def d_send(i):
        return pltpu.make_async_remote_copy(opart.at[i, pl.ds(PIECE, PIECE)], drx.at[i], ds_.at[i], dr.at[i],
                                            device_id=mate, device_id_type=MESH)

    def x_send(i):
        return pltpu.make_async_remote_copy(comb.at[i], xrx.at[i], xs.at[i], xr.at[i],
                                            device_id=peer, device_id_type=MESH)

    def p_send(n):
        return pltpu.make_async_remote_copy(pbuf.at[n], prx.at[n], ps.at[n], pr.at[n],
                                            device_id=mate, device_id_type=MESH)

    for n in range(6):
        w_copy(n).start()

    barrier = pltpu.get_barrier_semaphore()
    for other in (mate, peer):
        pl.semaphore_signal(barrier, inc=1, device_id=other, device_id_type=MESH)

    t = tok[...].astype(F32)
    inv = lax.rsqrt(jnp.sum(t * t, axis=-1, keepdims=True) * (1.0 / DIM) + NORM_EPS)
    for j in range(DIM // HD):
        sl = slice(j * HD, (j + 1) * HD)
        hid[:, sl] = (tok[:, sl].astype(F32) * inv * aux[j:j + 1, :]).astype(BF16)

    lane1 = lax.broadcasted_iota(jnp.int32, (1, HD), 1)
    freq = aux[DIM // HD + 2:DIM // HD + 3, :]

    def angle(b, carry):
        ang[pl.ds(b, 1), :] = freq * pos_s[b].astype(F32)
        return carry

    lax.fori_loop(0, SEQS, angle, 0)
    cosr[...] = jnp.cos(ang[...])
    sinr[...] = jnp.sin(ang[...]) * jnp.where(lane1 < HD // 2, -1.0, 1.0)

    row = lax.broadcasted_iota(jnp.int32, (2 * HALF, ROWS), 0)
    col = lax.broadcasted_iota(jnp.int32, (2 * HALF, ROWS), 1)
    half_of_row = jnp.where(row < HALF, core, 1 - core)
    kv_of_row = half_of_row * 2 + lax.rem(row, HALF) // 8
    colslot[...] = jnp.where(lax.rem(col, KVH) == kv_of_row, col // KVH, 1 << 20)

    qgain = aux[DIM // HD:DIM // HD + 1, :]
    kgain = aux[DIM // HD + 1:DIM // HD + 2, :]

    def norm_rope(x, gain):
        y = x * lax.rsqrt(jnp.mean(x * x, axis=-1, keepdims=True) + NORM_EPS) * gain
        y = y * cosr[...] + pltpu.roll(y, HD // 2, 1) * sinr[...]
        return y.astype(BF16).astype(F32)

    for n in range(6):
        w_copy(n).wait()
        k_copy(n).start()
        v_copy(n).start()
        proj = jnp.dot(hid[...], w_s[n], preferred_element_type=F32).astype(BF16).astype(F32)
        for j in range(WCH // HD):
            x = proj[:, j * HD:(j + 1) * HD]
            if n < 4:
                qmine[pl.ds(n * 4 + j, SEQS, stride=HALF), :] = norm_rope(x, qgain)
            else:
                y = norm_rope(x, kgain) if n == 4 else x
                for c in range(4):
                    rep[n - 4, pl.ds(c * KVH + j, SEQS, stride=4 * KVH), :] = y
        if n == 4:
            pl.semaphore_wait(barrier, 2)
            q_send().start()
    for i in range(6, NBLK):
        k_copy(i).start()
        v_copy(i).start()
    for n in range(4):
        wo_copy(n).start()
    start = me * SLOTS
    lane = lax.broadcasted_iota(jnp.int32, (HALF, HD), 1)
    lrow = lax.broadcasted_iota(jnp.int32, (HALF, HD), 0)
    lane8 = lax.broadcasted_iota(jnp.int32, (BLK, HD), 1)
    q_send().wait()

    def attend(i):
        k_copy(i).wait()
        v_copy(i).wait()
        ob = opart.at[i]
        for pair in range(BLK // 2):
            bs = [i * BLK + 2 * pair + z for z in range(2)]
            qf = [jnp.concatenate([qmine[pl.ds(pl.multiple_of(b * HALF, HALF), HALF), :],
                                   qmate[pl.ds(pl.multiple_of(b * HALF, HALF), HALF), :]], axis=0) for b in bs]
            zero = jnp.zeros((2 * HALF, HD), BF16)
            lhs = jnp.concatenate([jnp.concatenate([qf[0].astype(BF16), zero], axis=1),
                                   jnp.concatenate([zero, qf[1].astype(BF16)], axis=1)], axis=0)
            keys = jnp.concatenate([kv[bs[0]], kv[bs[1]]], axis=1)
            s = lax.dot_general(lhs, keys, (((1,), (1,)), ((), ())), preferred_element_type=F32)
            probs, extra, sums, peaks = [], [], [], []
            for z in range(2):
                b = bs[z]
                rel = pos_s[b] - start
                owner = jnp.logical_and(rel >= 0, rel < SLOTS)
                knew = jnp.concatenate(
                    [jnp.broadcast_to(rep[0, pl.ds(b * 4 * KVH + h, 1), :], (8, HD))
                     for h in (2 * core, 2 * core + 1, 2 - 2 * core, 3 - 2 * core)], axis=0)
                snew = jnp.sum(qf[z] * knew, axis=-1, keepdims=True)
                snew = jnp.where(owner, snew, NEG)
                sm = jnp.where(colslot[...] < rel, s[z * 2 * HALF:(z + 1) * 2 * HALF], NEG)
                peak = jnp.maximum(jnp.max(sm, axis=-1, keepdims=True), snew)
                safe = jnp.where(peak == NEG, 0.0, peak)
                p = jnp.exp2((sm - safe) * EXP_SCALE)
                pn = jnp.exp2((snew - safe) * EXP_SCALE)
                probs.append(p.astype(BF16))
                extra.append(pn.astype(BF16).astype(F32))
                sums.append(jnp.sum(p, axis=-1, keepdims=True) + pn)
                peaks.append(peak)
            values = jnp.concatenate([vv[bs[0]], vv[bs[1]]], axis=1)
            mixed = jnp.dot(jnp.concatenate(probs, axis=0), values, preferred_element_type=F32)
            for z in range(2):
                b = bs[z]
                vnew = jnp.concatenate(
                    [jnp.broadcast_to(rep[1, pl.ds(b * 4 * KVH + h, 1), :], (8, HD))
                     for h in (2 * core, 2 * core + 1, 2 - 2 * core, 3 - 2 * core)], axis=0)
                o = mixed[z * 2 * HALF:(z + 1) * 2 * HALF, z * HD:(z + 1) * HD] + extra[z] * vnew
                bb = 2 * pair + z
                for h in range(2):
                    hs = slice(h * HALF, (h + 1) * HALF)
                    ob[pl.ds(h * PIECE + bb, HALF, stride=BLK), :] = o[hs]
                    st = jnp.where(lane == lrow, peaks[z][hs], jnp.where(lane == lrow + HALF, sums[z][hs], 0.0))
                    ob[pl.ds(h * PIECE + HALF * BLK + bb, 1), :] = jnp.sum(st, axis=0, keepdims=True)

    def combine(i):
        d_send(i).wait_recv()
        s0 = opart[i, pl.ds(HALF * BLK, BLK), :]
        s1 = drx[i, pl.ds(HALF * BLK, BLK), :]
        peak = jnp.maximum(s0, s1)
        safe = jnp.where(peak == NEG, 0.0, peak)
        f0 = jnp.exp2((s0 - safe) * EXP_SCALE)
        f1 = jnp.exp2((s1 - safe) * EXP_SCALE)
        total = f0 * pltpu.roll(s0, HD - HALF, 1) + f1 * pltpu.roll(s1, HD - HALF, 1)
        comb[i, pl.ds(HALF * BLK, BLK), :] = jnp.where(
            lane8 < HALF, peak, jnp.where(lane8 < 2 * HALF, pltpu.roll(total, HALF, 1), 0.0))
        for j in range(HALF):
            rows = pl.ds(j * BLK, BLK)
            comb[i, rows, :] = bcast_col(f0, j) * opart[i, rows, :] + bcast_col(f1, j) * drx[i, rows, :]

    def finish(i):
        x_send(i).wait_recv()
        first = chip == 0

        def ordered(rows):
            mine, other = comb[i, rows, :], xrx[i, rows, :]
            return jnp.where(first, mine, other), jnp.where(first, other, mine)

        s0, s1 = ordered(pl.ds(HALF * BLK, BLK))
        peak = jnp.maximum(s0, s1)
        f0 = jnp.exp2((s0 - peak) * EXP_SCALE)
        f1 = jnp.exp2((s1 - peak) * EXP_SCALE)
        total = f0 * pltpu.roll(s0, HD - HALF, 1) + f1 * pltpu.roll(s1, HD - HALF, 1)
        g0, g1 = f0 / total, f1 / total
        for j in range(HALF):
            a, b = ordered(pl.ds(j * BLK, BLK))
            ofin[pl.ds(pl.multiple_of(i * BLK, BLK), BLK), j * HD:(j + 1) * HD] = bcast_col(g0, j) * a + bcast_col(g1, j) * b

    def step(i, carry):
        @pl.when(i < NBLK)
        def _():
            attend(i)

        @pl.when(jnp.logical_and(i >= 1, i < NBLK + 1))
        def _():
            combine(i - 1)

        @pl.when(i < NBLK)
        def _():
            d_send(i).start()

        @pl.when(i >= 3)
        def _():
            finish(i - 3)

        @pl.when(jnp.logical_and(i >= 1, i < NBLK + 1))
        def _():
            x_send(i - 1).start()

        return carry

    lax.fori_loop(0, NBLK + 3, step, 0)

    lhs = ofin[...].astype(BF16)
    for n in range(4):
        wo_copy(n).wait()
        pbuf[n] = jnp.dot(lhs, w_s[n], preferred_element_type=F32)
        p_send(n).start()
    for n in range(4):
        p_send(n).wait_recv()
        sl = slice(n * WCH, (n + 1) * WCH)
        bout[:, sl] = (tok[:, sl].astype(F32) + (pbuf[n] + prx[n])).astype(BF16)

    def drain(i, carry):
        d_send(i).wait_send()
        x_send(i).wait_send()
        return carry

    lax.fori_loop(0, NBLK, drain, 0)
    for n in range(4):
        p_send(n).wait_send()


def write_kernel(pos_s, kv, vv, rep, bin_, ko, vo, bo, nkv, kva, vva, ksem, vsem):
    start = lax.axis_index('sp') * SLOTS
    slot16 = lax.broadcasted_iota(jnp.int32, (4 * KVH, HD), 0) // KVH

    def put(i):
        for bb in range(BLK):
            b = i * BLK + bb
            rel = pos_s[b] - start

            @pl.when(jnp.logical_and(rel >= 0, rel < SLOTS))
            def _():
                base = pl.multiple_of(rel // 4 * (4 * KVH), 4 * KVH)
                mask = slot16 == lax.rem(rel, 4)
                for z, ref in enumerate((kv, vv)):
                    new = rep[z, pl.ds(b * 4 * KVH, 4 * KVH), :]
                    old = ref[b, pl.ds(base, 4 * KVH), :].astype(F32)
                    ref[b, pl.ds(base, 4 * KVH), :] = jnp.where(mask, new, old).astype(BF16)

    def copies(i):
        r = pl.ds(i * BLK, BLK)
        return (pltpu.make_async_copy(kv.at[r], ko.at[r], ksem.at[i]),
                pltpu.make_async_copy(vv.at[r], vo.at[r], vsem.at[i]))

    for i in range(NBLK + 1):
        if i < NBLK:
            put(i)
        if i > 0:
            for c in copies(i - 1):
                c.start()
    bo[...] = bin_[...]
    for b in range(SEQS):
        nkv[b] = jnp.concatenate([rep[0, pl.ds(b * 4 * KVH, KVH), :], rep[1, pl.ds(b * 4 * KVH, KVH), :]], axis=0).astype(BF16)
    for i in range(NBLK):
        for c in copies(i):
            c.wait()


def solution(mesh):
    cache_spec = P('dp', 'sp', None, None)
    inv_freq = (np.float64(ROPE_THETA) ** (-np.arange(HD // 2) * 2.0 / HD)).astype(np.float32)
    freq2 = np.concatenate([inv_freq, inv_freq])
    vm = pl.BlockSpec(memory_space=pltpu.VMEM)
    hbm = pl.BlockSpec(memory_space=pl.ANY)
    sm = pl.BlockSpec(memory_space=pltpu.SMEM)
    dma = pltpu.SemaphoreType.DMA

    def device_step(tokens, positions, k_cache, v_cache, w_q, w_k, w_v, w_o, attn_norm, q_norm, k_norm):
        aux = jnp.concatenate([attn_norm.astype(F32), q_norm.astype(F32), k_norm.astype(F32), freq2,
                               jnp.zeros((5 * HD,), F32)]).reshape(24, HD)
        in_hbm = lambda x: pltpu.with_memory_space_constraint(x, pltpu.HBM)
        in_vmem = lambda x: pltpu.with_memory_space_constraint(x, pltpu.VMEM)
        rows = (SEQS, ROWS, HD)
        kv, vv, rep, bout = pl.pallas_call(
            attend_kernel,
            out_shape=(pltpu.VMEM(rows, BF16), pltpu.VMEM(rows, BF16),
                       pltpu.VMEM((2, SEQS * 4 * KVH, HD), F32), pltpu.VMEM((SEQS, DIM), BF16)),
            in_specs=[sm, vm, vm] + [hbm] * 6,
            out_specs=(vm, vm, vm, vm),
            scratch_shapes=[
                pltpu.VMEM((6, DIM, WCH), BF16),
                pltpu.VMEM((SEQS, DIM), BF16),
                pltpu.VMEM((SEQS, HD), F32), pltpu.VMEM((SEQS, HD), F32), pltpu.VMEM((SEQS, HD), F32),
                pltpu.VMEM((SEQS * HALF, HD), F32), pltpu.VMEM((SEQS * HALF, HD), F32),
                pltpu.VMEM((2 * HALF, ROWS), jnp.int32),
                pltpu.VMEM((NBLK, 2 * PIECE, HD), F32),
                pltpu.VMEM((NBLK, PIECE, HD), F32), pltpu.VMEM((NBLK, PIECE, HD), F32), pltpu.VMEM((NBLK, PIECE, HD), F32),
                pltpu.VMEM((SEQS, HALF * HD), F32),
                pltpu.VMEM((4, SEQS, WCH), F32), pltpu.VMEM((4, SEQS, WCH), F32),
                dma((6,)), dma((NBLK,)), dma((NBLK,)), dma((4,)), dma, dma,
                dma((NBLK,)), dma((NBLK,)), dma((NBLK,)), dma((NBLK,)), dma((4,)), dma((4,)),
            ],
            compiler_params=pltpu.CompilerParams(collective_id=0, has_side_effects=True, vmem_limit_bytes=VMEM_LIMIT),
            name='attend',
        )(positions, tokens, aux, in_hbm(w_q), in_hbm(w_k), in_hbm(w_v), in_hbm(w_o),
          in_hbm(k_cache.reshape(rows)), in_hbm(v_cache.reshape(rows)))
        k_out, v_out, block_out, new_kv, _, _ = pl.pallas_call(
            write_kernel,
            out_shape=(pltpu.HBM(rows, BF16), pltpu.HBM(rows, BF16), jax.ShapeDtypeStruct((SEQS, DIM), BF16),
                       jax.ShapeDtypeStruct((SEQS, 2 * KVH, HD), BF16), pltpu.VMEM(rows, BF16), pltpu.VMEM(rows, BF16)),
            in_specs=[sm, vm, vm, vm, vm],
            out_specs=(hbm, hbm, vm, vm, vm, vm),
            input_output_aliases={1: 4, 2: 5},
            scratch_shapes=[dma((NBLK,)), dma((NBLK,))],
            compiler_params=pltpu.CompilerParams(vmem_limit_bytes=VMEM_LIMIT),
            name='write',
        )(positions, in_vmem(kv), in_vmem(vv), in_vmem(rep), in_vmem(bout))
        return block_out, k_out.reshape(k_cache.shape), v_out.reshape(v_cache.shape), new_kv.reshape(SEQS, 2, KVH, HD)

    return jax.shard_map(device_step, mesh=mesh, in_specs=(P('dp', None), P('dp'), cache_spec, cache_spec, P(), P(), P(), P(), P(), P(), P()), out_specs=(P('dp', None), cache_spec, cache_spec, P('dp', None, None, None)), check_vma=False)
```

```python
import functools

import jax
import jax.numpy as jnp
import numpy as np
from jax import lax
from jax.experimental import pallas as pl
from jax.experimental.pallas import tpu as pltpu
from jax.sharding import PartitionSpec as P

NORM_EPS = 1e-6
ROPE_THETA = 1000000.0
MESH = pl.DeviceIdType.MESH
BF16 = jnp.bfloat16
F32 = jnp.float32

SEQS = 64
DIM = 2048
HD = 128
KVH = 4
HALF = 16
SLOTS = 256
ROWS = SLOTS * KVH
BLK = 8
NBLK = SEQS // BLK
LAG = 6
WCH = 512
PIECE = (HALF + 1) * BLK
VMEM_LIMIT = 26 * 2**20
EXP_SCALE = HD ** -0.5 * 1.4426950408889634
NEG = -jnp.inf


def bcast_col(tile, col):
    return jnp.broadcast_to(tile[:, col:col + 1], (tile.shape[0], HD))


def attend_kernel(pos_h, tok_h, an_h, qn_h, kn_h, freq_h, wq, wk, wv, wo, kc, vc,
                  kv, vv, rep, bout,
                  pos_s, tok, an, qn, kn, freq, insem, w_s, hid, ang, cosr, sinr, qmine, qmate, colslot, opart, drx, comb, xrx, ofin, pbuf, prx,
                  wsem, ksem, vsem, wosem, qs, qr, ds_, dr, xs, xr, ps, pr):
    me = lax.axis_index('sp')
    core = lax.rem(me, 2)
    chip = me // 2
    mate = {'sp': me + 1 - 2 * core}
    peer = {'sp': me + 2 - 4 * chip}

    def w_copy(n):
        if n < 4:
            src = wq.at[:, pl.ds(pl.multiple_of(core * (HALF * HD) + n * WCH, WCH), WCH)]
        else:
            src = (wk, wv)[n - 4]
        return pltpu.make_async_copy(src, w_s.at[n], wsem.at[n])

    def wo_copy(n):
        src = wo.at[pl.ds(pl.multiple_of(core * (HALF * HD), HD), HALF * HD), pl.ds(n * WCH, WCH)]
        return pltpu.make_async_copy(src, w_s.at[n], wosem.at[n])

    def k_copy(i):
        return pltpu.make_async_copy(kc.at[pl.ds(i * BLK, BLK)], kv.at[pl.ds(i * BLK, BLK)], ksem.at[i])

    def v_copy(i):
        return pltpu.make_async_copy(vc.at[pl.ds(i * BLK, BLK)], vv.at[pl.ds(i * BLK, BLK)], vsem.at[i])

    def q_send():
        return pltpu.make_async_remote_copy(qmine, qmate, qs, qr, device_id=mate, device_id_type=MESH)

    def d_send(i):
        return pltpu.make_async_remote_copy(opart.at[i, pl.ds(PIECE, PIECE)], drx.at[i], ds_.at[i], dr.at[i],
                                            device_id=mate, device_id_type=MESH)

    def x_send(i):
        return pltpu.make_async_remote_copy(comb.at[i], xrx.at[i], xs.at[i], xr.at[i],
                                            device_id=peer, device_id_type=MESH)

    def p_send(n):
        return pltpu.make_async_remote_copy(pbuf.at[n], prx.at[n], ps.at[n], pr.at[n],
                                            device_id=mate, device_id_type=MESH)

    small = [pltpu.make_async_copy(a, b, insem.at[z]) for z, (a, b) in enumerate(
        ((tok_h, tok), (pos_h, pos_s), (an_h, an), (qn_h, qn), (kn_h, kn), (freq_h, freq)))]
    for c in small:
        c.start()
    for n in range(6):
        w_copy(n).start()

    barrier = pltpu.get_barrier_semaphore()
    for other in (mate, peer):
        pl.semaphore_signal(barrier, inc=1, device_id=other, device_id_type=MESH)

    for c in small:
        c.wait()

    t = tok[...].astype(F32)
    inv = lax.rsqrt(jnp.sum(t * t, axis=-1, keepdims=True) * (1.0 / DIM) + NORM_EPS)
    gains = an[...].astype(F32)
    for j in range(DIM // HD):
        sl = slice(j * HD, (j + 1) * HD)
        hid[:, sl] = (tok[:, sl].astype(F32) * inv * gains[j:j + 1, :]).astype(BF16)

    lane1 = lax.broadcasted_iota(jnp.int32, (1, HD), 1)

    def angle(b, carry):
        ang[pl.ds(b, 1), :] = freq[...] * pos_s[b].astype(F32)
        return carry

    lax.fori_loop(0, SEQS, angle, 0)
    cosr[...] = jnp.cos(ang[...])
    sinr[...] = jnp.sin(ang[...]) * jnp.where(lane1 < HD // 2, -1.0, 1.0)

    row = lax.broadcasted_iota(jnp.int32, (2 * HALF, ROWS), 0)
    col = lax.broadcasted_iota(jnp.int32, (2 * HALF, ROWS), 1)
    half_of_row = jnp.where(row < HALF, core, 1 - core)
    kv_of_row = half_of_row * 2 + lax.rem(row, HALF) // 8
    colslot[...] = jnp.where(lax.rem(col, KVH) == kv_of_row, col // KVH, 1 << 20)

    qgain = qn[...].astype(F32)
    kgain = kn[...].astype(F32)

    def norm_rope(x, gain):
        y = x * lax.rsqrt(jnp.mean(x * x, axis=-1, keepdims=True) + NORM_EPS) * gain
        y = y * cosr[...] + pltpu.roll(y, HD // 2, 1) * sinr[...]
        return y.astype(BF16).astype(F32)

    for n in range(6):
        w_copy(n).wait()
        k_copy(n).start()
        v_copy(n).start()
        proj = jnp.dot(hid[...], w_s[n], preferred_element_type=F32).astype(BF16).astype(F32)
        for j in range(WCH // HD):
            x = proj[:, j * HD:(j + 1) * HD]
            if n < 4:
                qmine[pl.ds(n * 4 + j, SEQS, stride=HALF), :] = norm_rope(x, qgain)
            else:
                y = norm_rope(x, kgain) if n == 4 else x
                for c in range(4):
                    rep[n - 4, pl.ds(c * KVH + j, SEQS, stride=4 * KVH), :] = y
        if n == 3:
            pl.semaphore_wait(barrier, 2)
            q_send().start()
    for i in range(6, NBLK):
        k_copy(i).start()
        v_copy(i).start()
    for n in range(4):
        wo_copy(n).start()
    start = me * SLOTS
    lane = lax.broadcasted_iota(jnp.int32, (HALF, HD), 1)
    lrow = lax.broadcasted_iota(jnp.int32, (HALF, HD), 0)
    lane8 = lax.broadcasted_iota(jnp.int32, (BLK, HD), 1)
    q_send().wait()

    def attend(i):
        k_copy(i).wait()
        v_copy(i).wait()
        ob = opart.at[i]
        for pair in range(BLK // 2):
            bs = [i * BLK + 2 * pair + z for z in range(2)]
            qf = [jnp.concatenate([qmine[pl.ds(pl.multiple_of(b * HALF, HALF), HALF), :],
                                   qmate[pl.ds(pl.multiple_of(b * HALF, HALF), HALF), :]], axis=0) for b in bs]
            zero = jnp.zeros((2 * HALF, HD), BF16)
            lhs = jnp.concatenate([jnp.concatenate([qf[0].astype(BF16), zero], axis=1),
                                   jnp.concatenate([zero, qf[1].astype(BF16)], axis=1)], axis=0)
            keys = jnp.concatenate([kv[bs[0]], kv[bs[1]]], axis=1)
            s = lax.dot_general(lhs, keys, (((1,), (1,)), ((), ())), preferred_element_type=F32)
            probs, extra, sums, peaks = [], [], [], []
            for z in range(2):
                b = bs[z]
                rel = pos_s[b] - start
                owner = jnp.logical_and(rel >= 0, rel < SLOTS)
                knew = jnp.concatenate(
                    [jnp.broadcast_to(rep[0, pl.ds(b * 4 * KVH + h, 1), :], (8, HD))
                     for h in (2 * core, 2 * core + 1, 2 - 2 * core, 3 - 2 * core)], axis=0)
                snew = jnp.sum(qf[z] * knew, axis=-1, keepdims=True)
                snew = jnp.where(owner, snew, NEG)
                sm = jnp.where(colslot[...] < rel, s[z * 2 * HALF:(z + 1) * 2 * HALF], NEG)
                peak = jnp.maximum(jnp.max(sm, axis=-1, keepdims=True), snew)
                safe = jnp.where(peak == NEG, 0.0, peak)
                p = jnp.exp2((sm - safe) * EXP_SCALE)
                pn = jnp.exp2((snew - safe) * EXP_SCALE)
                probs.append(p.astype(BF16))
                extra.append(pn.astype(BF16).astype(F32))
                sums.append(jnp.sum(p, axis=-1, keepdims=True) + pn)
                peaks.append(peak)
            values = jnp.concatenate([vv[bs[0]], vv[bs[1]]], axis=1)
            mixed = jnp.dot(jnp.concatenate(probs, axis=0), values, preferred_element_type=F32)
            for z in range(2):
                b = bs[z]
                vnew = jnp.concatenate(
                    [jnp.broadcast_to(rep[1, pl.ds(b * 4 * KVH + h, 1), :], (8, HD))
                     for h in (2 * core, 2 * core + 1, 2 - 2 * core, 3 - 2 * core)], axis=0)
                o = mixed[z * 2 * HALF:(z + 1) * 2 * HALF, z * HD:(z + 1) * HD] + extra[z] * vnew
                bb = 2 * pair + z
                for h in range(2):
                    hs = slice(h * HALF, (h + 1) * HALF)
                    ob[pl.ds(h * PIECE + bb, HALF, stride=BLK), :] = o[hs]
                    st = jnp.where(lane == lrow, peaks[z][hs], jnp.where(lane == lrow + HALF, sums[z][hs], 0.0))
                    ob[pl.ds(h * PIECE + HALF * BLK + bb, 1), :] = jnp.sum(st, axis=0, keepdims=True)

    def combine(i):
        d_send(i).wait_recv()
        s0 = opart[i, pl.ds(HALF * BLK, BLK), :]
        s1 = drx[i, pl.ds(HALF * BLK, BLK), :]
        peak = jnp.maximum(s0, s1)
        safe = jnp.where(peak == NEG, 0.0, peak)
        f0 = jnp.exp2((s0 - safe) * EXP_SCALE)
        f1 = jnp.exp2((s1 - safe) * EXP_SCALE)
        total = f0 * pltpu.roll(s0, HD - HALF, 1) + f1 * pltpu.roll(s1, HD - HALF, 1)
        comb[i, pl.ds(HALF * BLK, BLK), :] = jnp.where(
            lane8 < HALF, peak, jnp.where(lane8 < 2 * HALF, pltpu.roll(total, HALF, 1), 0.0))
        for j in range(HALF):
            rows = pl.ds(j * BLK, BLK)
            comb[i, rows, :] = bcast_col(f0, j) * opart[i, rows, :] + bcast_col(f1, j) * drx[i, rows, :]

    def finish(i):
        x_send(i).wait_recv()
        first = chip == 0

        def ordered(rows):
            mine, other = comb[i, rows, :], xrx[i, rows, :]
            return jnp.where(first, mine, other), jnp.where(first, other, mine)

        s0, s1 = ordered(pl.ds(HALF * BLK, BLK))
        peak = jnp.maximum(s0, s1)
        f0 = jnp.exp2((s0 - peak) * EXP_SCALE)
        f1 = jnp.exp2((s1 - peak) * EXP_SCALE)
        total = f0 * pltpu.roll(s0, HD - HALF, 1) + f1 * pltpu.roll(s1, HD - HALF, 1)
        g0, g1 = f0 / total, f1 / total
        for j in range(HALF):
            a, b = ordered(pl.ds(j * BLK, BLK))
            ofin[pl.ds(pl.multiple_of(i * BLK, BLK), BLK), j * HD:(j + 1) * HD] = bcast_col(g0, j) * a + bcast_col(g1, j) * b

    def step(i, carry):
        @pl.when(i < NBLK)
        def _():
            attend(i)

        @pl.when(jnp.logical_and(i >= 1, i < NBLK + 1))
        def _():
            combine(i - 1)

        @pl.when(i < NBLK)
        def _():
            d_send(i).start()

        @pl.when(i >= LAG)
        def _():
            finish(i - LAG)

        @pl.when(jnp.logical_and(i >= 1, i < NBLK + 1))
        def _():
            x_send(i - 1).start()

        return carry

    lax.fori_loop(0, NBLK + LAG, step, 0)

    lhs = ofin[...].astype(BF16)
    for n in range(4):
        wo_copy(n).wait()
        pbuf[n] = jnp.dot(lhs, w_s[n], preferred_element_type=F32)
        p_send(n).start()
    for n in range(4):
        p_send(n).wait_recv()
        sl = slice(n * WCH, (n + 1) * WCH)
        bout[:, sl] = (tok[:, sl].astype(F32) + (pbuf[n] + prx[n])).astype(BF16)

    def drain(i, carry):
        d_send(i).wait_send()
        x_send(i).wait_send()
        return carry

    lax.fori_loop(0, NBLK, drain, 0)
    for n in range(4):
        p_send(n).wait_send()


def write_kernel(pos_h, kv, vv, rep, bin_, ko, vo, bo, nkv, kva, vva, pos_s, nkv_s, patch, ksem, vsem, psem, osem):
    start = lax.axis_index('sp') * SLOTS
    slot16 = lax.broadcasted_iota(jnp.int32, (4 * KVH, HD), 0) // KVH

    def copies(i):
        r = pl.ds(i * BLK, BLK)
        return (pltpu.make_async_copy(kv.at[r], ko.at[r], ksem.at[i]),
                pltpu.make_async_copy(vv.at[r], vo.at[r], vsem.at[i]))

    pos_copy = pltpu.make_async_copy(pos_h, pos_s, osem.at[0])
    pos_copy.start()
    out_copy = pltpu.make_async_copy(bin_, bo, osem.at[1])
    out_copy.start()
    for c in copies(0):
        c.start()
    for b in range(SEQS):
        nkv_s[b] = jnp.concatenate([rep[0, pl.ds(b * 4 * KVH, KVH), :], rep[1, pl.ds(b * 4 * KVH, KVH), :]], axis=0).astype(BF16)
    pos_copy.wait()

    def each(i, do):
        for bb in range(BLK):
            b = i * BLK + bb
            rel = pos_s[b] - start

            @pl.when(jnp.logical_and(rel >= 0, rel < SLOTS))
            def _():
                base = pl.multiple_of(rel // 4 * (4 * KVH), 4 * KVH)
                mask = slot16 == lax.rem(rel, 4)
                for z, (ref, out) in enumerate(((kv, ko), (vv, vo))):
                    do(b, z, base, mask, ref, out)

    def merged(b, z, base, mask, ref):
        new = rep[z, pl.ds(b * 4 * KVH, 4 * KVH), :]
        old = ref[b, pl.ds(base, 4 * KVH), :].astype(F32)
        return jnp.where(mask, new, old).astype(BF16)

    def put(b, z, base, mask, ref, out):
        ref[b, pl.ds(base, 4 * KVH), :] = merged(b, z, base, mask, ref)

    def stage(b, z, base, mask, ref, out):
        patch[z, b] = merged(b, z, base, mask, ref)

    def patch_copy(b, z, base, out):
        return pltpu.make_async_copy(patch.at[z, b], out.at[b, pl.ds(base, 4 * KVH)], psem.at[z, b])

    for i in range(1, NBLK):
        each(i, put)
        if i > 1:
            for c in copies(i - 1):
                c.start()
    nkv_copy = pltpu.make_async_copy(nkv_s, nkv, osem.at[2])
    nkv_copy.start()
    each(0, stage)
    for c in copies(NBLK - 1):
        c.start()
    for c in copies(0):
        c.wait()
    each(0, lambda b, z, base, mask, ref, out: patch_copy(b, z, base, out).start())
    out_copy.wait()
    nkv_copy.wait()
    each(0, lambda b, z, base, mask, ref, out: patch_copy(b, z, base, out).wait())
    for i in range(1, NBLK):
        for c in copies(i):
            c.wait()


def solution(mesh):
    cache_spec = P('dp', 'sp', None, None)
    inv_freq = (np.float64(ROPE_THETA) ** (-np.arange(HD // 2) * 2.0 / HD)).astype(np.float32)
    freq2 = np.concatenate([inv_freq, inv_freq])
    vm = pl.BlockSpec(memory_space=pltpu.VMEM)
    hbm = pl.BlockSpec(memory_space=pl.ANY)
    dma = pltpu.SemaphoreType.DMA

    def device_step(tokens, positions, k_cache, v_cache, w_q, w_k, w_v, w_o, attn_norm, q_norm, k_norm):
        in_hbm = lambda x: pltpu.with_memory_space_constraint(x, pltpu.HBM)
        in_vmem = lambda x: pltpu.with_memory_space_constraint(x, pltpu.VMEM)
        rows = (SEQS, ROWS, HD)
        kv, vv, rep, bout = pl.pallas_call(
            attend_kernel,
            out_shape=(pltpu.VMEM(rows, BF16), pltpu.VMEM(rows, BF16),
                       pltpu.VMEM((2, SEQS * 4 * KVH, HD), F32), pltpu.VMEM((SEQS, DIM), BF16)),
            in_specs=[hbm] * 12,
            out_specs=(vm, vm, vm, vm),
            scratch_shapes=[
                pltpu.SMEM((SEQS,), jnp.int32), pltpu.VMEM((SEQS, DIM), BF16), pltpu.VMEM((DIM // HD, HD), BF16),
                pltpu.VMEM((1, HD), BF16), pltpu.VMEM((1, HD), BF16), pltpu.VMEM((1, HD), F32), dma((6,)),
                pltpu.VMEM((6, DIM, WCH), BF16),
                pltpu.VMEM((SEQS, DIM), BF16),
                pltpu.VMEM((SEQS, HD), F32), pltpu.VMEM((SEQS, HD), F32), pltpu.VMEM((SEQS, HD), F32),
                pltpu.VMEM((SEQS * HALF, HD), F32), pltpu.VMEM((SEQS * HALF, HD), F32),
                pltpu.VMEM((2 * HALF, ROWS), jnp.int32),
                pltpu.VMEM((NBLK, 2 * PIECE, HD), F32),
                pltpu.VMEM((NBLK, PIECE, HD), F32), pltpu.VMEM((NBLK, PIECE, HD), F32), pltpu.VMEM((NBLK, PIECE, HD), F32),
                pltpu.VMEM((SEQS, HALF * HD), F32),
                pltpu.VMEM((4, SEQS, WCH), F32), pltpu.VMEM((4, SEQS, WCH), F32),
                dma((6,)), dma((NBLK,)), dma((NBLK,)), dma((4,)), dma, dma,
                dma((NBLK,)), dma((NBLK,)), dma((NBLK,)), dma((NBLK,)), dma((4,)), dma((4,)),
            ],
            compiler_params=pltpu.CompilerParams(collective_id=0, has_side_effects=True, vmem_limit_bytes=VMEM_LIMIT),
            name='attend',
        )(in_hbm(positions), in_hbm(tokens), in_hbm(attn_norm.reshape(DIM // HD, HD)), in_hbm(q_norm.reshape(1, HD)),
          in_hbm(k_norm.reshape(1, HD)), in_hbm(jnp.asarray(freq2).reshape(1, HD)), in_hbm(w_q), in_hbm(w_k), in_hbm(w_v), in_hbm(w_o),
          in_hbm(k_cache.reshape(rows)), in_hbm(v_cache.reshape(rows)))
        k_out, v_out, block_out, new_kv, _, _ = pl.pallas_call(
            write_kernel,
            out_shape=(pltpu.HBM(rows, BF16), pltpu.HBM(rows, BF16), pltpu.HBM((SEQS, DIM), BF16),
                       pltpu.HBM((SEQS, 2 * KVH, HD), BF16), pltpu.VMEM(rows, BF16), pltpu.VMEM(rows, BF16)),
            in_specs=[hbm, vm, vm, vm, vm],
            out_specs=(hbm, hbm, hbm, hbm, vm, vm),
            input_output_aliases={1: 4, 2: 5},
            scratch_shapes=[pltpu.SMEM((SEQS,), jnp.int32), pltpu.VMEM((SEQS, 2 * KVH, HD), BF16),
                            pltpu.VMEM((2, BLK, 4 * KVH, HD), BF16),
                            dma((NBLK,)), dma((NBLK,)), dma((2, BLK)), dma((3,))],
            compiler_params=pltpu.CompilerParams(vmem_limit_bytes=VMEM_LIMIT),
            name='write',
        )(in_hbm(positions), in_vmem(kv), in_vmem(vv), in_vmem(rep), in_vmem(bout))
        return block_out, k_out.reshape(k_cache.shape), v_out.reshape(v_cache.shape), new_kv.reshape(SEQS, 2, KVH, HD)

    return jax.shard_map(device_step, mesh=mesh, in_specs=(P('dp', None), P('dp'), cache_spec, cache_spec, P(), P(), P(), P(), P(), P(), P()), out_specs=(P('dp', None), cache_spec, cache_spec, P('dp', None, None, None)), check_vma=False)
```

```python
import functools

import jax
import jax.numpy as jnp
import numpy as np
from jax import lax
from jax.experimental import pallas as pl
from jax.experimental.pallas import tpu as pltpu
from jax.sharding import PartitionSpec as P

NORM_EPS = 1e-6
ROPE_THETA = 1000000.0
MESH = pl.DeviceIdType.MESH
BF16 = jnp.bfloat16
F32 = jnp.float32

SEQS = 64
DIM = 2048
HD = 128
KVH = 4
HALF = 16
SLOTS = 256
ROWS = SLOTS * KVH
BLK = 8
NBLK = SEQS // BLK
AHEAD = 2
LAG = 6
WCH = 512
PIECE = (HALF + 1) * BLK
VMEM_LIMIT = 26 * 2**20
EXP_SCALE = HD ** -0.5 * 1.4426950408889634
NEG = -jnp.inf


def bcast_col(tile, col):
    return jnp.broadcast_to(tile[:, col:col + 1], (tile.shape[0], HD))


def attend_kernel(pos_h, tok_h, an_h, qn_h, kn_h, freq_h, wq, wk, wv, wo, kc, vc,
                  kv, vv, rep, bout,
                  pos_s, tok, an, qn, kn, freq, insem, w_s, hid, ang, cosr, sinr, qmine, qmate, colslot, opart, drx, comb, xrx, ofin, pbuf, prx,
                  wsem, ksem, vsem, wosem, qs, qr, ds_, dr, xs, xr, ps, pr):
    me = lax.axis_index('sp')
    core = lax.rem(me, 2)
    chip = me // 2
    mate = {'sp': me + 1 - 2 * core}
    peer = {'sp': me + 2 - 4 * chip}

    def w_copy(n):
        if n < 4:
            src = wq.at[:, pl.ds(pl.multiple_of(core * (HALF * HD) + n * WCH, WCH), WCH)]
        else:
            src = (wk, wv)[n - 4]
        return pltpu.make_async_copy(src, w_s.at[n], wsem.at[n])

    def wo_copy(n):
        src = wo.at[pl.ds(pl.multiple_of(core * (HALF * HD), HD), HALF * HD), pl.ds(n * WCH, WCH)]
        return pltpu.make_async_copy(src, w_s.at[n], wosem.at[n])

    def k_copy(i):
        return pltpu.make_async_copy(kc.at[pl.ds(i * BLK, BLK)], kv.at[pl.ds(i * BLK, BLK)], ksem.at[i])

    def v_copy(i):
        return pltpu.make_async_copy(vc.at[pl.ds(i * BLK, BLK)], vv.at[pl.ds(i * BLK, BLK)], vsem.at[i])

    def q_send():
        return pltpu.make_async_remote_copy(qmine, qmate, qs, qr, device_id=mate, device_id_type=MESH)

    def d_send(i):
        return pltpu.make_async_remote_copy(opart.at[i, pl.ds(PIECE, PIECE)], drx.at[i], ds_.at[i], dr.at[i],
                                            device_id=mate, device_id_type=MESH)

    def x_send(i):
        return pltpu.make_async_remote_copy(comb.at[i], xrx.at[i], xs.at[i], xr.at[i],
                                            device_id=peer, device_id_type=MESH)

    def p_send(n):
        return pltpu.make_async_remote_copy(pbuf.at[n], prx.at[n], ps.at[n], pr.at[n],
                                            device_id=mate, device_id_type=MESH)

    small = [pltpu.make_async_copy(a, b, insem.at[z]) for z, (a, b) in enumerate(
        ((tok_h, tok), (pos_h, pos_s), (an_h, an), (qn_h, qn), (kn_h, kn), (freq_h, freq)))]
    for c in small:
        c.start()
    for n in range(AHEAD):
        w_copy(n).start()

    barrier = pltpu.get_barrier_semaphore()
    for other in (mate, peer):
        pl.semaphore_signal(barrier, inc=1, device_id=other, device_id_type=MESH)

    for c in small:
        c.wait()

    t = tok[...].astype(F32)
    inv = lax.rsqrt(jnp.sum(t * t, axis=-1, keepdims=True) * (1.0 / DIM) + NORM_EPS)
    gains = an[...].astype(F32)
    for j in range(DIM // HD):
        sl = slice(j * HD, (j + 1) * HD)
        hid[:, sl] = (tok[:, sl].astype(F32) * inv * gains[j:j + 1, :]).astype(BF16)

    lane1 = lax.broadcasted_iota(jnp.int32, (1, HD), 1)

    def angle(b, carry):
        ang[pl.ds(b, 1), :] = freq[...] * pos_s[b].astype(F32)
        return carry

    lax.fori_loop(0, SEQS, angle, 0)
    cosr[...] = jnp.cos(ang[...])
    sinr[...] = jnp.sin(ang[...]) * jnp.where(lane1 < HD // 2, -1.0, 1.0)

    row = lax.broadcasted_iota(jnp.int32, (2 * HALF, ROWS), 0)
    col = lax.broadcasted_iota(jnp.int32, (2 * HALF, ROWS), 1)
    half_of_row = jnp.where(row < HALF, core, 1 - core)
    kv_of_row = half_of_row * 2 + lax.rem(row, HALF) // 8
    colslot[...] = jnp.where(lax.rem(col, KVH) == kv_of_row, col // KVH, 1 << 20)

    qgain = qn[...].astype(F32)
    kgain = kn[...].astype(F32)

    def norm_rope(x, gain):
        y = x * lax.rsqrt(jnp.mean(x * x, axis=-1, keepdims=True) + NORM_EPS) * gain
        y = y * cosr[...] + pltpu.roll(y, HD // 2, 1) * sinr[...]
        return y.astype(BF16).astype(F32)

    for n in range(6):
        w_copy(n).wait()
        if n + AHEAD < 6:
            w_copy(n + AHEAD).start()
        else:
            k_copy(n + AHEAD - 6).start()
            v_copy(n + AHEAD - 6).start()
        proj = jnp.dot(hid[...], w_s[n], preferred_element_type=F32).astype(BF16).astype(F32)
        for j in range(WCH // HD):
            x = proj[:, j * HD:(j + 1) * HD]
            if n < 4:
                qmine[pl.ds(n * 4 + j, SEQS, stride=HALF), :] = norm_rope(x, qgain)
            else:
                y = norm_rope(x, kgain) if n == 4 else x
                for c in range(4):
                    rep[n - 4, pl.ds(c * KVH + j, SEQS, stride=4 * KVH), :] = y
        if n == 3:
            pl.semaphore_wait(barrier, 2)
            q_send().start()
    start = me * SLOTS
    lane = lax.broadcasted_iota(jnp.int32, (HALF, HD), 1)
    lrow = lax.broadcasted_iota(jnp.int32, (HALF, HD), 0)
    lane8 = lax.broadcasted_iota(jnp.int32, (BLK, HD), 1)
    q_send().wait()

    def attend(i):
        k_copy(i).wait()
        v_copy(i).wait()

        @pl.when(i + AHEAD < NBLK)
        def _():
            k_copy(i + AHEAD).start()
            v_copy(i + AHEAD).start()

        @pl.when(i + AHEAD == NBLK)
        def _():
            for n in range(4):
                wo_copy(n).start()

        ob = opart.at[i]
        for pair in range(BLK // 2):
            bs = [i * BLK + 2 * pair + z for z in range(2)]
            qf = [jnp.concatenate([qmine[pl.ds(pl.multiple_of(b * HALF, HALF), HALF), :],
                                   qmate[pl.ds(pl.multiple_of(b * HALF, HALF), HALF), :]], axis=0) for b in bs]
            zero = jnp.zeros((2 * HALF, HD), BF16)
            lhs = jnp.concatenate([jnp.concatenate([qf[0].astype(BF16), zero], axis=1),
                                   jnp.concatenate([zero, qf[1].astype(BF16)], axis=1)], axis=0)
            keys = jnp.concatenate([kv[bs[0]], kv[bs[1]]], axis=1)
            s = lax.dot_general(lhs, keys, (((1,), (1,)), ((), ())), preferred_element_type=F32)
            probs, extra, sums, peaks = [], [], [], []
            for z in range(2):
                b = bs[z]
                rel = pos_s[b] - start
                owner = jnp.logical_and(rel >= 0, rel < SLOTS)
                knew = jnp.concatenate(
                    [jnp.broadcast_to(rep[0, pl.ds(b * 4 * KVH + h, 1), :], (8, HD))
                     for h in (2 * core, 2 * core + 1, 2 - 2 * core, 3 - 2 * core)], axis=0)
                snew = jnp.sum(qf[z] * knew, axis=-1, keepdims=True)
                snew = jnp.where(owner, snew, NEG)
                sm = jnp.where(colslot[...] < rel, s[z * 2 * HALF:(z + 1) * 2 * HALF], NEG)
                peak = jnp.maximum(jnp.max(sm, axis=-1, keepdims=True), snew)
                safe = jnp.where(peak == NEG, 0.0, peak)
                p = jnp.exp2((sm - safe) * EXP_SCALE)
                pn = jnp.exp2((snew - safe) * EXP_SCALE)
                probs.append(p.astype(BF16))
                extra.append(pn.astype(BF16).astype(F32))
                sums.append(jnp.sum(p, axis=-1, keepdims=True) + pn)
                peaks.append(peak)
            values = jnp.concatenate([vv[bs[0]], vv[bs[1]]], axis=1)
            mixed = jnp.dot(jnp.concatenate(probs, axis=0), values, preferred_element_type=F32)
            for z in range(2):
                b = bs[z]
                vnew = jnp.concatenate(
                    [jnp.broadcast_to(rep[1, pl.ds(b * 4 * KVH + h, 1), :], (8, HD))
                     for h in (2 * core, 2 * core + 1, 2 - 2 * core, 3 - 2 * core)], axis=0)
                o = mixed[z * 2 * HALF:(z + 1) * 2 * HALF, z * HD:(z + 1) * HD] + extra[z] * vnew
                bb = 2 * pair + z
                for h in range(2):
                    hs = slice(h * HALF, (h + 1) * HALF)
                    ob[pl.ds(h * PIECE + bb, HALF, stride=BLK), :] = o[hs]
                    st = jnp.where(lane == lrow, peaks[z][hs], jnp.where(lane == lrow + HALF, sums[z][hs], 0.0))
                    ob[pl.ds(h * PIECE + HALF * BLK + bb, 1), :] = jnp.sum(st, axis=0, keepdims=True)

    def combine(i):
        d_send(i).wait_recv()
        s0 = opart[i, pl.ds(HALF * BLK, BLK), :]
        s1 = drx[i, pl.ds(HALF * BLK, BLK), :]
        peak = jnp.maximum(s0, s1)
        safe = jnp.where(peak == NEG, 0.0, peak)
        f0 = jnp.exp2((s0 - safe) * EXP_SCALE)
        f1 = jnp.exp2((s1 - safe) * EXP_SCALE)
        total = f0 * pltpu.roll(s0, HD - HALF, 1) + f1 * pltpu.roll(s1, HD - HALF, 1)
        comb[i, pl.ds(HALF * BLK, BLK), :] = jnp.where(
            lane8 < HALF, peak, jnp.where(lane8 < 2 * HALF, pltpu.roll(total, HALF, 1), 0.0))
        for j in range(HALF):
            rows = pl.ds(j * BLK, BLK)
            comb[i, rows, :] = bcast_col(f0, j) * opart[i, rows, :] + bcast_col(f1, j) * drx[i, rows, :]

    def finish(i):
        x_send(i).wait_recv()
        first = chip == 0

        def ordered(rows):
            mine, other = comb[i, rows, :], xrx[i, rows, :]
            return jnp.where(first, mine, other), jnp.where(first, other, mine)

        s0, s1 = ordered(pl.ds(HALF * BLK, BLK))
        peak = jnp.maximum(s0, s1)
        f0 = jnp.exp2((s0 - peak) * EXP_SCALE)
        f1 = jnp.exp2((s1 - peak) * EXP_SCALE)
        total = f0 * pltpu.roll(s0, HD - HALF, 1) + f1 * pltpu.roll(s1, HD - HALF, 1)
        g0, g1 = f0 / total, f1 / total
        for j in range(HALF):
            a, b = ordered(pl.ds(j * BLK, BLK))
            ofin[pl.ds(pl.multiple_of(i * BLK, BLK), BLK), j * HD:(j + 1) * HD] = bcast_col(g0, j) * a + bcast_col(g1, j) * b

    def step(i, carry):
        @pl.when(i < NBLK)
        def _():
            attend(i)

        @pl.when(jnp.logical_and(i >= 1, i < NBLK + 1))
        def _():
            combine(i - 1)

        @pl.when(i < NBLK)
        def _():
            d_send(i).start()

        @pl.when(i >= LAG)
        def _():
            finish(i - LAG)

        @pl.when(jnp.logical_and(i >= 1, i < NBLK + 1))
        def _():
            x_send(i - 1).start()

        return carry

    lax.fori_loop(0, NBLK + LAG, step, 0)

    lhs = ofin[...].astype(BF16)
    for n in range(4):
        wo_copy(n).wait()
        pbuf[n] = jnp.dot(lhs, w_s[n], preferred_element_type=F32)
        p_send(n).start()
    for n in range(4):
        p_send(n).wait_recv()
        sl = slice(n * WCH, (n + 1) * WCH)
        bout[:, sl] = (tok[:, sl].astype(F32) + (pbuf[n] + prx[n])).astype(BF16)

    def drain(i, carry):
        d_send(i).wait_send()
        x_send(i).wait_send()
        return carry

    lax.fori_loop(0, NBLK, drain, 0)
    for n in range(4):
        p_send(n).wait_send()


def write_kernel(pos_h, kv, vv, rep, bin_, ko, vo, bo, nkv, kva, vva, pos_s, nkv_s, patch, ksem, vsem, psem, osem):
    start = lax.axis_index('sp') * SLOTS
    slot16 = lax.broadcasted_iota(jnp.int32, (4 * KVH, HD), 0) // KVH

    def copies(i):
        r = pl.ds(i * BLK, BLK)
        return (pltpu.make_async_copy(kv.at[r], ko.at[r], ksem.at[i]),
                pltpu.make_async_copy(vv.at[r], vo.at[r], vsem.at[i]))

    pos_copy = pltpu.make_async_copy(pos_h, pos_s, osem.at[0])
    pos_copy.start()
    out_copy = pltpu.make_async_copy(bin_, bo, osem.at[1])
    out_copy.start()
    for c in copies(0):
        c.start()
    for b in range(SEQS):
        nkv_s[b] = jnp.concatenate([rep[0, pl.ds(b * 4 * KVH, KVH), :], rep[1, pl.ds(b * 4 * KVH, KVH), :]], axis=0).astype(BF16)
    pos_copy.wait()

    def each(i, do):
        for bb in range(BLK):
            b = i * BLK + bb
            rel = pos_s[b] - start

            @pl.when(jnp.logical_and(rel >= 0, rel < SLOTS))
            def _():
                base = pl.multiple_of(rel // 4 * (4 * KVH), 4 * KVH)
                mask = slot16 == lax.rem(rel, 4)
                for z, (ref, out) in enumerate(((kv, ko), (vv, vo))):
                    do(b, z, base, mask, ref, out)

    def merged(b, z, base, mask, ref):
        new = rep[z, pl.ds(b * 4 * KVH, 4 * KVH), :]
        old = ref[b, pl.ds(base, 4 * KVH), :].astype(F32)
        return jnp.where(mask, new, old).astype(BF16)

    def put(b, z, base, mask, ref, out):
        ref[b, pl.ds(base, 4 * KVH), :] = merged(b, z, base, mask, ref)

    def stage(b, z, base, mask, ref, out):
        patch[z, b] = merged(b, z, base, mask, ref)

    def patch_copy(b, z, base, out):
        return pltpu.make_async_copy(patch.at[z, b], out.at[b, pl.ds(base, 4 * KVH)], psem.at[z, b])

    for i in range(1, NBLK):
        each(i, put)
        if i > 1:
            for c in copies(i - 1):
                c.start()
    nkv_copy = pltpu.make_async_copy(nkv_s, nkv, osem.at[2])
    nkv_copy.start()
    each(0, stage)
    for c in copies(NBLK - 1):
        c.start()
    for c in copies(0):
        c.wait()
    each(0, lambda b, z, base, mask, ref, out: patch_copy(b, z, base, out).start())
    out_copy.wait()
    nkv_copy.wait()
    each(0, lambda b, z, base, mask, ref, out: patch_copy(b, z, base, out).wait())
    for i in range(1, NBLK):
        for c in copies(i):
            c.wait()


def solution(mesh):
    cache_spec = P('dp', 'sp', None, None)
    inv_freq = (np.float64(ROPE_THETA) ** (-np.arange(HD // 2) * 2.0 / HD)).astype(np.float32)
    freq2 = np.concatenate([inv_freq, inv_freq])
    vm = pl.BlockSpec(memory_space=pltpu.VMEM)
    hbm = pl.BlockSpec(memory_space=pl.ANY)
    dma = pltpu.SemaphoreType.DMA

    def device_step(tokens, positions, k_cache, v_cache, w_q, w_k, w_v, w_o, attn_norm, q_norm, k_norm):
        in_hbm = lambda x: pltpu.with_memory_space_constraint(x, pltpu.HBM)
        in_vmem = lambda x: pltpu.with_memory_space_constraint(x, pltpu.VMEM)
        rows = (SEQS, ROWS, HD)
        kv, vv, rep, bout = pl.pallas_call(
            attend_kernel,
            out_shape=(pltpu.VMEM(rows, BF16), pltpu.VMEM(rows, BF16),
                       pltpu.VMEM((2, SEQS * 4 * KVH, HD), F32), pltpu.VMEM((SEQS, DIM), BF16)),
            in_specs=[hbm] * 12,
            out_specs=(vm, vm, vm, vm),
            scratch_shapes=[
                pltpu.SMEM((SEQS,), jnp.int32), pltpu.VMEM((SEQS, DIM), BF16), pltpu.VMEM((DIM // HD, HD), BF16),
                pltpu.VMEM((1, HD), BF16), pltpu.VMEM((1, HD), BF16), pltpu.VMEM((1, HD), F32), dma((6,)),
                pltpu.VMEM((6, DIM, WCH), BF16),
                pltpu.VMEM((SEQS, DIM), BF16),
                pltpu.VMEM((SEQS, HD), F32), pltpu.VMEM((SEQS, HD), F32), pltpu.VMEM((SEQS, HD), F32),
                pltpu.VMEM((SEQS * HALF, HD), F32), pltpu.VMEM((SEQS * HALF, HD), F32),
                pltpu.VMEM((2 * HALF, ROWS), jnp.int32),
                pltpu.VMEM((NBLK, 2 * PIECE, HD), F32),
                pltpu.VMEM((NBLK, PIECE, HD), F32), pltpu.VMEM((NBLK, PIECE, HD), F32), pltpu.VMEM((NBLK, PIECE, HD), F32),
                pltpu.VMEM((SEQS, HALF * HD), F32),
                pltpu.VMEM((4, SEQS, WCH), F32), pltpu.VMEM((4, SEQS, WCH), F32),
                dma((6,)), dma((NBLK,)), dma((NBLK,)), dma((4,)), dma, dma,
                dma((NBLK,)), dma((NBLK,)), dma((NBLK,)), dma((NBLK,)), dma((4,)), dma((4,)),
            ],
            compiler_params=pltpu.CompilerParams(collective_id=0, has_side_effects=True, vmem_limit_bytes=VMEM_LIMIT),
            name='attend',
        )(in_hbm(positions), in_hbm(tokens), in_hbm(attn_norm.reshape(DIM // HD, HD)), in_hbm(q_norm.reshape(1, HD)),
          in_hbm(k_norm.reshape(1, HD)), in_hbm(jnp.asarray(freq2).reshape(1, HD)), in_hbm(w_q), in_hbm(w_k), in_hbm(w_v), in_hbm(w_o),
          in_hbm(k_cache.reshape(rows)), in_hbm(v_cache.reshape(rows)))
        k_out, v_out, block_out, new_kv, _, _ = pl.pallas_call(
            write_kernel,
            out_shape=(pltpu.HBM(rows, BF16), pltpu.HBM(rows, BF16), pltpu.HBM((SEQS, DIM), BF16),
                       pltpu.HBM((SEQS, 2 * KVH, HD), BF16), pltpu.VMEM(rows, BF16), pltpu.VMEM(rows, BF16)),
            in_specs=[hbm, vm, vm, vm, vm],
            out_specs=(hbm, hbm, hbm, hbm, vm, vm),
            input_output_aliases={1: 4, 2: 5},
            scratch_shapes=[pltpu.SMEM((SEQS,), jnp.int32), pltpu.VMEM((SEQS, 2 * KVH, HD), BF16),
                            pltpu.VMEM((2, BLK, 4 * KVH, HD), BF16),
                            dma((NBLK,)), dma((NBLK,)), dma((2, BLK)), dma((3,))],
            compiler_params=pltpu.CompilerParams(vmem_limit_bytes=VMEM_LIMIT),
            name='write',
        )(in_hbm(positions), in_vmem(kv), in_vmem(vv), in_vmem(rep), in_vmem(bout))
        return block_out, k_out.reshape(k_cache.shape), v_out.reshape(v_cache.shape), new_kv.reshape(SEQS, 2, KVH, HD)

    return jax.shard_map(device_step, mesh=mesh, in_specs=(P('dp', None), P('dp'), cache_spec, cache_spec, P(), P(), P(), P(), P(), P(), P()), out_specs=(P('dp', None), cache_spec, cache_spec, P('dp', None, None, None)), check_vma=False)
```

```python
import functools

import jax
import jax.numpy as jnp
import numpy as np
from jax import lax
from jax.experimental import pallas as pl
from jax.experimental.pallas import tpu as pltpu
from jax.sharding import PartitionSpec as P

NORM_EPS = 1e-6
ROPE_THETA = 1000000.0
MESH = pl.DeviceIdType.MESH
BF16 = jnp.bfloat16
F32 = jnp.float32

SEQS = 64
DIM = 2048
HD = 128
KVH = 4
HALF = 16
SLOTS = 256
ROWS = SLOTS * KVH
BLK = 8
NBLK = SEQS // BLK
AHEAD = 2
LAG = 2
WCH = 512
PIECE = (HALF + 1) * BLK
VMEM_LIMIT = 26 * 2**20
EXP_SCALE = HD ** -0.5 * 1.4426950408889634
NEG = -jnp.inf


def bcast_col(tile, col):
    return jnp.broadcast_to(tile[:, col:col + 1], (tile.shape[0], HD))


def attend_kernel(pos_h, tok_h, an_h, qn_h, kn_h, freq_h, wq, wk, wv, wo, kc, vc,
                  kv, vv, rep, bout,
                  pos_s, tok, an, qn, kn, freq, insem, w_s, hid, ang, cosr, sinr, qmine, qmate, colslot, opart, drx, comb, xrx, ofin, pbuf, prx, sc, pr_s,
                  wsem, ksem, vsem, wosem, qs, qr, ds_, dr, xs, xr, ps, pr):
    me = lax.axis_index('sp')
    core = lax.rem(me, 2)
    chip = me // 2
    mate = {'sp': me + 1 - 2 * core}
    peer = {'sp': me + 2 - 4 * chip}

    def w_copy(n):
        if n < 4:
            src = wq.at[:, pl.ds(pl.multiple_of(core * (HALF * HD) + n * WCH, WCH), WCH)]
        else:
            src = (wk, wv)[n - 4]
        return pltpu.make_async_copy(src, w_s.at[n], wsem.at[n])

    def wo_copy(n):
        src = wo.at[pl.ds(pl.multiple_of(core * (HALF * HD), HD), HALF * HD), pl.ds(n * WCH, WCH)]
        return pltpu.make_async_copy(src, w_s.at[n], wosem.at[n])

    def k_copy(i):
        return pltpu.make_async_copy(kc.at[pl.ds(i * BLK, BLK)], kv.at[pl.ds(i * BLK, BLK)], ksem.at[i])

    def v_copy(i):
        return pltpu.make_async_copy(vc.at[pl.ds(i * BLK, BLK)], vv.at[pl.ds(i * BLK, BLK)], vsem.at[i])

    def q_send():
        return pltpu.make_async_remote_copy(qmine, qmate, qs, qr, device_id=mate, device_id_type=MESH)

    def d_send(i):
        return pltpu.make_async_remote_copy(opart.at[i, pl.ds(PIECE, PIECE)], drx.at[i], ds_.at[i], dr.at[i],
                                            device_id=mate, device_id_type=MESH)

    def x_send(i):
        return pltpu.make_async_remote_copy(comb.at[i], xrx.at[i], xs.at[i], xr.at[i],
                                            device_id=peer, device_id_type=MESH)

    def p_send(n):
        return pltpu.make_async_remote_copy(pbuf.at[n], prx.at[n], ps.at[n], pr.at[n],
                                            device_id=mate, device_id_type=MESH)

    small = [pltpu.make_async_copy(a, b, insem.at[z]) for z, (a, b) in enumerate(
        ((tok_h, tok), (pos_h, pos_s), (an_h, an), (qn_h, qn), (kn_h, kn), (freq_h, freq)))]
    for c in small:
        c.start()
    for n in range(AHEAD):
        w_copy(n).start()

    barrier = pltpu.get_barrier_semaphore()
    for other in (mate, peer):
        pl.semaphore_signal(barrier, inc=1, device_id=other, device_id_type=MESH)

    for c in small:
        c.wait()

    t = tok[...].astype(F32)
    inv = lax.rsqrt(jnp.sum(t * t, axis=-1, keepdims=True) * (1.0 / DIM) + NORM_EPS)
    gains = an[...].astype(F32)
    for j in range(DIM // HD):
        sl = slice(j * HD, (j + 1) * HD)
        hid[:, sl] = (tok[:, sl].astype(F32) * inv * gains[j:j + 1, :]).astype(BF16)

    lane1 = lax.broadcasted_iota(jnp.int32, (1, HD), 1)

    def angle(b, carry):
        ang[pl.ds(b, 1), :] = freq[...] * pos_s[b].astype(F32)
        return carry

    lax.fori_loop(0, SEQS, angle, 0)
    cosr[...] = jnp.cos(ang[...])
    sinr[...] = jnp.sin(ang[...]) * jnp.where(lane1 < HD // 2, -1.0, 1.0)

    row = lax.broadcasted_iota(jnp.int32, (2 * HALF, ROWS), 0)
    col = lax.broadcasted_iota(jnp.int32, (2 * HALF, ROWS), 1)
    half_of_row = jnp.where(row < HALF, core, 1 - core)
    kv_of_row = half_of_row * 2 + lax.rem(row, HALF) // 8
    colslot[...] = jnp.where(lax.rem(col, KVH) == kv_of_row, col // KVH, 1 << 20)

    qgain = qn[...].astype(F32)
    kgain = kn[...].astype(F32)

    def norm_rope(x, gain):
        y = x * lax.rsqrt(jnp.mean(x * x, axis=-1, keepdims=True) + NORM_EPS) * gain
        y = y * cosr[...] + pltpu.roll(y, HD // 2, 1) * sinr[...]
        return y.astype(BF16).astype(F32)

    for n in range(6):
        w_copy(n).wait()
        if n + AHEAD < 6:
            w_copy(n + AHEAD).start()
        else:
            k_copy(n + AHEAD - 6).start()
            v_copy(n + AHEAD - 6).start()
        proj = jnp.dot(hid[...], w_s[n], preferred_element_type=F32).astype(BF16).astype(F32)
        for j in range(WCH // HD):
            x = proj[:, j * HD:(j + 1) * HD]
            if n < 4:
                qmine[pl.ds(n * 4 + j, SEQS, stride=HALF), :] = norm_rope(x, qgain)
            else:
                y = norm_rope(x, kgain) if n == 4 else x
                for c in range(4):
                    rep[n - 4, pl.ds(c * KVH + j, SEQS, stride=4 * KVH), :] = y
        if n == 3:
            pl.semaphore_wait(barrier, 2)
            q_send().start()
    start = me * SLOTS
    lane = lax.broadcasted_iota(jnp.int32, (HALF, HD), 1)
    lrow = lax.broadcasted_iota(jnp.int32, (HALF, HD), 0)
    lane8 = lax.broadcasted_iota(jnp.int32, (BLK, HD), 1)
    q_send().wait()

    def attend(i):
        ob = opart.at[i]
        def load_q(pair):
            bs = [i * BLK + 2 * pair + z for z in range(2)]
            return bs, [jnp.concatenate([qmine[pl.ds(pl.multiple_of(b * HALF, HALF), HALF), :],
                                         qmate[pl.ds(pl.multiple_of(b * HALF, HALF), HALF), :]], axis=0) for b in bs]

        def new_rows(z, b):
            return jnp.concatenate([jnp.broadcast_to(rep[z, pl.ds(b * 4 * KVH + h, 1), :], (8, HD))
                                    for h in (2 * core, 2 * core + 1, 2 - 2 * core, 3 - 2 * core)], axis=0)

        def scores(pair):
            bs, qf = load_q(pair)
            zero = jnp.zeros((2 * HALF, HD), BF16)
            lhs = jnp.concatenate([jnp.concatenate([qf[0].astype(BF16), zero], axis=1),
                                   jnp.concatenate([zero, qf[1].astype(BF16)], axis=1)], axis=0)
            keys = jnp.concatenate([kv[bs[0]], kv[bs[1]]], axis=1)
            sc[pair % 2] = lax.dot_general(lhs, keys, (((1,), (1,)), ((), ())), preferred_element_type=F32)

        def soft(pair):
            bs, qf = load_q(pair)
            out = []
            for z in range(2):
                b = bs[z]
                rel = pos_s[b] - start
                owner = jnp.logical_and(rel >= 0, rel < SLOTS)
                snew = jnp.where(owner, jnp.sum(qf[z] * new_rows(0, b), axis=-1, keepdims=True), NEG)
                sm = jnp.where(colslot[...] < rel, sc[pair % 2, z * 2 * HALF:(z + 1) * 2 * HALF], NEG)
                peak = jnp.maximum(jnp.max(sm, axis=-1, keepdims=True), snew)
                safe = jnp.where(peak == NEG, 0.0, peak)
                p = jnp.exp2((sm - safe) * EXP_SCALE)
                pn = jnp.exp2((snew - safe) * EXP_SCALE)
                pr_s[pair % 2, z * 2 * HALF:(z + 1) * 2 * HALF, :] = p.astype(BF16)
                out.append((pn.astype(BF16).astype(F32), jnp.sum(p, axis=-1, keepdims=True) + pn, peak))
            return out

        def mix(pair, st3):
            bs = [i * BLK + 2 * pair + z for z in range(2)]
            values = jnp.concatenate([vv[bs[0]], vv[bs[1]]], axis=1)
            mixed = jnp.dot(pr_s[pair % 2], values, preferred_element_type=F32)
            for z in range(2):
                extra, total, peak = st3[z]
                o = mixed[z * 2 * HALF:(z + 1) * 2 * HALF, z * HD:(z + 1) * HD] + extra * new_rows(1, bs[z])
                bb = 2 * pair + z
                for h in range(2):
                    hs = slice(h * HALF, (h + 1) * HALF)
                    ob[pl.ds(h * PIECE + bb, HALF, stride=BLK), :] = o[hs]
                    st = jnp.where(lane == lrow, peak[hs], jnp.where(lane == lrow + HALF, total[hs], 0.0))
                    ob[pl.ds(h * PIECE + HALF * BLK + bb, 1), :] = jnp.sum(st, axis=0, keepdims=True)

        scores(0)
        for pair in range(BLK // 2):
            if pair + 1 < BLK // 2:
                scores(pair + 1)
            mix(pair, soft(pair))

    def combine(i):
        s0 = opart[i, pl.ds(HALF * BLK, BLK), :]
        s1 = drx[i, pl.ds(HALF * BLK, BLK), :]
        peak = jnp.maximum(s0, s1)
        safe = jnp.where(peak == NEG, 0.0, peak)
        f0 = jnp.exp2((s0 - safe) * EXP_SCALE)
        f1 = jnp.exp2((s1 - safe) * EXP_SCALE)
        total = f0 * pltpu.roll(s0, HD - HALF, 1) + f1 * pltpu.roll(s1, HD - HALF, 1)
        comb[i, pl.ds(HALF * BLK, BLK), :] = jnp.where(
            lane8 < HALF, peak, jnp.where(lane8 < 2 * HALF, pltpu.roll(total, HALF, 1), 0.0))
        for j in range(HALF):
            rows = pl.ds(j * BLK, BLK)
            comb[i, rows, :] = bcast_col(f0, j) * opart[i, rows, :] + bcast_col(f1, j) * drx[i, rows, :]

    def finish(i):
        first = chip == 0

        def ordered(rows):
            mine, other = comb[i, rows, :], xrx[i, rows, :]
            return jnp.where(first, mine, other), jnp.where(first, other, mine)

        s0, s1 = ordered(pl.ds(HALF * BLK, BLK))
        peak = jnp.maximum(s0, s1)
        f0 = jnp.exp2((s0 - peak) * EXP_SCALE)
        f1 = jnp.exp2((s1 - peak) * EXP_SCALE)
        total = f0 * pltpu.roll(s0, HD - HALF, 1) + f1 * pltpu.roll(s1, HD - HALF, 1)
        g0, g1 = f0 / total, f1 / total
        for j in range(HALF):
            a, b = ordered(pl.ds(j * BLK, BLK))
            ofin[pl.ds(pl.multiple_of(i * BLK, BLK), BLK), j * HD:(j + 1) * HD] = bcast_col(g0, j) * a + bcast_col(g1, j) * b

    def fetch(i):
        k_copy(i).wait()
        v_copy(i).wait()

        @pl.when(i + AHEAD < NBLK)
        def _():
            k_copy(i + AHEAD).start()
            v_copy(i + AHEAD).start()

        @pl.when(i + AHEAD == NBLK)
        def _():
            for n in range(4):
                wo_copy(n).start()

    def early(i, carry):
        fetch(i)
        attend(i)
        d_send(i).start()
        return carry

    def steady(i, carry):
        fetch(i)
        d_send(i - LAG).wait_recv()
        combine(i - LAG)
        attend(i)
        d_send(i).start()
        x_send(i - LAG).start()
        return carry

    lax.fori_loop(0, LAG, early, 0)
    lax.fori_loop(LAG, NBLK, steady, 0)

    def late(i, carry):
        d_send(i).wait_recv()
        combine(i)
        x_send(i).start()
        return carry

    lax.fori_loop(NBLK - LAG, NBLK, late, 0)

    def last(i, carry):
        x_send(i).wait_recv()
        finish(i)
        return carry

    lax.fori_loop(0, NBLK, last, 0)

    lhs = ofin[...].astype(BF16)
    for n in range(4):
        wo_copy(n).wait()
        pbuf[n] = jnp.dot(lhs, w_s[n], preferred_element_type=F32)
        p_send(n).start()
    for n in range(4):
        p_send(n).wait_recv()
        sl = slice(n * WCH, (n + 1) * WCH)
        bout[:, sl] = (tok[:, sl].astype(F32) + (pbuf[n] + prx[n])).astype(BF16)

    def drain(i, carry):
        d_send(i).wait_send()
        x_send(i).wait_send()
        return carry

    lax.fori_loop(0, NBLK, drain, 0)
    for n in range(4):
        p_send(n).wait_send()


def write_kernel(pos_h, kv, vv, rep, bin_, ko, vo, bo, nkv, kva, vva, pos_s, nkv_s, patch, ksem, vsem, psem, osem):
    start = lax.axis_index('sp') * SLOTS
    slot16 = lax.broadcasted_iota(jnp.int32, (4 * KVH, HD), 0) // KVH

    def copies(i):
        r = pl.ds(i * BLK, BLK)
        return (pltpu.make_async_copy(kv.at[r], ko.at[r], ksem.at[i]),
                pltpu.make_async_copy(vv.at[r], vo.at[r], vsem.at[i]))

    pos_copy = pltpu.make_async_copy(pos_h, pos_s, osem.at[0])
    pos_copy.start()
    out_copy = pltpu.make_async_copy(bin_, bo, osem.at[1])
    out_copy.start()
    for c in copies(0):
        c.start()
    for b in range(SEQS):
        nkv_s[b] = jnp.concatenate([rep[0, pl.ds(b * 4 * KVH, KVH), :], rep[1, pl.ds(b * 4 * KVH, KVH), :]], axis=0).astype(BF16)
    pos_copy.wait()

    def each(i, do):
        for bb in range(BLK):
            b = i * BLK + bb
            rel = pos_s[b] - start

            @pl.when(jnp.logical_and(rel >= 0, rel < SLOTS))
            def _():
                base = pl.multiple_of(rel // 4 * (4 * KVH), 4 * KVH)
                mask = slot16 == lax.rem(rel, 4)
                for z, (ref, out) in enumerate(((kv, ko), (vv, vo))):
                    do(b, z, base, mask, ref, out)

    def merged(b, z, base, mask, ref):
        new = rep[z, pl.ds(b * 4 * KVH, 4 * KVH), :]
        old = ref[b, pl.ds(base, 4 * KVH), :].astype(F32)
        return jnp.where(mask, new, old).astype(BF16)

    def put(b, z, base, mask, ref, out):
        ref[b, pl.ds(base, 4 * KVH), :] = merged(b, z, base, mask, ref)

    def stage(b, z, base, mask, ref, out):
        patch[z, b] = merged(b, z, base, mask, ref)

    def patch_copy(b, z, base, out):
        return pltpu.make_async_copy(patch.at[z, b], out.at[b, pl.ds(base, 4 * KVH)], psem.at[z, b])

    for i in range(1, NBLK):
        each(i, put)
        if i > 1:
            for c in copies(i - 1):
                c.start()
    nkv_copy = pltpu.make_async_copy(nkv_s, nkv, osem.at[2])
    nkv_copy.start()
    each(0, stage)
    for c in copies(NBLK - 1):
        c.start()
    for c in copies(0):
        c.wait()
    each(0, lambda b, z, base, mask, ref, out: patch_copy(b, z, base, out).start())
    out_copy.wait()
    nkv_copy.wait()
    each(0, lambda b, z, base, mask, ref, out: patch_copy(b, z, base, out).wait())
    for i in range(1, NBLK):
        for c in copies(i):
            c.wait()


def solution(mesh):
    cache_spec = P('dp', 'sp', None, None)
    inv_freq = (np.float64(ROPE_THETA) ** (-np.arange(HD // 2) * 2.0 / HD)).astype(np.float32)
    freq2 = np.concatenate([inv_freq, inv_freq])
    vm = pl.BlockSpec(memory_space=pltpu.VMEM)
    hbm = pl.BlockSpec(memory_space=pl.ANY)
    dma = pltpu.SemaphoreType.DMA

    def device_step(tokens, positions, k_cache, v_cache, w_q, w_k, w_v, w_o, attn_norm, q_norm, k_norm):
        in_hbm = lambda x: pltpu.with_memory_space_constraint(x, pltpu.HBM)
        in_vmem = lambda x: pltpu.with_memory_space_constraint(x, pltpu.VMEM)
        rows = (SEQS, ROWS, HD)
        kv, vv, rep, bout = pl.pallas_call(
            attend_kernel,
            out_shape=(pltpu.VMEM(rows, BF16), pltpu.VMEM(rows, BF16),
                       pltpu.VMEM((2, SEQS * 4 * KVH, HD), F32), pltpu.VMEM((SEQS, DIM), BF16)),
            in_specs=[hbm] * 12,
            out_specs=(vm, vm, vm, vm),
            scratch_shapes=[
                pltpu.SMEM((SEQS,), jnp.int32), pltpu.VMEM((SEQS, DIM), BF16), pltpu.VMEM((DIM // HD, HD), BF16),
                pltpu.VMEM((1, HD), BF16), pltpu.VMEM((1, HD), BF16), pltpu.VMEM((1, HD), F32), dma((6,)),
                pltpu.VMEM((6, DIM, WCH), BF16),
                pltpu.VMEM((SEQS, DIM), BF16),
                pltpu.VMEM((SEQS, HD), F32), pltpu.VMEM((SEQS, HD), F32), pltpu.VMEM((SEQS, HD), F32),
                pltpu.VMEM((SEQS * HALF, HD), F32), pltpu.VMEM((SEQS * HALF, HD), F32),
                pltpu.VMEM((2 * HALF, ROWS), jnp.int32),
                pltpu.VMEM((NBLK, 2 * PIECE, HD), F32),
                pltpu.VMEM((NBLK, PIECE, HD), F32), pltpu.VMEM((NBLK, PIECE, HD), F32), pltpu.VMEM((NBLK, PIECE, HD), F32),
                pltpu.VMEM((SEQS, HALF * HD), F32),
                pltpu.VMEM((4, SEQS, WCH), F32), pltpu.VMEM((4, SEQS, WCH), F32),
                pltpu.VMEM((2, 4 * HALF, ROWS), F32), pltpu.VMEM((2, 4 * HALF, ROWS), BF16),
                dma((6,)), dma((NBLK,)), dma((NBLK,)), dma((4,)), dma, dma,
                dma((NBLK,)), dma((NBLK,)), dma((NBLK,)), dma((NBLK,)), dma((4,)), dma((4,)),
            ],
            compiler_params=pltpu.CompilerParams(collective_id=0, has_side_effects=True, vmem_limit_bytes=VMEM_LIMIT),
            name='attend',
        )(in_hbm(positions), in_hbm(tokens), in_hbm(attn_norm.reshape(DIM // HD, HD)), in_hbm(q_norm.reshape(1, HD)),
          in_hbm(k_norm.reshape(1, HD)), in_hbm(jnp.asarray(freq2).reshape(1, HD)), in_hbm(w_q), in_hbm(w_k), in_hbm(w_v), in_hbm(w_o),
          in_hbm(k_cache.reshape(rows)), in_hbm(v_cache.reshape(rows)))
        k_out, v_out, block_out, new_kv, _, _ = pl.pallas_call(
            write_kernel,
            out_shape=(pltpu.HBM(rows, BF16), pltpu.HBM(rows, BF16), pltpu.HBM((SEQS, DIM), BF16),
                       pltpu.HBM((SEQS, 2 * KVH, HD), BF16), pltpu.VMEM(rows, BF16), pltpu.VMEM(rows, BF16)),
            in_specs=[hbm, vm, vm, vm, vm],
            out_specs=(hbm, hbm, hbm, hbm, vm, vm),
            input_output_aliases={1: 4, 2: 5},
            scratch_shapes=[pltpu.SMEM((SEQS,), jnp.int32), pltpu.VMEM((SEQS, 2 * KVH, HD), BF16),
                            pltpu.VMEM((2, BLK, 4 * KVH, HD), BF16),
                            dma((NBLK,)), dma((NBLK,)), dma((2, BLK)), dma((3,))],
            compiler_params=pltpu.CompilerParams(vmem_limit_bytes=VMEM_LIMIT),
            name='write',
        )(in_hbm(positions), in_vmem(kv), in_vmem(vv), in_vmem(rep), in_vmem(bout))
        return block_out, k_out.reshape(k_cache.shape), v_out.reshape(v_cache.shape), new_kv.reshape(SEQS, 2, KVH, HD)

    return jax.shard_map(device_step, mesh=mesh, in_specs=(P('dp', None), P('dp'), cache_spec, cache_spec, P(), P(), P(), P(), P(), P(), P()), out_specs=(P('dp', None), cache_spec, cache_spec, P('dp', None, None, None)), check_vma=False)
```

```python
import functools

import jax
import jax.numpy as jnp
import numpy as np
from jax import lax
from jax.experimental import pallas as pl
from jax.experimental.pallas import tpu as pltpu
from jax.sharding import PartitionSpec as P

NORM_EPS = 1e-6
ROPE_THETA = 1000000.0
MESH = pl.DeviceIdType.MESH
BF16 = jnp.bfloat16
F32 = jnp.float32

SEQS = 64
DIM = 2048
HD = 128
KVH = 4
HALF = 16
SLOTS = 256
ROWS = SLOTS * KVH
BLK = 8
NBLK = SEQS // BLK
AHEAD = 2
NX = 4
RING = 3
LAG = 2
WCH = 512
PIECE = (HALF + 1) * BLK
VMEM_LIMIT = 16 * 2**20
EXP_SCALE = HD ** -0.5 * 1.4426950408889634
NEG = -jnp.inf


def bcast_col(tile, col):
    return jnp.broadcast_to(tile[:, col:col + 1], (tile.shape[0], HD))


def attend_kernel(pos_h, tok_h, an_h, qn_h, kn_h, freq_h, wq, wk, wv, wo, kc, vc,
                  kv, vv, rep, wo_v, comb_a, comb_b, xrx,
                  pos_s, tok, an, qn, kn, freq, insem, w_s, hid, ang, cosr, sinr, qmine, qmate, colslot, opart, drx, sc, pr_s,
                  wsem, ksem, vsem, wosem, qs, qr, ds_, dr, xs, xr):
    me = lax.axis_index('sp')
    core = lax.rem(me, 2)
    chip = me // 2
    mate = {'sp': me + 1 - 2 * core}
    peer = {'sp': me + 2 - 4 * chip}

    def w_copy(n):
        if n < 4:
            src = wq.at[:, pl.ds(pl.multiple_of(core * (HALF * HD) + n * WCH, WCH), WCH)]
        else:
            src = (wk, wv)[n - 4]
        return pltpu.make_async_copy(src, w_s.at[n % RING], wsem.at[n])

    def wo_copy(n):
        src = wo.at[pl.ds(pl.multiple_of(core * (HALF * HD), HD), HALF * HD), pl.ds(n * WCH, WCH)]
        return pltpu.make_async_copy(src, wo_v.at[n], wosem.at[n])

    def k_copy(i):
        return pltpu.make_async_copy(kc.at[pl.ds(i * BLK, BLK)], kv.at[pl.ds(i * BLK, BLK)], ksem.at[i])

    def v_copy(i):
        return pltpu.make_async_copy(vc.at[pl.ds(i * BLK, BLK)], vv.at[pl.ds(i * BLK, BLK)], vsem.at[i])

    def q_send():
        return pltpu.make_async_remote_copy(qmine, qmate, qs, qr, device_id=mate, device_id_type=MESH)

    def d_send(i):
        return pltpu.make_async_remote_copy(opart.at[i, pl.ds(PIECE, PIECE)], drx.at[i], ds_.at[i], dr.at[i],
                                            device_id=mate, device_id_type=MESH)

    def x_send(i):
        return pltpu.make_async_remote_copy(comb_a.at[i], xrx.at[i], xs.at[i], xr.at[i],
                                            device_id=peer, device_id_type=MESH)

    small = [pltpu.make_async_copy(a, b, insem.at[z]) for z, (a, b) in enumerate(
        ((tok_h, tok), (pos_h, pos_s), (an_h, an), (qn_h, qn), (kn_h, kn), (freq_h, freq)))]
    for c in small:
        c.start()
    for n in range(AHEAD):
        w_copy(n).start()

    barrier = pltpu.get_barrier_semaphore()
    for other in (mate, peer):
        pl.semaphore_signal(barrier, inc=1, device_id=other, device_id_type=MESH)

    for c in small:
        c.wait()

    t = tok[...].astype(F32)
    inv = lax.rsqrt(jnp.sum(t * t, axis=-1, keepdims=True) * (1.0 / DIM) + NORM_EPS)
    gains = an[...].astype(F32)
    for j in range(DIM // HD):
        sl = slice(j * HD, (j + 1) * HD)
        hid[:, sl] = (tok[:, sl].astype(F32) * inv * gains[j:j + 1, :]).astype(BF16)

    lane1 = lax.broadcasted_iota(jnp.int32, (1, HD), 1)

    def angle(b, carry):
        ang[pl.ds(b, 1), :] = freq[...] * pos_s[b].astype(F32)
        return carry

    lax.fori_loop(0, SEQS, angle, 0)
    cosr[...] = jnp.cos(ang[...])
    sinr[...] = jnp.sin(ang[...]) * jnp.where(lane1 < HD // 2, -1.0, 1.0)

    row = lax.broadcasted_iota(jnp.int32, (2 * HALF, ROWS), 0)
    col = lax.broadcasted_iota(jnp.int32, (2 * HALF, ROWS), 1)
    half_of_row = jnp.where(row < HALF, core, 1 - core)
    kv_of_row = half_of_row * 2 + lax.rem(row, HALF) // 8
    colslot[...] = jnp.where(lax.rem(col, KVH) == kv_of_row, col // KVH, 1 << 20)

    qgain = qn[...].astype(F32)
    kgain = kn[...].astype(F32)

    def norm_rope(x, gain):
        y = x * lax.rsqrt(jnp.mean(x * x, axis=-1, keepdims=True) + NORM_EPS) * gain
        y = y * cosr[...] + pltpu.roll(y, HD // 2, 1) * sinr[...]
        return y.astype(BF16).astype(F32)

    for n in range(6):
        w_copy(n).wait()
        if n + AHEAD < 6:
            w_copy(n + AHEAD).start()
        else:
            k_copy(n + AHEAD - 6).start()
            v_copy(n + AHEAD - 6).start()
        proj = jnp.dot(hid[...], w_s[n % RING], preferred_element_type=F32).astype(BF16).astype(F32)
        for j in range(WCH // HD):
            x = proj[:, j * HD:(j + 1) * HD]
            if n < 4:
                qmine[pl.ds(n * 4 + j, SEQS, stride=HALF), :] = norm_rope(x, qgain)
            else:
                y = norm_rope(x, kgain) if n == 4 else x
                for c in range(4):
                    rep[n - 4, pl.ds(c * KVH + j, SEQS, stride=4 * KVH), :] = y
        if n == 3:
            pl.semaphore_wait(barrier, 2)
            q_send().start()
    start = me * SLOTS
    lane = lax.broadcasted_iota(jnp.int32, (HALF, HD), 1)
    lrow = lax.broadcasted_iota(jnp.int32, (HALF, HD), 0)
    lane8 = lax.broadcasted_iota(jnp.int32, (BLK, HD), 1)
    q_send().wait()

    def attend(i):
        ob = opart.at[i]
        def load_q(pair):
            bs = [i * BLK + 2 * pair + z for z in range(2)]
            return bs, [jnp.concatenate([qmine[pl.ds(pl.multiple_of(b * HALF, HALF), HALF), :],
                                         qmate[pl.ds(pl.multiple_of(b * HALF, HALF), HALF), :]], axis=0) for b in bs]

        def new_rows(z, b):
            return jnp.concatenate([jnp.broadcast_to(rep[z, pl.ds(b * 4 * KVH + h, 1), :], (8, HD))
                                    for h in (2 * core, 2 * core + 1, 2 - 2 * core, 3 - 2 * core)], axis=0)

        def scores(pair):
            bs, qf = load_q(pair)
            zero = jnp.zeros((2 * HALF, HD), BF16)
            lhs = jnp.concatenate([jnp.concatenate([qf[0].astype(BF16), zero], axis=1),
                                   jnp.concatenate([zero, qf[1].astype(BF16)], axis=1)], axis=0)
            keys = jnp.concatenate([kv[bs[0]], kv[bs[1]]], axis=1)
            sc[pair % 2] = lax.dot_general(lhs, keys, (((1,), (1,)), ((), ())), preferred_element_type=F32)

        def soft(pair):
            bs, qf = load_q(pair)
            out = []
            for z in range(2):
                b = bs[z]
                rel = pos_s[b] - start
                owner = jnp.logical_and(rel >= 0, rel < SLOTS)
                snew = jnp.where(owner, jnp.sum(qf[z] * new_rows(0, b), axis=-1, keepdims=True), NEG)
                sm = jnp.where(colslot[...] < rel, sc[pair % 2, z * 2 * HALF:(z + 1) * 2 * HALF], NEG)
                peak = jnp.maximum(jnp.max(sm, axis=-1, keepdims=True), snew)
                safe = jnp.where(peak == NEG, 0.0, peak)
                p = jnp.exp2((sm - safe) * EXP_SCALE)
                pn = jnp.exp2((snew - safe) * EXP_SCALE)
                pr_s[pair % 2, z * 2 * HALF:(z + 1) * 2 * HALF, :] = p.astype(BF16)
                out.append((pn.astype(BF16).astype(F32), jnp.sum(p, axis=-1, keepdims=True) + pn, peak))
            return out

        def mix(pair, st3):
            bs = [i * BLK + 2 * pair + z for z in range(2)]
            values = jnp.concatenate([vv[bs[0]], vv[bs[1]]], axis=1)
            mixed = jnp.dot(pr_s[pair % 2], values, preferred_element_type=F32)
            for z in range(2):
                extra, total, peak = st3[z]
                o = mixed[z * 2 * HALF:(z + 1) * 2 * HALF, z * HD:(z + 1) * HD] + extra * new_rows(1, bs[z])
                bb = 2 * pair + z
                for h in range(2):
                    hs = slice(h * HALF, (h + 1) * HALF)
                    ob[pl.ds(h * PIECE + bb, HALF, stride=BLK), :] = o[hs]
                    st = jnp.where(lane == lrow, peak[hs], jnp.where(lane == lrow + HALF, total[hs], 0.0))
                    ob[pl.ds(h * PIECE + HALF * BLK + bb, 1), :] = jnp.sum(st, axis=0, keepdims=True)

        scores(0)
        for pair in range(BLK // 2):
            if pair + 1 < BLK // 2:
                scores(pair + 1)
            mix(pair, soft(pair))

    def combine(i, comb, at):
        s0 = opart[i, pl.ds(HALF * BLK, BLK), :]
        s1 = drx[i, pl.ds(HALF * BLK, BLK), :]
        peak = jnp.maximum(s0, s1)
        safe = jnp.where(peak == NEG, 0.0, peak)
        f0 = jnp.exp2((s0 - safe) * EXP_SCALE)
        f1 = jnp.exp2((s1 - safe) * EXP_SCALE)
        total = f0 * pltpu.roll(s0, HD - HALF, 1) + f1 * pltpu.roll(s1, HD - HALF, 1)
        comb[at, pl.ds(HALF * BLK, BLK), :] = jnp.where(
            lane8 < HALF, peak, jnp.where(lane8 < 2 * HALF, pltpu.roll(total, HALF, 1), 0.0))
        for j in range(HALF):
            rows = pl.ds(j * BLK, BLK)
            comb[at, rows, :] = bcast_col(f0, j) * opart[i, rows, :] + bcast_col(f1, j) * drx[i, rows, :]

    def fetch(i):
        k_copy(i).wait()
        v_copy(i).wait()

        @pl.when(i + AHEAD < NBLK)
        def _():
            k_copy(i + AHEAD).start()
            v_copy(i + AHEAD).start()

        @pl.when(i + AHEAD == NBLK)
        def _():
            for n in range(4):
                wo_copy(n).start()

    def early(i, carry):
        fetch(i)
        attend(i)
        d_send(i).start()
        return carry

    def sending(i, carry):
        fetch(i)
        d_send(i - LAG).wait_recv()
        combine(i - LAG, comb_a, i - LAG)
        attend(i)
        d_send(i).start()
        x_send(i - LAG).start()
        return carry

    def keeping(i, carry):
        fetch(i)
        d_send(i - LAG).wait_recv()
        combine(i - LAG, comb_b, i - LAG - NX)
        attend(i)
        d_send(i).start()
        return carry

    def late(i, carry):
        d_send(i).wait_recv()
        combine(i, comb_b, i - NX)
        return carry

    lax.fori_loop(0, LAG, early, 0)
    lax.fori_loop(LAG, LAG + NX, sending, 0)
    lax.fori_loop(LAG + NX, NBLK, keeping, 0)
    lax.fori_loop(NBLK - LAG, NBLK, late, 0)

    for n in range(4):
        wo_copy(n).wait()

    def drain(i, carry):
        d_send(i).wait_send()
        return carry

    def drain_x(i, carry):
        x_send(i).wait()
        return carry

    lax.fori_loop(0, NBLK, drain, 0)
    lax.fori_loop(0, NX, drain_x, 0)


def last_merge(chip, comb, other_ref, i, ofin, at):
    first = chip == 0

    def ordered(rows):
        mine, other = comb[i, rows, :], other_ref[i, rows, :]
        return jnp.where(first, mine, other), jnp.where(first, other, mine)

    s0, s1 = ordered(pl.ds(HALF * BLK, BLK))
    peak = jnp.maximum(s0, s1)
    f0 = jnp.exp2((s0 - peak) * EXP_SCALE)
    f1 = jnp.exp2((s1 - peak) * EXP_SCALE)
    total = f0 * pltpu.roll(s0, HD - HALF, 1) + f1 * pltpu.roll(s1, HD - HALF, 1)
    g0, g1 = f0 / total, f1 / total
    for j in range(HALF):
        a, b = ordered(pl.ds(j * BLK, BLK))
        ofin[at * BLK:(at + 1) * BLK, j * HD:(j + 1) * HD] = bcast_col(g0, j) * a + bcast_col(g1, j) * b


def finish_kernel(tok_h, wo_v, oa, comb_b, xrx_b, bout, tok, ofin, pbuf, prx, insem, ps, pr):
    me = lax.axis_index('sp')
    core = lax.rem(me, 2)
    mate = {'sp': me + 1 - 2 * core}
    tok_copy = pltpu.make_async_copy(tok_h, tok, insem)
    tok_copy.start()
    barrier = pltpu.get_barrier_semaphore()
    pl.semaphore_signal(barrier, inc=1, device_id=mate, device_id_type=MESH)
    for i in range(NBLK - NX):
        last_merge(me // 2, comb_b, xrx_b, i, ofin, i)
    lhs = jnp.concatenate([oa[...].astype(BF16), ofin[...].astype(BF16)], axis=0)
    pl.semaphore_wait(barrier, 1)

    def p_send(n):
        return pltpu.make_async_remote_copy(pbuf.at[n], prx.at[n], ps.at[n], pr.at[n],
                                            device_id=mate, device_id_type=MESH)

    for n in range(4):
        pbuf[n] = jnp.dot(lhs, wo_v[n], preferred_element_type=F32)
        p_send(n).start()
    tok_copy.wait()
    for n in range(4):
        p_send(n).wait_recv()
        sl = slice(n * WCH, (n + 1) * WCH)
        bout[:, sl] = (tok[:, sl].astype(F32) + (pbuf[n] + prx[n])).astype(BF16)
    for n in range(4):
        p_send(n).wait_send()


def write_kernel(pos_h, kv, vv, rep, comb_a, xrx, wo_v, ko, vo, nkv, oa, kva, vva, pos_s, nkv_s, patch, ksem, vsem, psem, osem):
    start = lax.axis_index('sp') * SLOTS
    slot16 = lax.broadcasted_iota(jnp.int32, (4 * KVH, HD), 0) // KVH

    def copies(i):
        r = pl.ds(i * BLK, BLK)
        return (pltpu.make_async_copy(kv.at[r], ko.at[r], ksem.at[i]),
                pltpu.make_async_copy(vv.at[r], vo.at[r], vsem.at[i]))

    pos_copy = pltpu.make_async_copy(pos_h, pos_s, osem.at[0])
    pos_copy.start()
    for c in copies(0):
        c.start()
    for b in range(SEQS):
        nkv_s[b] = jnp.concatenate([rep[0, pl.ds(b * 4 * KVH, KVH), :], rep[1, pl.ds(b * 4 * KVH, KVH), :]], axis=0).astype(BF16)
    pos_copy.wait()

    def each(i, do):
        for bb in range(BLK):
            b = i * BLK + bb
            rel = pos_s[b] - start

            @pl.when(jnp.logical_and(rel >= 0, rel < SLOTS))
            def _():
                base = pl.multiple_of(rel // 4 * (4 * KVH), 4 * KVH)
                mask = slot16 == lax.rem(rel, 4)
                for z, (ref, out) in enumerate(((kv, ko), (vv, vo))):
                    do(b, z, base, mask, ref, out)

    def merged(b, z, base, mask, ref):
        new = rep[z, pl.ds(b * 4 * KVH, 4 * KVH), :]
        old = ref[b, pl.ds(base, 4 * KVH), :].astype(F32)
        return jnp.where(mask, new, old).astype(BF16)

    def put(b, z, base, mask, ref, out):
        ref[b, pl.ds(base, 4 * KVH), :] = merged(b, z, base, mask, ref)

    def stage(b, z, base, mask, ref, out):
        patch[z, b] = merged(b, z, base, mask, ref)

    def patch_copy(b, z, base, out):
        return pltpu.make_async_copy(patch.at[z, b], out.at[b, pl.ds(base, 4 * KVH)], psem.at[z, b])

    for i in range(1, NBLK):
        each(i, put)
        if i > 1:
            for c in copies(i - 1):
                c.start()
    nkv_copy = pltpu.make_async_copy(nkv_s, nkv, osem.at[1])
    nkv_copy.start()
    each(0, stage)
    for c in copies(NBLK - 1):
        c.start()
    for i in range(NX):
        last_merge(lax.axis_index('sp') // 2, comb_a, xrx, i, oa, i)
    for c in copies(0):
        c.wait()
    each(0, lambda b, z, base, mask, ref, out: patch_copy(b, z, base, out).start())
    nkv_copy.wait()
    each(0, lambda b, z, base, mask, ref, out: patch_copy(b, z, base, out).wait())
    for i in range(1, NBLK):
        for c in copies(i):
            c.wait()


def solution(mesh):
    cache_spec = P('dp', 'sp', None, None)
    inv_freq = (np.float64(ROPE_THETA) ** (-np.arange(HD // 2) * 2.0 / HD)).astype(np.float32)
    freq2 = np.concatenate([inv_freq, inv_freq])
    vm = pl.BlockSpec(memory_space=pltpu.VMEM)
    hbm = pl.BlockSpec(memory_space=pl.ANY)
    dma = pltpu.SemaphoreType.DMA

    def device_step(tokens, positions, k_cache, v_cache, w_q, w_k, w_v, w_o, attn_norm, q_norm, k_norm):
        in_hbm = lambda x: pltpu.with_memory_space_constraint(x, pltpu.HBM)
        in_vmem = lambda x: pltpu.with_memory_space_constraint(x, pltpu.VMEM)
        rows = (SEQS, ROWS, HD)
        piece = (PIECE, HD)
        kv, vv, rep, wo_v, comb_a, comb_b, xrx_a = pl.pallas_call(
            attend_kernel,
            out_shape=(pltpu.VMEM(rows, BF16), pltpu.VMEM(rows, BF16),
                       pltpu.VMEM((2, SEQS * 4 * KVH, HD), F32), pltpu.VMEM((4, HALF * HD, WCH), BF16),
                       pltpu.VMEM((NX,) + piece, F32), pltpu.VMEM((NBLK - NX,) + piece, F32), pltpu.VMEM((NX,) + piece, F32)),
            in_specs=[hbm] * 12,
            out_specs=(vm,) * 7,
            scratch_shapes=[
                pltpu.SMEM((SEQS,), jnp.int32), pltpu.VMEM((SEQS, DIM), BF16), pltpu.VMEM((DIM // HD, HD), BF16),
                pltpu.VMEM((1, HD), BF16), pltpu.VMEM((1, HD), BF16), pltpu.VMEM((1, HD), F32), dma((6,)),
                pltpu.VMEM((RING, DIM, WCH), BF16),
                pltpu.VMEM((SEQS, DIM), BF16),
                pltpu.VMEM((SEQS, HD), F32), pltpu.VMEM((SEQS, HD), F32), pltpu.VMEM((SEQS, HD), F32),
                pltpu.VMEM((SEQS * HALF, HD), F32), pltpu.VMEM((SEQS * HALF, HD), F32),
                pltpu.VMEM((2 * HALF, ROWS), jnp.int32),
                pltpu.VMEM((NBLK, 2 * PIECE, HD), F32),
                pltpu.VMEM((NBLK,) + piece, F32),
                pltpu.VMEM((2, 4 * HALF, ROWS), F32), pltpu.VMEM((2, 4 * HALF, ROWS), BF16),
                dma((6,)), dma((NBLK,)), dma((NBLK,)), dma((4,)), dma, dma,
                dma((NBLK,)), dma((NBLK,)), dma((NX,)), dma((NX,)),
            ],
            compiler_params=pltpu.CompilerParams(collective_id=0, has_side_effects=True, vmem_limit_bytes=VMEM_LIMIT),
            name='attend',
        )(in_hbm(positions), in_hbm(tokens), in_hbm(attn_norm.reshape(DIM // HD, HD)), in_hbm(q_norm.reshape(1, HD)),
          in_hbm(k_norm.reshape(1, HD)), in_hbm(jnp.asarray(freq2).reshape(1, HD)), in_hbm(w_q), in_hbm(w_k), in_hbm(w_v), in_hbm(w_o),
          in_hbm(k_cache.reshape(rows)), in_hbm(v_cache.reshape(rows)))
        xrx_b = lax.ppermute(comb_b, 'sp', [(0, 2), (2, 0), (1, 3), (3, 1)])
        k_out, v_out, new_kv, oa, _, _ = pl.pallas_call(
            write_kernel,
            out_shape=(pltpu.HBM(rows, BF16), pltpu.HBM(rows, BF16), pltpu.HBM((SEQS, 2 * KVH, HD), BF16),
                       pltpu.VMEM((NX * BLK, HALF * HD), F32), pltpu.VMEM(rows, BF16), pltpu.VMEM(rows, BF16)),
            in_specs=[hbm, vm, vm, vm, vm, vm, vm],
            out_specs=(hbm, hbm, hbm, vm, vm, vm),
            input_output_aliases={1: 4, 2: 5},
            scratch_shapes=[pltpu.SMEM((SEQS,), jnp.int32), pltpu.VMEM((SEQS, 2 * KVH, HD), BF16),
                            pltpu.VMEM((2, BLK, 4 * KVH, HD), BF16),
                            dma((NBLK,)), dma((NBLK,)), dma((2, BLK)), dma((2,))],
            compiler_params=pltpu.CompilerParams(vmem_limit_bytes=VMEM_LIMIT),
            cost_estimate=pl.CostEstimate(flops=10**10, bytes_accessed=2**25, transcendentals=0),
            name='write',
        )(in_hbm(positions), in_vmem(kv), in_vmem(vv), in_vmem(rep), in_vmem(comb_a), in_vmem(xrx_a), in_vmem(wo_v))
        block_out = pl.pallas_call(
            finish_kernel,
            out_shape=jax.ShapeDtypeStruct((SEQS, DIM), BF16),
            in_specs=[hbm, vm, vm, vm, vm],
            out_specs=vm,
            scratch_shapes=[pltpu.VMEM((SEQS, DIM), BF16), pltpu.VMEM(((NBLK - NX) * BLK, HALF * HD), F32),
                            pltpu.VMEM((4, SEQS, WCH), F32), pltpu.VMEM((4, SEQS, WCH), F32), dma, dma((4,)), dma((4,))],
            compiler_params=pltpu.CompilerParams(collective_id=1, has_side_effects=True, vmem_limit_bytes=VMEM_LIMIT),
            name='finish',
        )(in_hbm(tokens), in_vmem(wo_v), in_vmem(oa), in_vmem(comb_b), xrx_b)
        return block_out, k_out.reshape(k_cache.shape), v_out.reshape(v_cache.shape), new_kv.reshape(SEQS, 2, KVH, HD)

    return jax.shard_map(device_step, mesh=mesh, in_specs=(P('dp', None), P('dp'), cache_spec, cache_spec, P(), P(), P(), P(), P(), P(), P()), out_specs=(P('dp', None), cache_spec, cache_spec, P('dp', None, None, None)), check_vma=False)
```

```python
import functools

import jax
import jax.numpy as jnp
import numpy as np
from jax import lax
from jax.experimental import pallas as pl
from jax.experimental.pallas import tpu as pltpu
from jax.sharding import PartitionSpec as P

NORM_EPS = 1e-6
ROPE_THETA = 1000000.0
MESH = pl.DeviceIdType.MESH
BF16 = jnp.bfloat16
F32 = jnp.float32

SEQS = 64
DIM = 2048
HD = 128
KVH = 4
HALF = 16
SLOTS = 256
ROWS = SLOTS * KVH
BLK = 8
NBLK = SEQS // BLK
AHEAD = 2
NX = 4
NA, NB = 6, 7
RING = 3
LAG = 2
WCH = 512
PIECE = (HALF + 1) * BLK
VMEM_LIMIT = 14 * 2**20
EXP_SCALE = HD ** -0.5 * 1.4426950408889634
NEG = -jnp.inf


def bcast_col(tile, col):
    return jnp.broadcast_to(tile[:, col:col + 1], (tile.shape[0], HD))


def attend_kernel(pos_h, tok_h, an_h, qn_h, kn_h, freq_h, wq, wk, wv, wo, kc, vc,
                  kv, vv, rep, wo_v, comb_a, comb_b, xrx,
                  pos_s, tok, an, qn, kn, freq, insem, w_s, hid, ang, cosr, sinr, qmine, qmate, colslot, opart, drx, sc, pr_s,
                  wsem, ksem, vsem, wosem, qs, qr, ds_, dr, xs, xr):
    me = lax.axis_index('sp')
    core = lax.rem(me, 2)
    chip = me // 2
    mate = {'sp': me + 1 - 2 * core}
    peer = {'sp': me + 2 - 4 * chip}

    def w_copy(n):
        if n < 4:
            src = wq.at[:, pl.ds(pl.multiple_of(core * (HALF * HD) + n * WCH, WCH), WCH)]
        else:
            src = (wk, wv)[n - 4]
        return pltpu.make_async_copy(src, w_s.at[n % RING], wsem.at[n])

    def wo_copy(n):
        src = wo.at[pl.ds(pl.multiple_of(core * (HALF * HD), HD), HALF * HD), pl.ds(n * WCH, WCH)]
        return pltpu.make_async_copy(src, wo_v.at[n], wosem.at[n])

    def k_copy(i):
        return pltpu.make_async_copy(kc.at[pl.ds(i * BLK, BLK)], kv.at[pl.ds(i * BLK, BLK)], ksem.at[i])

    def v_copy(i):
        return pltpu.make_async_copy(vc.at[pl.ds(i * BLK, BLK)], vv.at[pl.ds(i * BLK, BLK)], vsem.at[i])

    def q_send():
        return pltpu.make_async_remote_copy(qmine, qmate, qs, qr, device_id=mate, device_id_type=MESH)

    def d_send(i):
        return pltpu.make_async_remote_copy(opart.at[i, pl.ds(PIECE, PIECE)], drx.at[i], ds_.at[i], dr.at[i],
                                            device_id=mate, device_id_type=MESH)

    def x_send(i):
        return pltpu.make_async_remote_copy(comb_a.at[i], xrx.at[i], xs.at[i], xr.at[i],
                                            device_id=peer, device_id_type=MESH)

    small = [pltpu.make_async_copy(a, b, insem.at[z]) for z, (a, b) in enumerate(
        ((tok_h, tok), (pos_h, pos_s), (an_h, an), (qn_h, qn), (kn_h, kn), (freq_h, freq)))]
    for c in small:
        c.start()
    for n in range(AHEAD):
        w_copy(n).start()

    barrier = pltpu.get_barrier_semaphore()
    for other in (mate, peer):
        pl.semaphore_signal(barrier, inc=1, device_id=other, device_id_type=MESH)

    for c in small:
        c.wait()

    t = tok[...].astype(F32)
    inv = lax.rsqrt(jnp.sum(t * t, axis=-1, keepdims=True) * (1.0 / DIM) + NORM_EPS)
    gains = an[...].astype(F32)
    for j in range(DIM // HD):
        sl = slice(j * HD, (j + 1) * HD)
        hid[:, sl] = (tok[:, sl].astype(F32) * inv * gains[j:j + 1, :]).astype(BF16)

    lane1 = lax.broadcasted_iota(jnp.int32, (1, HD), 1)

    def angle(b, carry):
        ang[pl.ds(b, 1), :] = freq[...] * pos_s[b].astype(F32)
        return carry

    lax.fori_loop(0, SEQS, angle, 0)
    cosr[...] = jnp.cos(ang[...])
    sinr[...] = jnp.sin(ang[...]) * jnp.where(lane1 < HD // 2, -1.0, 1.0)

    row = lax.broadcasted_iota(jnp.int32, (2 * HALF, ROWS), 0)
    col = lax.broadcasted_iota(jnp.int32, (2 * HALF, ROWS), 1)
    half_of_row = jnp.where(row < HALF, core, 1 - core)
    kv_of_row = half_of_row * 2 + lax.rem(row, HALF) // 8
    colslot[...] = jnp.where(lax.rem(col, KVH) == kv_of_row, col // KVH, 1 << 20)

    qgain = qn[...].astype(F32)
    kgain = kn[...].astype(F32)

    def norm_rope(x, gain):
        y = x * lax.rsqrt(jnp.mean(x * x, axis=-1, keepdims=True) + NORM_EPS) * gain
        y = y * cosr[...] + pltpu.roll(y, HD // 2, 1) * sinr[...]
        return y.astype(BF16).astype(F32)

    for n in range(6):
        w_copy(n).wait()
        if n + AHEAD < 6:
            w_copy(n + AHEAD).start()
        else:
            k_copy(n + AHEAD - 6).start()
            v_copy(n + AHEAD - 6).start()
        proj = jnp.dot(hid[...], w_s[n % RING], preferred_element_type=F32).astype(BF16).astype(F32)
        for j in range(WCH // HD):
            x = proj[:, j * HD:(j + 1) * HD]
            if n < 4:
                qmine[pl.ds(n * 4 + j, SEQS, stride=HALF), :] = norm_rope(x, qgain)
            else:
                y = norm_rope(x, kgain) if n == 4 else x
                for c in range(4):
                    rep[n - 4, pl.ds(c * KVH + j, SEQS, stride=4 * KVH), :] = y
        if n == 3:
            pl.semaphore_wait(barrier, 2)
            q_send().start()
    start = me * SLOTS
    lane = lax.broadcasted_iota(jnp.int32, (HALF, HD), 1)
    lrow = lax.broadcasted_iota(jnp.int32, (HALF, HD), 0)
    lane8 = lax.broadcasted_iota(jnp.int32, (BLK, HD), 1)
    q_send().wait()

    def attend(i):
        ob = opart.at[i]
        def load_q(pair):
            bs = [i * BLK + 2 * pair + z for z in range(2)]
            return bs, [jnp.concatenate([qmine[pl.ds(pl.multiple_of(b * HALF, HALF), HALF), :],
                                         qmate[pl.ds(pl.multiple_of(b * HALF, HALF), HALF), :]], axis=0) for b in bs]

        def new_rows(z, b):
            return jnp.concatenate([jnp.broadcast_to(rep[z, pl.ds(b * 4 * KVH + h, 1), :], (8, HD))
                                    for h in (2 * core, 2 * core + 1, 2 - 2 * core, 3 - 2 * core)], axis=0)

        def scores(pair):
            bs, qf = load_q(pair)
            zero = jnp.zeros((2 * HALF, HD), BF16)
            lhs = jnp.concatenate([jnp.concatenate([qf[0].astype(BF16), zero], axis=1),
                                   jnp.concatenate([zero, qf[1].astype(BF16)], axis=1)], axis=0)
            keys = jnp.concatenate([kv[bs[0]], kv[bs[1]]], axis=1)
            sc[pair % 2] = lax.dot_general(lhs, keys, (((1,), (1,)), ((), ())), preferred_element_type=F32)

        def soft(pair):
            bs, qf = load_q(pair)
            out = []
            for z in range(2):
                b = bs[z]
                rel = pos_s[b] - start
                owner = jnp.logical_and(rel >= 0, rel < SLOTS)
                snew = jnp.where(owner, jnp.sum(qf[z] * new_rows(0, b), axis=-1, keepdims=True), NEG)
                sm = jnp.where(colslot[...] < rel, sc[pair % 2, z * 2 * HALF:(z + 1) * 2 * HALF], NEG)
                peak = jnp.maximum(jnp.max(sm, axis=-1, keepdims=True), snew)
                safe = jnp.where(peak == NEG, 0.0, peak)
                p = jnp.exp2((sm - safe) * EXP_SCALE)
                pn = jnp.exp2((snew - safe) * EXP_SCALE)
                pr_s[pair % 2, z * 2 * HALF:(z + 1) * 2 * HALF, :] = p.astype(BF16)
                out.append((pn.astype(BF16).astype(F32), jnp.sum(p, axis=-1, keepdims=True) + pn, peak))
            return out

        def mix(pair, st3):
            bs = [i * BLK + 2 * pair + z for z in range(2)]
            values = jnp.concatenate([vv[bs[0]], vv[bs[1]]], axis=1)
            mixed = jnp.dot(pr_s[pair % 2], values, preferred_element_type=F32)
            for z in range(2):
                extra, total, peak = st3[z]
                o = mixed[z * 2 * HALF:(z + 1) * 2 * HALF, z * HD:(z + 1) * HD] + extra * new_rows(1, bs[z])
                bb = 2 * pair + z
                for h in range(2):
                    hs = slice(h * HALF, (h + 1) * HALF)
                    ob[pl.ds(h * PIECE + bb, HALF, stride=BLK), :] = o[hs]
                    st = jnp.where(lane == lrow, peak[hs], jnp.where(lane == lrow + HALF, total[hs], 0.0))
                    ob[pl.ds(h * PIECE + HALF * BLK + bb, 1), :] = jnp.sum(st, axis=0, keepdims=True)

        scores(0)
        for pair in range(BLK // 2):
            if pair + 1 < BLK // 2:
                scores(pair + 1)
            mix(pair, soft(pair))

    def combine(i, comb, at):
        s0 = opart[i, pl.ds(HALF * BLK, BLK), :]
        s1 = drx[i, pl.ds(HALF * BLK, BLK), :]
        peak = jnp.maximum(s0, s1)
        safe = jnp.where(peak == NEG, 0.0, peak)
        f0 = jnp.exp2((s0 - safe) * EXP_SCALE)
        f1 = jnp.exp2((s1 - safe) * EXP_SCALE)
        total = f0 * pltpu.roll(s0, HD - HALF, 1) + f1 * pltpu.roll(s1, HD - HALF, 1)
        comb[at, pl.ds(HALF * BLK, BLK), :] = jnp.where(
            lane8 < HALF, peak, jnp.where(lane8 < 2 * HALF, pltpu.roll(total, HALF, 1), 0.0))
        for j in range(HALF):
            rows = pl.ds(j * BLK, BLK)
            comb[at, rows, :] = bcast_col(f0, j) * opart[i, rows, :] + bcast_col(f1, j) * drx[i, rows, :]

    def fetch(i):
        k_copy(i).wait()
        v_copy(i).wait()

        @pl.when(i + AHEAD < NBLK)
        def _():
            k_copy(i + AHEAD).start()
            v_copy(i + AHEAD).start()

        @pl.when(i + AHEAD == NBLK)
        def _():
            for n in range(4):
                wo_copy(n).start()

    def early(i, carry):
        fetch(i)
        attend(i)
        d_send(i).start()
        return carry

    def sending(i, carry):
        fetch(i)
        d_send(i - LAG).wait_recv()
        combine(i - LAG, comb_a, i - LAG)
        attend(i)
        d_send(i).start()
        x_send(i - LAG).start()
        return carry

    def keeping(i, carry):
        fetch(i)
        d_send(i - LAG).wait_recv()
        combine(i - LAG, comb_b, i - LAG - NX)
        attend(i)
        d_send(i).start()
        return carry

    def late(i, carry):
        d_send(i).wait_recv()
        combine(i, comb_b, i - NX)
        return carry

    lax.fori_loop(0, LAG, early, 0)
    lax.fori_loop(LAG, LAG + NX, sending, 0)
    lax.fori_loop(LAG + NX, NBLK, keeping, 0)
    lax.fori_loop(NBLK - LAG, NBLK, late, 0)

    for n in range(4):
        wo_copy(n).wait()

    def drain(i, carry):
        d_send(i).wait_send()
        return carry

    def drain_x(i, carry):
        x_send(i).wait()
        return carry

    lax.fori_loop(0, NBLK, drain, 0)
    lax.fori_loop(0, NX, drain_x, 0)


def last_merge(chip, comb, other_ref, i, ofin, at):
    first = chip == 0

    def ordered(rows):
        mine, other = comb[i, rows, :], other_ref[i, rows, :]
        return jnp.where(first, mine, other), jnp.where(first, other, mine)

    s0, s1 = ordered(pl.ds(HALF * BLK, BLK))
    peak = jnp.maximum(s0, s1)
    f0 = jnp.exp2((s0 - peak) * EXP_SCALE)
    f1 = jnp.exp2((s1 - peak) * EXP_SCALE)
    total = f0 * pltpu.roll(s0, HD - HALF, 1) + f1 * pltpu.roll(s1, HD - HALF, 1)
    g0, g1 = f0 / total, f1 / total
    for j in range(HALF):
        a, b = ordered(pl.ds(j * BLK, BLK))
        ofin[at * BLK:(at + 1) * BLK, j * HD:(j + 1) * HD] = bcast_col(g0, j) * a + bcast_col(g1, j) * b


def block_copies(i, kv, vv, ko, vo, ksem, vsem):
    r = pl.ds(i * BLK, BLK)
    return (pltpu.make_async_copy(kv.at[r], ko.at[r], ksem.at[i]),
            pltpu.make_async_copy(vv.at[r], vo.at[r], vsem.at[i]))


def product_kernel(kv, vv, ki, vi, oa, comb_b, xrx_b, wo_v, ko, vo, part, ofin, ksem, vsem):
    for i in range(NA, NB):
        for c in block_copies(i, kv, vv, ko, vo, ksem, vsem):
            c.start()
    for i in range(NBLK - NX):
        last_merge(lax.axis_index('sp') // 2, comb_b, xrx_b, i, ofin, i)
    lhs = jnp.concatenate([oa[...].astype(BF16), ofin[...].astype(BF16)], axis=0)
    for n in range(4):
        part[:, n * WCH:(n + 1) * WCH] = jnp.dot(lhs, wo_v[n], preferred_element_type=F32)
    for i in range(NA, NB):
        for c in block_copies(i, kv, vv, ko, vo, ksem, vsem):
            c.wait()


def rest_kernel(kv, vv, ki, vi, ko, vo, ksem, vsem):
    for i in range(NB, NBLK):
        for c in block_copies(i, kv, vv, ko, vo, ksem, vsem):
            c.start()
    for i in range(NB, NBLK):
        for c in block_copies(i, kv, vv, ko, vo, ksem, vsem):
            c.wait()


def write_kernel(pos_h, kv, vv, rep, comb_a, xrx, wo_v, ko, vo, nkv, oa, kva, vva, wo_a, pos_s, nkv_s, patch, ksem, vsem, psem, osem):
    start = lax.axis_index('sp') * SLOTS
    slot16 = lax.broadcasted_iota(jnp.int32, (4 * KVH, HD), 0) // KVH

    def copies(i):
        return block_copies(i, kv, vv, ko, vo, ksem, vsem)

    pos_copy = pltpu.make_async_copy(pos_h, pos_s, osem.at[0])
    pos_copy.start()
    for c in copies(0):
        c.start()
    for b in range(SEQS):
        nkv_s[b] = jnp.concatenate([rep[0, pl.ds(b * 4 * KVH, KVH), :], rep[1, pl.ds(b * 4 * KVH, KVH), :]], axis=0).astype(BF16)
    pos_copy.wait()

    def each(i, do):
        for bb in range(BLK):
            b = i * BLK + bb
            rel = pos_s[b] - start

            @pl.when(jnp.logical_and(rel >= 0, rel < SLOTS))
            def _():
                base = pl.multiple_of(rel // 4 * (4 * KVH), 4 * KVH)
                mask = slot16 == lax.rem(rel, 4)
                for z, (ref, out) in enumerate(((kv, ko), (vv, vo))):
                    do(b, z, base, mask, ref, out)

    def merged(b, z, base, mask, ref):
        new = rep[z, pl.ds(b * 4 * KVH, 4 * KVH), :]
        old = ref[b, pl.ds(base, 4 * KVH), :].astype(F32)
        return jnp.where(mask, new, old).astype(BF16)

    def put(b, z, base, mask, ref, out):
        ref[b, pl.ds(base, 4 * KVH), :] = merged(b, z, base, mask, ref)

    def stage(b, z, base, mask, ref, out):
        patch[z, b] = merged(b, z, base, mask, ref)

    def patch_copy(b, z, base, out):
        return pltpu.make_async_copy(patch.at[z, b], out.at[b, pl.ds(base, 4 * KVH)], psem.at[z, b])

    for i in range(1, NBLK):
        each(i, put)
        if 1 < i <= NA:
            for c in copies(i - 1):
                c.start()
    nkv_copy = pltpu.make_async_copy(nkv_s, nkv, osem.at[1])
    nkv_copy.start()
    each(0, stage)
    for i in range(NX):
        last_merge(lax.axis_index('sp') // 2, comb_a, xrx, i, oa, i)
    for c in copies(0):
        c.wait()
    each(0, lambda b, z, base, mask, ref, out: patch_copy(b, z, base, out).start())
    nkv_copy.wait()
    each(0, lambda b, z, base, mask, ref, out: patch_copy(b, z, base, out).wait())
    for i in range(1, NA):
        for c in copies(i):
            c.wait()


def solution(mesh):
    cache_spec = P('dp', 'sp', None, None)
    inv_freq = (np.float64(ROPE_THETA) ** (-np.arange(HD // 2) * 2.0 / HD)).astype(np.float32)
    freq2 = np.concatenate([inv_freq, inv_freq])
    vm = pl.BlockSpec(memory_space=pltpu.VMEM)
    hbm = pl.BlockSpec(memory_space=pl.ANY)
    dma = pltpu.SemaphoreType.DMA

    def device_step(tokens, positions, k_cache, v_cache, w_q, w_k, w_v, w_o, attn_norm, q_norm, k_norm):
        in_hbm = lambda x: pltpu.with_memory_space_constraint(x, pltpu.HBM)
        in_vmem = lambda x: pltpu.with_memory_space_constraint(x, pltpu.VMEM)
        rows = (SEQS, ROWS, HD)
        piece = (PIECE, HD)
        kv, vv, rep, wo_v, comb_a, comb_b, xrx_a = pl.pallas_call(
            attend_kernel,
            out_shape=(pltpu.VMEM(rows, BF16), pltpu.VMEM(rows, BF16),
                       pltpu.VMEM((2, SEQS * 4 * KVH, HD), F32), pltpu.VMEM((4, HALF * HD, WCH), BF16),
                       pltpu.VMEM((NX,) + piece, F32), pltpu.VMEM((NBLK - NX,) + piece, F32), pltpu.VMEM((NX,) + piece, F32)),
            in_specs=[hbm] * 12,
            out_specs=(vm,) * 7,
            scratch_shapes=[
                pltpu.SMEM((SEQS,), jnp.int32), pltpu.VMEM((SEQS, DIM), BF16), pltpu.VMEM((DIM // HD, HD), BF16),
                pltpu.VMEM((1, HD), BF16), pltpu.VMEM((1, HD), BF16), pltpu.VMEM((1, HD), F32), dma((6,)),
                pltpu.VMEM((RING, DIM, WCH), BF16),
                pltpu.VMEM((SEQS, DIM), BF16),
                pltpu.VMEM((SEQS, HD), F32), pltpu.VMEM((SEQS, HD), F32), pltpu.VMEM((SEQS, HD), F32),
                pltpu.VMEM((SEQS * HALF, HD), F32), pltpu.VMEM((SEQS * HALF, HD), F32),
                pltpu.VMEM((2 * HALF, ROWS), jnp.int32),
                pltpu.VMEM((NBLK, 2 * PIECE, HD), F32),
                pltpu.VMEM((NBLK,) + piece, F32),
                pltpu.VMEM((2, 4 * HALF, ROWS), F32), pltpu.VMEM((2, 4 * HALF, ROWS), BF16),
                dma((6,)), dma((NBLK,)), dma((NBLK,)), dma((4,)), dma, dma,
                dma((NBLK,)), dma((NBLK,)), dma((NX,)), dma((NX,)),
            ],
            compiler_params=pltpu.CompilerParams(collective_id=0, has_side_effects=True, vmem_limit_bytes=VMEM_LIMIT),
            name='attend',
        )(in_hbm(positions), in_hbm(tokens), in_hbm(attn_norm.reshape(DIM // HD, HD)), in_hbm(q_norm.reshape(1, HD)),
          in_hbm(k_norm.reshape(1, HD)), in_hbm(jnp.asarray(freq2).reshape(1, HD)), in_hbm(w_q), in_hbm(w_k), in_hbm(w_v), in_hbm(w_o),
          in_hbm(k_cache.reshape(rows)), in_hbm(v_cache.reshape(rows)))
        xrx_b = lax.ppermute(comb_b, 'sp', [(0, 2), (2, 0), (1, 3), (3, 1)])
        k_out, v_out, new_kv, oa, kv, vv, wo_v = pl.pallas_call(
            write_kernel,
            out_shape=(pltpu.HBM(rows, BF16), pltpu.HBM(rows, BF16), pltpu.HBM((SEQS, 2 * KVH, HD), BF16),
                       pltpu.VMEM((NX * BLK, HALF * HD), F32), pltpu.VMEM(rows, BF16), pltpu.VMEM(rows, BF16),
                       pltpu.VMEM((4, HALF * HD, WCH), BF16)),
            in_specs=[hbm, vm, vm, vm, vm, vm, vm],
            out_specs=(hbm, hbm, hbm, vm, vm, vm, vm),
            input_output_aliases={1: 4, 2: 5, 6: 6},
            scratch_shapes=[pltpu.SMEM((SEQS,), jnp.int32), pltpu.VMEM((SEQS, 2 * KVH, HD), BF16),
                            pltpu.VMEM((2, BLK, 4 * KVH, HD), BF16),
                            dma((NBLK,)), dma((NBLK,)), dma((2, BLK)), dma((2,))],
            compiler_params=pltpu.CompilerParams(vmem_limit_bytes=VMEM_LIMIT),
            cost_estimate=pl.CostEstimate(flops=10**10, bytes_accessed=2**25, transcendentals=0),
            name='write',
        )(in_hbm(positions), in_vmem(kv), in_vmem(vv), in_vmem(rep), in_vmem(comb_a), in_vmem(xrx_a), in_vmem(wo_v))
        k_out, v_out, part = pl.pallas_call(
            product_kernel,
            out_shape=(pltpu.HBM(rows, BF16), pltpu.HBM(rows, BF16), pltpu.VMEM((SEQS, DIM), F32)),
            in_specs=[vm, vm, hbm, hbm, vm, vm, vm, vm],
            out_specs=(hbm, hbm, vm),
            input_output_aliases={2: 0, 3: 1},
            scratch_shapes=[pltpu.VMEM(((NBLK - NX) * BLK, HALF * HD), F32), dma((NBLK,)), dma((NBLK,))],
            compiler_params=pltpu.CompilerParams(vmem_limit_bytes=VMEM_LIMIT),
            cost_estimate=pl.CostEstimate(flops=2 * SEQS * DIM * DIM, bytes_accessed=2**22, transcendentals=0),
            name='product',
        )(in_vmem(kv), in_vmem(vv), k_out, v_out, in_vmem(oa), in_vmem(comb_b), in_vmem(xrx_b), in_vmem(wo_v))
        other = lax.ppermute(part, 'sp', [(0, 1), (1, 0), (2, 3), (3, 2)])
        k_out, v_out = pl.pallas_call(
            rest_kernel,
            out_shape=(pltpu.HBM(rows, BF16), pltpu.HBM(rows, BF16)),
            in_specs=[vm, vm, hbm, hbm],
            out_specs=(hbm, hbm),
            input_output_aliases={2: 0, 3: 1},
            scratch_shapes=[dma((NBLK,)), dma((NBLK,))],
            compiler_params=pltpu.CompilerParams(vmem_limit_bytes=VMEM_LIMIT),
            cost_estimate=pl.CostEstimate(flops=10**9, bytes_accessed=2**22, transcendentals=0),
            name='rest',
        )(in_vmem(kv), in_vmem(vv), k_out, v_out)
        block_out = (tokens.astype(F32) + (part + other)).astype(BF16)
        return block_out, k_out.reshape(k_cache.shape), v_out.reshape(v_cache.shape), new_kv.reshape(SEQS, 2, KVH, HD)

    return jax.shard_map(device_step, mesh=mesh, in_specs=(P('dp', None), P('dp'), cache_spec, cache_spec, P(), P(), P(), P(), P(), P(), P()), out_specs=(P('dp', None), cache_spec, cache_spec, P('dp', None, None, None)), check_vma=False)
```

```python
import functools

import jax
import jax.numpy as jnp
import numpy as np
from jax import lax
from jax.experimental import pallas as pl
from jax.experimental.pallas import tpu as pltpu
from jax.sharding import PartitionSpec as P

NORM_EPS = 1e-6
ROPE_THETA = 1000000.0
MESH = pl.DeviceIdType.MESH
BF16 = jnp.bfloat16
F32 = jnp.float32

SEQS = 64
DIM = 2048
HD = 128
KVH = 4
HALF = 16
SLOTS = 256
ROWS = SLOTS * KVH
BLK = 8
NBLK = SEQS // BLK
AHEAD = 2
NX = 4
NA, NB = 6, 7
NW = 5
WAHEAD = 3
RING = 4
LAG = 2
WCH = 512
PIECE = (HALF + 1) * BLK
VMEM_LIMIT = 14 * 2**20
EXP_SCALE = HD ** -0.5 * 1.4426950408889634
NEG = -jnp.inf


def bcast_col(tile, col):
    return jnp.broadcast_to(tile[:, col:col + 1], (tile.shape[0], HD))


def attend_kernel(pos_h, tok_h, an_h, qn_h, kn_h, freq_h, wq, wk, wv, wo, kc, vc,
                  kv, vv, rep, wo_v, comb_a, comb_b, xrx,
                  pos_s, tok, an, qn, kn, freq, insem, proj, w_s, hid, ang, cosr, sinr, qmine, qmate, colslot, opart, drx, sc, pr_s,
                  wsem, ksem, vsem, wosem, qs, qr, ds_, dr, xs, xr):
    me = lax.axis_index('sp')
    core = lax.rem(me, 2)
    chip = me // 2
    mate = {'sp': me + 1 - 2 * core}
    peer = {'sp': me + 2 - 4 * chip}

    def w_copy(n, src=None):
        if n < 4:
            src = wq.at[:, pl.ds(pl.multiple_of(core * (HALF * HD) + n * WCH, WCH), WCH)]
        return pltpu.make_async_copy(src, w_s.at[n % RING], wsem.at[n])

    def w_start(n):
        if n < 4:
            w_copy(n).start()
        else:
            @pl.when(core == 0)
            def _():
                w_copy(n, wk).start()

            @pl.when(core == 1)
            def _():
                w_copy(n, wv).start()

    def wo_copy(n):
        src = wo.at[pl.ds(pl.multiple_of(core * (HALF * HD), HD), HALF * HD), pl.ds(n * WCH, WCH)]
        return pltpu.make_async_copy(src, wo_v.at[n], wosem.at[n])

    def k_copy(i):
        return pltpu.make_async_copy(kc.at[pl.ds(i * BLK, BLK)], kv.at[pl.ds(i * BLK, BLK)], ksem.at[i])

    def v_copy(i):
        return pltpu.make_async_copy(vc.at[pl.ds(i * BLK, BLK)], vv.at[pl.ds(i * BLK, BLK)], vsem.at[i])

    def q_send(h):
        return pltpu.make_async_remote_copy(qmine.at[h], qmate.at[h], qs.at[h], qr.at[h], device_id=mate, device_id_type=MESH)

    def new_send():
        return pltpu.make_async_remote_copy(rep.at[core], rep.at[core], qs.at[2], qr.at[2], device_id=mate, device_id_type=MESH)

    def d_send(i):
        return pltpu.make_async_remote_copy(opart.at[i, pl.ds(PIECE, PIECE)], drx.at[i], ds_.at[i], dr.at[i],
                                            device_id=mate, device_id_type=MESH)

    def x_send(i):
        return pltpu.make_async_remote_copy(comb_a.at[i], xrx.at[i], xs.at[i], xr.at[i],
                                            device_id=peer, device_id_type=MESH)

    small = [pltpu.make_async_copy(a, b, insem.at[z]) for z, (a, b) in enumerate(
        ((tok_h, tok), (pos_h, pos_s), (an_h, an), (qn_h, qn), (kn_h, kn), (freq_h, freq)))]
    for c in small:
        c.start()
    for n in range(WAHEAD):
        w_start(n)

    barrier = pltpu.get_barrier_semaphore()
    for other in (mate, peer):
        pl.semaphore_signal(barrier, inc=1, device_id=other, device_id_type=MESH)

    for c in small[1:]:
        c.wait()
    lane1 = lax.broadcasted_iota(jnp.int32, (1, HD), 1)

    def angle(b, carry):
        ang[pl.ds(b, 1), :] = freq[...] * pos_s[b].astype(F32)
        return carry

    lax.fori_loop(0, SEQS, angle, 0, unroll=8)
    cosr[...] = jnp.cos(ang[...])
    sinr[...] = jnp.sin(ang[...]) * jnp.where(lane1 < HD // 2, -1.0, 1.0)

    row = lax.broadcasted_iota(jnp.int32, (2 * HALF, ROWS), 0)
    col = lax.broadcasted_iota(jnp.int32, (2 * HALF, ROWS), 1)
    half_of_row = jnp.where(row < HALF, core, 1 - core)
    kv_of_row = half_of_row * 2 + lax.rem(row, HALF) // 8
    colslot[...] = jnp.where(lax.rem(col, KVH) == kv_of_row, col // KVH, 1 << 20)

    small[0].wait()
    t = tok[...].astype(F32)
    inv = lax.rsqrt(jnp.sum(t * t, axis=-1, keepdims=True) * (1.0 / DIM) + NORM_EPS)
    gains = an[...].astype(F32)
    for j in range(DIM // HD):
        sl = slice(j * HD, (j + 1) * HD)
        hid[:, sl] = (tok[:, sl].astype(F32) * inv * gains[j:j + 1, :]).astype(BF16)

    qgain = qn[...].astype(F32)
    kgain = kn[...].astype(F32)

    def norm_rope(x, gain):
        y = x * lax.rsqrt(jnp.mean(x * x, axis=-1, keepdims=True) + NORM_EPS) * gain
        y = y * cosr[...] + pltpu.roll(y, HD // 2, 1) * sinr[...]
        return y.astype(BF16).astype(F32)

    def post(n):
        for j in range(WCH // HD):
            x = proj[n % 2, :, j * HD:(j + 1) * HD].astype(BF16).astype(F32)
            if n < 4:
                qmine.at[n // 2][pl.ds(n % 2 * 4 + j, SEQS, stride=8), :] = norm_rope(x, qgain)
            else:
                rep.at[core][pl.ds(j, SEQS, stride=KVH), :] = jnp.where(core == 0, norm_rope(x, kgain), x)

    for n in range(NW):
        w_copy(n, wk).wait()
        if n + WAHEAD < NW:
            w_start(n + WAHEAD)
        elif n + WAHEAD - NW < AHEAD:
            k_copy(n + WAHEAD - NW).start()
            v_copy(n + WAHEAD - NW).start()
        proj[n % 2] = jnp.dot(hid[...], w_s[n % RING], preferred_element_type=F32)
        if n > 0:
            post(n - 1)
        if n == 2:
            pl.semaphore_wait(barrier, 2)
            q_send(0).start()
        if n == 4:
            q_send(1).start()
    for i in range(WAHEAD, AHEAD):
        k_copy(i).start()
        v_copy(i).start()
    post(NW - 1)
    new_send().start()
    start = me * SLOTS
    lane = lax.broadcasted_iota(jnp.int32, (HALF, HD), 1)
    lrow = lax.broadcasted_iota(jnp.int32, (HALF, HD), 0)
    lane8 = lax.broadcasted_iota(jnp.int32, (BLK, HD), 1)
    for h in range(2):
        q_send(h).wait()
    new_send().wait()

    def attend(i):
        ob = opart.at[i]
        def load_q(pair):
            bs = [i * BLK + 2 * pair + z for z in range(2)]
            return bs, [jnp.concatenate([ref[h, pl.ds(pl.multiple_of(b * 8, 8), 8), :]
                                         for ref in (qmine, qmate) for h in range(2)], axis=0) for b in bs]

        def new_rows(z, b):
            return jnp.concatenate([jnp.broadcast_to(rep[z, pl.ds(b * KVH + h, 1), :], (8, HD))
                                    for h in (2 * core, 2 * core + 1, 2 - 2 * core, 3 - 2 * core)], axis=0)

        def scores(pair):
            bs, qf = load_q(pair)
            zero = jnp.zeros((2 * HALF, HD), BF16)
            lhs = jnp.concatenate([jnp.concatenate([qf[0].astype(BF16), zero], axis=1),
                                   jnp.concatenate([zero, qf[1].astype(BF16)], axis=1)], axis=0)
            keys = jnp.concatenate([kv[bs[0]], kv[bs[1]]], axis=1)
            sc[pair % 2] = lax.dot_general(lhs, keys, (((1,), (1,)), ((), ())), preferred_element_type=F32)

        def soft(pair):
            bs, qf = load_q(pair)
            out = []
            for z in range(2):
                b = bs[z]
                rel = pos_s[b] - start
                owner = jnp.logical_and(rel >= 0, rel < SLOTS)
                snew = jnp.where(owner, jnp.sum(qf[z] * new_rows(0, b), axis=-1, keepdims=True), NEG)
                sm = jnp.where(colslot[...] < rel, sc[pair % 2, z * 2 * HALF:(z + 1) * 2 * HALF], NEG)
                peak = jnp.maximum(jnp.max(sm, axis=-1, keepdims=True), snew)
                safe = jnp.where(peak == NEG, 0.0, peak)
                p = jnp.exp2((sm - safe) * EXP_SCALE)
                pn = jnp.exp2((snew - safe) * EXP_SCALE)
                pr_s[pair % 2, z * 2 * HALF:(z + 1) * 2 * HALF, :] = p.astype(BF16)
                out.append((pn.astype(BF16).astype(F32), jnp.sum(p, axis=-1, keepdims=True) + pn, peak))
            return out

        def mix(pair, st3):
            bs = [i * BLK + 2 * pair + z for z in range(2)]
            values = jnp.concatenate([vv[bs[0]], vv[bs[1]]], axis=1)
            mixed = jnp.dot(pr_s[pair % 2], values, preferred_element_type=F32)
            for z in range(2):
                extra, total, peak = st3[z]
                o = mixed[z * 2 * HALF:(z + 1) * 2 * HALF, z * HD:(z + 1) * HD] + extra * new_rows(1, bs[z])
                bb = 2 * pair + z
                for h in range(2):
                    hs = slice(h * HALF, (h + 1) * HALF)
                    ob[pl.ds(h * PIECE + bb, HALF, stride=BLK), :] = o[hs]
                    st = jnp.where(lane == lrow, peak[hs], jnp.where(lane == lrow + HALF, total[hs], 0.0))
                    ob[pl.ds(h * PIECE + HALF * BLK + bb, 1), :] = jnp.sum(st, axis=0, keepdims=True)

        scores(0)
        for pair in range(BLK // 2):
            if pair + 1 < BLK // 2:
                scores(pair + 1)
            mix(pair, soft(pair))

    def combine(i, comb, at):
        s0 = opart[i, pl.ds(HALF * BLK, BLK), :]
        s1 = drx[i, pl.ds(HALF * BLK, BLK), :]
        peak = jnp.maximum(s0, s1)
        safe = jnp.where(peak == NEG, 0.0, peak)
        f0 = jnp.exp2((s0 - safe) * EXP_SCALE)
        f1 = jnp.exp2((s1 - safe) * EXP_SCALE)
        total = f0 * pltpu.roll(s0, HD - HALF, 1) + f1 * pltpu.roll(s1, HD - HALF, 1)
        comb[at, pl.ds(HALF * BLK, BLK), :] = jnp.where(
            lane8 < HALF, peak, jnp.where(lane8 < 2 * HALF, pltpu.roll(total, HALF, 1), 0.0))
        for j in range(HALF):
            rows = pl.ds(j * BLK, BLK)
            comb[at, rows, :] = bcast_col(f0, j) * opart[i, rows, :] + bcast_col(f1, j) * drx[i, rows, :]

    def fetch(i):
        k_copy(i).wait()
        v_copy(i).wait()

        @pl.when(i + AHEAD < NBLK)
        def _():
            k_copy(i + AHEAD).start()
            v_copy(i + AHEAD).start()

        @pl.when(i + AHEAD == NBLK)
        def _():
            for n in range(4):
                wo_copy(n).start()

    def early(i, carry):
        fetch(i)
        attend(i)
        d_send(i).start()
        return carry

    def sending(i, carry):
        fetch(i)
        d_send(i - LAG).wait_recv()
        combine(i - LAG, comb_a, i - LAG)
        attend(i)
        d_send(i).start()
        x_send(i - LAG).start()
        return carry

    def keeping(i, carry):
        fetch(i)
        d_send(i - LAG).wait_recv()
        combine(i - LAG, comb_b, i - LAG - NX)
        attend(i)
        d_send(i).start()
        return carry

    def late(i, carry):
        d_send(i).wait_recv()
        combine(i, comb_b, i - NX)
        return carry

    lax.fori_loop(0, LAG, early, 0)
    lax.fori_loop(LAG, LAG + NX, sending, 0)
    lax.fori_loop(LAG + NX, NBLK, keeping, 0)
    lax.fori_loop(NBLK - LAG, NBLK, late, 0)

    for n in range(4):
        wo_copy(n).wait()

    def drain(i, carry):
        d_send(i).wait_send()
        return carry

    def drain_x(i, carry):
        x_send(i).wait()
        return carry

    lax.fori_loop(0, NBLK, drain, 0)
    lax.fori_loop(0, NX, drain_x, 0)


def last_merge(chip, comb, other_ref, i, ofin, at):
    first = chip == 0

    def ordered(rows):
        mine, other = comb[i, rows, :], other_ref[i, rows, :]
        return jnp.where(first, mine, other), jnp.where(first, other, mine)

    s0, s1 = ordered(pl.ds(HALF * BLK, BLK))
    peak = jnp.maximum(s0, s1)
    f0 = jnp.exp2((s0 - peak) * EXP_SCALE)
    f1 = jnp.exp2((s1 - peak) * EXP_SCALE)
    total = f0 * pltpu.roll(s0, HD - HALF, 1) + f1 * pltpu.roll(s1, HD - HALF, 1)
    g0, g1 = f0 / total, f1 / total
    for j in range(HALF):
        a, b = ordered(pl.ds(j * BLK, BLK))
        ofin[at * BLK:(at + 1) * BLK, j * HD:(j + 1) * HD] = bcast_col(g0, j) * a + bcast_col(g1, j) * b


def block_copies(i, kv, vv, ko, vo, ksem, vsem):
    r = pl.ds(i * BLK, BLK)
    return (pltpu.make_async_copy(kv.at[r], ko.at[r], ksem.at[i]),
            pltpu.make_async_copy(vv.at[r], vo.at[r], vsem.at[i]))


def product_kernel(kv, vv, ki, vi, oa, comb_b, xrx_b, wo_v, ko, vo, part, ofin, ksem, vsem):
    for i in range(NA, NB):
        for c in block_copies(i, kv, vv, ko, vo, ksem, vsem):
            c.start()
    for i in range(NBLK - NX):
        last_merge(lax.axis_index('sp') // 2, comb_b, xrx_b, i, ofin, i)
    lhs = jnp.concatenate([oa[...].astype(BF16), ofin[...].astype(BF16)], axis=0)
    for n in range(4):
        part[:, n * WCH:(n + 1) * WCH] = jnp.dot(lhs, wo_v[n], preferred_element_type=F32)
    for i in range(NA, NB):
        for c in block_copies(i, kv, vv, ko, vo, ksem, vsem):
            c.wait()


def rest_kernel(kv, vv, ki, vi, ko, vo, ksem, vsem):
    for i in range(NB, NBLK):
        for c in block_copies(i, kv, vv, ko, vo, ksem, vsem):
            c.start()
    for i in range(NB, NBLK):
        for c in block_copies(i, kv, vv, ko, vo, ksem, vsem):
            c.wait()


def write_kernel(pos_h, kv, vv, rep, comb_a, xrx, wo_v, ko, vo, nkv, oa, kva, vva, wo_a, pos_s, nkv_s, patch, ksem, vsem, psem, osem):
    start = lax.axis_index('sp') * SLOTS
    slot16 = lax.broadcasted_iota(jnp.int32, (4 * KVH, HD), 0) // KVH

    def copies(i):
        return block_copies(i, kv, vv, ko, vo, ksem, vsem)

    pos_copy = pltpu.make_async_copy(pos_h, pos_s, osem.at[0])
    pos_copy.start()
    for c in copies(0):
        c.start()
    for b in range(SEQS):
        nkv_s[b] = jnp.concatenate([rep[0, pl.ds(b * KVH, KVH), :], rep[1, pl.ds(b * KVH, KVH), :]], axis=0).astype(BF16)
    pos_copy.wait()

    def each(i, do):
        for bb in range(BLK):
            b = i * BLK + bb
            rel = pos_s[b] - start

            @pl.when(jnp.logical_and(rel >= 0, rel < SLOTS))
            def _():
                base = pl.multiple_of(rel // 4 * (4 * KVH), 4 * KVH)
                mask = slot16 == lax.rem(rel, 4)
                for z, (ref, out) in enumerate(((kv, ko), (vv, vo))):
                    do(b, z, base, mask, ref, out)

    def merged(b, z, base, mask, ref):
        new = jnp.concatenate([rep[z, pl.ds(b * KVH, KVH), :]] * 4, axis=0)
        old = ref[b, pl.ds(base, 4 * KVH), :].astype(F32)
        return jnp.where(mask, new, old).astype(BF16)

    def put(b, z, base, mask, ref, out):
        ref[b, pl.ds(base, 4 * KVH), :] = merged(b, z, base, mask, ref)

    def stage(b, z, base, mask, ref, out):
        patch[z, b] = merged(b, z, base, mask, ref)

    def patch_copy(b, z, base, out):
        return pltpu.make_async_copy(patch.at[z, b], out.at[b, pl.ds(base, 4 * KVH)], psem.at[z, b])

    for i in range(1, NBLK):
        each(i, put)
        if 1 < i <= NA:
            for c in copies(i - 1):
                c.start()
    nkv_copy = pltpu.make_async_copy(nkv_s, nkv, osem.at[1])
    nkv_copy.start()
    each(0, stage)
    for i in range(NX):
        last_merge(lax.axis_index('sp') // 2, comb_a, xrx, i, oa, i)
    for c in copies(0):
        c.wait()
    each(0, lambda b, z, base, mask, ref, out: patch_copy(b, z, base, out).start())
    nkv_copy.wait()
    each(0, lambda b, z, base, mask, ref, out: patch_copy(b, z, base, out).wait())
    for i in range(1, NA):
        for c in copies(i):
            c.wait()


def solution(mesh):
    cache_spec = P('dp', 'sp', None, None)
    inv_freq = (np.float64(ROPE_THETA) ** (-np.arange(HD // 2) * 2.0 / HD)).astype(np.float32)
    freq2 = np.concatenate([inv_freq, inv_freq])
    vm = pl.BlockSpec(memory_space=pltpu.VMEM)
    hbm = pl.BlockSpec(memory_space=pl.ANY)
    dma = pltpu.SemaphoreType.DMA

    def device_step(tokens, positions, k_cache, v_cache, w_q, w_k, w_v, w_o, attn_norm, q_norm, k_norm):
        in_hbm = lambda x: pltpu.with_memory_space_constraint(x, pltpu.HBM)
        in_vmem = lambda x: pltpu.with_memory_space_constraint(x, pltpu.VMEM)
        rows = (SEQS, ROWS, HD)
        piece = (PIECE, HD)
        kv, vv, rep, wo_v, comb_a, comb_b, xrx_a = pl.pallas_call(
            attend_kernel,
            out_shape=(pltpu.VMEM(rows, BF16), pltpu.VMEM(rows, BF16),
                       pltpu.VMEM((2, SEQS * KVH, HD), F32), pltpu.VMEM((4, HALF * HD, WCH), BF16),
                       pltpu.VMEM((NX,) + piece, F32), pltpu.VMEM((NBLK - NX,) + piece, F32), pltpu.VMEM((NX,) + piece, F32)),
            in_specs=[hbm] * 12,
            out_specs=(vm,) * 7,
            scratch_shapes=[
                pltpu.SMEM((SEQS,), jnp.int32), pltpu.VMEM((SEQS, DIM), BF16), pltpu.VMEM((DIM // HD, HD), BF16),
                pltpu.VMEM((1, HD), BF16), pltpu.VMEM((1, HD), BF16), pltpu.VMEM((1, HD), F32), dma((6,)),
                pltpu.VMEM((2, SEQS, WCH), F32),
                pltpu.VMEM((RING, DIM, WCH), BF16),
                pltpu.VMEM((SEQS, DIM), BF16),
                pltpu.VMEM((SEQS, HD), F32), pltpu.VMEM((SEQS, HD), F32), pltpu.VMEM((SEQS, HD), F32),
                pltpu.VMEM((2, SEQS * 8, HD), F32), pltpu.VMEM((2, SEQS * 8, HD), F32),
                pltpu.VMEM((2 * HALF, ROWS), jnp.int32),
                pltpu.VMEM((NBLK, 2 * PIECE, HD), F32),
                pltpu.VMEM((NBLK,) + piece, F32),
                pltpu.VMEM((2, 4 * HALF, ROWS), F32), pltpu.VMEM((2, 4 * HALF, ROWS), BF16),
                dma((NW,)), dma((NBLK,)), dma((NBLK,)), dma((4,)), dma((3,)), dma((3,)),
                dma((NBLK,)), dma((NBLK,)), dma((NX,)), dma((NX,)),
            ],
            compiler_params=pltpu.CompilerParams(collective_id=0, has_side_effects=True, vmem_limit_bytes=VMEM_LIMIT),
            name='attend',
        )(in_hbm(positions), in_hbm(tokens), in_hbm(attn_norm.reshape(DIM // HD, HD)), in_hbm(q_norm.reshape(1, HD)),
          in_hbm(k_norm.reshape(1, HD)), in_hbm(jnp.asarray(freq2).reshape(1, HD)), in_hbm(w_q), in_hbm(w_k), in_hbm(w_v), in_hbm(w_o),
          in_hbm(k_cache.reshape(rows)), in_hbm(v_cache.reshape(rows)))
        xrx_b = lax.ppermute(comb_b, 'sp', [(0, 2), (2, 0), (1, 3), (3, 1)])
        k_out, v_out, new_kv, oa, kv, vv, wo_v = pl.pallas_call(
            write_kernel,
            out_shape=(pltpu.HBM(rows, BF16), pltpu.HBM(rows, BF16), pltpu.HBM((SEQS, 2 * KVH, HD), BF16),
                       pltpu.VMEM((NX * BLK, HALF * HD), F32), pltpu.VMEM(rows, BF16), pltpu.VMEM(rows, BF16),
                       pltpu.VMEM((4, HALF * HD, WCH), BF16)),
            in_specs=[hbm, vm, vm, vm, vm, vm, vm],
            out_specs=(hbm, hbm, hbm, vm, vm, vm, vm),
            input_output_aliases={1: 4, 2: 5, 6: 6},
            scratch_shapes=[pltpu.SMEM((SEQS,), jnp.int32), pltpu.VMEM((SEQS, 2 * KVH, HD), BF16),
                            pltpu.VMEM((2, BLK, 4 * KVH, HD), BF16),
                            dma((NBLK,)), dma((NBLK,)), dma((2, BLK)), dma((2,))],
            compiler_params=pltpu.CompilerParams(vmem_limit_bytes=VMEM_LIMIT),
            cost_estimate=pl.CostEstimate(flops=10**10, bytes_accessed=2**25, transcendentals=0),
            name='write',
        )(in_hbm(positions), in_vmem(kv), in_vmem(vv), in_vmem(rep), in_vmem(comb_a), in_vmem(xrx_a), in_vmem(wo_v))
        k_out, v_out, part = pl.pallas_call(
            product_kernel,
            out_shape=(pltpu.HBM(rows, BF16), pltpu.HBM(rows, BF16), pltpu.VMEM((SEQS, DIM), F32)),
            in_specs=[vm, vm, hbm, hbm, vm, vm, vm, vm],
            out_specs=(hbm, hbm, vm),
            input_output_aliases={2: 0, 3: 1},
            scratch_shapes=[pltpu.VMEM(((NBLK - NX) * BLK, HALF * HD), F32), dma((NBLK,)), dma((NBLK,))],
            compiler_params=pltpu.CompilerParams(vmem_limit_bytes=VMEM_LIMIT),
            cost_estimate=pl.CostEstimate(flops=2 * SEQS * DIM * DIM, bytes_accessed=2**22, transcendentals=0),
            name='product',
        )(in_vmem(kv), in_vmem(vv), k_out, v_out, in_vmem(oa), in_vmem(comb_b), in_vmem(xrx_b), in_vmem(wo_v))
        other = lax.ppermute(part, 'sp', [(0, 1), (1, 0), (2, 3), (3, 2)])
        k_out, v_out = pl.pallas_call(
            rest_kernel,
            out_shape=(pltpu.HBM(rows, BF16), pltpu.HBM(rows, BF16)),
            in_specs=[vm, vm, hbm, hbm],
            out_specs=(hbm, hbm),
            input_output_aliases={2: 0, 3: 1},
            scratch_shapes=[dma((NBLK,)), dma((NBLK,))],
            compiler_params=pltpu.CompilerParams(vmem_limit_bytes=VMEM_LIMIT),
            cost_estimate=pl.CostEstimate(flops=10**9, bytes_accessed=2**22, transcendentals=0),
            name='rest',
        )(in_vmem(kv), in_vmem(vv), k_out, v_out)
        block_out = (tokens.astype(F32) + (part + other)).astype(BF16)
        return block_out, k_out.reshape(k_cache.shape), v_out.reshape(v_cache.shape), new_kv.reshape(SEQS, 2, KVH, HD)

    return jax.shard_map(device_step, mesh=mesh, in_specs=(P('dp', None), P('dp'), cache_spec, cache_spec, P(), P(), P(), P(), P(), P(), P()), out_specs=(P('dp', None), cache_spec, cache_spec, P('dp', None, None, None)), check_vma=False)
```

```python
import functools

import jax
import jax.numpy as jnp
import numpy as np
from jax import lax
from jax.experimental import pallas as pl
from jax.experimental.pallas import tpu as pltpu
from jax.sharding import PartitionSpec as P

NORM_EPS = 1e-6
ROPE_THETA = 1000000.0
MESH = pl.DeviceIdType.MESH
BF16 = jnp.bfloat16
F32 = jnp.float32

SEQS = 64
DIM = 2048
HD = 128
KVH = 4
HALF = 16
SLOTS = 256
ROWS = SLOTS * KVH
BLK = 8
NBLK = SEQS // BLK
AHEAD = 4
NX = 3
NA = 7
NW = 5
WAHEAD = 3
RING = 4
LAG = 2
WCH = 512
PIECE = (HALF + 1) * BLK
VMEM_LIMIT = 14 * 2**20
EXP_SCALE = HD ** -0.5 * 1.4426950408889634
NEG = -jnp.inf


def bcast_col(tile, col):
    return jnp.broadcast_to(tile[:, col:col + 1], (tile.shape[0], HD))


def attend_kernel(pos_h, tok_h, an_h, qn_h, kn_h, freq_h, wq, wk, wv, wo, kc, vc,
                  kv, vv, rep, wo_v, comb_a, comb_b, xrx,
                  pos_s, tok, an, qn, kn, freq, insem, proj, w_s, hid, ang, cosr, sinr, qmine, qmate, colslot, opart, drx, sc, pr_s,
                  wsem, ksem, vsem, wosem, qs, qr, ds_, dr, xs, xr):
    me = lax.axis_index('sp')
    core = lax.rem(me, 2)
    chip = me // 2
    mate = {'sp': me + 1 - 2 * core}
    peer = {'sp': me + 2 - 4 * chip}

    def w_copy(n, src=None):
        if n < 4:
            src = wq.at[:, pl.ds(pl.multiple_of(core * (HALF * HD) + n * WCH, WCH), WCH)]
        return pltpu.make_async_copy(src, w_s.at[n % RING], wsem.at[n])

    def w_start(n):
        if n < 4:
            w_copy(n).start()
        else:
            @pl.when(core == 0)
            def _():
                w_copy(n, wk).start()

            @pl.when(core == 1)
            def _():
                w_copy(n, wv).start()

    def wo_copy(n):
        src = wo.at[pl.ds(pl.multiple_of(core * (HALF * HD), HD), HALF * HD), pl.ds(n * WCH, WCH)]
        return pltpu.make_async_copy(src, wo_v.at[n], wosem.at[n])

    def k_copy(i):
        return pltpu.make_async_copy(kc.at[pl.ds(i * BLK, BLK)], kv.at[pl.ds(i * BLK, BLK)], ksem.at[i])

    def v_copy(i):
        return pltpu.make_async_copy(vc.at[pl.ds(i * BLK, BLK)], vv.at[pl.ds(i * BLK, BLK)], vsem.at[i])

    def q_send(h):
        return pltpu.make_async_remote_copy(qmine.at[h], qmate.at[h], qs.at[h], qr.at[h], device_id=mate, device_id_type=MESH)

    def new_send():
        return pltpu.make_async_remote_copy(rep.at[core], rep.at[core], qs.at[2], qr.at[2], device_id=mate, device_id_type=MESH)

    def d_send(i):
        return pltpu.make_async_remote_copy(opart.at[i, pl.ds(PIECE, PIECE)], drx.at[i], ds_.at[i], dr.at[i],
                                            device_id=mate, device_id_type=MESH)

    def x_send(i):
        return pltpu.make_async_remote_copy(comb_a.at[i], xrx.at[i], xs.at[i], xr.at[i],
                                            device_id=peer, device_id_type=MESH)

    small = [pltpu.make_async_copy(a, b, insem.at[z]) for z, (a, b) in enumerate(
        ((tok_h, tok), (pos_h, pos_s), (an_h, an), (qn_h, qn), (kn_h, kn), (freq_h, freq)))]
    for c in small:
        c.start()
    for n in range(WAHEAD):
        w_start(n)

    barrier = pltpu.get_barrier_semaphore()
    for other in (mate, peer):
        pl.semaphore_signal(barrier, inc=1, device_id=other, device_id_type=MESH)

    for c in small[1:]:
        c.wait()
    lane1 = lax.broadcasted_iota(jnp.int32, (1, HD), 1)

    def angle(b, carry):
        ang[pl.ds(b, 1), :] = freq[...] * pos_s[b].astype(F32)
        return carry

    lax.fori_loop(0, SEQS, angle, 0, unroll=8)
    cosr[...] = jnp.cos(ang[...])
    sinr[...] = jnp.sin(ang[...]) * jnp.where(lane1 < HD // 2, -1.0, 1.0)

    row = lax.broadcasted_iota(jnp.int32, (2 * HALF, ROWS), 0)
    col = lax.broadcasted_iota(jnp.int32, (2 * HALF, ROWS), 1)
    half_of_row = jnp.where(row < HALF, core, 1 - core)
    kv_of_row = half_of_row * 2 + lax.rem(row, HALF) // 8
    colslot[...] = jnp.where(lax.rem(col, KVH) == kv_of_row, col // KVH, 1 << 20)

    small[0].wait()
    t = tok[...].astype(F32)
    inv = lax.rsqrt(jnp.sum(t * t, axis=-1, keepdims=True) * (1.0 / DIM) + NORM_EPS)
    gains = an[...].astype(F32)
    for j in range(DIM // HD):
        sl = slice(j * HD, (j + 1) * HD)
        hid[:, sl] = (tok[:, sl].astype(F32) * inv * gains[j:j + 1, :]).astype(BF16)

    qgain = qn[...].astype(F32)
    kgain = kn[...].astype(F32)

    def norm_rope(x, gain):
        y = x * lax.rsqrt(jnp.mean(x * x, axis=-1, keepdims=True) + NORM_EPS) * gain
        y = y * cosr[...] + pltpu.roll(y, HD // 2, 1) * sinr[...]
        return y.astype(BF16).astype(F32)

    def post(n):
        for j in range(WCH // HD):
            x = proj[n % 2, :, j * HD:(j + 1) * HD].astype(BF16).astype(F32)
            if n < 4:
                qmine.at[n // 2][pl.ds(n % 2 * 4 + j, SEQS, stride=8), :] = norm_rope(x, qgain)
            else:
                rep.at[core][pl.ds(j, SEQS, stride=KVH), :] = jnp.where(core == 0, norm_rope(x, kgain), x)

    for n in range(NW):
        w_copy(n, wk).wait()
        if n + WAHEAD < NW:
            w_start(n + WAHEAD)
        elif n + WAHEAD - NW < AHEAD:
            k_copy(n + WAHEAD - NW).start()
            v_copy(n + WAHEAD - NW).start()
        proj[n % 2] = jnp.dot(hid[...], w_s[n % RING], preferred_element_type=F32)
        if n > 0:
            post(n - 1)
        if n == 2:
            pl.semaphore_wait(barrier, 2)
            q_send(0).start()
        if n == 4:
            q_send(1).start()
    for i in range(min(WAHEAD, AHEAD), AHEAD):
        k_copy(i).start()
        v_copy(i).start()
    post(NW - 1)
    new_send().start()
    start = me * SLOTS
    lane = lax.broadcasted_iota(jnp.int32, (HALF, HD), 1)
    lrow = lax.broadcasted_iota(jnp.int32, (HALF, HD), 0)
    lane8 = lax.broadcasted_iota(jnp.int32, (BLK, HD), 1)
    for h in range(2):
        q_send(h).wait()
    new_send().wait()

    def attend(i, first=False):
        ob = opart.at[i]
        def load_q(pair, at):
            bs = [at * BLK + 2 * pair + z for z in range(2)]
            return bs, [jnp.concatenate([ref[h, pl.ds(pl.multiple_of(b * 8, 8), 8), :]
                                         for ref in (qmine, qmate) for h in range(2)], axis=0) for b in bs]

        def new_rows(z, b):
            return jnp.concatenate([jnp.broadcast_to(rep[z, pl.ds(b * KVH + h, 1), :], (8, HD))
                                    for h in (2 * core, 2 * core + 1, 2 - 2 * core, 3 - 2 * core)], axis=0)

        def scores(pair, at):
            bs, qf = load_q(pair, at)
            zero = jnp.zeros((2 * HALF, HD), BF16)
            lhs = jnp.concatenate([jnp.concatenate([qf[0].astype(BF16), zero], axis=1),
                                   jnp.concatenate([zero, qf[1].astype(BF16)], axis=1)], axis=0)
            keys = jnp.concatenate([kv[bs[0]], kv[bs[1]]], axis=1)
            sc[pair % 2] = lax.dot_general(lhs, keys, (((1,), (1,)), ((), ())), preferred_element_type=F32)

        def soft(pair):
            bs, qf = load_q(pair, i)
            out = []
            for z in range(2):
                b = bs[z]
                rel = pos_s[b] - start
                owner = jnp.logical_and(rel >= 0, rel < SLOTS)
                snew = jnp.where(owner, jnp.sum(qf[z] * new_rows(0, b), axis=-1, keepdims=True), NEG)
                sm = jnp.where(colslot[...] < rel, sc[pair % 2, z * 2 * HALF:(z + 1) * 2 * HALF], NEG)
                peak = jnp.maximum(jnp.max(sm, axis=-1, keepdims=True), snew)
                safe = jnp.where(peak == NEG, 0.0, peak)
                p = jnp.exp2((sm - safe) * EXP_SCALE)
                pn = jnp.exp2((snew - safe) * EXP_SCALE)
                pr_s[pair % 2, z * 2 * HALF:(z + 1) * 2 * HALF, :] = p.astype(BF16)
                out.append((pn.astype(BF16).astype(F32), jnp.sum(p, axis=-1, keepdims=True) + pn, peak))
            return out

        def mix(pair, st3):
            bs = [i * BLK + 2 * pair + z for z in range(2)]
            values = jnp.concatenate([vv[bs[0]], vv[bs[1]]], axis=1)
            mixed = jnp.dot(pr_s[pair % 2], values, preferred_element_type=F32)
            for z in range(2):
                extra, total, peak = st3[z]
                o = mixed[z * 2 * HALF:(z + 1) * 2 * HALF, z * HD:(z + 1) * HD] + extra * new_rows(1, bs[z])
                bb = 2 * pair + z
                for h in range(2):
                    hs = slice(h * HALF, (h + 1) * HALF)
                    ob[pl.ds(h * PIECE + bb, HALF, stride=BLK), :] = o[hs]
                    st = jnp.where(lane == lrow, peak[hs], jnp.where(lane == lrow + HALF, total[hs], 0.0))
                    ob[pl.ds(h * PIECE + HALF * BLK + bb, 1), :] = jnp.sum(st, axis=0, keepdims=True)

        if first:
            scores(0, i)
            return
        for pair in range(BLK // 2):
            if pair + 1 < BLK // 2:
                scores(pair + 1, i)
            else:
                scores(0, jnp.minimum(i + 1, NBLK - 1))
            mix(pair, soft(pair))

    def combine(i, comb, at):
        s0 = opart[i, pl.ds(HALF * BLK, BLK), :]
        s1 = drx[i, pl.ds(HALF * BLK, BLK), :]
        peak = jnp.maximum(s0, s1)
        safe = jnp.where(peak == NEG, 0.0, peak)
        f0 = jnp.exp2((s0 - safe) * EXP_SCALE)
        f1 = jnp.exp2((s1 - safe) * EXP_SCALE)
        total = f0 * pltpu.roll(s0, HD - HALF, 1) + f1 * pltpu.roll(s1, HD - HALF, 1)
        comb[at, pl.ds(HALF * BLK, BLK), :] = jnp.where(
            lane8 < HALF, peak, jnp.where(lane8 < 2 * HALF, pltpu.roll(total, HALF, 1), 0.0))
        for j in range(HALF):
            rows = pl.ds(j * BLK, BLK)
            comb[at, rows, :] = bcast_col(f0, j) * opart[i, rows, :] + bcast_col(f1, j) * drx[i, rows, :]

    def fetch(i):
        @pl.when(i + 1 < NBLK)
        def _():
            k_copy(i + 1).wait()

        v_copy(i).wait()

        @pl.when(i + AHEAD < NBLK)
        def _():
            k_copy(i + AHEAD).start()
            v_copy(i + AHEAD).start()

        @pl.when(i + AHEAD == NBLK)
        def _():
            for n in range(4):
                wo_copy(n).start()

    def early(i, carry):
        fetch(i)
        attend(i)
        d_send(i).start()
        return carry

    def sending(i, carry):
        fetch(i)
        d_send(i - LAG).wait_recv()
        combine(i - LAG, comb_a, i - LAG)
        attend(i)
        d_send(i).start()
        x_send(i - LAG).start()
        return carry

    def keeping(i, carry):
        fetch(i)
        d_send(i - LAG).wait_recv()
        combine(i - LAG, comb_b, i - LAG - NX)
        attend(i)
        d_send(i).start()
        return carry

    def late(i, carry):
        d_send(i).wait_recv()
        combine(i, comb_b, i - NX)
        return carry

    k_copy(0).wait()
    attend(0, first=True)
    lax.fori_loop(0, LAG, early, 0)
    lax.fori_loop(LAG, LAG + NX, sending, 0)
    lax.fori_loop(LAG + NX, NBLK, keeping, 0)
    lax.fori_loop(NBLK - LAG, NBLK, late, 0)

    for n in range(4):
        wo_copy(n).wait()

    def drain(i, carry):
        d_send(i).wait_send()
        return carry

    def drain_x(i, carry):
        x_send(i).wait()
        return carry

    lax.fori_loop(0, NBLK, drain, 0)
    lax.fori_loop(0, NX, drain_x, 0)


def last_merge(chip, comb, other_ref, i, ofin, at):
    first = chip == 0

    def ordered(rows):
        mine, other = comb[i, rows, :], other_ref[i, rows, :]
        return jnp.where(first, mine, other), jnp.where(first, other, mine)

    s0, s1 = ordered(pl.ds(HALF * BLK, BLK))
    peak = jnp.maximum(s0, s1)
    f0 = jnp.exp2((s0 - peak) * EXP_SCALE)
    f1 = jnp.exp2((s1 - peak) * EXP_SCALE)
    total = f0 * pltpu.roll(s0, HD - HALF, 1) + f1 * pltpu.roll(s1, HD - HALF, 1)
    g0, g1 = f0 / total, f1 / total
    for j in range(HALF):
        a, b = ordered(pl.ds(j * BLK, BLK))
        ofin[at * BLK:(at + 1) * BLK, j * HD:(j + 1) * HD] = bcast_col(g0, j) * a + bcast_col(g1, j) * b


def block_copies(i, kv, vv, ko, vo, ksem, vsem):
    r = pl.ds(i * BLK, BLK)
    return (pltpu.make_async_copy(kv.at[r], ko.at[r], ksem.at[i]),
            pltpu.make_async_copy(vv.at[r], vo.at[r], vsem.at[i]))


def product_kernel(kv, vv, ki, vi, oa, comb_b, xrx_b, wo_v, ko, vo, part, ofin, ksem, vsem):
    block_copies(NA, kv, vv, ko, vo, ksem, vsem)[0].start()
    for i in range(NBLK - NX):
        last_merge(lax.axis_index('sp') // 2, comb_b, xrx_b, i, ofin, i)
    lhs = jnp.concatenate([oa[...].astype(BF16), ofin[...].astype(BF16)], axis=0)
    for n in range(4):
        part[:, n * WCH:(n + 1) * WCH] = jnp.dot(lhs, wo_v[n], preferred_element_type=F32)
    block_copies(NA, kv, vv, ko, vo, ksem, vsem)[0].wait()


def rest_kernel(kv, vv, ki, vi, ko, vo, ksem, vsem):
    copy = block_copies(NA, kv, vv, ko, vo, ksem, vsem)[1]
    copy.start()
    copy.wait()


def write_kernel(pos_h, kv, vv, rep, comb_a, xrx, wo_v, ko, vo, nkv, oa, kva, vva, wo_a, pos_s, nkv_s, patch, ksem, vsem, psem, osem):
    start = lax.axis_index('sp') * SLOTS
    slot16 = lax.broadcasted_iota(jnp.int32, (4 * KVH, HD), 0) // KVH

    def copies(i):
        return block_copies(i, kv, vv, ko, vo, ksem, vsem)

    pos_copy = pltpu.make_async_copy(pos_h, pos_s, osem.at[0])
    pos_copy.start()
    for c in copies(0):
        c.start()
    for b in range(SEQS):
        nkv_s[b] = jnp.concatenate([rep[0, pl.ds(b * KVH, KVH), :], rep[1, pl.ds(b * KVH, KVH), :]], axis=0).astype(BF16)
    pos_copy.wait()

    def each(i, do):
        for bb in range(BLK):
            b = i * BLK + bb
            rel = pos_s[b] - start

            @pl.when(jnp.logical_and(rel >= 0, rel < SLOTS))
            def _():
                base = pl.multiple_of(rel // 4 * (4 * KVH), 4 * KVH)
                mask = slot16 == lax.rem(rel, 4)
                for z, (ref, out) in enumerate(((kv, ko), (vv, vo))):
                    do(b, z, base, mask, ref, out)

    def merged(b, z, base, mask, ref):
        new = jnp.concatenate([rep[z, pl.ds(b * KVH, KVH), :]] * 4, axis=0)
        old = ref[b, pl.ds(base, 4 * KVH), :].astype(F32)
        return jnp.where(mask, new, old).astype(BF16)

    def put(b, z, base, mask, ref, out):
        ref[b, pl.ds(base, 4 * KVH), :] = merged(b, z, base, mask, ref)

    def stage(b, z, base, mask, ref, out):
        patch[z, b] = merged(b, z, base, mask, ref)

    def patch_copy(b, z, base, out):
        return pltpu.make_async_copy(patch.at[z, b], out.at[b, pl.ds(base, 4 * KVH)], psem.at[z, b])

    for i in range(1, NBLK):
        each(i, put)
        if 1 < i <= NA:
            for c in copies(i - 1):
                c.start()
    nkv_copy = pltpu.make_async_copy(nkv_s, nkv, osem.at[1])
    nkv_copy.start()
    each(0, stage)
    for i in range(NX):
        last_merge(lax.axis_index('sp') // 2, comb_a, xrx, i, oa, i)
    for c in copies(0):
        c.wait()
    each(0, lambda b, z, base, mask, ref, out: patch_copy(b, z, base, out).start())
    nkv_copy.wait()
    each(0, lambda b, z, base, mask, ref, out: patch_copy(b, z, base, out).wait())
    for i in range(1, NA):
        for c in copies(i):
            c.wait()


def solution(mesh):
    cache_spec = P('dp', 'sp', None, None)
    inv_freq = (np.float64(ROPE_THETA) ** (-np.arange(HD // 2) * 2.0 / HD)).astype(np.float32)
    freq2 = np.concatenate([inv_freq, inv_freq])
    vm = pl.BlockSpec(memory_space=pltpu.VMEM)
    hbm = pl.BlockSpec(memory_space=pl.ANY)
    dma = pltpu.SemaphoreType.DMA

    def device_step(tokens, positions, k_cache, v_cache, w_q, w_k, w_v, w_o, attn_norm, q_norm, k_norm):
        in_hbm = lambda x: pltpu.with_memory_space_constraint(x, pltpu.HBM)
        in_vmem = lambda x: pltpu.with_memory_space_constraint(x, pltpu.VMEM)
        rows = (SEQS, ROWS, HD)
        piece = (PIECE, HD)
        kv, vv, rep, wo_v, comb_a, comb_b, xrx_a = pl.pallas_call(
            attend_kernel,
            out_shape=(pltpu.VMEM(rows, BF16), pltpu.VMEM(rows, BF16),
                       pltpu.VMEM((2, SEQS * KVH, HD), F32), pltpu.VMEM((4, HALF * HD, WCH), BF16),
                       pltpu.VMEM((NX,) + piece, F32), pltpu.VMEM((NBLK - NX,) + piece, F32), pltpu.VMEM((NX,) + piece, F32)),
            in_specs=[hbm] * 12,
            out_specs=(vm,) * 7,
            scratch_shapes=[
                pltpu.SMEM((SEQS,), jnp.int32), pltpu.VMEM((SEQS, DIM), BF16), pltpu.VMEM((DIM // HD, HD), BF16),
                pltpu.VMEM((1, HD), BF16), pltpu.VMEM((1, HD), BF16), pltpu.VMEM((1, HD), F32), dma((6,)),
                pltpu.VMEM((2, SEQS, WCH), F32),
                pltpu.VMEM((RING, DIM, WCH), BF16),
                pltpu.VMEM((SEQS, DIM), BF16),
                pltpu.VMEM((SEQS, HD), F32), pltpu.VMEM((SEQS, HD), F32), pltpu.VMEM((SEQS, HD), F32),
                pltpu.VMEM((2, SEQS * 8, HD), F32), pltpu.VMEM((2, SEQS * 8, HD), F32),
                pltpu.VMEM((2 * HALF, ROWS), jnp.int32),
                pltpu.VMEM((NBLK, 2 * PIECE, HD), F32),
                pltpu.VMEM((NBLK,) + piece, F32),
                pltpu.VMEM((2, 4 * HALF, ROWS), F32), pltpu.VMEM((2, 4 * HALF, ROWS), BF16),
                dma((NW,)), dma((NBLK,)), dma((NBLK,)), dma((4,)), dma((3,)), dma((3,)),
                dma((NBLK,)), dma((NBLK,)), dma((NX,)), dma((NX,)),
            ],
            compiler_params=pltpu.CompilerParams(collective_id=0, has_side_effects=True, vmem_limit_bytes=VMEM_LIMIT),
            name='attend',
        )(in_hbm(positions), in_hbm(tokens), in_hbm(attn_norm.reshape(DIM // HD, HD)), in_hbm(q_norm.reshape(1, HD)),
          in_hbm(k_norm.reshape(1, HD)), in_hbm(jnp.asarray(freq2).reshape(1, HD)), in_hbm(w_q), in_hbm(w_k), in_hbm(w_v), in_hbm(w_o),
          in_hbm(k_cache.reshape(rows)), in_hbm(v_cache.reshape(rows)))
        xrx_b = lax.ppermute(comb_b, 'sp', [(0, 2), (2, 0), (1, 3), (3, 1)])
        k_out, v_out, new_kv, oa, kv, vv, wo_v = pl.pallas_call(
            write_kernel,
            out_shape=(pltpu.HBM(rows, BF16), pltpu.HBM(rows, BF16), pltpu.HBM((SEQS, 2 * KVH, HD), BF16),
                       pltpu.VMEM((NX * BLK, HALF * HD), F32), pltpu.VMEM(rows, BF16), pltpu.VMEM(rows, BF16),
                       pltpu.VMEM((4, HALF * HD, WCH), BF16)),
            in_specs=[hbm, vm, vm, vm, vm, vm, vm],
            out_specs=(hbm, hbm, hbm, vm, vm, vm, vm),
            input_output_aliases={1: 4, 2: 5, 6: 6},
            scratch_shapes=[pltpu.SMEM((SEQS,), jnp.int32), pltpu.VMEM((SEQS, 2 * KVH, HD), BF16),
                            pltpu.VMEM((2, BLK, 4 * KVH, HD), BF16),
                            dma((NBLK,)), dma((NBLK,)), dma((2, BLK)), dma((2,))],
            compiler_params=pltpu.CompilerParams(vmem_limit_bytes=VMEM_LIMIT),
            cost_estimate=pl.CostEstimate(flops=10**10, bytes_accessed=2**25, transcendentals=0),
            name='write',
        )(in_hbm(positions), in_vmem(kv), in_vmem(vv), in_vmem(rep), in_vmem(comb_a), in_vmem(xrx_a), in_vmem(wo_v))
        k_out, v_out, part = pl.pallas_call(
            product_kernel,
            out_shape=(pltpu.HBM(rows, BF16), pltpu.HBM(rows, BF16), pltpu.VMEM((SEQS, DIM), F32)),
            in_specs=[vm, vm, hbm, hbm, vm, vm, vm, vm],
            out_specs=(hbm, hbm, vm),
            input_output_aliases={2: 0, 3: 1},
            scratch_shapes=[pltpu.VMEM(((NBLK - NX) * BLK, HALF * HD), F32), dma((NBLK,)), dma((NBLK,))],
            compiler_params=pltpu.CompilerParams(vmem_limit_bytes=VMEM_LIMIT),
            cost_estimate=pl.CostEstimate(flops=2 * SEQS * DIM * DIM, bytes_accessed=2**22, transcendentals=0),
            name='product',
        )(in_vmem(kv), in_vmem(vv), k_out, v_out, in_vmem(oa), in_vmem(comb_b), in_vmem(xrx_b), in_vmem(wo_v))
        other = lax.ppermute(part, 'sp', [(0, 1), (1, 0), (2, 3), (3, 2)])
        k_out, v_out = pl.pallas_call(
            rest_kernel,
            out_shape=(pltpu.HBM(rows, BF16), pltpu.HBM(rows, BF16)),
            in_specs=[vm, vm, hbm, hbm],
            out_specs=(hbm, hbm),
            input_output_aliases={2: 0, 3: 1},
            scratch_shapes=[dma((NBLK,)), dma((NBLK,))],
            compiler_params=pltpu.CompilerParams(vmem_limit_bytes=VMEM_LIMIT),
            cost_estimate=pl.CostEstimate(flops=10**9, bytes_accessed=2**22, transcendentals=0),
            name='rest',
        )(in_vmem(kv), in_vmem(vv), k_out, v_out)
        block_out = (tokens.astype(F32) + (part + other)).astype(BF16)
        return block_out, k_out.reshape(k_cache.shape), v_out.reshape(v_cache.shape), new_kv.reshape(SEQS, 2, KVH, HD)

    return jax.shard_map(device_step, mesh=mesh, in_specs=(P('dp', None), P('dp'), cache_spec, cache_spec, P(), P(), P(), P(), P(), P(), P()), out_specs=(P('dp', None), cache_spec, cache_spec, P('dp', None, None, None)), check_vma=False)
```

```python
import functools

import jax
import jax.numpy as jnp
import numpy as np
from jax import lax
from jax.experimental import pallas as pl
from jax.experimental.pallas import tpu as pltpu
from jax.sharding import PartitionSpec as P

NORM_EPS = 1e-6
ROPE_THETA = 1000000.0
MESH = pl.DeviceIdType.MESH
BF16 = jnp.bfloat16
F32 = jnp.float32

SEQS = 64
DIM = 2048
HD = 128
KVH = 4
HALF = 16
SLOTS = 256
ROWS = SLOTS * KVH
BLK = 8
NBLK = SEQS // BLK
AHEAD = 3
NX = 4
NA = 6
NW = 5
WAHEAD = 3
RING = 4
LAG = 2
WCH = 512
PIECE = (HALF + 1) * BLK
VMEM_LIMIT = 14 * 2**20
EXP_SCALE = HD ** -0.5 * 1.4426950408889634
NEG = -jnp.inf


def bcast_col(tile, col):
    return jnp.broadcast_to(tile[:, col:col + 1], (tile.shape[0], HD))


def attend_kernel(pos_h, tok_h, an_h, qn_h, kn_h, freq_h, wq, wk, wv, wo, kc, vc,
                  kv, vv, rep, wo_v, comb_a, comb_b, xrx,
                  pos_s, tok, an, qn, kn, freq, insem, proj, w_s, hid, ang, cosr, sinr, qmine, qmate, colslot, opart, drx, sc, pr_s,
                  wsem, ksem, vsem, wosem, qs, qr, ds_, dr, xs, xr):
    me = lax.axis_index('sp')
    core = lax.rem(me, 2)
    chip = me // 2
    mate = {'sp': me + 1 - 2 * core}
    peer = {'sp': me + 2 - 4 * chip}

    def w_copy(n, src=None):
        if n < 4:
            src = wq.at[:, pl.ds(pl.multiple_of(core * (HALF * HD) + n * WCH, WCH), WCH)]
        return pltpu.make_async_copy(src, w_s.at[n % RING], wsem.at[n])

    def w_start(n):
        if n < 4:
            w_copy(n).start()
        else:
            @pl.when(core == 0)
            def _():
                w_copy(n, wk).start()

            @pl.when(core == 1)
            def _():
                w_copy(n, wv).start()

    def wo_copy(n):
        src = wo.at[pl.ds(pl.multiple_of(core * (HALF * HD), HD), HALF * HD), pl.ds(n * WCH, WCH)]
        return pltpu.make_async_copy(src, wo_v.at[n], wosem.at[n])

    def k_copy(i):
        return pltpu.make_async_copy(kc.at[pl.ds(i * BLK, BLK)], kv.at[pl.ds(i * BLK, BLK)], ksem.at[i])

    def v_copy(i):
        return pltpu.make_async_copy(vc.at[pl.ds(i * BLK, BLK)], vv.at[pl.ds(i * BLK, BLK)], vsem.at[i])

    def q_send(h):
        return pltpu.make_async_remote_copy(qmine.at[h], qmate.at[h], qs.at[h], qr.at[h], device_id=mate, device_id_type=MESH)

    def new_send():
        return pltpu.make_async_remote_copy(rep.at[core], rep.at[core], qs.at[2], qr.at[2], device_id=mate, device_id_type=MESH)

    def d_send(i):
        return pltpu.make_async_remote_copy(opart.at[i, pl.ds(PIECE, PIECE)], drx.at[i], ds_.at[i], dr.at[i],
                                            device_id=mate, device_id_type=MESH)

    def x_send(i):
        return pltpu.make_async_remote_copy(comb_a.at[i], xrx.at[i], xs.at[i], xr.at[i],
                                            device_id=peer, device_id_type=MESH)

    small = [pltpu.make_async_copy(a, b, insem.at[z]) for z, (a, b) in enumerate(
        ((tok_h, tok), (pos_h, pos_s), (an_h, an), (qn_h, qn), (kn_h, kn), (freq_h, freq)))]
    for c in small:
        c.start()
    for n in range(WAHEAD):
        w_start(n)

    barrier = pltpu.get_barrier_semaphore()
    for other in (mate, peer):
        pl.semaphore_signal(barrier, inc=1, device_id=other, device_id_type=MESH)

    for c in small[1:]:
        c.wait()
    lane1 = lax.broadcasted_iota(jnp.int32, (1, HD), 1)

    def angle(b, carry):
        ang[pl.ds(b, 1), :] = freq[...] * pos_s[b].astype(F32)
        return carry

    lax.fori_loop(0, SEQS, angle, 0, unroll=8)
    cosr[...] = jnp.cos(ang[...])
    sinr[...] = jnp.sin(ang[...]) * jnp.where(lane1 < HD // 2, -1.0, 1.0)

    row = lax.broadcasted_iota(jnp.int32, (2 * HALF, ROWS), 0)
    col = lax.broadcasted_iota(jnp.int32, (2 * HALF, ROWS), 1)
    half_of_row = jnp.where(row < HALF, core, 1 - core)
    kv_of_row = half_of_row * 2 + lax.rem(row, HALF) // 8
    colslot[...] = jnp.where(lax.rem(col, KVH) == kv_of_row, col // KVH, 1 << 20)

    small[0].wait()
    t = tok[...].astype(F32)
    inv = lax.rsqrt(jnp.sum(t * t, axis=-1, keepdims=True) * (1.0 / DIM) + NORM_EPS)
    gains = an[...].astype(F32)
    for j in range(DIM // HD):
        sl = slice(j * HD, (j + 1) * HD)
        hid[:, sl] = (tok[:, sl].astype(F32) * inv * gains[j:j + 1, :]).astype(BF16)

    qgain = qn[...].astype(F32)
    kgain = kn[...].astype(F32)

    def norm_rope(x, gain):
        y = x * lax.rsqrt(jnp.mean(x * x, axis=-1, keepdims=True) + NORM_EPS) * gain
        y = y * cosr[...] + pltpu.roll(y, HD // 2, 1) * sinr[...]
        return y.astype(BF16).astype(F32)

    def post(n):
        for j in range(WCH // HD):
            x = proj[n % 2, :, j * HD:(j + 1) * HD].astype(BF16).astype(F32)
            if n < 4:
                qmine.at[n // 2][pl.ds(n % 2 * 4 + j, SEQS, stride=8), :] = norm_rope(x, qgain)
            else:
                rep.at[core][pl.ds(j, SEQS, stride=KVH), :] = jnp.where(core == 0, norm_rope(x, kgain), x)

    for n in range(NW):
        w_copy(n, wk).wait()
        if n + WAHEAD < NW:
            w_start(n + WAHEAD)
        elif n + WAHEAD - NW < AHEAD:
            k_copy(n + WAHEAD - NW).start()
            v_copy(n + WAHEAD - NW).start()
        proj[n % 2] = jnp.dot(hid[...], w_s[n % RING], preferred_element_type=F32)
        if n > 0:
            post(n - 1)
        if n == 2:
            pl.semaphore_wait(barrier, 2)
            q_send(0).start()
        if n == 4:
            q_send(1).start()
    for i in range(min(WAHEAD, AHEAD), AHEAD):
        k_copy(i).start()
        v_copy(i).start()
    post(NW - 1)
    new_send().start()
    start = me * SLOTS
    lane = lax.broadcasted_iota(jnp.int32, (HALF, HD), 1)
    lrow = lax.broadcasted_iota(jnp.int32, (HALF, HD), 0)
    lane8 = lax.broadcasted_iota(jnp.int32, (BLK, HD), 1)
    for h in range(2):
        q_send(h).wait()
    new_send().wait()

    def attend(i, first=False):
        ob = opart.at[i]
        def load_q(pair, at):
            bs = [at * BLK + 2 * pair + z for z in range(2)]
            return bs, [jnp.concatenate([ref[h, pl.ds(pl.multiple_of(b * 8, 8), 8), :]
                                         for ref in (qmine, qmate) for h in range(2)], axis=0) for b in bs]

        def new_rows(z, b):
            return jnp.concatenate([jnp.broadcast_to(rep[z, pl.ds(b * KVH + h, 1), :], (8, HD))
                                    for h in (2 * core, 2 * core + 1, 2 - 2 * core, 3 - 2 * core)], axis=0)

        def scores(pair, at):
            bs, qf = load_q(pair, at)
            zero = jnp.zeros((2 * HALF, HD), BF16)
            lhs = jnp.concatenate([jnp.concatenate([qf[0].astype(BF16), zero], axis=1),
                                   jnp.concatenate([zero, qf[1].astype(BF16)], axis=1)], axis=0)
            keys = jnp.concatenate([kv[bs[0]], kv[bs[1]]], axis=1)
            sc[pair % 2] = lax.dot_general(lhs, keys, (((1,), (1,)), ((), ())), preferred_element_type=F32)

        def soft(pair):
            bs, qf = load_q(pair, i)
            out = []
            for z in range(2):
                b = bs[z]
                rel = pos_s[b] - start
                owner = jnp.logical_and(rel >= 0, rel < SLOTS)
                snew = jnp.where(owner, jnp.sum(qf[z] * new_rows(0, b), axis=-1, keepdims=True), NEG)
                sm = jnp.where(colslot[...] < rel, sc[pair % 2, z * 2 * HALF:(z + 1) * 2 * HALF], NEG)
                peak = jnp.maximum(jnp.max(sm, axis=-1, keepdims=True), snew)
                safe = jnp.where(peak == NEG, 0.0, peak)
                p = jnp.exp2((sm - safe) * EXP_SCALE)
                pn = jnp.exp2((snew - safe) * EXP_SCALE)
                pr_s[pair % 2, z * 2 * HALF:(z + 1) * 2 * HALF, :] = p.astype(BF16)
                out.append((pn.astype(BF16).astype(F32), jnp.sum(p, axis=-1, keepdims=True) + pn, peak))
            return out

        def mix(pair, st3):
            bs = [i * BLK + 2 * pair + z for z in range(2)]
            values = jnp.concatenate([vv[bs[0]], vv[bs[1]]], axis=1)
            mixed = jnp.dot(pr_s[pair % 2], values, preferred_element_type=F32)
            for z in range(2):
                extra, total, peak = st3[z]
                o = mixed[z * 2 * HALF:(z + 1) * 2 * HALF, z * HD:(z + 1) * HD] + extra * new_rows(1, bs[z])
                bb = 2 * pair + z
                for h in range(2):
                    hs = slice(h * HALF, (h + 1) * HALF)
                    ob[pl.ds(h * PIECE + bb, HALF, stride=BLK), :] = o[hs]
                    st = jnp.where(lane == lrow, peak[hs], jnp.where(lane == lrow + HALF, total[hs], 0.0))
                    ob[pl.ds(h * PIECE + HALF * BLK + bb, 1), :] = jnp.sum(st, axis=0, keepdims=True)

        if first:
            scores(0, i)
            return
        for pair in range(BLK // 2):
            if pair + 1 < BLK // 2:
                scores(pair + 1, i)
            else:
                scores(0, jnp.minimum(i + 1, NBLK - 1))
            mix(pair, soft(pair))

    def combine(i, comb, at):
        s0 = opart[i, pl.ds(HALF * BLK, BLK), :]
        s1 = drx[i, pl.ds(HALF * BLK, BLK), :]
        peak = jnp.maximum(s0, s1)
        safe = jnp.where(peak == NEG, 0.0, peak)
        f0 = jnp.exp2((s0 - safe) * EXP_SCALE)
        f1 = jnp.exp2((s1 - safe) * EXP_SCALE)
        total = f0 * pltpu.roll(s0, HD - HALF, 1) + f1 * pltpu.roll(s1, HD - HALF, 1)
        comb[at, pl.ds(HALF * BLK, BLK), :] = jnp.where(
            lane8 < HALF, peak, jnp.where(lane8 < 2 * HALF, pltpu.roll(total, HALF, 1), 0.0))
        for j in range(HALF):
            rows = pl.ds(j * BLK, BLK)
            comb[at, rows, :] = bcast_col(f0, j) * opart[i, rows, :] + bcast_col(f1, j) * drx[i, rows, :]

    def fetch(i):
        @pl.when(i + 1 < NBLK)
        def _():
            k_copy(i + 1).wait()

        v_copy(i).wait()

        @pl.when(i + AHEAD < NBLK)
        def _():
            k_copy(i + AHEAD).start()
            v_copy(i + AHEAD).start()

        @pl.when(i == NBLK - 1)
        def _():
            for n in range(4):
                wo_copy(n).start()

    def early(i, carry):
        fetch(i)
        attend(i)
        d_send(i).start()
        return carry

    def sending(i, carry):
        fetch(i)
        d_send(i - LAG).wait_recv()
        combine(i - LAG, comb_a, i - LAG)
        attend(i)
        d_send(i).start()
        x_send(i - LAG).start()
        return carry

    def keeping(i, carry):
        fetch(i)
        d_send(i - LAG).wait_recv()
        combine(i - LAG, comb_b, i - LAG - NX)
        attend(i)
        d_send(i).start()
        return carry

    def late(i, carry):
        d_send(i).wait_recv()
        combine(i, comb_b, i - NX)
        return carry

    k_copy(0).wait()
    attend(0, first=True)
    lax.fori_loop(0, LAG, early, 0)
    lax.fori_loop(LAG, LAG + NX, sending, 0)
    lax.fori_loop(LAG + NX, NBLK, keeping, 0)
    lax.fori_loop(NBLK - LAG, NBLK, late, 0)

    for n in range(4):
        wo_copy(n).wait()

    def drain(i, carry):
        d_send(i).wait_send()
        return carry

    def drain_x(i, carry):
        x_send(i).wait()
        return carry

    lax.fori_loop(0, NBLK, drain, 0)
    lax.fori_loop(0, NX, drain_x, 0)


def last_merge(chip, comb, other_ref, i, ofin, at):
    first = chip == 0

    def ordered(rows):
        mine, other = comb[i, rows, :], other_ref[i, rows, :]
        return jnp.where(first, mine, other), jnp.where(first, other, mine)

    s0, s1 = ordered(pl.ds(HALF * BLK, BLK))
    peak = jnp.maximum(s0, s1)
    f0 = jnp.exp2((s0 - peak) * EXP_SCALE)
    f1 = jnp.exp2((s1 - peak) * EXP_SCALE)
    total = f0 * pltpu.roll(s0, HD - HALF, 1) + f1 * pltpu.roll(s1, HD - HALF, 1)
    g0, g1 = f0 / total, f1 / total
    for j in range(HALF):
        a, b = ordered(pl.ds(j * BLK, BLK))
        ofin[at * BLK:(at + 1) * BLK, j * HD:(j + 1) * HD] = bcast_col(g0, j) * a + bcast_col(g1, j) * b


def block_copies(i, kv, vv, ko, vo, ksem, vsem):
    r = pl.ds(i * BLK, BLK)
    return (pltpu.make_async_copy(kv.at[r], ko.at[r], ksem.at[i]),
            pltpu.make_async_copy(vv.at[r], vo.at[r], vsem.at[i]))


def product_kernel(kv, vv, ki, vi, oa, comb_b, xrx_b, wo_v, ko, vo, part, ofin, ksem, vsem):
    for c in block_copies(NA, kv, vv, ko, vo, ksem, vsem):
        c.start()
    for i in range(NBLK - NX):
        last_merge(lax.axis_index('sp') // 2, comb_b, xrx_b, i, ofin, i)
    lhs = jnp.concatenate([oa[...].astype(BF16), ofin[...].astype(BF16)], axis=0)
    for n in range(4):
        part[:, n * WCH:(n + 1) * WCH] = jnp.dot(lhs, wo_v[n], preferred_element_type=F32)
    for c in block_copies(NA, kv, vv, ko, vo, ksem, vsem):
        c.wait()


def rest_kernel(kv, vv, ki, vi, ko, vo, ksem, vsem):
    for c in block_copies(NA + 1, kv, vv, ko, vo, ksem, vsem):
        c.start()
    for c in block_copies(NA + 1, kv, vv, ko, vo, ksem, vsem):
        c.wait()


def write_kernel(pos_h, kv, vv, rep, comb_a, xrx, wo_v, ko, vo, nkv, oa, kva, vva, wo_a, pos_s, nkv_s, patch, ksem, vsem, psem, osem):
    start = lax.axis_index('sp') * SLOTS
    slot16 = lax.broadcasted_iota(jnp.int32, (4 * KVH, HD), 0) // KVH

    def copies(i):
        return block_copies(i, kv, vv, ko, vo, ksem, vsem)

    pos_copy = pltpu.make_async_copy(pos_h, pos_s, osem.at[0])
    pos_copy.start()
    for c in copies(0):
        c.start()
    for b in range(SEQS):
        nkv_s[b] = jnp.concatenate([rep[0, pl.ds(b * KVH, KVH), :], rep[1, pl.ds(b * KVH, KVH), :]], axis=0).astype(BF16)
    pos_copy.wait()

    def each(i, do):
        for bb in range(BLK):
            b = i * BLK + bb
            rel = pos_s[b] - start

            @pl.when(jnp.logical_and(rel >= 0, rel < SLOTS))
            def _():
                base = pl.multiple_of(rel // 4 * (4 * KVH), 4 * KVH)
                mask = slot16 == lax.rem(rel, 4)
                for z, (ref, out) in enumerate(((kv, ko), (vv, vo))):
                    do(b, z, base, mask, ref, out)

    def merged(b, z, base, mask, ref):
        new = jnp.concatenate([rep[z, pl.ds(b * KVH, KVH), :]] * 4, axis=0)
        old = ref[b, pl.ds(base, 4 * KVH), :].astype(F32)
        return jnp.where(mask, new, old).astype(BF16)

    def put(b, z, base, mask, ref, out):
        ref[b, pl.ds(base, 4 * KVH), :] = merged(b, z, base, mask, ref)

    def stage(b, z, base, mask, ref, out):
        patch[z, b] = merged(b, z, base, mask, ref)

    def patch_copy(b, z, base, out):
        return pltpu.make_async_copy(patch.at[z, b], out.at[b, pl.ds(base, 4 * KVH)], psem.at[z, b])

    for i in range(1, NBLK):
        each(i, put)
        if 1 < i <= NA:
            for c in copies(i - 1):
                c.start()
    nkv_copy = pltpu.make_async_copy(nkv_s, nkv, osem.at[1])
    nkv_copy.start()
    each(0, stage)
    for i in range(NX):
        last_merge(lax.axis_index('sp') // 2, comb_a, xrx, i, oa, i)
    for c in copies(0):
        c.wait()
    each(0, lambda b, z, base, mask, ref, out: patch_copy(b, z, base, out).start())
    nkv_copy.wait()
    each(0, lambda b, z, base, mask, ref, out: patch_copy(b, z, base, out).wait())
    for i in range(1, NA):
        for c in copies(i):
            c.wait()


def solution(mesh):
    cache_spec = P('dp', 'sp', None, None)
    inv_freq = (np.float64(ROPE_THETA) ** (-np.arange(HD // 2) * 2.0 / HD)).astype(np.float32)
    freq2 = np.concatenate([inv_freq, inv_freq])
    vm = pl.BlockSpec(memory_space=pltpu.VMEM)
    hbm = pl.BlockSpec(memory_space=pl.ANY)
    dma = pltpu.SemaphoreType.DMA

    def device_step(tokens, positions, k_cache, v_cache, w_q, w_k, w_v, w_o, attn_norm, q_norm, k_norm):
        in_hbm = lambda x: pltpu.with_memory_space_constraint(x, pltpu.HBM)
        in_vmem = lambda x: pltpu.with_memory_space_constraint(x, pltpu.VMEM)
        rows = (SEQS, ROWS, HD)
        piece = (PIECE, HD)
        kv, vv, rep, wo_v, comb_a, comb_b, xrx_a = pl.pallas_call(
            attend_kernel,
            out_shape=(pltpu.VMEM(rows, BF16), pltpu.VMEM(rows, BF16),
                       pltpu.VMEM((2, SEQS * KVH, HD), F32), pltpu.VMEM((4, HALF * HD, WCH), BF16),
                       pltpu.VMEM((NX,) + piece, F32), pltpu.VMEM((NBLK - NX,) + piece, F32), pltpu.VMEM((NX,) + piece, F32)),
            in_specs=[hbm] * 12,
            out_specs=(vm,) * 7,
            scratch_shapes=[
                pltpu.SMEM((SEQS,), jnp.int32), pltpu.VMEM((SEQS, DIM), BF16), pltpu.VMEM((DIM // HD, HD), BF16),
                pltpu.VMEM((1, HD), BF16), pltpu.VMEM((1, HD), BF16), pltpu.VMEM((1, HD), F32), dma((6,)),
                pltpu.VMEM((2, SEQS, WCH), F32),
                pltpu.VMEM((RING, DIM, WCH), BF16),
                pltpu.VMEM((SEQS, DIM), BF16),
                pltpu.VMEM((SEQS, HD), F32), pltpu.VMEM((SEQS, HD), F32), pltpu.VMEM((SEQS, HD), F32),
                pltpu.VMEM((2, SEQS * 8, HD), F32), pltpu.VMEM((2, SEQS * 8, HD), F32),
                pltpu.VMEM((2 * HALF, ROWS), jnp.int32),
                pltpu.VMEM((NBLK, 2 * PIECE, HD), F32),
                pltpu.VMEM((NBLK,) + piece, F32),
                pltpu.VMEM((2, 4 * HALF, ROWS), F32), pltpu.VMEM((2, 4 * HALF, ROWS), BF16),
                dma((NW,)), dma((NBLK,)), dma((NBLK,)), dma((4,)), dma((3,)), dma((3,)),
                dma((NBLK,)), dma((NBLK,)), dma((NX,)), dma((NX,)),
            ],
            compiler_params=pltpu.CompilerParams(collective_id=0, has_side_effects=True, vmem_limit_bytes=VMEM_LIMIT),
            name='attend',
        )(in_hbm(positions), in_hbm(tokens), in_hbm(attn_norm.reshape(DIM // HD, HD)), in_hbm(q_norm.reshape(1, HD)),
          in_hbm(k_norm.reshape(1, HD)), in_hbm(jnp.asarray(freq2).reshape(1, HD)), in_hbm(w_q), in_hbm(w_k), in_hbm(w_v), in_hbm(w_o),
          in_hbm(k_cache.reshape(rows)), in_hbm(v_cache.reshape(rows)))
        xrx_b = lax.ppermute(comb_b, 'sp', [(0, 2), (2, 0), (1, 3), (3, 1)])
        k_out, v_out, new_kv, oa, kv, vv, wo_v = pl.pallas_call(
            write_kernel,
            out_shape=(pltpu.HBM(rows, BF16), pltpu.HBM(rows, BF16), pltpu.HBM((SEQS, 2 * KVH, HD), BF16),
                       pltpu.VMEM((NX * BLK, HALF * HD), F32), pltpu.VMEM(rows, BF16), pltpu.VMEM(rows, BF16),
                       pltpu.VMEM((4, HALF * HD, WCH), BF16)),
            in_specs=[hbm, vm, vm, vm, vm, vm, vm],
            out_specs=(hbm, hbm, hbm, vm, vm, vm, vm),
            input_output_aliases={1: 4, 2: 5, 6: 6},
            scratch_shapes=[pltpu.SMEM((SEQS,), jnp.int32), pltpu.VMEM((SEQS, 2 * KVH, HD), BF16),
                            pltpu.VMEM((2, BLK, 4 * KVH, HD), BF16),
                            dma((NBLK,)), dma((NBLK,)), dma((2, BLK)), dma((2,))],
            compiler_params=pltpu.CompilerParams(vmem_limit_bytes=VMEM_LIMIT),
            cost_estimate=pl.CostEstimate(flops=10**10, bytes_accessed=2**25, transcendentals=0),
            name='write',
        )(in_hbm(positions), in_vmem(kv), in_vmem(vv), in_vmem(rep), in_vmem(comb_a), in_vmem(xrx_a), in_vmem(wo_v))
        k_out, v_out, part = pl.pallas_call(
            product_kernel,
            out_shape=(pltpu.HBM(rows, BF16), pltpu.HBM(rows, BF16), pltpu.VMEM((SEQS, DIM), F32)),
            in_specs=[vm, vm, hbm, hbm, vm, vm, vm, vm],
            out_specs=(hbm, hbm, vm),
            input_output_aliases={2: 0, 3: 1},
            scratch_shapes=[pltpu.VMEM(((NBLK - NX) * BLK, HALF * HD), F32), dma((NBLK,)), dma((NBLK,))],
            compiler_params=pltpu.CompilerParams(vmem_limit_bytes=VMEM_LIMIT),
            cost_estimate=pl.CostEstimate(flops=2 * SEQS * DIM * DIM, bytes_accessed=2**22, transcendentals=0),
            name='product',
        )(in_vmem(kv), in_vmem(vv), k_out, v_out, in_vmem(oa), in_vmem(comb_b), in_vmem(xrx_b), in_vmem(wo_v))
        other = lax.ppermute(part, 'sp', [(0, 1), (1, 0), (2, 3), (3, 2)])
        k_out, v_out = pl.pallas_call(
            rest_kernel,
            out_shape=(pltpu.HBM(rows, BF16), pltpu.HBM(rows, BF16)),
            in_specs=[vm, vm, hbm, hbm],
            out_specs=(hbm, hbm),
            input_output_aliases={2: 0, 3: 1},
            scratch_shapes=[dma((NBLK,)), dma((NBLK,))],
            compiler_params=pltpu.CompilerParams(vmem_limit_bytes=VMEM_LIMIT),
            cost_estimate=pl.CostEstimate(flops=10**9, bytes_accessed=2**22, transcendentals=0),
            name='rest',
        )(in_vmem(kv), in_vmem(vv), k_out, v_out)
        block_out = (tokens.astype(F32) + (part + other)).astype(BF16)
        return block_out, k_out.reshape(k_cache.shape), v_out.reshape(v_cache.shape), new_kv.reshape(SEQS, 2, KVH, HD)

    return jax.shard_map(device_step, mesh=mesh, in_specs=(P('dp', None), P('dp'), cache_spec, cache_spec, P(), P(), P(), P(), P(), P(), P()), out_specs=(P('dp', None), cache_spec, cache_spec, P('dp', None, None, None)), check_vma=False)
```

```python
import functools

import jax
import jax.numpy as jnp
import numpy as np
from jax import lax
from jax.experimental import pallas as pl
from jax.experimental.pallas import tpu as pltpu
from jax.sharding import PartitionSpec as P

NORM_EPS = 1e-6
ROPE_THETA = 1000000.0
MESH = pl.DeviceIdType.MESH
BF16 = jnp.bfloat16
F32 = jnp.float32

SEQS = 64
DIM = 2048
HD = 128
KVH = 4
HALF = 16
SLOTS = 256
ROWS = SLOTS * KVH
BLK = 8
NBLK = SEQS // BLK
AHEAD = 5
NX = 8
NA = 6
NW = 5
WAHEAD = 3
RING = 4
LAG = 3
WCH = 512
CB = 4
NCB = SEQS // CB
PIECE = HALF * CB + 8
VMEM_LIMIT = 14 * 2**20
EXP_SCALE = HD ** -0.5 * 1.4426950408889634
NEG = -jnp.inf


def bcast_col(tile, col):
    return jnp.broadcast_to(tile[:, col:col + 1], (tile.shape[0], HD))


def attend_kernel(pos_h, tok_h, an_h, qn_h, kn_h, freq_h, wq, wk, wv, wo, kc, vc,
                  kv, vv, rep, wo_v, comb_a, comb_b, xrx,
                  pos_s, tok, an, qn, kn, freq, insem, proj, w_s, hid, ang, cosr, sinr, qmine, qmate, colslot, opart, drx, sc, pr_s,
                  wsem, ksem, vsem, wosem, qs, qr, ds_, dr, xs, xr):
    me = lax.axis_index('sp')
    core = lax.rem(me, 2)
    chip = me // 2
    mate = {'sp': me + 1 - 2 * core}
    peer = {'sp': me + 2 - 4 * chip}

    def w_copy(n, src=None):
        if n < 4:
            src = wq.at[:, pl.ds(pl.multiple_of(core * (HALF * HD) + n * WCH, WCH), WCH)]
        return pltpu.make_async_copy(src, w_s.at[n % RING], wsem.at[n])

    def w_start(n):
        if n < 4:
            w_copy(n).start()
        else:
            @pl.when(core == 0)
            def _():
                w_copy(n, wk).start()

            @pl.when(core == 1)
            def _():
                w_copy(n, wv).start()

    def wo_copy(n):
        src = wo.at[pl.ds(pl.multiple_of(core * (HALF * HD), HD), HALF * HD), pl.ds(n * WCH, WCH)]
        return pltpu.make_async_copy(src, wo_v.at[n], wosem.at[n])

    def k_copy(i):
        return pltpu.make_async_copy(kc.at[pl.ds(i * CB, CB)], kv.at[pl.ds(i * CB, CB)], ksem.at[i])

    def v_copy(i):
        return pltpu.make_async_copy(vc.at[pl.ds(i * CB, CB)], vv.at[pl.ds(i * CB, CB)], vsem.at[i])

    def q_send(h):
        return pltpu.make_async_remote_copy(qmine.at[h], qmate.at[h], qs.at[h], qr.at[h], device_id=mate, device_id_type=MESH)

    def new_send():
        return pltpu.make_async_remote_copy(rep.at[core], rep.at[core], qs.at[2], qr.at[2], device_id=mate, device_id_type=MESH)

    def d_send(i):
        return pltpu.make_async_remote_copy(opart.at[i, pl.ds(PIECE, PIECE)], drx.at[i], ds_.at[i], dr.at[i],
                                            device_id=mate, device_id_type=MESH)

    def x_send(i):
        return pltpu.make_async_remote_copy(comb_a.at[i], xrx.at[i], xs.at[i], xr.at[i],
                                            device_id=peer, device_id_type=MESH)

    small = [pltpu.make_async_copy(a, b, insem.at[z]) for z, (a, b) in enumerate(
        ((tok_h, tok), (pos_h, pos_s), (an_h, an), (qn_h, qn), (kn_h, kn), (freq_h, freq)))]
    for c in small:
        c.start()
    for n in range(WAHEAD):
        w_start(n)

    barrier = pltpu.get_barrier_semaphore()
    for other in (mate, peer):
        pl.semaphore_signal(barrier, inc=1, device_id=other, device_id_type=MESH)

    for c in small[1:]:
        c.wait()
    lane1 = lax.broadcasted_iota(jnp.int32, (1, HD), 1)

    def angle(b, carry):
        ang[pl.ds(b, 1), :] = freq[...] * pos_s[b].astype(F32)
        return carry

    lax.fori_loop(0, SEQS, angle, 0, unroll=8)
    cosr[...] = jnp.cos(ang[...])
    sinr[...] = jnp.sin(ang[...]) * jnp.where(lane1 < HD // 2, -1.0, 1.0)

    row = lax.broadcasted_iota(jnp.int32, (2 * HALF, ROWS), 0)
    col = lax.broadcasted_iota(jnp.int32, (2 * HALF, ROWS), 1)
    half_of_row = jnp.where(row < HALF, core, 1 - core)
    kv_of_row = half_of_row * 2 + lax.rem(row, HALF) // 8
    colslot[...] = jnp.where(lax.rem(col, KVH) == kv_of_row, col // KVH, 1 << 20)

    small[0].wait()
    t = tok[...].astype(F32)
    inv = lax.rsqrt(jnp.sum(t * t, axis=-1, keepdims=True) * (1.0 / DIM) + NORM_EPS)
    gains = an[...].astype(F32)
    for j in range(DIM // HD):
        sl = slice(j * HD, (j + 1) * HD)
        hid[:, sl] = (tok[:, sl].astype(F32) * inv * gains[j:j + 1, :]).astype(BF16)

    qgain = qn[...].astype(F32)
    kgain = kn[...].astype(F32)

    def norm_rope(x, gain):
        y = x * lax.rsqrt(jnp.mean(x * x, axis=-1, keepdims=True) + NORM_EPS) * gain
        y = y * cosr[...] + pltpu.roll(y, HD // 2, 1) * sinr[...]
        return y.astype(BF16).astype(F32)

    def post(n):
        for j in range(WCH // HD):
            x = proj[n % 2, :, j * HD:(j + 1) * HD].astype(BF16).astype(F32)
            if n < 4:
                qmine.at[n // 2][pl.ds(n % 2 * 4 + j, SEQS, stride=8), :] = norm_rope(x, qgain)
            else:
                rep.at[core][pl.ds(j, SEQS, stride=KVH), :] = jnp.where(core == 0, norm_rope(x, kgain), x)

    for n in range(NW):
        w_copy(n, wk).wait()
        if n + WAHEAD < NW:
            w_start(n + WAHEAD)
        else:
            k_copy(n + WAHEAD - NW).start()
            v_copy(n + WAHEAD - NW).start()
        proj[n % 2] = jnp.dot(hid[...], w_s[n % RING], preferred_element_type=F32)
        if n > 0:
            post(n - 1)
        if n == 2:
            pl.semaphore_wait(barrier, 2)
            q_send(0).start()
        if n == 4:
            q_send(1).start()
    for i in range(WAHEAD, AHEAD):
        k_copy(i).start()
        v_copy(i).start()
    post(NW - 1)
    new_send().start()
    start = me * SLOTS
    lane = lax.broadcasted_iota(jnp.int32, (HALF, HD), 1)
    lrow = lax.broadcasted_iota(jnp.int32, (HALF, HD), 0)
    lane8 = lax.broadcasted_iota(jnp.int32, (8, HD), 1)
    for h in range(2):
        q_send(h).wait()
    new_send().wait()

    def attend(i, first=False):
        ob = opart.at[i]
        def load_q(pair, at):
            bs = [at * CB + 2 * pair + z for z in range(2)]
            return bs, [jnp.concatenate([ref[h, pl.ds(pl.multiple_of(b * 8, 8), 8), :]
                                         for ref in (qmine, qmate) for h in range(2)], axis=0) for b in bs]

        def new_rows(z, b):
            return jnp.concatenate([jnp.broadcast_to(rep[z, pl.ds(b * KVH + h, 1), :], (8, HD))
                                    for h in (2 * core, 2 * core + 1, 2 - 2 * core, 3 - 2 * core)], axis=0)

        def scores(pair, at):
            bs, qf = load_q(pair, at)
            zero = jnp.zeros((2 * HALF, HD), BF16)
            lhs = jnp.concatenate([jnp.concatenate([qf[0].astype(BF16), zero], axis=1),
                                   jnp.concatenate([zero, qf[1].astype(BF16)], axis=1)], axis=0)
            keys = jnp.concatenate([kv[bs[0]], kv[bs[1]]], axis=1)
            sc[pair % 2] = lax.dot_general(lhs, keys, (((1,), (1,)), ((), ())), preferred_element_type=F32)

        def soft(pair):
            bs, qf = load_q(pair, i)
            out = []
            for z in range(2):
                b = bs[z]
                rel = pos_s[b] - start
                owner = jnp.logical_and(rel >= 0, rel < SLOTS)
                snew = jnp.where(owner, jnp.sum(qf[z] * new_rows(0, b), axis=-1, keepdims=True), NEG)
                sm = jnp.where(colslot[...] < rel, sc[pair % 2, z * 2 * HALF:(z + 1) * 2 * HALF], NEG)
                peak = jnp.maximum(jnp.max(sm, axis=-1, keepdims=True), snew)
                safe = jnp.where(peak == NEG, 0.0, peak)
                p = jnp.exp2((sm - safe) * EXP_SCALE)
                pn = jnp.exp2((snew - safe) * EXP_SCALE)
                pr_s[pair % 2, z * 2 * HALF:(z + 1) * 2 * HALF, :] = p.astype(BF16)
                out.append((pn.astype(BF16).astype(F32), jnp.sum(p, axis=-1, keepdims=True) + pn, peak))
            return out

        def mix(pair, st3):
            bs = [i * CB + 2 * pair + z for z in range(2)]
            values = jnp.concatenate([vv[bs[0]], vv[bs[1]]], axis=1)
            mixed = jnp.dot(pr_s[pair % 2], values, preferred_element_type=F32)
            for z in range(2):
                extra, total, peak = st3[z]
                o = mixed[z * 2 * HALF:(z + 1) * 2 * HALF, z * HD:(z + 1) * HD] + extra * new_rows(1, bs[z])
                bb = 2 * pair + z
                for h in range(2):
                    hs = slice(h * HALF, (h + 1) * HALF)
                    ob[pl.ds(h * PIECE + bb, HALF, stride=CB), :] = o[hs]
                    st = jnp.where(lane == lrow // 2, peak[hs], jnp.where(lane == lrow // 2 + HALF // 2, total[hs], 0.0))
                    for w in range(2):
                        ob[pl.ds(h * PIECE + HALF * CB + w * CB + bb, 1), :] = jnp.sum(
                            jnp.where(lrow % 2 == w, st, 0.0), axis=0, keepdims=True)

        if first:
            scores(0, i)
            return
        for pair in range(CB // 2):
            if pair + 1 < CB // 2:
                scores(pair + 1, i)
            else:
                scores(0, jnp.minimum(i + 1, NCB - 1))
            mix(pair, soft(pair))

    def combine(i, comb, at):
        s0 = opart[i, pl.ds(HALF * CB, 8), :]
        s1 = drx[i, pl.ds(HALF * CB, 8), :]
        peak = jnp.maximum(s0, s1)
        safe = jnp.where(peak == NEG, 0.0, peak)
        f0 = jnp.exp2((s0 - safe) * EXP_SCALE)
        f1 = jnp.exp2((s1 - safe) * EXP_SCALE)
        total = f0 * pltpu.roll(s0, HD - HALF // 2, 1) + f1 * pltpu.roll(s1, HD - HALF // 2, 1)
        comb[at, pl.ds(HALF * CB, 8), :] = jnp.where(
            lane8 < HALF // 2, peak, jnp.where(lane8 < HALF, pltpu.roll(total, HALF // 2, 1), 0.0))
        for u in range(HALF // 2):
            rows = pl.ds(u * 8, 8)
            comb[at, rows, :] = bcast_col(f0, u) * opart[i, rows, :] + bcast_col(f1, u) * drx[i, rows, :]

    def fetch(i):
        @pl.when(i + 1 < NCB)
        def _():
            k_copy(i + 1).wait()

        v_copy(i).wait()

        @pl.when(i + AHEAD < NCB)
        def _():
            k_copy(i + AHEAD).start()
            v_copy(i + AHEAD).start()

        @pl.when(i == NCB - 1)
        def _():
            for n in range(4):
                wo_copy(n).start()

    def early(i, carry):
        fetch(i)
        attend(i)
        d_send(i).start()
        return carry

    def sending(i, carry):
        fetch(i)
        d_send(i - LAG).wait_recv()
        combine(i - LAG, comb_a, i - LAG)
        attend(i)
        d_send(i).start()
        x_send(i - LAG).start()
        return carry

    def keeping(i, carry):
        fetch(i)
        d_send(i - LAG).wait_recv()
        combine(i - LAG, comb_b, i - LAG - NX)
        attend(i)
        d_send(i).start()
        return carry

    def late(i, carry):
        d_send(i).wait_recv()
        combine(i, comb_b, i - NX)
        return carry

    k_copy(0).wait()
    attend(0, first=True)
    lax.fori_loop(0, LAG, early, 0)
    lax.fori_loop(LAG, LAG + NX, sending, 0)
    lax.fori_loop(LAG + NX, NCB, keeping, 0)
    lax.fori_loop(NCB - LAG, NCB, late, 0)

    for n in range(4):
        wo_copy(n).wait()

    def drain(i, carry):
        d_send(i).wait_send()
        return carry

    def drain_x(i, carry):
        x_send(i).wait()
        return carry

    lax.fori_loop(0, NCB, drain, 0)
    lax.fori_loop(0, NX, drain_x, 0)


def last_merge(chip, comb, other_ref, i, ofin, at):
    first = chip == 0

    def ordered(rows):
        mine, other = comb[i, rows, :], other_ref[i, rows, :]
        return jnp.where(first, mine, other), jnp.where(first, other, mine)

    s0, s1 = ordered(pl.ds(HALF * CB, 8))
    peak = jnp.maximum(s0, s1)
    f0 = jnp.exp2((s0 - peak) * EXP_SCALE)
    f1 = jnp.exp2((s1 - peak) * EXP_SCALE)
    total = f0 * pltpu.roll(s0, HD - HALF // 2, 1) + f1 * pltpu.roll(s1, HD - HALF // 2, 1)
    g0, g1 = f0 / total, f1 / total
    for u in range(HALF // 2):
        a, b = ordered(pl.ds(u * 8, 8))
        o = bcast_col(g0, u) * a + bcast_col(g1, u) * b
        for w in range(2):
            j = 2 * u + w
            ofin[at * CB:(at + 1) * CB, j * HD:(j + 1) * HD] = o[w * CB:(w + 1) * CB]


def block_copies(i, kv, vv, ko, vo, ksem, vsem):
    r = pl.ds(i * BLK, BLK)
    return (pltpu.make_async_copy(kv.at[r], ko.at[r], ksem.at[i]),
            pltpu.make_async_copy(vv.at[r], vo.at[r], vsem.at[i]))


def product_kernel(kv, vv, ki, vi, oa, comb_b, xrx_b, wo_v, ko, vo, part, ofin, ksem, vsem):
    for c in block_copies(NA, kv, vv, ko, vo, ksem, vsem):
        c.start()
    for i in range(NCB - NX):
        last_merge(lax.axis_index('sp') // 2, comb_b, xrx_b, i, ofin, i)
    lhs = jnp.concatenate([oa[...].astype(BF16), ofin[...].astype(BF16)], axis=0)
    for n in range(4):
        part[:, n * WCH:(n + 1) * WCH] = jnp.dot(lhs, wo_v[n], preferred_element_type=F32)
    for c in block_copies(NA, kv, vv, ko, vo, ksem, vsem):
        c.wait()


def rest_kernel(kv, vv, ki, vi, ko, vo, ksem, vsem):
    for c in block_copies(NA + 1, kv, vv, ko, vo, ksem, vsem):
        c.start()
    for c in block_copies(NA + 1, kv, vv, ko, vo, ksem, vsem):
        c.wait()


def write_kernel(pos_h, kv, vv, rep, comb_a, xrx, wo_v, ko, vo, nkv, oa, kva, vva, wo_a, pos_s, nkv_s, patch, ksem, vsem, psem, osem):
    start = lax.axis_index('sp') * SLOTS
    slot16 = lax.broadcasted_iota(jnp.int32, (4 * KVH, HD), 0) // KVH

    def copies(i):
        return block_copies(i, kv, vv, ko, vo, ksem, vsem)

    pos_copy = pltpu.make_async_copy(pos_h, pos_s, osem.at[0])
    pos_copy.start()
    for c in copies(0):
        c.start()
    for b in range(SEQS):
        nkv_s[b] = jnp.concatenate([rep[0, pl.ds(b * KVH, KVH), :], rep[1, pl.ds(b * KVH, KVH), :]], axis=0).astype(BF16)
    pos_copy.wait()

    def each(i, do):
        for bb in range(BLK):
            b = i * BLK + bb
            rel = pos_s[b] - start

            @pl.when(jnp.logical_and(rel >= 0, rel < SLOTS))
            def _():
                base = pl.multiple_of(rel // 4 * (4 * KVH), 4 * KVH)
                mask = slot16 == lax.rem(rel, 4)
                for z, (ref, out) in enumerate(((kv, ko), (vv, vo))):
                    do(b, z, base, mask, ref, out)

    def merged(b, z, base, mask, ref):
        new = jnp.concatenate([rep[z, pl.ds(b * KVH, KVH), :]] * 4, axis=0)
        old = ref[b, pl.ds(base, 4 * KVH), :].astype(F32)
        return jnp.where(mask, new, old).astype(BF16)

    def put(b, z, base, mask, ref, out):
        ref[b, pl.ds(base, 4 * KVH), :] = merged(b, z, base, mask, ref)

    def stage(b, z, base, mask, ref, out):
        patch[z, b] = merged(b, z, base, mask, ref)

    def patch_copy(b, z, base, out):
        return pltpu.make_async_copy(patch.at[z, b], out.at[b, pl.ds(base, 4 * KVH)], psem.at[z, b])

    for i in range(1, NBLK):
        each(i, put)
        if 1 < i <= NA:
            for c in copies(i - 1):
                c.start()
    nkv_copy = pltpu.make_async_copy(nkv_s, nkv, osem.at[1])
    nkv_copy.start()
    each(0, stage)
    for i in range(NX):
        last_merge(lax.axis_index('sp') // 2, comb_a, xrx, i, oa, i)
    for c in copies(0):
        c.wait()
    each(0, lambda b, z, base, mask, ref, out: patch_copy(b, z, base, out).start())
    nkv_copy.wait()
    each(0, lambda b, z, base, mask, ref, out: patch_copy(b, z, base, out).wait())
    for i in range(1, NA):
        for c in copies(i):
            c.wait()


def solution(mesh):
    cache_spec = P('dp', 'sp', None, None)
    inv_freq = (np.float64(ROPE_THETA) ** (-np.arange(HD // 2) * 2.0 / HD)).astype(np.float32)
    freq2 = np.concatenate([inv_freq, inv_freq])
    vm = pl.BlockSpec(memory_space=pltpu.VMEM)
    hbm = pl.BlockSpec(memory_space=pl.ANY)
    dma = pltpu.SemaphoreType.DMA

    def device_step(tokens, positions, k_cache, v_cache, w_q, w_k, w_v, w_o, attn_norm, q_norm, k_norm):
        in_hbm = lambda x: pltpu.with_memory_space_constraint(x, pltpu.HBM)
        in_vmem = lambda x: pltpu.with_memory_space_constraint(x, pltpu.VMEM)
        rows = (SEQS, ROWS, HD)
        piece = (PIECE, HD)
        kv, vv, rep, wo_v, comb_a, comb_b, xrx_a = pl.pallas_call(
            attend_kernel,
            out_shape=(pltpu.VMEM(rows, BF16), pltpu.VMEM(rows, BF16),
                       pltpu.VMEM((2, SEQS * KVH, HD), F32), pltpu.VMEM((4, HALF * HD, WCH), BF16),
                       pltpu.VMEM((NX,) + piece, F32), pltpu.VMEM((NCB - NX,) + piece, F32), pltpu.VMEM((NX,) + piece, F32)),
            in_specs=[hbm] * 12,
            out_specs=(vm,) * 7,
            scratch_shapes=[
                pltpu.SMEM((SEQS,), jnp.int32), pltpu.VMEM((SEQS, DIM), BF16), pltpu.VMEM((DIM // HD, HD), BF16),
                pltpu.VMEM((1, HD), BF16), pltpu.VMEM((1, HD), BF16), pltpu.VMEM((1, HD), F32), dma((6,)),
                pltpu.VMEM((2, SEQS, WCH), F32),
                pltpu.VMEM((RING, DIM, WCH), BF16),
                pltpu.VMEM((SEQS, DIM), BF16),
                pltpu.VMEM((SEQS, HD), F32), pltpu.VMEM((SEQS, HD), F32), pltpu.VMEM((SEQS, HD), F32),
                pltpu.VMEM((2, SEQS * 8, HD), F32), pltpu.VMEM((2, SEQS * 8, HD), F32),
                pltpu.VMEM((2 * HALF, ROWS), jnp.int32),
                pltpu.VMEM((NCB, 2 * PIECE, HD), F32),
                pltpu.VMEM((NCB,) + piece, F32),
                pltpu.VMEM((2, 4 * HALF, ROWS), F32), pltpu.VMEM((2, 4 * HALF, ROWS), BF16),
                dma((NW,)), dma((NCB,)), dma((NCB,)), dma((4,)), dma((3,)), dma((3,)),
                dma((NCB,)), dma((NCB,)), dma((NX,)), dma((NX,)),
            ],
            compiler_params=pltpu.CompilerParams(collective_id=0, has_side_effects=True, vmem_limit_bytes=VMEM_LIMIT),
            name='attend',
        )(in_hbm(positions), in_hbm(tokens), in_hbm(attn_norm.reshape(DIM // HD, HD)), in_hbm(q_norm.reshape(1, HD)),
          in_hbm(k_norm.reshape(1, HD)), in_hbm(jnp.asarray(freq2).reshape(1, HD)), in_hbm(w_q), in_hbm(w_k), in_hbm(w_v), in_hbm(w_o),
          in_hbm(k_cache.reshape(rows)), in_hbm(v_cache.reshape(rows)))
        xrx_b = lax.ppermute(comb_b, 'sp', [(0, 2), (2, 0), (1, 3), (3, 1)])
        k_out, v_out, new_kv, oa, kv, vv, wo_v = pl.pallas_call(
            write_kernel,
            out_shape=(pltpu.HBM(rows, BF16), pltpu.HBM(rows, BF16), pltpu.HBM((SEQS, 2 * KVH, HD), BF16),
                       pltpu.VMEM((NX * CB, HALF * HD), F32), pltpu.VMEM(rows, BF16), pltpu.VMEM(rows, BF16),
                       pltpu.VMEM((4, HALF * HD, WCH), BF16)),
            in_specs=[hbm, vm, vm, vm, vm, vm, vm],
            out_specs=(hbm, hbm, hbm, vm, vm, vm, vm),
            input_output_aliases={1: 4, 2: 5, 6: 6},
            scratch_shapes=[pltpu.SMEM((SEQS,), jnp.int32), pltpu.VMEM((SEQS, 2 * KVH, HD), BF16),
                            pltpu.VMEM((2, BLK, 4 * KVH, HD), BF16),
                            dma((NBLK,)), dma((NBLK,)), dma((2, BLK)), dma((2,))],
            compiler_params=pltpu.CompilerParams(vmem_limit_bytes=VMEM_LIMIT),
            cost_estimate=pl.CostEstimate(flops=10**10, bytes_accessed=2**25, transcendentals=0),
            name='write',
        )(in_hbm(positions), in_vmem(kv), in_vmem(vv), in_vmem(rep), in_vmem(comb_a), in_vmem(xrx_a), in_vmem(wo_v))
        k_out, v_out, part = pl.pallas_call(
            product_kernel,
            out_shape=(pltpu.HBM(rows, BF16), pltpu.HBM(rows, BF16), pltpu.VMEM((SEQS, DIM), F32)),
            in_specs=[vm, vm, hbm, hbm, vm, vm, vm, vm],
            out_specs=(hbm, hbm, vm),
            input_output_aliases={2: 0, 3: 1},
            scratch_shapes=[pltpu.VMEM(((NCB - NX) * CB, HALF * HD), F32), dma((NBLK,)), dma((NBLK,))],
            compiler_params=pltpu.CompilerParams(vmem_limit_bytes=VMEM_LIMIT),
            cost_estimate=pl.CostEstimate(flops=2 * SEQS * DIM * DIM, bytes_accessed=2**22, transcendentals=0),
            name='product',
        )(in_vmem(kv), in_vmem(vv), k_out, v_out, in_vmem(oa), in_vmem(comb_b), in_vmem(xrx_b), in_vmem(wo_v))
        other = lax.ppermute(part, 'sp', [(0, 1), (1, 0), (2, 3), (3, 2)])
        k_out, v_out = pl.pallas_call(
            rest_kernel,
            out_shape=(pltpu.HBM(rows, BF16), pltpu.HBM(rows, BF16)),
            in_specs=[vm, vm, hbm, hbm],
            out_specs=(hbm, hbm),
            input_output_aliases={2: 0, 3: 1},
            scratch_shapes=[dma((NBLK,)), dma((NBLK,))],
            compiler_params=pltpu.CompilerParams(vmem_limit_bytes=VMEM_LIMIT),
            cost_estimate=pl.CostEstimate(flops=10**9, bytes_accessed=2**22, transcendentals=0),
            name='rest',
        )(in_vmem(kv), in_vmem(vv), k_out, v_out)
        block_out = (tokens.astype(F32) + (part + other)).astype(BF16)
        return block_out, k_out.reshape(k_cache.shape), v_out.reshape(v_cache.shape), new_kv.reshape(SEQS, 2, KVH, HD)

    return jax.shard_map(device_step, mesh=mesh, in_specs=(P('dp', None), P('dp'), cache_spec, cache_spec, P(), P(), P(), P(), P(), P(), P()), out_specs=(P('dp', None), cache_spec, cache_spec, P('dp', None, None, None)), check_vma=False)
```

```python
import functools

import jax
import jax.numpy as jnp
import numpy as np
from jax import lax
from jax.experimental import pallas as pl
from jax.experimental.pallas import tpu as pltpu
from jax.sharding import PartitionSpec as P

NORM_EPS = 1e-6
ROPE_THETA = 1000000.0
MESH = pl.DeviceIdType.MESH
BF16 = jnp.bfloat16
F32 = jnp.float32

SEQS = 64
DIM = 2048
HD = 128
KVH = 4
HALF = 16
SLOTS = 256
ROWS = SLOTS * KVH
BLK = 8
NBLK = SEQS // BLK
AHEAD = 3
NX = 4
NA = 6
NW = 5
WAHEAD = 3
RING = 4
LAG = 2
WCH = 512
PIECE = (HALF + 1) * BLK
VMEM_LIMIT = 14 * 2**20
EXP_SCALE = HD ** -0.5 * 1.4426950408889634
NEG = -jnp.inf


def bcast_col(tile, col):
    return jnp.broadcast_to(tile[:, col:col + 1], (tile.shape[0], HD))


def attend_kernel(pos_h, tok_h, an_h, qn_h, kn_h, freq_h, wq, wk, wv, wo, kc, vc,
                  kv, vv, rep, wo_v, comb_a, comb_b, xrx,
                  pos_s, tok, an, qn, kn, freq, insem, proj, w_s, hid, ang, cosr, sinr, qmine, qmate, colslot, opart, drx, sc, pr_s,
                  wsem, ksem, vsem, wosem, qs, qr, ds_, dr, xs, xr):
    me = lax.axis_index('sp')
    core = lax.rem(me, 2)
    chip = me // 2
    mate = {'sp': me + 1 - 2 * core}
    peer = {'sp': me + 2 - 4 * chip}

    def w_copy(n, src=None):
        if n < 4:
            src = wq.at[:, pl.ds(pl.multiple_of(core * (HALF * HD) + n * WCH, WCH), WCH)]
        return pltpu.make_async_copy(src, w_s.at[n % RING], wsem.at[n])

    def w_start(n):
        if n < 4:
            w_copy(n).start()
        else:
            @pl.when(core == 0)
            def _():
                w_copy(n, wk).start()

            @pl.when(core == 1)
            def _():
                w_copy(n, wv).start()

    def wo_copy(n):
        src = wo.at[pl.ds(pl.multiple_of(core * (HALF * HD), HD), HALF * HD), pl.ds(n * WCH, WCH)]
        return pltpu.make_async_copy(src, wo_v.at[n], wosem.at[n])

    def k_copy(i):
        return pltpu.make_async_copy(kc.at[pl.ds(i * BLK, BLK)], kv.at[pl.ds(i * BLK, BLK)], ksem.at[i])

    def v_copy(i):
        return pltpu.make_async_copy(vc.at[pl.ds(i * BLK, BLK)], vv.at[pl.ds(i * BLK, BLK)], vsem.at[i])

    def q_send(h):
        return pltpu.make_async_remote_copy(qmine.at[h], qmate.at[h], qs.at[h], qr.at[h], device_id=mate, device_id_type=MESH)

    def new_send():
        return pltpu.make_async_remote_copy(rep.at[core], rep.at[core], qs.at[2], qr.at[2], device_id=mate, device_id_type=MESH)

    def d_send(i):
        return pltpu.make_async_remote_copy(opart.at[i, pl.ds(PIECE, PIECE)], drx.at[i], ds_.at[i], dr.at[i],
                                            device_id=mate, device_id_type=MESH)

    def x_send(i):
        return pltpu.make_async_remote_copy(comb_a.at[i], xrx.at[i], xs.at[i], xr.at[i],
                                            device_id=peer, device_id_type=MESH)

    small = [pltpu.make_async_copy(a, b, insem.at[z]) for z, (a, b) in enumerate(
        ((tok_h, tok), (an_h, an), (pos_h, pos_s), (qn_h, qn), (kn_h, kn), (freq_h, freq)))]
    for c in small:
        c.start()
    for n in range(WAHEAD):
        w_start(n)

    barrier = pltpu.get_barrier_semaphore()
    for other in (mate, peer):
        pl.semaphore_signal(barrier, inc=1, device_id=other, device_id_type=MESH)

    small[0].wait()
    small[1].wait()
    t = tok[...].astype(F32)
    inv = lax.rsqrt(jnp.sum(t * t, axis=-1, keepdims=True) * (1.0 / DIM) + NORM_EPS)
    gains = an[...].astype(F32)
    for j in range(DIM // HD):
        sl = slice(j * HD, (j + 1) * HD)
        hid[:, sl] = (tok[:, sl].astype(F32) * inv * gains[j:j + 1, :]).astype(BF16)

    def tables():
        for c in small[2:]:
            c.wait()
        lane1 = lax.broadcasted_iota(jnp.int32, (1, HD), 1)

        def angle(b, carry):
            ang[pl.ds(b, 1), :] = freq[...] * pos_s[b].astype(F32)
            return carry

        lax.fori_loop(0, SEQS, angle, 0, unroll=8)
        cosr[...] = jnp.cos(ang[...])
        sinr[...] = jnp.sin(ang[...]) * jnp.where(lane1 < HD // 2, -1.0, 1.0)

        row = lax.broadcasted_iota(jnp.int32, (2 * HALF, ROWS), 0)
        col = lax.broadcasted_iota(jnp.int32, (2 * HALF, ROWS), 1)
        half_of_row = jnp.where(row < HALF, core, 1 - core)
        kv_of_row = half_of_row * 2 + lax.rem(row, HALF) // 8
        colslot[...] = jnp.where(lax.rem(col, KVH) == kv_of_row, col // KVH, 1 << 20)

    def norm_rope(x, gain):
        y = x * lax.rsqrt(jnp.mean(x * x, axis=-1, keepdims=True) + NORM_EPS) * gain
        y = y * cosr[...] + pltpu.roll(y, HD // 2, 1) * sinr[...]
        return y.astype(BF16).astype(F32)

    def post(n):
        for j in range(WCH // HD):
            x = proj[n % 2, :, j * HD:(j + 1) * HD].astype(BF16).astype(F32)
            if n < 4:
                qmine.at[n // 2][pl.ds(n % 2 * 4 + j, SEQS, stride=8), :] = norm_rope(x, qgain)
            else:
                rep.at[core][pl.ds(j, SEQS, stride=KVH), :] = jnp.where(core == 0, norm_rope(x, kgain), x)

    def multiply(n):
        w_copy(n, wk).wait()
        if n + WAHEAD < NW:
            w_start(n + WAHEAD)
        elif n >= NW - 2:
            k_copy(n - NW + 2).start()
            v_copy(n - NW + 2).start()
        proj[n % 2] = jnp.dot(hid[...], w_s[n % RING], preferred_element_type=F32)

    multiply(0)
    tables()
    qgain = qn[...].astype(F32)
    kgain = kn[...].astype(F32)
    multiply(1)
    post(0)
    multiply(2)
    post(1)
    pl.semaphore_wait(barrier, 2)
    q_send(0).start()
    multiply(3)
    post(2)
    post(3)
    q_send(1).start()
    multiply(4)
    for i in range(2, AHEAD):
        k_copy(i).start()
        v_copy(i).start()
    post(4)
    new_send().start()
    start = me * SLOTS
    lane = lax.broadcasted_iota(jnp.int32, (HALF, HD), 1)
    lrow = lax.broadcasted_iota(jnp.int32, (HALF, HD), 0)
    lane8 = lax.broadcasted_iota(jnp.int32, (BLK, HD), 1)
    for h in range(2):
        q_send(h).wait()

    def attend(i, first=False):
        ob = opart.at[i]
        def load_q(pair, at):
            bs = [at * BLK + 2 * pair + z for z in range(2)]
            return bs, [jnp.concatenate([ref[h, pl.ds(pl.multiple_of(b * 8, 8), 8), :]
                                         for ref in (qmine, qmate) for h in range(2)], axis=0) for b in bs]

        def new_rows(z, b):
            return jnp.concatenate([jnp.broadcast_to(rep[z, pl.ds(b * KVH + h, 1), :], (8, HD))
                                    for h in (2 * core, 2 * core + 1, 2 - 2 * core, 3 - 2 * core)], axis=0)

        def scores(pair, at):
            bs, qf = load_q(pair, at)
            zero = jnp.zeros((2 * HALF, HD), BF16)
            lhs = jnp.concatenate([jnp.concatenate([qf[0].astype(BF16), zero], axis=1),
                                   jnp.concatenate([zero, qf[1].astype(BF16)], axis=1)], axis=0)
            keys = jnp.concatenate([kv[bs[0]], kv[bs[1]]], axis=1)
            sc[pair % 2] = lax.dot_general(lhs, keys, (((1,), (1,)), ((), ())), preferred_element_type=F32)

        def soft(pair):
            bs, qf = load_q(pair, i)
            out = []
            for z in range(2):
                b = bs[z]
                rel = pos_s[b] - start
                owner = jnp.logical_and(rel >= 0, rel < SLOTS)
                snew = jnp.where(owner, jnp.sum(qf[z] * new_rows(0, b), axis=-1, keepdims=True), NEG)
                sm = jnp.where(colslot[...] < rel, sc[pair % 2, z * 2 * HALF:(z + 1) * 2 * HALF], NEG)
                peak = jnp.maximum(jnp.max(sm, axis=-1, keepdims=True), snew)
                safe = jnp.where(peak == NEG, 0.0, peak)
                p = jnp.exp2((sm - safe) * EXP_SCALE)
                pn = jnp.exp2((snew - safe) * EXP_SCALE)
                pr_s[pair % 2, z * 2 * HALF:(z + 1) * 2 * HALF, :] = p.astype(BF16)
                out.append((pn.astype(BF16).astype(F32), jnp.sum(p, axis=-1, keepdims=True) + pn, peak))
            return out

        def mix(pair, st3):
            bs = [i * BLK + 2 * pair + z for z in range(2)]
            values = jnp.concatenate([vv[bs[0]], vv[bs[1]]], axis=1)
            mixed = jnp.dot(pr_s[pair % 2], values, preferred_element_type=F32)
            for z in range(2):
                extra, total, peak = st3[z]
                o = mixed[z * 2 * HALF:(z + 1) * 2 * HALF, z * HD:(z + 1) * HD] + extra * new_rows(1, bs[z])
                bb = 2 * pair + z
                for h in range(2):
                    hs = slice(h * HALF, (h + 1) * HALF)
                    ob[pl.ds(h * PIECE + bb, HALF, stride=BLK), :] = o[hs]
                    st = jnp.where(lane == lrow, peak[hs], jnp.where(lane == lrow + HALF, total[hs], 0.0))
                    ob[pl.ds(h * PIECE + HALF * BLK + bb, 1), :] = jnp.sum(st, axis=0, keepdims=True)

        if first:
            scores(0, i)
            return
        for pair in range(BLK // 2):
            if pair + 1 < BLK // 2:
                scores(pair + 1, i)
            else:
                scores(0, jnp.minimum(i + 1, NBLK - 1))
            mix(pair, soft(pair))

    def combine(i, comb, at):
        s0 = opart[i, pl.ds(HALF * BLK, BLK), :]
        s1 = drx[i, pl.ds(HALF * BLK, BLK), :]
        peak = jnp.maximum(s0, s1)
        safe = jnp.where(peak == NEG, 0.0, peak)
        f0 = jnp.exp2((s0 - safe) * EXP_SCALE)
        f1 = jnp.exp2((s1 - safe) * EXP_SCALE)
        total = f0 * pltpu.roll(s0, HD - HALF, 1) + f1 * pltpu.roll(s1, HD - HALF, 1)
        comb[at, pl.ds(HALF * BLK, BLK), :] = jnp.where(
            lane8 < HALF, peak, jnp.where(lane8 < 2 * HALF, pltpu.roll(total, HALF, 1), 0.0))
        for j in range(HALF):
            rows = pl.ds(j * BLK, BLK)
            comb[at, rows, :] = bcast_col(f0, j) * opart[i, rows, :] + bcast_col(f1, j) * drx[i, rows, :]

    def fetch(i):
        @pl.when(i + 1 < NBLK)
        def _():
            k_copy(i + 1).wait()

        v_copy(i).wait()

        @pl.when(i + AHEAD < NBLK)
        def _():
            k_copy(i + AHEAD).start()
            v_copy(i + AHEAD).start()

        @pl.when(i == NBLK - 1)
        def _():
            for n in range(4):
                wo_copy(n).start()

    def early(i, carry):
        fetch(i)
        attend(i)
        d_send(i).start()
        return carry

    def sending(i, carry):
        fetch(i)
        d_send(i - LAG).wait_recv()
        combine(i - LAG, comb_a, i - LAG)
        attend(i)
        d_send(i).start()
        x_send(i - LAG).start()
        return carry

    def keeping(i, carry):
        fetch(i)
        d_send(i - LAG).wait_recv()
        combine(i - LAG, comb_b, i - LAG - NX)
        attend(i)
        d_send(i).start()
        return carry

    def late(i, carry):
        d_send(i).wait_recv()
        combine(i, comb_b, i - NX)
        return carry

    k_copy(0).wait()
    attend(0, first=True)
    new_send().wait()
    lax.fori_loop(0, LAG, early, 0)
    lax.fori_loop(LAG, LAG + NX, sending, 0)
    lax.fori_loop(LAG + NX, NBLK, keeping, 0)
    lax.fori_loop(NBLK - LAG, NBLK, late, 0)

    for n in range(4):
        wo_copy(n).wait()

    def drain(i, carry):
        d_send(i).wait_send()
        return carry

    def drain_x(i, carry):
        x_send(i).wait()
        return carry

    lax.fori_loop(0, NBLK, drain, 0)
    lax.fori_loop(0, NX, drain_x, 0)


def last_merge(chip, comb, other_ref, i, ofin, at):
    first = chip == 0

    def ordered(rows):
        mine, other = comb[i, rows, :], other_ref[i, rows, :]
        return jnp.where(first, mine, other), jnp.where(first, other, mine)

    s0, s1 = ordered(pl.ds(HALF * BLK, BLK))
    peak = jnp.maximum(s0, s1)
    f0 = jnp.exp2((s0 - peak) * EXP_SCALE)
    f1 = jnp.exp2((s1 - peak) * EXP_SCALE)
    total = f0 * pltpu.roll(s0, HD - HALF, 1) + f1 * pltpu.roll(s1, HD - HALF, 1)
    g0, g1 = f0 / total, f1 / total
    for j in range(HALF):
        a, b = ordered(pl.ds(j * BLK, BLK))
        ofin[at * BLK:(at + 1) * BLK, j * HD:(j + 1) * HD] = bcast_col(g0, j) * a + bcast_col(g1, j) * b


def block_copies(i, kv, vv, ko, vo, ksem, vsem):
    r = pl.ds(i * BLK, BLK)
    return (pltpu.make_async_copy(kv.at[r], ko.at[r], ksem.at[i]),
            pltpu.make_async_copy(vv.at[r], vo.at[r], vsem.at[i]))


def product_kernel(kv, vv, ki, vi, oa, comb_b, xrx_b, wo_v, ko, vo, part, ofin, ksem, vsem):
    for c in block_copies(NA, kv, vv, ko, vo, ksem, vsem):
        c.start()
    for i in range(NBLK - NX):
        last_merge(lax.axis_index('sp') // 2, comb_b, xrx_b, i, ofin, i)
    lhs = jnp.concatenate([oa[...].astype(BF16), ofin[...].astype(BF16)], axis=0)
    for n in range(4):
        part[:, n * WCH:(n + 1) * WCH] = jnp.dot(lhs, wo_v[n], preferred_element_type=F32)
    for c in block_copies(NA, kv, vv, ko, vo, ksem, vsem):
        c.wait()


def rest_kernel(kv, vv, ki, vi, ko, vo, ksem, vsem):
    for c in block_copies(NA + 1, kv, vv, ko, vo, ksem, vsem):
        c.start()
    for c in block_copies(NA + 1, kv, vv, ko, vo, ksem, vsem):
        c.wait()


def write_kernel(pos_h, kv, vv, rep, comb_a, xrx, wo_v, ko, vo, nkv, oa, kva, vva, wo_a, pos_s, nkv_s, patch, ksem, vsem, psem, osem):
    start = lax.axis_index('sp') * SLOTS
    slot16 = lax.broadcasted_iota(jnp.int32, (4 * KVH, HD), 0) // KVH

    def copies(i):
        return block_copies(i, kv, vv, ko, vo, ksem, vsem)

    pos_copy = pltpu.make_async_copy(pos_h, pos_s, osem.at[0])
    pos_copy.start()
    for c in copies(0):
        c.start()
    for b in range(SEQS):
        nkv_s[b] = jnp.concatenate([rep[0, pl.ds(b * KVH, KVH), :], rep[1, pl.ds(b * KVH, KVH), :]], axis=0).astype(BF16)
    pos_copy.wait()

    def each(i, do):
        for bb in range(BLK):
            b = i * BLK + bb
            rel = pos_s[b] - start

            @pl.when(jnp.logical_and(rel >= 0, rel < SLOTS))
            def _():
                base = pl.multiple_of(rel // 4 * (4 * KVH), 4 * KVH)
                mask = slot16 == lax.rem(rel, 4)
                for z, (ref, out) in enumerate(((kv, ko), (vv, vo))):
                    do(b, z, base, mask, ref, out)

    def merged(b, z, base, mask, ref):
        new = jnp.concatenate([rep[z, pl.ds(b * KVH, KVH), :]] * 4, axis=0)
        old = ref[b, pl.ds(base, 4 * KVH), :].astype(F32)
        return jnp.where(mask, new, old).astype(BF16)

    def put(b, z, base, mask, ref, out):
        ref[b, pl.ds(base, 4 * KVH), :] = merged(b, z, base, mask, ref)

    def stage(b, z, base, mask, ref, out):
        patch[z, b] = merged(b, z, base, mask, ref)

    def patch_copy(b, z, base, out):
        return pltpu.make_async_copy(patch.at[z, b], out.at[b, pl.ds(base, 4 * KVH)], psem.at[z, b])

    for i in range(1, NBLK):
        each(i, put)
        if 1 < i <= NA:
            for c in copies(i - 1):
                c.start()
    nkv_copy = pltpu.make_async_copy(nkv_s, nkv, osem.at[1])
    nkv_copy.start()
    each(0, stage)
    for i in range(NX):
        last_merge(lax.axis_index('sp') // 2, comb_a, xrx, i, oa, i)
    for c in copies(0):
        c.wait()
    each(0, lambda b, z, base, mask, ref, out: patch_copy(b, z, base, out).start())
    nkv_copy.wait()
    each(0, lambda b, z, base, mask, ref, out: patch_copy(b, z, base, out).wait())
    for i in range(1, NA):
        for c in copies(i):
            c.wait()


def solution(mesh):
    cache_spec = P('dp', 'sp', None, None)
    inv_freq = (np.float64(ROPE_THETA) ** (-np.arange(HD // 2) * 2.0 / HD)).astype(np.float32)
    freq2 = np.concatenate([inv_freq, inv_freq])
    vm = pl.BlockSpec(memory_space=pltpu.VMEM)
    hbm = pl.BlockSpec(memory_space=pl.ANY)
    dma = pltpu.SemaphoreType.DMA

    def device_step(tokens, positions, k_cache, v_cache, w_q, w_k, w_v, w_o, attn_norm, q_norm, k_norm):
        in_hbm = lambda x: pltpu.with_memory_space_constraint(x, pltpu.HBM)
        in_vmem = lambda x: pltpu.with_memory_space_constraint(x, pltpu.VMEM)
        rows = (SEQS, ROWS, HD)
        piece = (PIECE, HD)
        kv, vv, rep, wo_v, comb_a, comb_b, xrx_a = pl.pallas_call(
            attend_kernel,
            out_shape=(pltpu.VMEM(rows, BF16), pltpu.VMEM(rows, BF16),
                       pltpu.VMEM((2, SEQS * KVH, HD), F32), pltpu.VMEM((4, HALF * HD, WCH), BF16),
                       pltpu.VMEM((NX,) + piece, F32), pltpu.VMEM((NBLK - NX,) + piece, F32), pltpu.VMEM((NX,) + piece, F32)),
            in_specs=[hbm] * 12,
            out_specs=(vm,) * 7,
            scratch_shapes=[
                pltpu.SMEM((SEQS,), jnp.int32), pltpu.VMEM((SEQS, DIM), BF16), pltpu.VMEM((DIM // HD, HD), BF16),
                pltpu.VMEM((1, HD), BF16), pltpu.VMEM((1, HD), BF16), pltpu.VMEM((1, HD), F32), dma((6,)),
                pltpu.VMEM((2, SEQS, WCH), F32),
                pltpu.VMEM((RING, DIM, WCH), BF16),
                pltpu.VMEM((SEQS, DIM), BF16),
                pltpu.VMEM((SEQS, HD), F32), pltpu.VMEM((SEQS, HD), F32), pltpu.VMEM((SEQS, HD), F32),
                pltpu.VMEM((2, SEQS * 8, HD), F32), pltpu.VMEM((2, SEQS * 8, HD), F32),
                pltpu.VMEM((2 * HALF, ROWS), jnp.int32),
                pltpu.VMEM((NBLK, 2 * PIECE, HD), F32),
                pltpu.VMEM((NBLK,) + piece, F32),
                pltpu.VMEM((2, 4 * HALF, ROWS), F32), pltpu.VMEM((2, 4 * HALF, ROWS), BF16),
                dma((NW,)), dma((NBLK,)), dma((NBLK,)), dma((4,)), dma((3,)), dma((3,)),
                dma((NBLK,)), dma((NBLK,)), dma((NX,)), dma((NX,)),
            ],
            compiler_params=pltpu.CompilerParams(collective_id=0, has_side_effects=True, vmem_limit_bytes=VMEM_LIMIT),
            name='attend',
        )(in_hbm(positions), in_hbm(tokens), in_hbm(attn_norm.reshape(DIM // HD, HD)), in_hbm(q_norm.reshape(1, HD)),
          in_hbm(k_norm.reshape(1, HD)), in_hbm(jnp.asarray(freq2).reshape(1, HD)), in_hbm(w_q), in_hbm(w_k), in_hbm(w_v), in_hbm(w_o),
          in_hbm(k_cache.reshape(rows)), in_hbm(v_cache.reshape(rows)))
        xrx_b = lax.ppermute(comb_b, 'sp', [(0, 2), (2, 0), (1, 3), (3, 1)])
        k_out, v_out, new_kv, oa, kv, vv, wo_v = pl.pallas_call(
            write_kernel,
            out_shape=(pltpu.HBM(rows, BF16), pltpu.HBM(rows, BF16), pltpu.HBM((SEQS, 2 * KVH, HD), BF16),
                       pltpu.VMEM((NX * BLK, HALF * HD), F32), pltpu.VMEM(rows, BF16), pltpu.VMEM(rows, BF16),
                       pltpu.VMEM((4, HALF * HD, WCH), BF16)),
            in_specs=[hbm, vm, vm, vm, vm, vm, vm],
            out_specs=(hbm, hbm, hbm, vm, vm, vm, vm),
            input_output_aliases={1: 4, 2: 5, 6: 6},
            scratch_shapes=[pltpu.SMEM((SEQS,), jnp.int32), pltpu.VMEM((SEQS, 2 * KVH, HD), BF16),
                            pltpu.VMEM((2, BLK, 4 * KVH, HD), BF16),
                            dma((NBLK,)), dma((NBLK,)), dma((2, BLK)), dma((2,))],
            compiler_params=pltpu.CompilerParams(vmem_limit_bytes=VMEM_LIMIT),
            cost_estimate=pl.CostEstimate(flops=10**10, bytes_accessed=2**25, transcendentals=0),
            name='write',
        )(in_hbm(positions), in_vmem(kv), in_vmem(vv), in_vmem(rep), in_vmem(comb_a), in_vmem(xrx_a), in_vmem(wo_v))
        k_out, v_out, part = pl.pallas_call(
            product_kernel,
            out_shape=(pltpu.HBM(rows, BF16), pltpu.HBM(rows, BF16), pltpu.VMEM((SEQS, DIM), F32)),
            in_specs=[vm, vm, hbm, hbm, vm, vm, vm, vm],
            out_specs=(hbm, hbm, vm),
            input_output_aliases={2: 0, 3: 1},
            scratch_shapes=[pltpu.VMEM(((NBLK - NX) * BLK, HALF * HD), F32), dma((NBLK,)), dma((NBLK,))],
            compiler_params=pltpu.CompilerParams(vmem_limit_bytes=VMEM_LIMIT),
            cost_estimate=pl.CostEstimate(flops=2 * SEQS * DIM * DIM, bytes_accessed=2**22, transcendentals=0),
            name='product',
        )(in_vmem(kv), in_vmem(vv), k_out, v_out, in_vmem(oa), in_vmem(comb_b), in_vmem(xrx_b), in_vmem(wo_v))
        other = lax.ppermute(part, 'sp', [(0, 1), (1, 0), (2, 3), (3, 2)])
        k_out, v_out = pl.pallas_call(
            rest_kernel,
            out_shape=(pltpu.HBM(rows, BF16), pltpu.HBM(rows, BF16)),
            in_specs=[vm, vm, hbm, hbm],
            out_specs=(hbm, hbm),
            input_output_aliases={2: 0, 3: 1},
            scratch_shapes=[dma((NBLK,)), dma((NBLK,))],
            compiler_params=pltpu.CompilerParams(vmem_limit_bytes=VMEM_LIMIT),
            cost_estimate=pl.CostEstimate(flops=10**9, bytes_accessed=2**22, transcendentals=0),
            name='rest',
        )(in_vmem(kv), in_vmem(vv), k_out, v_out)
        block_out = (tokens.astype(F32) + (part + other)).astype(BF16)
        return block_out, k_out.reshape(k_cache.shape), v_out.reshape(v_cache.shape), new_kv.reshape(SEQS, 2, KVH, HD)

    return jax.shard_map(device_step, mesh=mesh, in_specs=(P('dp', None), P('dp'), cache_spec, cache_spec, P(), P(), P(), P(), P(), P(), P()), out_specs=(P('dp', None), cache_spec, cache_spec, P('dp', None, None, None)), check_vma=False)
```

```python
import functools

import jax
import jax.numpy as jnp
import numpy as np
from jax import lax
from jax.experimental import pallas as pl
from jax.experimental.pallas import tpu as pltpu
from jax.sharding import PartitionSpec as P

NORM_EPS = 1e-6
ROPE_THETA = 1000000.0
MESH = pl.DeviceIdType.MESH
BF16 = jnp.bfloat16
F32 = jnp.float32

SEQS = 64
DIM = 2048
HD = 128
KVH = 4
HALF = 16
SLOTS = 256
ROWS = SLOTS * KVH
BLK = 8
NBLK = SEQS // BLK
AHEAD = 4
NX = 3
NA = 7
NW = 5
WAHEAD = 3
RING = 4
LAG = 2
WCH = 512
PIECE = (HALF + 1) * BLK
VMEM_LIMIT = 14 * 2**20
EXP_SCALE = HD ** -0.5 * 1.4426950408889634
NEG = -jnp.inf


def bcast_col(tile, col):
    return jnp.broadcast_to(tile[:, col:col + 1], (tile.shape[0], HD))


def attend_kernel(pos_h, tok_h, an_h, qn_h, kn_h, freq_h, wq, wk, wv, wo, kc, vc,
                  kv, vv, rep, wo_v, comb_a, comb_b, xrx,
                  pos_s, tok, an, qn, kn, freq, insem, proj, w_s, hid, ang, cosr, sinr, qmine, qmate, colslot, opart, drx, sc, pr_s,
                  wsem, ksem, vsem, wosem, qs, qr, ds_, dr, xs, xr):
    me = lax.axis_index('sp')
    core = lax.rem(me, 2)
    chip = me // 2
    mate = {'sp': me + 1 - 2 * core}
    peer = {'sp': me + 2 - 4 * chip}

    def w_copy(n, src=None):
        if n < 4:
            src = wq.at[:, pl.ds(pl.multiple_of(core * (HALF * HD) + n * WCH, WCH), WCH)]
        return pltpu.make_async_copy(src, w_s.at[n % RING], wsem.at[n])

    def w_start(n):
        if n < 4:
            w_copy(n).start()
        else:
            @pl.when(core == 0)
            def _():
                w_copy(n, wk).start()

            @pl.when(core == 1)
            def _():
                w_copy(n, wv).start()

    def wo_copy(n):
        src = wo.at[pl.ds(pl.multiple_of(core * (HALF * HD), HD), HALF * HD), pl.ds(n * WCH, WCH)]
        return pltpu.make_async_copy(src, wo_v.at[n], wosem.at[n])

    def k_copy(i):
        return pltpu.make_async_copy(kc.at[pl.ds(i * BLK, BLK)], kv.at[pl.ds(i * BLK, BLK)], ksem.at[i])

    def v_copy(i):
        return pltpu.make_async_copy(vc.at[pl.ds(i * BLK, BLK)], vv.at[pl.ds(i * BLK, BLK)], vsem.at[i])

    def q_send(h):
        return pltpu.make_async_remote_copy(qmine.at[h], qmate.at[h], qs.at[h], qr.at[h], device_id=mate, device_id_type=MESH)

    def new_send():
        return pltpu.make_async_remote_copy(rep.at[core], rep.at[core], qs.at[2], qr.at[2], device_id=mate, device_id_type=MESH)

    def d_send(i):
        return pltpu.make_async_remote_copy(opart.at[i, pl.ds(PIECE, PIECE)], drx.at[i], ds_.at[i], dr.at[i],
                                            device_id=mate, device_id_type=MESH)

    def x_send(i):
        return pltpu.make_async_remote_copy(comb_a.at[i], xrx.at[i], xs.at[i], xr.at[i],
                                            device_id=peer, device_id_type=MESH)

    small = [pltpu.make_async_copy(a, b, insem.at[z]) for z, (a, b) in enumerate(
        ((tok_h, tok), (an_h, an), (pos_h, pos_s), (qn_h, qn), (kn_h, kn), (freq_h, freq)))]
    for c in small:
        c.start()
    for n in range(WAHEAD):
        w_start(n)

    barrier = pltpu.get_barrier_semaphore()
    for other in (mate, peer):
        pl.semaphore_signal(barrier, inc=1, device_id=other, device_id_type=MESH)

    small[0].wait()
    small[1].wait()
    t = tok[...].astype(F32)
    inv = lax.rsqrt(jnp.sum(t * t, axis=-1, keepdims=True) * (1.0 / DIM) + NORM_EPS)
    gains = an[...].astype(F32)
    for j in range(DIM // HD):
        sl = slice(j * HD, (j + 1) * HD)
        hid[:, sl] = (tok[:, sl].astype(F32) * inv * gains[j:j + 1, :]).astype(BF16)

    def tables():
        for c in small[2:]:
            c.wait()
        lane1 = lax.broadcasted_iota(jnp.int32, (1, HD), 1)

        def angle(b, carry):
            ang[pl.ds(b, 1), :] = freq[...] * pos_s[b].astype(F32)
            return carry

        lax.fori_loop(0, SEQS, angle, 0, unroll=8)
        cosr[...] = jnp.cos(ang[...])
        sinr[...] = jnp.sin(ang[...]) * jnp.where(lane1 < HD // 2, -1.0, 1.0)

        row = lax.broadcasted_iota(jnp.int32, (2 * HALF, ROWS), 0)
        col = lax.broadcasted_iota(jnp.int32, (2 * HALF, ROWS), 1)
        half_of_row = jnp.where(row < HALF, core, 1 - core)
        kv_of_row = half_of_row * 2 + lax.rem(row, HALF) // 8
        colslot[...] = jnp.where(lax.rem(col, KVH) == kv_of_row, col // KVH, 1 << 20)

    def norm_rope(x, gain):
        y = x * lax.rsqrt(jnp.mean(x * x, axis=-1, keepdims=True) + NORM_EPS) * gain
        y = y * cosr[...] + pltpu.roll(y, HD // 2, 1) * sinr[...]
        return y.astype(BF16).astype(F32)

    def post(n):
        for j in range(WCH // HD):
            x = proj[n % 2, :, j * HD:(j + 1) * HD].astype(BF16).astype(F32)
            if n < 4:
                qmine.at[n // 2][pl.ds(n % 2 * 4 + j, SEQS, stride=8), :] = norm_rope(x, qgain)
            else:
                rep.at[core][pl.ds(j, SEQS, stride=KVH), :] = jnp.where(core == 0, norm_rope(x, kgain), x)

    def multiply(n):
        w_copy(n, wk).wait()
        if n + WAHEAD < NW:
            w_start(n + WAHEAD)
        else:
            k_copy(n + WAHEAD - NW).start()
            v_copy(n + WAHEAD - NW).start()
        proj[n % 2] = jnp.dot(hid[...], w_s[n % RING], preferred_element_type=F32)

    multiply(0)
    tables()
    qgain = qn[...].astype(F32)
    kgain = kn[...].astype(F32)
    multiply(1)
    post(0)
    multiply(2)
    post(1)
    pl.semaphore_wait(barrier, 2)
    q_send(0).start()
    multiply(3)
    post(2)
    post(3)
    q_send(1).start()
    multiply(4)
    for i in range(WAHEAD, AHEAD):
        k_copy(i).start()
        v_copy(i).start()
    post(4)
    new_send().start()
    start = me * SLOTS
    lane = lax.broadcasted_iota(jnp.int32, (HALF, HD), 1)
    lrow = lax.broadcasted_iota(jnp.int32, (HALF, HD), 0)
    lane8 = lax.broadcasted_iota(jnp.int32, (BLK, HD), 1)
    for h in range(2):
        q_send(h).wait()

    def attend(i, first=False):
        ob = opart.at[i]
        def load_q(pair, at):
            bs = [at * BLK + 2 * pair + z for z in range(2)]
            return bs, [jnp.concatenate([ref[h, pl.ds(pl.multiple_of(b * 8, 8), 8), :]
                                         for ref in (qmine, qmate) for h in range(2)], axis=0) for b in bs]

        def new_rows(z, b):
            return jnp.concatenate([jnp.broadcast_to(rep[z, pl.ds(b * KVH + h, 1), :], (8, HD))
                                    for h in (2 * core, 2 * core + 1, 2 - 2 * core, 3 - 2 * core)], axis=0)

        def scores(pair, at):
            bs, qf = load_q(pair, at)
            zero = jnp.zeros((2 * HALF, HD), BF16)
            lhs = jnp.concatenate([jnp.concatenate([qf[0].astype(BF16), zero], axis=1),
                                   jnp.concatenate([zero, qf[1].astype(BF16)], axis=1)], axis=0)
            keys = jnp.concatenate([kv[bs[0]], kv[bs[1]]], axis=1)
            sc[pair % 2] = lax.dot_general(lhs, keys, (((1,), (1,)), ((), ())), preferred_element_type=F32)

        def soft(pair):
            bs, qf = load_q(pair, i)
            out = []
            for z in range(2):
                b = bs[z]
                rel = pos_s[b] - start
                owner = jnp.logical_and(rel >= 0, rel < SLOTS)
                snew = jnp.where(owner, jnp.sum(qf[z] * new_rows(0, b), axis=-1, keepdims=True), NEG)
                sm = jnp.where(colslot[...] < rel, sc[pair % 2, z * 2 * HALF:(z + 1) * 2 * HALF], NEG)
                peak = jnp.maximum(jnp.max(sm, axis=-1, keepdims=True), snew)
                safe = jnp.where(peak == NEG, 0.0, peak)
                p = jnp.exp2((sm - safe) * EXP_SCALE)
                pn = jnp.exp2((snew - safe) * EXP_SCALE)
                pr_s[pair % 2, z * 2 * HALF:(z + 1) * 2 * HALF, :] = p.astype(BF16)
                out.append((pn.astype(BF16).astype(F32), jnp.sum(p, axis=-1, keepdims=True) + pn, peak))
            return out

        def mix(pair, st3):
            bs = [i * BLK + 2 * pair + z for z in range(2)]
            values = jnp.concatenate([vv[bs[0]], vv[bs[1]]], axis=1)
            mixed = jnp.dot(pr_s[pair % 2], values, preferred_element_type=F32)
            for z in range(2):
                extra, total, peak = st3[z]
                o = mixed[z * 2 * HALF:(z + 1) * 2 * HALF, z * HD:(z + 1) * HD] + extra * new_rows(1, bs[z])
                bb = 2 * pair + z
                for h in range(2):
                    hs = slice(h * HALF, (h + 1) * HALF)
                    ob[pl.ds(h * PIECE + bb, HALF, stride=BLK), :] = o[hs]
                    st = jnp.where(lane == lrow, peak[hs], jnp.where(lane == lrow + HALF, total[hs], 0.0))
                    ob[pl.ds(h * PIECE + HALF * BLK + bb, 1), :] = jnp.sum(st, axis=0, keepdims=True)

        if first:
            scores(0, i)
            return
        for pair in range(BLK // 2):
            if pair + 1 < BLK // 2:
                scores(pair + 1, i)
            else:
                scores(0, jnp.minimum(i + 1, NBLK - 1))
            mix(pair, soft(pair))

    def combine(i, comb, at):
        s0 = opart[i, pl.ds(HALF * BLK, BLK), :]
        s1 = drx[i, pl.ds(HALF * BLK, BLK), :]
        peak = jnp.maximum(s0, s1)
        safe = jnp.where(peak == NEG, 0.0, peak)
        f0 = jnp.exp2((s0 - safe) * EXP_SCALE)
        f1 = jnp.exp2((s1 - safe) * EXP_SCALE)
        total = f0 * pltpu.roll(s0, HD - HALF, 1) + f1 * pltpu.roll(s1, HD - HALF, 1)
        comb[at, pl.ds(HALF * BLK, BLK), :] = jnp.where(
            lane8 < HALF, peak, jnp.where(lane8 < 2 * HALF, pltpu.roll(total, HALF, 1), 0.0))
        for j in range(HALF):
            rows = pl.ds(j * BLK, BLK)
            comb[at, rows, :] = bcast_col(f0, j) * opart[i, rows, :] + bcast_col(f1, j) * drx[i, rows, :]

    def fetch(i):
        @pl.when(i + 1 < NBLK)
        def _():
            k_copy(i + 1).wait()

        v_copy(i).wait()

        @pl.when(i + AHEAD < NBLK)
        def _():
            k_copy(i + AHEAD).start()
            v_copy(i + AHEAD).start()

        @pl.when(i + AHEAD == NBLK)
        def _():
            for n in range(4):
                wo_copy(n).start()

    def early(i, carry):
        fetch(i)
        attend(i)
        d_send(i).start()
        return carry

    def sending(i, carry):
        fetch(i)
        d_send(i - LAG).wait_recv()
        combine(i - LAG, comb_a, i - LAG)
        attend(i)
        d_send(i).start()
        x_send(i - LAG).start()
        return carry

    def keeping(i, carry):
        fetch(i)
        d_send(i - LAG).wait_recv()
        combine(i - LAG, comb_b, i - LAG - NX)
        attend(i)
        d_send(i).start()
        return carry

    def late(i, carry):
        d_send(i).wait_recv()
        combine(i, comb_b, i - NX)
        return carry

    k_copy(0).wait()
    attend(0, first=True)
    new_send().wait()
    lax.fori_loop(0, LAG, early, 0)
    lax.fori_loop(LAG, LAG + NX, sending, 0)
    lax.fori_loop(LAG + NX, NBLK, keeping, 0)
    lax.fori_loop(NBLK - LAG, NBLK, late, 0)

    for n in range(4):
        wo_copy(n).wait()

    def drain(i, carry):
        d_send(i).wait_send()
        return carry

    def drain_x(i, carry):
        x_send(i).wait()
        return carry

    lax.fori_loop(0, NBLK, drain, 0)
    lax.fori_loop(0, NX, drain_x, 0)


def last_merge(chip, comb, other_ref, i, ofin, at):
    first = chip == 0

    def ordered(rows):
        mine, other = comb[i, rows, :], other_ref[i, rows, :]
        return jnp.where(first, mine, other), jnp.where(first, other, mine)

    s0, s1 = ordered(pl.ds(HALF * BLK, BLK))
    peak = jnp.maximum(s0, s1)
    f0 = jnp.exp2((s0 - peak) * EXP_SCALE)
    f1 = jnp.exp2((s1 - peak) * EXP_SCALE)
    total = f0 * pltpu.roll(s0, HD - HALF, 1) + f1 * pltpu.roll(s1, HD - HALF, 1)
    g0, g1 = f0 / total, f1 / total
    for j in range(HALF):
        a, b = ordered(pl.ds(j * BLK, BLK))
        ofin[at * BLK:(at + 1) * BLK, j * HD:(j + 1) * HD] = bcast_col(g0, j) * a + bcast_col(g1, j) * b


def block_copies(i, kv, vv, ko, vo, ksem, vsem):
    r = pl.ds(i * BLK, BLK)
    return (pltpu.make_async_copy(kv.at[r], ko.at[r], ksem.at[i]),
            pltpu.make_async_copy(vv.at[r], vo.at[r], vsem.at[i]))


def product_kernel(kv, vv, ki, vi, oa, comb_b, xrx_b, wo_v, ko, vo, part, ofin, ksem, vsem):
    block_copies(NA, kv, vv, ko, vo, ksem, vsem)[0].start()
    for i in range(NBLK - NX):
        last_merge(lax.axis_index('sp') // 2, comb_b, xrx_b, i, ofin, i)
    lhs = jnp.concatenate([oa[...].astype(BF16), ofin[...].astype(BF16)], axis=0)
    for n in range(4):
        part[:, n * WCH:(n + 1) * WCH] = jnp.dot(lhs, wo_v[n], preferred_element_type=F32)
    block_copies(NA, kv, vv, ko, vo, ksem, vsem)[0].wait()


def rest_kernel(kv, vv, ki, vi, ko, vo, ksem, vsem):
    copy = block_copies(NA, kv, vv, ko, vo, ksem, vsem)[1]
    copy.start()
    copy.wait()


def write_kernel(pos_h, kv, vv, rep, comb_a, xrx, wo_v, ko, vo, nkv, oa, kva, vva, wo_a, pos_s, nkv_s, patch, ksem, vsem, psem, osem):
    start = lax.axis_index('sp') * SLOTS
    slot16 = lax.broadcasted_iota(jnp.int32, (4 * KVH, HD), 0) // KVH

    def copies(i):
        return block_copies(i, kv, vv, ko, vo, ksem, vsem)

    pos_copy = pltpu.make_async_copy(pos_h, pos_s, osem.at[0])
    pos_copy.start()
    for c in copies(0):
        c.start()
    for b in range(SEQS):
        nkv_s[b] = jnp.concatenate([rep[0, pl.ds(b * KVH, KVH), :], rep[1, pl.ds(b * KVH, KVH), :]], axis=0).astype(BF16)
    pos_copy.wait()

    def each(i, do):
        for bb in range(BLK):
            b = i * BLK + bb
            rel = pos_s[b] - start

            @pl.when(jnp.logical_and(rel >= 0, rel < SLOTS))
            def _():
                base = pl.multiple_of(rel // 4 * (4 * KVH), 4 * KVH)
                mask = slot16 == lax.rem(rel, 4)
                for z, (ref, out) in enumerate(((kv, ko), (vv, vo))):
                    do(b, z, base, mask, ref, out)

    def merged(b, z, base, mask, ref):
        new = jnp.concatenate([rep[z, pl.ds(b * KVH, KVH), :]] * 4, axis=0)
        old = ref[b, pl.ds(base, 4 * KVH), :].astype(F32)
        return jnp.where(mask, new, old).astype(BF16)

    def put(b, z, base, mask, ref, out):
        ref[b, pl.ds(base, 4 * KVH), :] = merged(b, z, base, mask, ref)

    def stage(b, z, base, mask, ref, out):
        patch[z, b] = merged(b, z, base, mask, ref)

    def patch_copy(b, z, base, out):
        return pltpu.make_async_copy(patch.at[z, b], out.at[b, pl.ds(base, 4 * KVH)], psem.at[z, b])

    for i in range(1, NBLK):
        each(i, put)
        if 1 < i <= NA:
            for c in copies(i - 1):
                c.start()
    nkv_copy = pltpu.make_async_copy(nkv_s, nkv, osem.at[1])
    nkv_copy.start()
    each(0, stage)
    for i in range(NX):
        last_merge(lax.axis_index('sp') // 2, comb_a, xrx, i, oa, i)
    for c in copies(0):
        c.wait()
    each(0, lambda b, z, base, mask, ref, out: patch_copy(b, z, base, out).start())
    nkv_copy.wait()
    each(0, lambda b, z, base, mask, ref, out: patch_copy(b, z, base, out).wait())
    for i in range(1, NA):
        for c in copies(i):
            c.wait()


def solution(mesh):
    cache_spec = P('dp', 'sp', None, None)
    inv_freq = (np.float64(ROPE_THETA) ** (-np.arange(HD // 2) * 2.0 / HD)).astype(np.float32)
    freq2 = np.concatenate([inv_freq, inv_freq])
    vm = pl.BlockSpec(memory_space=pltpu.VMEM)
    hbm = pl.BlockSpec(memory_space=pl.ANY)
    dma = pltpu.SemaphoreType.DMA

    def device_step(tokens, positions, k_cache, v_cache, w_q, w_k, w_v, w_o, attn_norm, q_norm, k_norm):
        in_hbm = lambda x: pltpu.with_memory_space_constraint(x, pltpu.HBM)
        in_vmem = lambda x: pltpu.with_memory_space_constraint(x, pltpu.VMEM)
        rows = (SEQS, ROWS, HD)
        piece = (PIECE, HD)
        kv, vv, rep, wo_v, comb_a, comb_b, xrx_a = pl.pallas_call(
            attend_kernel,
            out_shape=(pltpu.VMEM(rows, BF16), pltpu.VMEM(rows, BF16),
                       pltpu.VMEM((2, SEQS * KVH, HD), F32), pltpu.VMEM((4, HALF * HD, WCH), BF16),
                       pltpu.VMEM((NX,) + piece, F32), pltpu.VMEM((NBLK - NX,) + piece, F32), pltpu.VMEM((NX,) + piece, F32)),
            in_specs=[hbm] * 12,
            out_specs=(vm,) * 7,
            scratch_shapes=[
                pltpu.SMEM((SEQS,), jnp.int32), pltpu.VMEM((SEQS, DIM), BF16), pltpu.VMEM((DIM // HD, HD), BF16),
                pltpu.VMEM((1, HD), BF16), pltpu.VMEM((1, HD), BF16), pltpu.VMEM((1, HD), F32), dma((6,)),
                pltpu.VMEM((2, SEQS, WCH), F32),
                pltpu.VMEM((RING, DIM, WCH), BF16),
                pltpu.VMEM((SEQS, DIM), BF16),
                pltpu.VMEM((SEQS, HD), F32), pltpu.VMEM((SEQS, HD), F32), pltpu.VMEM((SEQS, HD), F32),
                pltpu.VMEM((2, SEQS * 8, HD), F32), pltpu.VMEM((2, SEQS * 8, HD), F32),
                pltpu.VMEM((2 * HALF, ROWS), jnp.int32),
                pltpu.VMEM((NBLK, 2 * PIECE, HD), F32),
                pltpu.VMEM((NBLK,) + piece, F32),
                pltpu.VMEM((2, 4 * HALF, ROWS), F32), pltpu.VMEM((2, 4 * HALF, ROWS), BF16),
                dma((NW,)), dma((NBLK,)), dma((NBLK,)), dma((4,)), dma((3,)), dma((3,)),
                dma((NBLK,)), dma((NBLK,)), dma((NX,)), dma((NX,)),
            ],
            compiler_params=pltpu.CompilerParams(collective_id=0, has_side_effects=True, vmem_limit_bytes=VMEM_LIMIT),
            name='attend',
        )(in_hbm(positions), in_hbm(tokens), in_hbm(attn_norm.reshape(DIM // HD, HD)), in_hbm(q_norm.reshape(1, HD)),
          in_hbm(k_norm.reshape(1, HD)), in_hbm(jnp.asarray(freq2).reshape(1, HD)), in_hbm(w_q), in_hbm(w_k), in_hbm(w_v), in_hbm(w_o),
          in_hbm(k_cache.reshape(rows)), in_hbm(v_cache.reshape(rows)))
        xrx_b = lax.ppermute(comb_b, 'sp', [(0, 2), (2, 0), (1, 3), (3, 1)])
        k_out, v_out, new_kv, oa, kv, vv, wo_v = pl.pallas_call(
            write_kernel,
            out_shape=(pltpu.HBM(rows, BF16), pltpu.HBM(rows, BF16), pltpu.HBM((SEQS, 2 * KVH, HD), BF16),
                       pltpu.VMEM((NX * BLK, HALF * HD), F32), pltpu.VMEM(rows, BF16), pltpu.VMEM(rows, BF16),
                       pltpu.VMEM((4, HALF * HD, WCH), BF16)),
            in_specs=[hbm, vm, vm, vm, vm, vm, vm],
            out_specs=(hbm, hbm, hbm, vm, vm, vm, vm),
            input_output_aliases={1: 4, 2: 5, 6: 6},
            scratch_shapes=[pltpu.SMEM((SEQS,), jnp.int32), pltpu.VMEM((SEQS, 2 * KVH, HD), BF16),
                            pltpu.VMEM((2, BLK, 4 * KVH, HD), BF16),
                            dma((NBLK,)), dma((NBLK,)), dma((2, BLK)), dma((2,))],
            compiler_params=pltpu.CompilerParams(vmem_limit_bytes=VMEM_LIMIT),
            cost_estimate=pl.CostEstimate(flops=10**10, bytes_accessed=2**25, transcendentals=0),
            name='write',
        )(in_hbm(positions), in_vmem(kv), in_vmem(vv), in_vmem(rep), in_vmem(comb_a), in_vmem(xrx_a), in_vmem(wo_v))
        k_out, v_out, part = pl.pallas_call(
            product_kernel,
            out_shape=(pltpu.HBM(rows, BF16), pltpu.HBM(rows, BF16), pltpu.VMEM((SEQS, DIM), F32)),
            in_specs=[vm, vm, hbm, hbm, vm, vm, vm, vm],
            out_specs=(hbm, hbm, vm),
            input_output_aliases={2: 0, 3: 1},
            scratch_shapes=[pltpu.VMEM(((NBLK - NX) * BLK, HALF * HD), F32), dma((NBLK,)), dma((NBLK,))],
            compiler_params=pltpu.CompilerParams(vmem_limit_bytes=VMEM_LIMIT),
            cost_estimate=pl.CostEstimate(flops=2 * SEQS * DIM * DIM, bytes_accessed=2**22, transcendentals=0),
            name='product',
        )(in_vmem(kv), in_vmem(vv), k_out, v_out, in_vmem(oa), in_vmem(comb_b), in_vmem(xrx_b), in_vmem(wo_v))
        other = lax.ppermute(part, 'sp', [(0, 1), (1, 0), (2, 3), (3, 2)])
        k_out, v_out = pl.pallas_call(
            rest_kernel,
            out_shape=(pltpu.HBM(rows, BF16), pltpu.HBM(rows, BF16)),
            in_specs=[vm, vm, hbm, hbm],
            out_specs=(hbm, hbm),
            input_output_aliases={2: 0, 3: 1},
            scratch_shapes=[dma((NBLK,)), dma((NBLK,))],
            compiler_params=pltpu.CompilerParams(vmem_limit_bytes=VMEM_LIMIT),
            cost_estimate=pl.CostEstimate(flops=10**9, bytes_accessed=2**22, transcendentals=0),
            name='rest',
        )(in_vmem(kv), in_vmem(vv), k_out, v_out)
        block_out = (tokens.astype(F32) + (part + other)).astype(BF16)
        return block_out, k_out.reshape(k_cache.shape), v_out.reshape(v_cache.shape), new_kv.reshape(SEQS, 2, KVH, HD)

    return jax.shard_map(device_step, mesh=mesh, in_specs=(P('dp', None), P('dp'), cache_spec, cache_spec, P(), P(), P(), P(), P(), P(), P()), out_specs=(P('dp', None), cache_spec, cache_spec, P('dp', None, None, None)), check_vma=False)
```

```python
import functools

import jax
import jax.numpy as jnp
import numpy as np
from jax import lax
from jax.experimental import pallas as pl
from jax.experimental.pallas import tpu as pltpu
from jax.sharding import PartitionSpec as P

NORM_EPS = 1e-6
ROPE_THETA = 1000000.0
MESH = pl.DeviceIdType.MESH
BF16 = jnp.bfloat16
F32 = jnp.float32

SEQS = 64
DIM = 2048
HD = 128
KVH = 4
HALF = 16
SLOTS = 256
ROWS = SLOTS * KVH
BLK = 8
NBLK = SEQS // BLK
AHEAD = 4
NX = 3
NA = 7
NW = 5
WAHEAD = 3
RING = 4
LAG = 2
WCH = 512
PIECE = (HALF + 1) * BLK
VMEM_LIMIT = 14 * 2**20
EXP_SCALE = HD ** -0.5 * 1.4426950408889634
NEG = -jnp.inf


def bcast_col(tile, col):
    return jnp.broadcast_to(tile[:, col:col + 1], (tile.shape[0], HD))


def attend_kernel(pos_h, tok_h, an_h, qn_h, kn_h, freq_h, wq, wk, wv, wo, kc, vc,
                  kv, vv, rep, wo_v, comb_a, comb_b, xrx,
                  pos_s, tok, an, qn, kn, freq, insem, proj, w_s, hid, ang, cosr, sinr, qmine, qmate, colslot, opart, drx, sc, pr_s,
                  wsem, ksem, vsem, wosem, qs, qr, ds_, dr, xs, xr):
    me = lax.axis_index('sp')
    core = lax.rem(me, 2)
    chip = me // 2
    mate = {'sp': me + 1 - 2 * core}
    peer = {'sp': me + 2 - 4 * chip}

    def w_copy(n, src=None):
        if n < 4:
            src = wq.at[:, pl.ds(pl.multiple_of(core * (HALF * HD) + n * WCH, WCH), WCH)]
        return pltpu.make_async_copy(src, w_s.at[n % RING], wsem.at[n])

    def w_start(n):
        if n < 4:
            w_copy(n).start()
        else:
            @pl.when(core == 0)
            def _():
                w_copy(n, wk).start()

            @pl.when(core == 1)
            def _():
                w_copy(n, wv).start()

    def wo_copy(n):
        src = wo.at[pl.ds(pl.multiple_of(core * (HALF * HD), HD), HALF * HD), pl.ds(n * WCH, WCH)]
        return pltpu.make_async_copy(src, wo_v.at[n], wosem.at[n])

    def k_copy(i):
        return pltpu.make_async_copy(kc.at[pl.ds(i * BLK, BLK)], kv.at[pl.ds(i * BLK, BLK)], ksem.at[i])

    def v_copy(i):
        return pltpu.make_async_copy(vc.at[pl.ds(i * BLK, BLK)], vv.at[pl.ds(i * BLK, BLK)], vsem.at[i])

    def q_send(h):
        return pltpu.make_async_remote_copy(qmine.at[h], qmate.at[h], qs.at[h], qr.at[h], device_id=mate, device_id_type=MESH)

    def new_send():
        return pltpu.make_async_remote_copy(rep.at[core], rep.at[core], qs.at[2], qr.at[2], device_id=mate, device_id_type=MESH)

    def d_send(i):
        return pltpu.make_async_remote_copy(opart.at[i, pl.ds(PIECE, PIECE)], drx.at[i], ds_.at[i], dr.at[i],
                                            device_id=mate, device_id_type=MESH)

    def x_send(i):
        return pltpu.make_async_remote_copy(comb_a.at[i], xrx.at[i], xs.at[i], xr.at[i],
                                            device_id=peer, device_id_type=MESH)

    small = [pltpu.make_async_copy(a, b, insem.at[z]) for z, (a, b) in enumerate(
        ((tok_h, tok), (an_h, an), (pos_h, pos_s), (qn_h, qn), (kn_h, kn), (freq_h, freq)))]
    for c in small:
        c.start()
    for n in range(WAHEAD):
        w_start(n)

    barrier = pltpu.get_barrier_semaphore()
    for other in (mate, peer):
        pl.semaphore_signal(barrier, inc=1, device_id=other, device_id_type=MESH)

    small[0].wait()
    small[1].wait()
    t = tok[...].astype(F32)
    inv = lax.rsqrt(jnp.sum(t * t, axis=-1, keepdims=True) * (1.0 / DIM) + NORM_EPS)
    gains = an[...].astype(F32)
    for j in range(DIM // HD):
        sl = slice(j * HD, (j + 1) * HD)
        hid[:, sl] = (tok[:, sl].astype(F32) * inv * gains[j:j + 1, :]).astype(BF16)

    def tables():
        for c in small[2:]:
            c.wait()
        lane1 = lax.broadcasted_iota(jnp.int32, (1, HD), 1)

        def angle(b, carry):
            ang[pl.ds(b, 1), :] = freq[...] * pos_s[b].astype(F32)
            return carry

        lax.fori_loop(0, SEQS, angle, 0, unroll=8)
        cosr[...] = jnp.cos(ang[...])
        sinr[...] = jnp.sin(ang[...]) * jnp.where(lane1 < HD // 2, -1.0, 1.0)

        row = lax.broadcasted_iota(jnp.int32, (2 * HALF, ROWS), 0)
        col = lax.broadcasted_iota(jnp.int32, (2 * HALF, ROWS), 1)
        half_of_row = jnp.where(row < HALF, core, 1 - core)
        kv_of_row = half_of_row * 2 + lax.rem(row, HALF) // 8
        colslot[...] = jnp.where(lax.rem(col, KVH) == kv_of_row, col // KVH, 1 << 20)

    def norm_rope(x, gain):
        y = x * lax.rsqrt(jnp.mean(x * x, axis=-1, keepdims=True) + NORM_EPS) * gain
        y = y * cosr[...] + pltpu.roll(y, HD // 2, 1) * sinr[...]
        return y.astype(BF16).astype(F32)

    def post(n):
        for j in range(WCH // HD):
            x = proj[n % 2, :, j * HD:(j + 1) * HD].astype(BF16).astype(F32)
            if n < 4:
                qmine.at[n // 2][pl.ds(n % 2 * 4 + j, SEQS, stride=8), :] = norm_rope(x, qgain)
            else:
                rep.at[core][pl.ds(j, SEQS, stride=KVH), :] = jnp.where(core == 0, norm_rope(x, kgain), x)

    def multiply(n):
        w_copy(n, wk).wait()
        if n + WAHEAD < NW:
            w_start(n + WAHEAD)
        else:
            k_copy(n + WAHEAD - NW).start()
            v_copy(n + WAHEAD - NW).start()
        proj[n % 2] = jnp.dot(hid[...], w_s[n % RING], preferred_element_type=F32)

    multiply(0)
    tables()
    qgain = qn[...].astype(F32)
    kgain = kn[...].astype(F32)
    multiply(1)
    post(0)
    multiply(2)
    post(1)
    pl.semaphore_wait(barrier, 2)
    q_send(0).start()
    multiply(3)
    post(2)
    post(3)
    q_send(1).start()
    multiply(4)
    for i in range(WAHEAD, AHEAD):
        k_copy(i).start()
        v_copy(i).start()
    post(4)
    new_send().start()
    start = me * SLOTS
    lane = lax.broadcasted_iota(jnp.int32, (HALF, HD), 1)
    lrow = lax.broadcasted_iota(jnp.int32, (HALF, HD), 0)
    lane8 = lax.broadcasted_iota(jnp.int32, (BLK, HD), 1)
    for h in range(2):
        q_send(h).wait()

    def attend(i, first=False):
        ob = opart.at[i]
        def load_q(pair, at):
            bs = [at * BLK + 2 * pair + z for z in range(2)]
            return bs, [jnp.concatenate([ref[h, pl.ds(pl.multiple_of(b * 8, 8), 8), :]
                                         for ref in (qmine, qmate) for h in range(2)], axis=0) for b in bs]

        def new_rows(z, b):
            return jnp.concatenate([jnp.broadcast_to(rep[z, pl.ds(b * KVH + h, 1), :], (8, HD))
                                    for h in (2 * core, 2 * core + 1, 2 - 2 * core, 3 - 2 * core)], axis=0)

        def scores(pair, at):
            bs, qf = load_q(pair, at)
            zero = jnp.zeros((2 * HALF, HD), BF16)
            lhs = jnp.concatenate([jnp.concatenate([qf[0].astype(BF16), zero], axis=1),
                                   jnp.concatenate([zero, qf[1].astype(BF16)], axis=1)], axis=0)
            keys = jnp.concatenate([kv[bs[0]], kv[bs[1]]], axis=1)
            sc[pair % 2] = lax.dot_general(lhs, keys, (((1,), (1,)), ((), ())), preferred_element_type=F32)

        def soft(pair):
            bs, qf = load_q(pair, i)
            out = []
            for z in range(2):
                b = bs[z]
                rel = pos_s[b] - start
                owner = jnp.logical_and(rel >= 0, rel < SLOTS)
                snew = jnp.where(owner, jnp.sum(qf[z] * new_rows(0, b), axis=-1, keepdims=True), NEG)
                sm = jnp.where(colslot[...] < rel, sc[pair % 2, z * 2 * HALF:(z + 1) * 2 * HALF], NEG)
                peak = jnp.maximum(jnp.max(sm, axis=-1, keepdims=True), snew)
                safe = jnp.where(peak == NEG, 0.0, peak)
                p = jnp.exp2((sm - safe) * EXP_SCALE)
                pn = jnp.exp2((snew - safe) * EXP_SCALE)
                pr_s[pair % 2, z * 2 * HALF:(z + 1) * 2 * HALF, :] = p.astype(BF16)
                out.append((pn.astype(BF16).astype(F32), jnp.sum(p, axis=-1, keepdims=True) + pn, peak))
            return out

        def mix(pair, st3):
            bs = [i * BLK + 2 * pair + z for z in range(2)]
            values = jnp.concatenate([vv[bs[0]], vv[bs[1]]], axis=1)
            mixed = jnp.dot(pr_s[pair % 2], values, preferred_element_type=F32)
            for z in range(2):
                extra, total, peak = st3[z]
                o = mixed[z * 2 * HALF:(z + 1) * 2 * HALF, z * HD:(z + 1) * HD] + extra * new_rows(1, bs[z])
                bb = 2 * pair + z
                for h in range(2):
                    hs = slice(h * HALF, (h + 1) * HALF)
                    ob[pl.ds(h * PIECE + bb, HALF, stride=BLK), :] = o[hs]
                    st = jnp.where(lane == lrow, peak[hs], jnp.where(lane == lrow + HALF, total[hs], 0.0))
                    ob[pl.ds(h * PIECE + HALF * BLK + bb, 1), :] = jnp.sum(st, axis=0, keepdims=True)

        if first:
            scores(0, i)
            return
        for pair in range(BLK // 2):
            if pair + 1 < BLK // 2:
                scores(pair + 1, i)
            else:
                scores(0, jnp.minimum(i + 1, NBLK - 1))
            mix(pair, soft(pair))

    def combine(i, comb, at):
        s0 = opart[i, pl.ds(HALF * BLK, BLK), :]
        s1 = drx[i, pl.ds(HALF * BLK, BLK), :]
        peak = jnp.maximum(s0, s1)
        safe = jnp.where(peak == NEG, 0.0, peak)
        f0 = jnp.exp2((s0 - safe) * EXP_SCALE)
        f1 = jnp.exp2((s1 - safe) * EXP_SCALE)
        total = f0 * pltpu.roll(s0, HD - HALF, 1) + f1 * pltpu.roll(s1, HD - HALF, 1)
        comb[at, pl.ds(HALF * BLK, BLK), :] = jnp.where(
            lane8 < HALF, peak, jnp.where(lane8 < 2 * HALF, pltpu.roll(total, HALF, 1), 0.0))
        for j in range(HALF):
            rows = pl.ds(j * BLK, BLK)
            comb[at, rows, :] = bcast_col(f0, j) * opart[i, rows, :] + bcast_col(f1, j) * drx[i, rows, :]

    def fetch(i):
        @pl.when(i + 1 < NBLK)
        def _():
            k_copy(i + 1).wait()

        v_copy(i).wait()

        @pl.when(i + AHEAD < NBLK)
        def _():
            k_copy(i + AHEAD).start()
            v_copy(i + AHEAD).start()

        @pl.when(i == NBLK - 2)
        def _():
            for n in range(4):
                wo_copy(n).start()

    def early(i, carry):
        fetch(i)
        attend(i)
        d_send(i).start()
        return carry

    def sending(i, carry):
        fetch(i)
        d_send(i - LAG).wait_recv()
        combine(i - LAG, comb_a, i - LAG)
        attend(i)
        d_send(i).start()
        x_send(i - LAG).start()
        return carry

    def keeping(i, carry):
        fetch(i)
        d_send(i - LAG).wait_recv()
        combine(i - LAG, comb_b, i - LAG - NX)
        attend(i)
        d_send(i).start()
        return carry

    def late(i, carry):
        d_send(i).wait_recv()
        combine(i, comb_b, i - NX)
        return carry

    k_copy(0).wait()
    attend(0, first=True)
    new_send().wait()
    lax.fori_loop(0, LAG, early, 0)
    lax.fori_loop(LAG, LAG + NX, sending, 0)
    lax.fori_loop(LAG + NX, NBLK, keeping, 0)
    lax.fori_loop(NBLK - LAG, NBLK, late, 0)

    for n in range(4):
        wo_copy(n).wait()

    def drain(i, carry):
        d_send(i).wait_send()
        return carry

    def drain_x(i, carry):
        x_send(i).wait()
        return carry

    lax.fori_loop(0, NBLK, drain, 0)
    lax.fori_loop(0, NX, drain_x, 0)


def last_merge(chip, comb, other_ref, i, ofin, at):
    first = chip == 0

    def ordered(rows):
        mine, other = comb[i, rows, :], other_ref[i, rows, :]
        return jnp.where(first, mine, other), jnp.where(first, other, mine)

    s0, s1 = ordered(pl.ds(HALF * BLK, BLK))
    peak = jnp.maximum(s0, s1)
    f0 = jnp.exp2((s0 - peak) * EXP_SCALE)
    f1 = jnp.exp2((s1 - peak) * EXP_SCALE)
    total = f0 * pltpu.roll(s0, HD - HALF, 1) + f1 * pltpu.roll(s1, HD - HALF, 1)
    g0, g1 = f0 / total, f1 / total
    for j in range(HALF):
        a, b = ordered(pl.ds(j * BLK, BLK))
        ofin[at * BLK:(at + 1) * BLK, j * HD:(j + 1) * HD] = bcast_col(g0, j) * a + bcast_col(g1, j) * b


def block_copies(i, kv, vv, ko, vo, ksem, vsem):
    r = pl.ds(i * BLK, BLK)
    return (pltpu.make_async_copy(kv.at[r], ko.at[r], ksem.at[i]),
            pltpu.make_async_copy(vv.at[r], vo.at[r], vsem.at[i]))


def product_kernel(kv, vv, ki, vi, oa, comb_b, xrx_b, wo_v, ko, vo, part, ofin, ksem, vsem):
    block_copies(NA, kv, vv, ko, vo, ksem, vsem)[0].start()
    for i in range(NBLK - NX):
        last_merge(lax.axis_index('sp') // 2, comb_b, xrx_b, i, ofin, i)
    lhs = jnp.concatenate([oa[...].astype(BF16), ofin[...].astype(BF16)], axis=0)
    for n in range(4):
        part[:, n * WCH:(n + 1) * WCH] = jnp.dot(lhs, wo_v[n], preferred_element_type=F32)
    block_copies(NA, kv, vv, ko, vo, ksem, vsem)[0].wait()


def rest_kernel(kv, vv, ki, vi, ko, vo, ksem, vsem):
    copy = block_copies(NA, kv, vv, ko, vo, ksem, vsem)[1]
    copy.start()
    copy.wait()


def write_kernel(pos_h, kv, vv, rep, comb_a, xrx, wo_v, ko, vo, nkv, oa, kva, vva, wo_a, pos_s, nkv_s, patch, ksem, vsem, psem, osem):
    start = lax.axis_index('sp') * SLOTS
    slot16 = lax.broadcasted_iota(jnp.int32, (4 * KVH, HD), 0) // KVH

    def copies(i):
        return block_copies(i, kv, vv, ko, vo, ksem, vsem)

    pos_copy = pltpu.make_async_copy(pos_h, pos_s, osem.at[0])
    pos_copy.start()
    for c in copies(0):
        c.start()
    for b in range(SEQS):
        nkv_s[b] = jnp.concatenate([rep[0, pl.ds(b * KVH, KVH), :], rep[1, pl.ds(b * KVH, KVH), :]], axis=0).astype(BF16)
    pos_copy.wait()

    def each(i, do):
        for bb in range(BLK):
            b = i * BLK + bb
            rel = pos_s[b] - start

            @pl.when(jnp.logical_and(rel >= 0, rel < SLOTS))
            def _():
                base = pl.multiple_of(rel // 4 * (4 * KVH), 4 * KVH)
                mask = slot16 == lax.rem(rel, 4)
                for z, (ref, out) in enumerate(((kv, ko), (vv, vo))):
                    do(b, z, base, mask, ref, out)

    def merged(b, z, base, mask, ref):
        new = jnp.concatenate([rep[z, pl.ds(b * KVH, KVH), :]] * 4, axis=0)
        old = ref[b, pl.ds(base, 4 * KVH), :].astype(F32)
        return jnp.where(mask, new, old).astype(BF16)

    def put(b, z, base, mask, ref, out):
        ref[b, pl.ds(base, 4 * KVH), :] = merged(b, z, base, mask, ref)

    def stage(b, z, base, mask, ref, out):
        patch[z, b] = merged(b, z, base, mask, ref)

    def patch_copy(b, z, base, out):
        return pltpu.make_async_copy(patch.at[z, b], out.at[b, pl.ds(base, 4 * KVH)], psem.at[z, b])

    for i in range(1, NBLK):
        each(i, put)
        if 1 < i <= NA:
            for c in copies(i - 1):
                c.start()
    nkv_copy = pltpu.make_async_copy(nkv_s, nkv, osem.at[1])
    nkv_copy.start()
    each(0, stage)
    for i in range(NX):
        last_merge(lax.axis_index('sp') // 2, comb_a, xrx, i, oa, i)
    for c in copies(0):
        c.wait()
    each(0, lambda b, z, base, mask, ref, out: patch_copy(b, z, base, out).start())
    nkv_copy.wait()
    each(0, lambda b, z, base, mask, ref, out: patch_copy(b, z, base, out).wait())
    for i in range(1, NA):
        for c in copies(i):
            c.wait()


def solution(mesh):
    cache_spec = P('dp', 'sp', None, None)
    inv_freq = (np.float64(ROPE_THETA) ** (-np.arange(HD // 2) * 2.0 / HD)).astype(np.float32)
    freq2 = np.concatenate([inv_freq, inv_freq])
    vm = pl.BlockSpec(memory_space=pltpu.VMEM)
    hbm = pl.BlockSpec(memory_space=pl.ANY)
    dma = pltpu.SemaphoreType.DMA

    def device_step(tokens, positions, k_cache, v_cache, w_q, w_k, w_v, w_o, attn_norm, q_norm, k_norm):
        in_hbm = lambda x: pltpu.with_memory_space_constraint(x, pltpu.HBM)
        in_vmem = lambda x: pltpu.with_memory_space_constraint(x, pltpu.VMEM)
        rows = (SEQS, ROWS, HD)
        piece = (PIECE, HD)
        kv, vv, rep, wo_v, comb_a, comb_b, xrx_a = pl.pallas_call(
            attend_kernel,
            out_shape=(pltpu.VMEM(rows, BF16), pltpu.VMEM(rows, BF16),
                       pltpu.VMEM((2, SEQS * KVH, HD), F32), pltpu.VMEM((4, HALF * HD, WCH), BF16),
                       pltpu.VMEM((NX,) + piece, F32), pltpu.VMEM((NBLK - NX,) + piece, F32), pltpu.VMEM((NX,) + piece, F32)),
            in_specs=[hbm] * 12,
            out_specs=(vm,) * 7,
            scratch_shapes=[
                pltpu.SMEM((SEQS,), jnp.int32), pltpu.VMEM((SEQS, DIM), BF16), pltpu.VMEM((DIM // HD, HD), BF16),
                pltpu.VMEM((1, HD), BF16), pltpu.VMEM((1, HD), BF16), pltpu.VMEM((1, HD), F32), dma((6,)),
                pltpu.VMEM((2, SEQS, WCH), F32),
                pltpu.VMEM((RING, DIM, WCH), BF16),
                pltpu.VMEM((SEQS, DIM), BF16),
                pltpu.VMEM((SEQS, HD), F32), pltpu.VMEM((SEQS, HD), F32), pltpu.VMEM((SEQS, HD), F32),
                pltpu.VMEM((2, SEQS * 8, HD), F32), pltpu.VMEM((2, SEQS * 8, HD), F32),
                pltpu.VMEM((2 * HALF, ROWS), jnp.int32),
                pltpu.VMEM((NBLK, 2 * PIECE, HD), F32),
                pltpu.VMEM((NBLK,) + piece, F32),
                pltpu.VMEM((2, 4 * HALF, ROWS), F32), pltpu.VMEM((2, 4 * HALF, ROWS), BF16),
                dma((NW,)), dma((NBLK,)), dma((NBLK,)), dma((4,)), dma((3,)), dma((3,)),
                dma((NBLK,)), dma((NBLK,)), dma((NX,)), dma((NX,)),
            ],
            compiler_params=pltpu.CompilerParams(collective_id=0, has_side_effects=True, vmem_limit_bytes=VMEM_LIMIT),
            name='attend',
        )(in_hbm(positions), in_hbm(tokens), in_hbm(attn_norm.reshape(DIM // HD, HD)), in_hbm(q_norm.reshape(1, HD)),
          in_hbm(k_norm.reshape(1, HD)), in_hbm(jnp.asarray(freq2).reshape(1, HD)), in_hbm(w_q), in_hbm(w_k), in_hbm(w_v), in_hbm(w_o),
          in_hbm(k_cache.reshape(rows)), in_hbm(v_cache.reshape(rows)))
        xrx_b = lax.ppermute(comb_b, 'sp', [(0, 2), (2, 0), (1, 3), (3, 1)])
        k_out, v_out, new_kv, oa, kv, vv, wo_v = pl.pallas_call(
            write_kernel,
            out_shape=(pltpu.HBM(rows, BF16), pltpu.HBM(rows, BF16), pltpu.HBM((SEQS, 2 * KVH, HD), BF16),
                       pltpu.VMEM((NX * BLK, HALF * HD), F32), pltpu.VMEM(rows, BF16), pltpu.VMEM(rows, BF16),
                       pltpu.VMEM((4, HALF * HD, WCH), BF16)),
            in_specs=[hbm, vm, vm, vm, vm, vm, vm],
            out_specs=(hbm, hbm, hbm, vm, vm, vm, vm),
            input_output_aliases={1: 4, 2: 5, 6: 6},
            scratch_shapes=[pltpu.SMEM((SEQS,), jnp.int32), pltpu.VMEM((SEQS, 2 * KVH, HD), BF16),
                            pltpu.VMEM((2, BLK, 4 * KVH, HD), BF16),
                            dma((NBLK,)), dma((NBLK,)), dma((2, BLK)), dma((2,))],
            compiler_params=pltpu.CompilerParams(vmem_limit_bytes=VMEM_LIMIT),
            cost_estimate=pl.CostEstimate(flops=10**10, bytes_accessed=2**25, transcendentals=0),
            name='write',
        )(in_hbm(positions), in_vmem(kv), in_vmem(vv), in_vmem(rep), in_vmem(comb_a), in_vmem(xrx_a), in_vmem(wo_v))
        k_out, v_out, part = pl.pallas_call(
            product_kernel,
            out_shape=(pltpu.HBM(rows, BF16), pltpu.HBM(rows, BF16), pltpu.VMEM((SEQS, DIM), F32)),
            in_specs=[vm, vm, hbm, hbm, vm, vm, vm, vm],
            out_specs=(hbm, hbm, vm),
            input_output_aliases={2: 0, 3: 1},
            scratch_shapes=[pltpu.VMEM(((NBLK - NX) * BLK, HALF * HD), F32), dma((NBLK,)), dma((NBLK,))],
            compiler_params=pltpu.CompilerParams(vmem_limit_bytes=VMEM_LIMIT),
            cost_estimate=pl.CostEstimate(flops=2 * SEQS * DIM * DIM, bytes_accessed=2**22, transcendentals=0),
            name='product',
        )(in_vmem(kv), in_vmem(vv), k_out, v_out, in_vmem(oa), in_vmem(comb_b), in_vmem(xrx_b), in_vmem(wo_v))
        other = lax.ppermute(part, 'sp', [(0, 1), (1, 0), (2, 3), (3, 2)])
        k_out, v_out = pl.pallas_call(
            rest_kernel,
            out_shape=(pltpu.HBM(rows, BF16), pltpu.HBM(rows, BF16)),
            in_specs=[vm, vm, hbm, hbm],
            out_specs=(hbm, hbm),
            input_output_aliases={2: 0, 3: 1},
            scratch_shapes=[dma((NBLK,)), dma((NBLK,))],
            compiler_params=pltpu.CompilerParams(vmem_limit_bytes=VMEM_LIMIT),
            cost_estimate=pl.CostEstimate(flops=10**9, bytes_accessed=2**22, transcendentals=0),
            name='rest',
        )(in_vmem(kv), in_vmem(vv), k_out, v_out)
        block_out = (tokens.astype(F32) + (part + other)).astype(BF16)
        return block_out, k_out.reshape(k_cache.shape), v_out.reshape(v_cache.shape), new_kv.reshape(SEQS, 2, KVH, HD)

    return jax.shard_map(device_step, mesh=mesh, in_specs=(P('dp', None), P('dp'), cache_spec, cache_spec, P(), P(), P(), P(), P(), P(), P()), out_specs=(P('dp', None), cache_spec, cache_spec, P('dp', None, None, None)), check_vma=False)
```

```python
import functools

import jax
import jax.numpy as jnp
import numpy as np
from jax import lax
from jax.experimental import pallas as pl
from jax.experimental.pallas import tpu as pltpu
from jax.sharding import PartitionSpec as P

NORM_EPS = 1e-6
ROPE_THETA = 1000000.0
MESH = pl.DeviceIdType.MESH
BF16 = jnp.bfloat16
F32 = jnp.float32

SEQS = 64
DIM = 2048
HD = 128
KVH = 4
HALF = 16
SLOTS = 256
ROWS = SLOTS * KVH
BLK = 8
NBLK = SEQS // BLK
AHEAD = 4
NX = 3
NA = 6
NW = 5
WAHEAD = 3
RING = 4
LAG = 2
WCH = 512
PIECE = (HALF + 1) * BLK
VMEM_LIMIT = 14 * 2**20
EXP_SCALE = HD ** -0.5 * 1.4426950408889634
NEG = -jnp.inf


def bcast_col(tile, col):
    return jnp.broadcast_to(tile[:, col:col + 1], (tile.shape[0], HD))


def attend_kernel(pos_h, tok_h, an_h, qn_h, kn_h, freq_h, wq, wk, wv, wo, kc, vc,
                  kv, vv, rep, wo_v, comb_a, comb_b, xrx,
                  pos_s, tok, an, qn, kn, freq, insem, proj, w_s, hid, ang, cosr, sinr, qmine, qmate, colslot, opart, drx, sc, pr_s,
                  wsem, ksem, vsem, wosem, qs, qr, ds_, dr, xs, xr):
    me = lax.axis_index('sp')
    core = lax.rem(me, 2)
    chip = me // 2
    mate = {'sp': me + 1 - 2 * core}
    peer = {'sp': me + 2 - 4 * chip}

    def w_copy(n, src=None):
        if n < 4:
            src = wq.at[:, pl.ds(pl.multiple_of(core * (HALF * HD) + n * WCH, WCH), WCH)]
        return pltpu.make_async_copy(src, w_s.at[n % RING], wsem.at[n])

    def w_start(n):
        if n < 4:
            w_copy(n).start()
        else:
            @pl.when(core == 0)
            def _():
                w_copy(n, wk).start()

            @pl.when(core == 1)
            def _():
                w_copy(n, wv).start()

    def wo_copy(n):
        src = wo.at[pl.ds(pl.multiple_of(core * (HALF * HD), HD), HALF * HD), pl.ds(n * WCH, WCH)]
        return pltpu.make_async_copy(src, wo_v.at[n], wosem.at[n])

    def k_copy(i):
        return pltpu.make_async_copy(kc.at[pl.ds(i * BLK, BLK)], kv.at[pl.ds(i * BLK, BLK)], ksem.at[i])

    def v_copy(i):
        return pltpu.make_async_copy(vc.at[pl.ds(i * BLK, BLK)], vv.at[pl.ds(i * BLK, BLK)], vsem.at[i])

    def q_send(h):
        return pltpu.make_async_remote_copy(qmine.at[h], qmate.at[h], qs.at[h], qr.at[h], device_id=mate, device_id_type=MESH)

    def new_send():
        return pltpu.make_async_remote_copy(rep.at[core], rep.at[core], qs.at[2], qr.at[2], device_id=mate, device_id_type=MESH)

    def d_send(i):
        return pltpu.make_async_remote_copy(opart.at[i, pl.ds(PIECE, PIECE)], drx.at[i], ds_.at[i], dr.at[i],
                                            device_id=mate, device_id_type=MESH)

    def x_send(i):
        return pltpu.make_async_remote_copy(comb_a.at[i], xrx.at[i], xs.at[i], xr.at[i],
                                            device_id=peer, device_id_type=MESH)

    small = [pltpu.make_async_copy(a, b, insem.at[z]) for z, (a, b) in enumerate(
        ((tok_h, tok), (an_h, an), (pos_h, pos_s), (qn_h, qn), (kn_h, kn), (freq_h, freq)))]
    for c in small:
        c.start()
    for n in range(WAHEAD):
        w_start(n)

    barrier = pltpu.get_barrier_semaphore()
    for other in (mate, peer):
        pl.semaphore_signal(barrier, inc=1, device_id=other, device_id_type=MESH)

    small[0].wait()
    small[1].wait()
    t = tok[...].astype(F32)
    inv = lax.rsqrt(jnp.sum(t * t, axis=-1, keepdims=True) * (1.0 / DIM) + NORM_EPS)
    gains = an[...].astype(F32)
    for j in range(DIM // HD):
        sl = slice(j * HD, (j + 1) * HD)
        hid[:, sl] = (tok[:, sl].astype(F32) * inv * gains[j:j + 1, :]).astype(BF16)

    def tables():
        for c in small[2:]:
            c.wait()
        lane1 = lax.broadcasted_iota(jnp.int32, (1, HD), 1)

        def angle(b, carry):
            ang[pl.ds(b, 1), :] = freq[...] * pos_s[b].astype(F32)
            return carry

        lax.fori_loop(0, SEQS, angle, 0, unroll=8)
        cosr[...] = jnp.cos(ang[...])
        sinr[...] = jnp.sin(ang[...]) * jnp.where(lane1 < HD // 2, -1.0, 1.0)

        row = lax.broadcasted_iota(jnp.int32, (2 * HALF, ROWS), 0)
        col = lax.broadcasted_iota(jnp.int32, (2 * HALF, ROWS), 1)
        half_of_row = jnp.where(row < HALF, core, 1 - core)
        kv_of_row = half_of_row * 2 + lax.rem(row, HALF) // 8
        colslot[...] = jnp.where(lax.rem(col, KVH) == kv_of_row, col // KVH, 1 << 20)

    def norm_rope(x, gain):
        y = x * lax.rsqrt(jnp.mean(x * x, axis=-1, keepdims=True) + NORM_EPS) * gain
        y = y * cosr[...] + pltpu.roll(y, HD // 2, 1) * sinr[...]
        return y.astype(BF16).astype(F32)

    def post(n):
        for j in range(WCH // HD):
            x = proj[n % 2, :, j * HD:(j + 1) * HD].astype(BF16).astype(F32)
            if n < 4:
                qmine.at[n // 2][pl.ds(n % 2 * 4 + j, SEQS, stride=8), :] = norm_rope(x, qgain)
            else:
                rep.at[core][pl.ds(j, SEQS, stride=KVH), :] = jnp.where(core == 0, norm_rope(x, kgain), x)

    def multiply(n):
        w_copy(n, wk).wait()
        if n + WAHEAD < NW:
            w_start(n + WAHEAD)
        else:
            k_copy(n + WAHEAD - NW).start()
            v_copy(n + WAHEAD - NW).start()
        proj[n % 2] = jnp.dot(hid[...], w_s[n % RING], preferred_element_type=F32)

    multiply(0)
    tables()
    qgain = qn[...].astype(F32)
    kgain = kn[...].astype(F32)
    multiply(1)
    post(0)
    multiply(2)
    post(1)
    pl.semaphore_wait(barrier, 2)
    q_send(0).start()
    multiply(3)
    post(2)
    post(3)
    q_send(1).start()
    multiply(4)
    for i in range(WAHEAD, AHEAD):
        k_copy(i).start()
        v_copy(i).start()
    post(4)
    new_send().start()
    start = me * SLOTS
    lane = lax.broadcasted_iota(jnp.int32, (HALF, HD), 1)
    lrow = lax.broadcasted_iota(jnp.int32, (HALF, HD), 0)
    lane8 = lax.broadcasted_iota(jnp.int32, (BLK, HD), 1)
    for h in range(2):
        q_send(h).wait()

    def attend(i, first=False):
        ob = opart.at[i]
        def load_q(pair, at):
            bs = [at * BLK + 2 * pair + z for z in range(2)]
            return bs, [jnp.concatenate([ref[h, pl.ds(pl.multiple_of(b * 8, 8), 8), :]
                                         for ref in (qmine, qmate) for h in range(2)], axis=0) for b in bs]

        def new_rows(z, b):
            return jnp.concatenate([jnp.broadcast_to(rep[z, pl.ds(b * KVH + h, 1), :], (8, HD))
                                    for h in (2 * core, 2 * core + 1, 2 - 2 * core, 3 - 2 * core)], axis=0)

        def scores(pair, at):
            bs, qf = load_q(pair, at)
            zero = jnp.zeros((2 * HALF, HD), BF16)
            lhs = jnp.concatenate([jnp.concatenate([qf[0].astype(BF16), zero], axis=1),
                                   jnp.concatenate([zero, qf[1].astype(BF16)], axis=1)], axis=0)
            keys = jnp.concatenate([kv[bs[0]], kv[bs[1]]], axis=1)
            sc[pair % 2] = lax.dot_general(lhs, keys, (((1,), (1,)), ((), ())), preferred_element_type=F32)

        def soft(pair):
            bs, qf = load_q(pair, i)
            out = []
            for z in range(2):
                b = bs[z]
                rel = pos_s[b] - start
                owner = jnp.logical_and(rel >= 0, rel < SLOTS)
                snew = jnp.where(owner, jnp.sum(qf[z] * new_rows(0, b), axis=-1, keepdims=True), NEG)
                sm = jnp.where(colslot[...] < rel, sc[pair % 2, z * 2 * HALF:(z + 1) * 2 * HALF], NEG)
                peak = jnp.maximum(jnp.max(sm, axis=-1, keepdims=True), snew)
                safe = jnp.where(peak == NEG, 0.0, peak)
                p = jnp.exp2((sm - safe) * EXP_SCALE)
                pn = jnp.exp2((snew - safe) * EXP_SCALE)
                pr_s[pair % 2, z * 2 * HALF:(z + 1) * 2 * HALF, :] = p.astype(BF16)
                out.append((pn.astype(BF16).astype(F32), jnp.sum(p, axis=-1, keepdims=True) + pn, peak))
            return out

        def mix(pair, st3):
            bs = [i * BLK + 2 * pair + z for z in range(2)]
            values = jnp.concatenate([vv[bs[0]], vv[bs[1]]], axis=1)
            mixed = jnp.dot(pr_s[pair % 2], values, preferred_element_type=F32)
            for z in range(2):
                extra, total, peak = st3[z]
                o = mixed[z * 2 * HALF:(z + 1) * 2 * HALF, z * HD:(z + 1) * HD] + extra * new_rows(1, bs[z])
                bb = 2 * pair + z
                for h in range(2):
                    hs = slice(h * HALF, (h + 1) * HALF)
                    ob[pl.ds(h * PIECE + bb, HALF, stride=BLK), :] = o[hs]
                    st = jnp.where(lane == lrow, peak[hs], jnp.where(lane == lrow + HALF, total[hs], 0.0))
                    ob[pl.ds(h * PIECE + HALF * BLK + bb, 1), :] = jnp.sum(st, axis=0, keepdims=True)

        if first:
            scores(0, i)
            return
        for pair in range(BLK // 2):
            if pair + 1 < BLK // 2:
                scores(pair + 1, i)
            else:
                scores(0, jnp.minimum(i + 1, NBLK - 1))
            mix(pair, soft(pair))

    def combine(i, comb, at):
        s0 = opart[i, pl.ds(HALF * BLK, BLK), :]
        s1 = drx[i, pl.ds(HALF * BLK, BLK), :]
        peak = jnp.maximum(s0, s1)
        safe = jnp.where(peak == NEG, 0.0, peak)
        f0 = jnp.exp2((s0 - safe) * EXP_SCALE)
        f1 = jnp.exp2((s1 - safe) * EXP_SCALE)
        total = f0 * pltpu.roll(s0, HD - HALF, 1) + f1 * pltpu.roll(s1, HD - HALF, 1)
        comb[at, pl.ds(HALF * BLK, BLK), :] = jnp.where(
            lane8 < HALF, peak, jnp.where(lane8 < 2 * HALF, pltpu.roll(total, HALF, 1), 0.0))
        for j in range(HALF):
            rows = pl.ds(j * BLK, BLK)
            comb[at, rows, :] = bcast_col(f0, j) * opart[i, rows, :] + bcast_col(f1, j) * drx[i, rows, :]

    def fetch(i):
        @pl.when(i + 1 < NBLK)
        def _():
            k_copy(i + 1).wait()

        v_copy(i).wait()

        @pl.when(i + AHEAD < NBLK)
        def _():
            k_copy(i + AHEAD).start()
            v_copy(i + AHEAD).start()

        @pl.when(i + AHEAD == NBLK)
        def _():
            for n in range(4):
                wo_copy(n).start()

    def early(i, carry):
        fetch(i)
        attend(i)
        d_send(i).start()
        return carry

    def sending(i, carry):
        fetch(i)
        attend(i)
        d_send(i).start()
        d_send(i - 1).wait_recv()
        combine(i - 1, comb_a, i - 1)
        x_send(i - 1).start()
        return carry

    def keeping(i, carry):
        fetch(i)
        d_send(i - LAG).wait_recv()
        combine(i - LAG, comb_b, i - LAG - NX)
        attend(i)
        d_send(i).start()
        return carry

    def late(i, carry):
        d_send(i).wait_recv()
        combine(i, comb_b, i - NX)
        return carry

    k_copy(0).wait()
    attend(0, first=True)
    new_send().wait()
    early(0, 0)
    lax.fori_loop(1, 1 + NX, sending, 0)
    lax.fori_loop(1 + NX, LAG + NX, early, 0)
    lax.fori_loop(LAG + NX, NBLK, keeping, 0)
    lax.fori_loop(NBLK - LAG, NBLK, late, 0)

    for n in range(4):
        wo_copy(n).wait()

    def drain(i, carry):
        d_send(i).wait_send()
        return carry

    def drain_x(i, carry):
        x_send(i).wait()
        return carry

    lax.fori_loop(0, NBLK, drain, 0)
    lax.fori_loop(0, NX, drain_x, 0)


def last_merge(chip, comb, other_ref, i, ofin, at):
    first = chip == 0

    def ordered(rows):
        mine, other = comb[i, rows, :], other_ref[i, rows, :]
        return jnp.where(first, mine, other), jnp.where(first, other, mine)

    s0, s1 = ordered(pl.ds(HALF * BLK, BLK))
    peak = jnp.maximum(s0, s1)
    f0 = jnp.exp2((s0 - peak) * EXP_SCALE)
    f1 = jnp.exp2((s1 - peak) * EXP_SCALE)
    total = f0 * pltpu.roll(s0, HD - HALF, 1) + f1 * pltpu.roll(s1, HD - HALF, 1)
    g0, g1 = f0 / total, f1 / total
    for j in range(HALF):
        a, b = ordered(pl.ds(j * BLK, BLK))
        ofin[at * BLK:(at + 1) * BLK, j * HD:(j + 1) * HD] = bcast_col(g0, j) * a + bcast_col(g1, j) * b


def block_copies(i, kv, vv, ko, vo, ksem, vsem):
    r = pl.ds(i * BLK, BLK)
    return (pltpu.make_async_copy(kv.at[r], ko.at[r], ksem.at[i]),
            pltpu.make_async_copy(vv.at[r], vo.at[r], vsem.at[i]))


def product_kernel(kv, vv, ki, vi, oa, comb_b, xrx_b, wo_v, ko, vo, part, ofin, ksem, vsem):
    block_copies(NA, kv, vv, ko, vo, ksem, vsem)[1].start()
    for i in range(NBLK - NX):
        last_merge(lax.axis_index('sp') // 2, comb_b, xrx_b, i, ofin, i)
    lhs = jnp.concatenate([oa[...].astype(BF16), ofin[...].astype(BF16)], axis=0)
    for n in range(4):
        part[:, n * WCH:(n + 1) * WCH] = jnp.dot(lhs, wo_v[n], preferred_element_type=F32)
    block_copies(NA, kv, vv, ko, vo, ksem, vsem)[1].wait()


def rest_kernel(kv, vv, ki, vi, ko, vo, ksem, vsem):
    for c in block_copies(NA + 1, kv, vv, ko, vo, ksem, vsem):
        c.start()
    for c in block_copies(NA + 1, kv, vv, ko, vo, ksem, vsem):
        c.wait()


def write_kernel(pos_h, kv, vv, rep, comb_a, xrx, wo_v, ko, vo, nkv, oa, kva, vva, wo_a, pos_s, nkv_s, patch, ksem, vsem, psem, osem):
    start = lax.axis_index('sp') * SLOTS
    slot16 = lax.broadcasted_iota(jnp.int32, (4 * KVH, HD), 0) // KVH

    def copies(i):
        return block_copies(i, kv, vv, ko, vo, ksem, vsem)

    pos_copy = pltpu.make_async_copy(pos_h, pos_s, osem.at[0])
    pos_copy.start()
    for c in copies(0):
        c.start()
    for b in range(SEQS):
        nkv_s[b] = jnp.concatenate([rep[0, pl.ds(b * KVH, KVH), :], rep[1, pl.ds(b * KVH, KVH), :]], axis=0).astype(BF16)
    pos_copy.wait()

    def each(i, do):
        for bb in range(BLK):
            b = i * BLK + bb
            rel = pos_s[b] - start

            @pl.when(jnp.logical_and(rel >= 0, rel < SLOTS))
            def _():
                base = pl.multiple_of(rel // 4 * (4 * KVH), 4 * KVH)
                mask = slot16 == lax.rem(rel, 4)
                for z, (ref, out) in enumerate(((kv, ko), (vv, vo))):
                    do(b, z, base, mask, ref, out)

    def merged(b, z, base, mask, ref):
        new = jnp.concatenate([rep[z, pl.ds(b * KVH, KVH), :]] * 4, axis=0)
        old = ref[b, pl.ds(base, 4 * KVH), :].astype(F32)
        return jnp.where(mask, new, old).astype(BF16)

    def put(b, z, base, mask, ref, out):
        ref[b, pl.ds(base, 4 * KVH), :] = merged(b, z, base, mask, ref)

    def stage(b, z, base, mask, ref, out):
        patch[z, b] = merged(b, z, base, mask, ref)

    def patch_copy(b, z, base, out):
        return pltpu.make_async_copy(patch.at[z, b], out.at[b, pl.ds(base, 4 * KVH)], psem.at[z, b])

    for i in range(1, NBLK):
        each(i, put)
        if 1 < i <= NA:
            for c in copies(i - 1):
                c.start()
    copies(NA)[0].start()
    nkv_copy = pltpu.make_async_copy(nkv_s, nkv, osem.at[1])
    nkv_copy.start()
    each(0, stage)
    for i in range(NX):
        last_merge(lax.axis_index('sp') // 2, comb_a, xrx, i, oa, i)
    for c in copies(0):
        c.wait()
    each(0, lambda b, z, base, mask, ref, out: patch_copy(b, z, base, out).start())
    nkv_copy.wait()
    each(0, lambda b, z, base, mask, ref, out: patch_copy(b, z, base, out).wait())
    for i in range(1, NA):
        for c in copies(i):
            c.wait()
    copies(NA)[0].wait()


def solution(mesh):
    cache_spec = P('dp', 'sp', None, None)
    inv_freq = (np.float64(ROPE_THETA) ** (-np.arange(HD // 2) * 2.0 / HD)).astype(np.float32)
    freq2 = np.concatenate([inv_freq, inv_freq])
    vm = pl.BlockSpec(memory_space=pltpu.VMEM)
    hbm = pl.BlockSpec(memory_space=pl.ANY)
    dma = pltpu.SemaphoreType.DMA

    def device_step(tokens, positions, k_cache, v_cache, w_q, w_k, w_v, w_o, attn_norm, q_norm, k_norm):
        in_hbm = lambda x: pltpu.with_memory_space_constraint(x, pltpu.HBM)
        in_vmem = lambda x: pltpu.with_memory_space_constraint(x, pltpu.VMEM)
        rows = (SEQS, ROWS, HD)
        piece = (PIECE, HD)
        kv, vv, rep, wo_v, comb_a, comb_b, xrx_a = pl.pallas_call(
            attend_kernel,
            out_shape=(pltpu.VMEM(rows, BF16), pltpu.VMEM(rows, BF16),
                       pltpu.VMEM((2, SEQS * KVH, HD), F32), pltpu.VMEM((4, HALF * HD, WCH), BF16),
                       pltpu.VMEM((NX,) + piece, F32), pltpu.VMEM((NBLK - NX,) + piece, F32), pltpu.VMEM((NX,) + piece, F32)),
            in_specs=[hbm] * 12,
            out_specs=(vm,) * 7,
            scratch_shapes=[
                pltpu.SMEM((SEQS,), jnp.int32), pltpu.VMEM((SEQS, DIM), BF16), pltpu.VMEM((DIM // HD, HD), BF16),
                pltpu.VMEM((1, HD), BF16), pltpu.VMEM((1, HD), BF16), pltpu.VMEM((1, HD), F32), dma((6,)),
                pltpu.VMEM((2, SEQS, WCH), F32),
                pltpu.VMEM((RING, DIM, WCH), BF16),
                pltpu.VMEM((SEQS, DIM), BF16),
                pltpu.VMEM((SEQS, HD), F32), pltpu.VMEM((SEQS, HD), F32), pltpu.VMEM((SEQS, HD), F32),
                pltpu.VMEM((2, SEQS * 8, HD), F32), pltpu.VMEM((2, SEQS * 8, HD), F32),
                pltpu.VMEM((2 * HALF, ROWS), jnp.int32),
                pltpu.VMEM((NBLK, 2 * PIECE, HD), F32),
                pltpu.VMEM((NBLK,) + piece, F32),
                pltpu.VMEM((2, 4 * HALF, ROWS), F32), pltpu.VMEM((2, 4 * HALF, ROWS), BF16),
                dma((NW,)), dma((NBLK,)), dma((NBLK,)), dma((4,)), dma((3,)), dma((3,)),
                dma((NBLK,)), dma((NBLK,)), dma((NX,)), dma((NX,)),
            ],
            compiler_params=pltpu.CompilerParams(collective_id=0, has_side_effects=True, vmem_limit_bytes=VMEM_LIMIT),
            name='attend',
        )(in_hbm(positions), in_hbm(tokens), in_hbm(attn_norm.reshape(DIM // HD, HD)), in_hbm(q_norm.reshape(1, HD)),
          in_hbm(k_norm.reshape(1, HD)), in_hbm(jnp.asarray(freq2).reshape(1, HD)), in_hbm(w_q), in_hbm(w_k), in_hbm(w_v), in_hbm(w_o),
          in_hbm(k_cache.reshape(rows)), in_hbm(v_cache.reshape(rows)))
        xrx_b = lax.ppermute(comb_b, 'sp', [(0, 2), (2, 0), (1, 3), (3, 1)])
        k_out, v_out, new_kv, oa, kv, vv, wo_v = pl.pallas_call(
            write_kernel,
            out_shape=(pltpu.HBM(rows, BF16), pltpu.HBM(rows, BF16), pltpu.HBM((SEQS, 2 * KVH, HD), BF16),
                       pltpu.VMEM((NX * BLK, HALF * HD), F32), pltpu.VMEM(rows, BF16), pltpu.VMEM(rows, BF16),
                       pltpu.VMEM((4, HALF * HD, WCH), BF16)),
            in_specs=[hbm, vm, vm, vm, vm, vm, vm],
            out_specs=(hbm, hbm, hbm, vm, vm, vm, vm),
            input_output_aliases={1: 4, 2: 5, 6: 6},
            scratch_shapes=[pltpu.SMEM((SEQS,), jnp.int32), pltpu.VMEM((SEQS, 2 * KVH, HD), BF16),
                            pltpu.VMEM((2, BLK, 4 * KVH, HD), BF16),
                            dma((NBLK,)), dma((NBLK,)), dma((2, BLK)), dma((2,))],
            compiler_params=pltpu.CompilerParams(vmem_limit_bytes=VMEM_LIMIT),
            cost_estimate=pl.CostEstimate(flops=10**10, bytes_accessed=2**25, transcendentals=0),
            name='write',
        )(in_hbm(positions), in_vmem(kv), in_vmem(vv), in_vmem(rep), in_vmem(comb_a), in_vmem(xrx_a), in_vmem(wo_v))
        k_out, v_out, part = pl.pallas_call(
            product_kernel,
            out_shape=(pltpu.HBM(rows, BF16), pltpu.HBM(rows, BF16), pltpu.VMEM((SEQS, DIM), F32)),
            in_specs=[vm, vm, hbm, hbm, vm, vm, vm, vm],
            out_specs=(hbm, hbm, vm),
            input_output_aliases={2: 0, 3: 1},
            scratch_shapes=[pltpu.VMEM(((NBLK - NX) * BLK, HALF * HD), F32), dma((NBLK,)), dma((NBLK,))],
            compiler_params=pltpu.CompilerParams(vmem_limit_bytes=VMEM_LIMIT),
            cost_estimate=pl.CostEstimate(flops=2 * SEQS * DIM * DIM, bytes_accessed=2**22, transcendentals=0),
            name='product',
        )(in_vmem(kv), in_vmem(vv), k_out, v_out, in_vmem(oa), in_vmem(comb_b), in_vmem(xrx_b), in_vmem(wo_v))
        other = lax.ppermute(part, 'sp', [(0, 1), (1, 0), (2, 3), (3, 2)])
        k_out, v_out = pl.pallas_call(
            rest_kernel,
            out_shape=(pltpu.HBM(rows, BF16), pltpu.HBM(rows, BF16)),
            in_specs=[vm, vm, hbm, hbm],
            out_specs=(hbm, hbm),
            input_output_aliases={2: 0, 3: 1},
            scratch_shapes=[dma((NBLK,)), dma((NBLK,))],
            compiler_params=pltpu.CompilerParams(vmem_limit_bytes=VMEM_LIMIT),
            cost_estimate=pl.CostEstimate(flops=10**9, bytes_accessed=2**22, transcendentals=0),
            name='rest',
        )(in_vmem(kv), in_vmem(vv), k_out, v_out)
        block_out = (tokens.astype(F32) + (part + other)).astype(BF16)
        return block_out, k_out.reshape(k_cache.shape), v_out.reshape(v_cache.shape), new_kv.reshape(SEQS, 2, KVH, HD)

    return jax.shard_map(device_step, mesh=mesh, in_specs=(P('dp', None), P('dp'), cache_spec, cache_spec, P(), P(), P(), P(), P(), P(), P()), out_specs=(P('dp', None), cache_spec, cache_spec, P('dp', None, None, None)), check_vma=False)
```

```python
import functools

import jax
import jax.numpy as jnp
import numpy as np
from jax import lax
from jax.experimental import pallas as pl
from jax.experimental.pallas import tpu as pltpu
from jax.sharding import PartitionSpec as P

NORM_EPS = 1e-6
ROPE_THETA = 1000000.0
MESH = pl.DeviceIdType.MESH
BF16 = jnp.bfloat16
F32 = jnp.float32

SEQS = 64
DIM = 2048
HD = 128
KVH = 4
HALF = 16
SLOTS = 256
ROWS = SLOTS * KVH
BLK = 8
NBLK = SEQS // BLK
AHEAD = 4
NX = 3
NA = 6
WSPLIT = 2
NW = 5
WAHEAD = 3
RING = 4
LAG = 2
WCH = 512
PIECE = (HALF + 1) * BLK
VMEM_LIMIT = 14 * 2**20
EXP_SCALE = HD ** -0.5 * 1.4426950408889634
NEG = -jnp.inf


def bcast_col(tile, col):
    return jnp.broadcast_to(tile[:, col:col + 1], (tile.shape[0], HD))


def out_weight_copy(n, core, wo, wo_v, wosem):
    src = wo.at[pl.ds(pl.multiple_of(core * (HALF * HD), HD), HALF * HD), pl.ds(n * WCH, WCH)]
    return pltpu.make_async_copy(src, wo_v.at[n], wosem.at[n])


def attend_kernel(pos_h, tok_h, an_h, qn_h, kn_h, freq_h, wq, wk, wv, wo, kc, vc,
                  kv, vv, rep, wo_v, comb_a, comb_b, xrx,
                  pos_s, tok, an, qn, kn, freq, insem, proj, w_s, hid, ang, cosr, sinr, qmine, qmate, colslot, opart, drx, sc, pr_s,
                  wsem, ksem, vsem, wosem, qs, qr, ds_, dr, xs, xr):
    me = lax.axis_index('sp')
    core = lax.rem(me, 2)
    chip = me // 2
    mate = {'sp': me + 1 - 2 * core}
    peer = {'sp': me + 2 - 4 * chip}

    def w_copy(n, src=None):
        if n < 4:
            src = wq.at[:, pl.ds(pl.multiple_of(core * (HALF * HD) + n * WCH, WCH), WCH)]
        return pltpu.make_async_copy(src, w_s.at[n % RING], wsem.at[n])

    def w_start(n):
        if n < 4:
            w_copy(n).start()
        else:
            @pl.when(core == 0)
            def _():
                w_copy(n, wk).start()

            @pl.when(core == 1)
            def _():
                w_copy(n, wv).start()

    def wo_copy(n):
        return out_weight_copy(n, core, wo, wo_v, wosem)

    def k_copy(i):
        return pltpu.make_async_copy(kc.at[pl.ds(i * BLK, BLK)], kv.at[pl.ds(i * BLK, BLK)], ksem.at[i])

    def v_copy(i):
        return pltpu.make_async_copy(vc.at[pl.ds(i * BLK, BLK)], vv.at[pl.ds(i * BLK, BLK)], vsem.at[i])

    def q_send(h):
        return pltpu.make_async_remote_copy(qmine.at[h], qmate.at[h], qs.at[h], qr.at[h], device_id=mate, device_id_type=MESH)

    def new_send():
        return pltpu.make_async_remote_copy(rep.at[core], rep.at[core], qs.at[2], qr.at[2], device_id=mate, device_id_type=MESH)

    def d_send(i):
        return pltpu.make_async_remote_copy(opart.at[i, pl.ds(PIECE, PIECE)], drx.at[i], ds_.at[i], dr.at[i],
                                            device_id=mate, device_id_type=MESH)

    def x_send(i):
        return pltpu.make_async_remote_copy(comb_a.at[i], xrx.at[i], xs.at[i], xr.at[i],
                                            device_id=peer, device_id_type=MESH)

    small = [pltpu.make_async_copy(a, b, insem.at[z]) for z, (a, b) in enumerate(
        ((tok_h, tok), (an_h, an), (pos_h, pos_s), (qn_h, qn), (kn_h, kn), (freq_h, freq)))]
    for c in small:
        c.start()
    for n in range(WAHEAD):
        w_start(n)

    barrier = pltpu.get_barrier_semaphore()
    for other in (mate, peer):
        pl.semaphore_signal(barrier, inc=1, device_id=other, device_id_type=MESH)

    small[0].wait()
    small[1].wait()
    t = tok[...].astype(F32)
    inv = lax.rsqrt(jnp.sum(t * t, axis=-1, keepdims=True) * (1.0 / DIM) + NORM_EPS)
    gains = an[...].astype(F32)
    for j in range(DIM // HD):
        sl = slice(j * HD, (j + 1) * HD)
        hid[:, sl] = (tok[:, sl].astype(F32) * inv * gains[j:j + 1, :]).astype(BF16)

    def tables():
        for c in small[2:]:
            c.wait()
        lane1 = lax.broadcasted_iota(jnp.int32, (1, HD), 1)

        def angle(b, carry):
            ang[pl.ds(b, 1), :] = freq[...] * pos_s[b].astype(F32)
            return carry

        lax.fori_loop(0, SEQS, angle, 0, unroll=8)
        cosr[...] = jnp.cos(ang[...])
        sinr[...] = jnp.sin(ang[...]) * jnp.where(lane1 < HD // 2, -1.0, 1.0)

        row = lax.broadcasted_iota(jnp.int32, (2 * HALF, ROWS), 0)
        col = lax.broadcasted_iota(jnp.int32, (2 * HALF, ROWS), 1)
        half_of_row = jnp.where(row < HALF, core, 1 - core)
        kv_of_row = half_of_row * 2 + lax.rem(row, HALF) // 8
        colslot[...] = jnp.where(lax.rem(col, KVH) == kv_of_row, col // KVH, 1 << 20)

    def norm_rope(x, gain):
        y = x * lax.rsqrt(jnp.mean(x * x, axis=-1, keepdims=True) + NORM_EPS) * gain
        y = y * cosr[...] + pltpu.roll(y, HD // 2, 1) * sinr[...]
        return y.astype(BF16).astype(F32)

    def post(n):
        for j in range(WCH // HD):
            x = proj[n % 2, :, j * HD:(j + 1) * HD].astype(BF16).astype(F32)
            if n < 4:
                qmine.at[n // 2][pl.ds(n % 2 * 4 + j, SEQS, stride=8), :] = norm_rope(x, qgain)
            else:
                rep.at[core][pl.ds(j, SEQS, stride=KVH), :] = jnp.where(core == 0, norm_rope(x, kgain), x)

    def multiply(n):
        w_copy(n, wk).wait()
        if n + WAHEAD < NW:
            w_start(n + WAHEAD)
        else:
            k_copy(n + WAHEAD - NW).start()
            v_copy(n + WAHEAD - NW).start()
        proj[n % 2] = jnp.dot(hid[...], w_s[n % RING], preferred_element_type=F32)

    multiply(0)
    tables()
    qgain = qn[...].astype(F32)
    kgain = kn[...].astype(F32)
    multiply(1)
    post(0)
    multiply(2)
    post(1)
    pl.semaphore_wait(barrier, 2)
    q_send(0).start()
    multiply(3)
    post(2)
    post(3)
    q_send(1).start()
    multiply(4)
    for i in range(WAHEAD, AHEAD):
        k_copy(i).start()
        v_copy(i).start()
    post(4)
    new_send().start()
    start = me * SLOTS
    lane = lax.broadcasted_iota(jnp.int32, (HALF, HD), 1)
    lrow = lax.broadcasted_iota(jnp.int32, (HALF, HD), 0)
    lane8 = lax.broadcasted_iota(jnp.int32, (BLK, HD), 1)
    for h in range(2):
        q_send(h).wait()

    def attend(i, first=False):
        ob = opart.at[i]
        def load_q(pair, at):
            bs = [at * BLK + 2 * pair + z for z in range(2)]
            return bs, [jnp.concatenate([ref[h, pl.ds(pl.multiple_of(b * 8, 8), 8), :]
                                         for ref in (qmine, qmate) for h in range(2)], axis=0) for b in bs]

        def new_rows(z, b):
            return jnp.concatenate([jnp.broadcast_to(rep[z, pl.ds(b * KVH + h, 1), :], (8, HD))
                                    for h in (2 * core, 2 * core + 1, 2 - 2 * core, 3 - 2 * core)], axis=0)

        def scores(pair, at):
            bs, qf = load_q(pair, at)
            zero = jnp.zeros((2 * HALF, HD), BF16)
            lhs = jnp.concatenate([jnp.concatenate([qf[0].astype(BF16), zero], axis=1),
                                   jnp.concatenate([zero, qf[1].astype(BF16)], axis=1)], axis=0)
            keys = jnp.concatenate([kv[bs[0]], kv[bs[1]]], axis=1)
            sc[pair % 2] = lax.dot_general(lhs, keys, (((1,), (1,)), ((), ())), preferred_element_type=F32)

        def soft(pair):
            bs, qf = load_q(pair, i)
            out = []
            for z in range(2):
                b = bs[z]
                rel = pos_s[b] - start
                owner = jnp.logical_and(rel >= 0, rel < SLOTS)
                snew = jnp.where(owner, jnp.sum(qf[z] * new_rows(0, b), axis=-1, keepdims=True), NEG)
                sm = jnp.where(colslot[...] < rel, sc[pair % 2, z * 2 * HALF:(z + 1) * 2 * HALF], NEG)
                peak = jnp.maximum(jnp.max(sm, axis=-1, keepdims=True), snew)
                safe = jnp.where(peak == NEG, 0.0, peak)
                p = jnp.exp2((sm - safe) * EXP_SCALE)
                pn = jnp.exp2((snew - safe) * EXP_SCALE)
                pr_s[pair % 2, z * 2 * HALF:(z + 1) * 2 * HALF, :] = p.astype(BF16)
                out.append((pn.astype(BF16).astype(F32), jnp.sum(p, axis=-1, keepdims=True) + pn, peak))
            return out

        def mix(pair, st3):
            bs = [i * BLK + 2 * pair + z for z in range(2)]
            values = jnp.concatenate([vv[bs[0]], vv[bs[1]]], axis=1)
            mixed = jnp.dot(pr_s[pair % 2], values, preferred_element_type=F32)
            for z in range(2):
                extra, total, peak = st3[z]
                o = mixed[z * 2 * HALF:(z + 1) * 2 * HALF, z * HD:(z + 1) * HD] + extra * new_rows(1, bs[z])
                bb = 2 * pair + z
                for h in range(2):
                    hs = slice(h * HALF, (h + 1) * HALF)
                    ob[pl.ds(h * PIECE + bb, HALF, stride=BLK), :] = o[hs]
                    st = jnp.where(lane == lrow, peak[hs], jnp.where(lane == lrow + HALF, total[hs], 0.0))
                    ob[pl.ds(h * PIECE + HALF * BLK + bb, 1), :] = jnp.sum(st, axis=0, keepdims=True)

        if first:
            scores(0, i)
            return
        for pair in range(BLK // 2):
            if pair + 1 < BLK // 2:
                scores(pair + 1, i)
            else:
                scores(0, jnp.minimum(i + 1, NBLK - 1))
            mix(pair, soft(pair))

    def combine(i, comb, at):
        s0 = opart[i, pl.ds(HALF * BLK, BLK), :]
        s1 = drx[i, pl.ds(HALF * BLK, BLK), :]
        peak = jnp.maximum(s0, s1)
        safe = jnp.where(peak == NEG, 0.0, peak)
        f0 = jnp.exp2((s0 - safe) * EXP_SCALE)
        f1 = jnp.exp2((s1 - safe) * EXP_SCALE)
        total = f0 * pltpu.roll(s0, HD - HALF, 1) + f1 * pltpu.roll(s1, HD - HALF, 1)
        comb[at, pl.ds(HALF * BLK, BLK), :] = jnp.where(
            lane8 < HALF, peak, jnp.where(lane8 < 2 * HALF, pltpu.roll(total, HALF, 1), 0.0))
        for j in range(HALF):
            rows = pl.ds(j * BLK, BLK)
            comb[at, rows, :] = bcast_col(f0, j) * opart[i, rows, :] + bcast_col(f1, j) * drx[i, rows, :]

    def fetch(i):
        @pl.when(i + 1 < NBLK)
        def _():
            k_copy(i + 1).wait()

        v_copy(i).wait()

        @pl.when(i + AHEAD < NBLK)
        def _():
            k_copy(i + AHEAD).start()
            v_copy(i + AHEAD).start()

        @pl.when(i + AHEAD == NBLK)
        def _():
            for n in range(WSPLIT):
                wo_copy(n).start()

    def early(i, carry):
        fetch(i)
        attend(i)
        d_send(i).start()
        return carry

    def sending(i, carry):
        fetch(i)
        attend(i)
        d_send(i).start()
        d_send(i - 1).wait_recv()
        combine(i - 1, comb_a, i - 1)
        x_send(i - 1).start()
        return carry

    def keeping(i, carry):
        fetch(i)
        d_send(i - LAG).wait_recv()
        combine(i - LAG, comb_b, i - LAG - NX)
        attend(i)
        d_send(i).start()
        return carry

    def late(i, carry):
        d_send(i).wait_recv()
        combine(i, comb_b, i - NX)
        return carry

    k_copy(0).wait()
    attend(0, first=True)
    new_send().wait()
    early(0, 0)
    lax.fori_loop(1, 1 + NX, sending, 0)
    lax.fori_loop(1 + NX, LAG + NX, early, 0)
    lax.fori_loop(LAG + NX, NBLK, keeping, 0)
    lax.fori_loop(NBLK - LAG, NBLK, late, 0)

    for n in range(WSPLIT):
        wo_copy(n).wait()

    def drain(i, carry):
        d_send(i).wait_send()
        return carry

    def drain_x(i, carry):
        x_send(i).wait()
        return carry

    lax.fori_loop(0, NBLK, drain, 0)
    lax.fori_loop(0, NX, drain_x, 0)


def last_merge(chip, comb, other_ref, i, ofin, at):
    first = chip == 0

    def ordered(rows):
        mine, other = comb[i, rows, :], other_ref[i, rows, :]
        return jnp.where(first, mine, other), jnp.where(first, other, mine)

    s0, s1 = ordered(pl.ds(HALF * BLK, BLK))
    peak = jnp.maximum(s0, s1)
    f0 = jnp.exp2((s0 - peak) * EXP_SCALE)
    f1 = jnp.exp2((s1 - peak) * EXP_SCALE)
    total = f0 * pltpu.roll(s0, HD - HALF, 1) + f1 * pltpu.roll(s1, HD - HALF, 1)
    g0, g1 = f0 / total, f1 / total
    for j in range(HALF):
        a, b = ordered(pl.ds(j * BLK, BLK))
        ofin[at * BLK:(at + 1) * BLK, j * HD:(j + 1) * HD] = bcast_col(g0, j) * a + bcast_col(g1, j) * b


def block_copies(i, kv, vv, ko, vo, ksem, vsem):
    r = pl.ds(i * BLK, BLK)
    return (pltpu.make_async_copy(kv.at[r], ko.at[r], ksem.at[i]),
            pltpu.make_async_copy(vv.at[r], vo.at[r], vsem.at[i]))


def product_kernel(kv, vv, ki, vi, oa, comb_b, xrx_b, wo_v, ko, vo, part, ofin, ksem, vsem):
    for c in block_copies(NA, kv, vv, ko, vo, ksem, vsem):
        c.start()
    for i in range(NBLK - NX):
        last_merge(lax.axis_index('sp') // 2, comb_b, xrx_b, i, ofin, i)
    lhs = jnp.concatenate([oa[...].astype(BF16), ofin[...].astype(BF16)], axis=0)
    for n in range(4):
        part[:, n * WCH:(n + 1) * WCH] = jnp.dot(lhs, wo_v[n], preferred_element_type=F32)
    for c in block_copies(NA, kv, vv, ko, vo, ksem, vsem):
        c.wait()


def rest_kernel(kv, vv, ki, vi, ko, vo, ksem, vsem):
    for c in block_copies(NA + 1, kv, vv, ko, vo, ksem, vsem):
        c.start()
    for c in block_copies(NA + 1, kv, vv, ko, vo, ksem, vsem):
        c.wait()


def write_kernel(pos_h, kv, vv, rep, comb_a, xrx, wo_v, wo, ko, vo, nkv, oa, kva, vva, wo_a, pos_s, nkv_s, patch, ksem, vsem, psem, osem, wosem):
    start = lax.axis_index('sp') * SLOTS
    slot16 = lax.broadcasted_iota(jnp.int32, (4 * KVH, HD), 0) // KVH

    def copies(i):
        return block_copies(i, kv, vv, ko, vo, ksem, vsem)

    pos_copy = pltpu.make_async_copy(pos_h, pos_s, osem.at[0])
    pos_copy.start()
    for c in copies(0):
        c.start()
    for b in range(SEQS):
        nkv_s[b] = jnp.concatenate([rep[0, pl.ds(b * KVH, KVH), :], rep[1, pl.ds(b * KVH, KVH), :]], axis=0).astype(BF16)
    pos_copy.wait()

    def each(i, do):
        for bb in range(BLK):
            b = i * BLK + bb
            rel = pos_s[b] - start

            @pl.when(jnp.logical_and(rel >= 0, rel < SLOTS))
            def _():
                base = pl.multiple_of(rel // 4 * (4 * KVH), 4 * KVH)
                mask = slot16 == lax.rem(rel, 4)
                for z, (ref, out) in enumerate(((kv, ko), (vv, vo))):
                    do(b, z, base, mask, ref, out)

    def merged(b, z, base, mask, ref):
        new = jnp.concatenate([rep[z, pl.ds(b * KVH, KVH), :]] * 4, axis=0)
        old = ref[b, pl.ds(base, 4 * KVH), :].astype(F32)
        return jnp.where(mask, new, old).astype(BF16)

    def put(b, z, base, mask, ref, out):
        ref[b, pl.ds(base, 4 * KVH), :] = merged(b, z, base, mask, ref)

    def stage(b, z, base, mask, ref, out):
        patch[z, b] = merged(b, z, base, mask, ref)

    def patch_copy(b, z, base, out):
        return pltpu.make_async_copy(patch.at[z, b], out.at[b, pl.ds(base, 4 * KVH)], psem.at[z, b])

    for i in range(1, NBLK):
        each(i, put)
        if 1 < i <= NA:
            for c in copies(i - 1):
                c.start()
    core = lax.rem(lax.axis_index('sp'), 2)
    for n in range(WSPLIT, 4):
        out_weight_copy(n, core, wo, wo_v, wosem).start()
    nkv_copy = pltpu.make_async_copy(nkv_s, nkv, osem.at[1])
    nkv_copy.start()
    each(0, stage)
    for i in range(NX):
        last_merge(lax.axis_index('sp') // 2, comb_a, xrx, i, oa, i)
    for c in copies(0):
        c.wait()
    each(0, lambda b, z, base, mask, ref, out: patch_copy(b, z, base, out).start())
    nkv_copy.wait()
    each(0, lambda b, z, base, mask, ref, out: patch_copy(b, z, base, out).wait())
    for i in range(1, NA):
        for c in copies(i):
            c.wait()
    for n in range(WSPLIT, 4):
        out_weight_copy(n, core, wo, wo_v, wosem).wait()


def solution(mesh):
    cache_spec = P('dp', 'sp', None, None)
    inv_freq = (np.float64(ROPE_THETA) ** (-np.arange(HD // 2) * 2.0 / HD)).astype(np.float32)
    freq2 = np.concatenate([inv_freq, inv_freq])
    vm = pl.BlockSpec(memory_space=pltpu.VMEM)
    hbm = pl.BlockSpec(memory_space=pl.ANY)
    dma = pltpu.SemaphoreType.DMA

    def device_step(tokens, positions, k_cache, v_cache, w_q, w_k, w_v, w_o, attn_norm, q_norm, k_norm):
        in_hbm = lambda x: pltpu.with_memory_space_constraint(x, pltpu.HBM)
        in_vmem = lambda x: pltpu.with_memory_space_constraint(x, pltpu.VMEM)
        rows = (SEQS, ROWS, HD)
        piece = (PIECE, HD)
        kv, vv, rep, wo_v, comb_a, comb_b, xrx_a = pl.pallas_call(
            attend_kernel,
            out_shape=(pltpu.VMEM(rows, BF16), pltpu.VMEM(rows, BF16),
                       pltpu.VMEM((2, SEQS * KVH, HD), F32), pltpu.VMEM((4, HALF * HD, WCH), BF16),
                       pltpu.VMEM((NX,) + piece, F32), pltpu.VMEM((NBLK - NX,) + piece, F32), pltpu.VMEM((NX,) + piece, F32)),
            in_specs=[hbm] * 12,
            out_specs=(vm,) * 7,
            scratch_shapes=[
                pltpu.SMEM((SEQS,), jnp.int32), pltpu.VMEM((SEQS, DIM), BF16), pltpu.VMEM((DIM // HD, HD), BF16),
                pltpu.VMEM((1, HD), BF16), pltpu.VMEM((1, HD), BF16), pltpu.VMEM((1, HD), F32), dma((6,)),
                pltpu.VMEM((2, SEQS, WCH), F32),
                pltpu.VMEM((RING, DIM, WCH), BF16),
                pltpu.VMEM((SEQS, DIM), BF16),
                pltpu.VMEM((SEQS, HD), F32), pltpu.VMEM((SEQS, HD), F32), pltpu.VMEM((SEQS, HD), F32),
                pltpu.VMEM((2, SEQS * 8, HD), F32), pltpu.VMEM((2, SEQS * 8, HD), F32),
                pltpu.VMEM((2 * HALF, ROWS), jnp.int32),
                pltpu.VMEM((NBLK, 2 * PIECE, HD), F32),
                pltpu.VMEM((NBLK,) + piece, F32),
                pltpu.VMEM((2, 4 * HALF, ROWS), F32), pltpu.VMEM((2, 4 * HALF, ROWS), BF16),
                dma((NW,)), dma((NBLK,)), dma((NBLK,)), dma((4,)), dma((3,)), dma((3,)),
                dma((NBLK,)), dma((NBLK,)), dma((NX,)), dma((NX,)),
            ],
            compiler_params=pltpu.CompilerParams(collective_id=0, has_side_effects=True, vmem_limit_bytes=VMEM_LIMIT),
            name='attend',
        )(in_hbm(positions), in_hbm(tokens), in_hbm(attn_norm.reshape(DIM // HD, HD)), in_hbm(q_norm.reshape(1, HD)),
          in_hbm(k_norm.reshape(1, HD)), in_hbm(jnp.asarray(freq2).reshape(1, HD)), in_hbm(w_q), in_hbm(w_k), in_hbm(w_v), in_hbm(w_o),
          in_hbm(k_cache.reshape(rows)), in_hbm(v_cache.reshape(rows)))
        xrx_b = lax.ppermute(comb_b, 'sp', [(0, 2), (2, 0), (1, 3), (3, 1)])
        k_out, v_out, new_kv, oa, kv, vv, wo_v = pl.pallas_call(
            write_kernel,
            out_shape=(pltpu.HBM(rows, BF16), pltpu.HBM(rows, BF16), pltpu.HBM((SEQS, 2 * KVH, HD), BF16),
                       pltpu.VMEM((NX * BLK, HALF * HD), F32), pltpu.VMEM(rows, BF16), pltpu.VMEM(rows, BF16),
                       pltpu.VMEM((4, HALF * HD, WCH), BF16)),
            in_specs=[hbm, vm, vm, vm, vm, vm, vm, hbm],
            out_specs=(hbm, hbm, hbm, vm, vm, vm, vm),
            input_output_aliases={1: 4, 2: 5, 6: 6},
            scratch_shapes=[pltpu.SMEM((SEQS,), jnp.int32), pltpu.VMEM((SEQS, 2 * KVH, HD), BF16),
                            pltpu.VMEM((2, BLK, 4 * KVH, HD), BF16),
                            dma((NBLK,)), dma((NBLK,)), dma((2, BLK)), dma((2,)), dma((4,))],
            compiler_params=pltpu.CompilerParams(vmem_limit_bytes=VMEM_LIMIT),
            cost_estimate=pl.CostEstimate(flops=10**10, bytes_accessed=2**25, transcendentals=0),
            name='write',
        )(in_hbm(positions), in_vmem(kv), in_vmem(vv), in_vmem(rep), in_vmem(comb_a), in_vmem(xrx_a), in_vmem(wo_v), in_hbm(w_o))
        k_out, v_out, part = pl.pallas_call(
            product_kernel,
            out_shape=(pltpu.HBM(rows, BF16), pltpu.HBM(rows, BF16), pltpu.VMEM((SEQS, DIM), F32)),
            in_specs=[vm, vm, hbm, hbm, vm, vm, vm, vm],
            out_specs=(hbm, hbm, vm),
            input_output_aliases={2: 0, 3: 1},
            scratch_shapes=[pltpu.VMEM(((NBLK - NX) * BLK, HALF * HD), F32), dma((NBLK,)), dma((NBLK,))],
            compiler_params=pltpu.CompilerParams(vmem_limit_bytes=VMEM_LIMIT),
            cost_estimate=pl.CostEstimate(flops=2 * SEQS * DIM * DIM, bytes_accessed=2**22, transcendentals=0),
            name='product',
        )(in_vmem(kv), in_vmem(vv), k_out, v_out, in_vmem(oa), in_vmem(comb_b), in_vmem(xrx_b), in_vmem(wo_v))
        other = lax.ppermute(part, 'sp', [(0, 1), (1, 0), (2, 3), (3, 2)])
        k_out, v_out = pl.pallas_call(
            rest_kernel,
            out_shape=(pltpu.HBM(rows, BF16), pltpu.HBM(rows, BF16)),
            in_specs=[vm, vm, hbm, hbm],
            out_specs=(hbm, hbm),
            input_output_aliases={2: 0, 3: 1},
            scratch_shapes=[dma((NBLK,)), dma((NBLK,))],
            compiler_params=pltpu.CompilerParams(vmem_limit_bytes=VMEM_LIMIT),
            cost_estimate=pl.CostEstimate(flops=10**9, bytes_accessed=2**22, transcendentals=0),
            name='rest',
        )(in_vmem(kv), in_vmem(vv), k_out, v_out)
        block_out = (tokens.astype(F32) + (part + other)).astype(BF16)
        return block_out, k_out.reshape(k_cache.shape), v_out.reshape(v_cache.shape), new_kv.reshape(SEQS, 2, KVH, HD)

    return jax.shard_map(device_step, mesh=mesh, in_specs=(P('dp', None), P('dp'), cache_spec, cache_spec, P(), P(), P(), P(), P(), P(), P()), out_specs=(P('dp', None), cache_spec, cache_spec, P('dp', None, None, None)), check_vma=False)
```

```python
import functools

import jax
import jax.numpy as jnp
import numpy as np
from jax import lax
from jax.experimental import pallas as pl
from jax.experimental.pallas import tpu as pltpu
from jax.sharding import PartitionSpec as P

NORM_EPS = 1e-6
ROPE_THETA = 1000000.0
MESH = pl.DeviceIdType.MESH
BF16 = jnp.bfloat16
F32 = jnp.float32

SEQS = 64
DIM = 2048
HD = 128
KVH = 4
HALF = 16
SLOTS = 256
ROWS = SLOTS * KVH
BLK = 8
NBLK = SEQS // BLK
AHEAD = 4
NX = 4
NA = 6
WSPLIT = 4
NW = 5
WAHEAD = 3
RING = 4
LAG = 2
WCH = 512
PIECE = (HALF + 1) * BLK
VMEM_LIMIT = 14 * 2**20
EXP_SCALE = HD ** -0.5 * 1.4426950408889634
NEG = -jnp.inf


def bcast_col(tile, col):
    return jnp.broadcast_to(tile[:, col:col + 1], (tile.shape[0], HD))


def out_weight_copy(n, core, wo, wo_v, wosem):
    src = wo.at[pl.ds(pl.multiple_of(core * (HALF * HD), HD), HALF * HD), pl.ds(n * WCH, WCH)]
    return pltpu.make_async_copy(src, wo_v.at[n], wosem.at[n])


def attend_kernel(pos_h, tok_h, an_h, qn_h, kn_h, freq_h, wq, wk, wv, wo, kc, vc,
                  kv, vv, rep, wo_v, comb_a, comb_b, xrx,
                  pos_s, tok, an, qn, kn, freq, insem, proj, w_s, hid, ang, cosr, sinr, qmine, qmate, colslot, opart, drx, sc, pr_s,
                  wsem, ksem, vsem, wosem, qs, qr, ds_, dr, xs, xr):
    me = lax.axis_index('sp')
    core = lax.rem(me, 2)
    chip = me // 2
    mate = {'sp': me + 1 - 2 * core}
    peer = {'sp': me + 2 - 4 * chip}

    def w_copy(n, src=None):
        if n < 4:
            src = wq.at[:, pl.ds(pl.multiple_of(core * (HALF * HD) + n * WCH, WCH), WCH)]
        return pltpu.make_async_copy(src, w_s.at[n % RING], wsem.at[n])

    def w_start(n):
        if n < 4:
            w_copy(n).start()
        else:
            @pl.when(core == 0)
            def _():
                w_copy(n, wk).start()

            @pl.when(core == 1)
            def _():
                w_copy(n, wv).start()

    def wo_copy(n):
        return out_weight_copy(n, core, wo, wo_v, wosem)

    def k_copy(i):
        return pltpu.make_async_copy(kc.at[pl.ds(i * BLK, BLK)], kv.at[pl.ds(i * BLK, BLK)], ksem.at[i])

    def v_copy(i):
        return pltpu.make_async_copy(vc.at[pl.ds(i * BLK, BLK)], vv.at[pl.ds(i * BLK, BLK)], vsem.at[i])

    def q_send(h):
        return pltpu.make_async_remote_copy(qmine.at[h], qmate.at[h], qs.at[h], qr.at[h], device_id=mate, device_id_type=MESH)

    def new_send():
        return pltpu.make_async_remote_copy(rep.at[core], rep.at[core], qs.at[2], qr.at[2], device_id=mate, device_id_type=MESH)

    def d_send(i):
        return pltpu.make_async_remote_copy(opart.at[i, pl.ds(PIECE, PIECE)], drx.at[i], ds_.at[i], dr.at[i],
                                            device_id=mate, device_id_type=MESH)

    def x_send(i):
        return pltpu.make_async_remote_copy(comb_a.at[i], xrx.at[i], xs.at[i], xr.at[i],
                                            device_id=peer, device_id_type=MESH)

    small = [pltpu.make_async_copy(a, b, insem.at[z]) for z, (a, b) in enumerate(
        ((tok_h, tok), (an_h, an), (pos_h, pos_s), (qn_h, qn), (kn_h, kn), (freq_h, freq)))]
    for c in small:
        c.start()
    for n in range(WAHEAD):
        w_start(n)

    barrier = pltpu.get_barrier_semaphore()
    for other in (mate, peer):
        pl.semaphore_signal(barrier, inc=1, device_id=other, device_id_type=MESH)

    small[0].wait()
    small[1].wait()
    t = tok[...].astype(F32)
    inv = lax.rsqrt(jnp.sum(t * t, axis=-1, keepdims=True) * (1.0 / DIM) + NORM_EPS)
    gains = an[...].astype(F32)
    for j in range(DIM // HD):
        sl = slice(j * HD, (j + 1) * HD)
        hid[:, sl] = (tok[:, sl].astype(F32) * inv * gains[j:j + 1, :]).astype(BF16)

    def tables():
        for c in small[2:]:
            c.wait()
        lane1 = lax.broadcasted_iota(jnp.int32, (1, HD), 1)

        def angle(b, carry):
            ang[pl.ds(b, 1), :] = freq[...] * pos_s[b].astype(F32)
            return carry

        lax.fori_loop(0, SEQS, angle, 0, unroll=8)
        cosr[...] = jnp.cos(ang[...])
        sinr[...] = jnp.sin(ang[...]) * jnp.where(lane1 < HD // 2, -1.0, 1.0)

        row = lax.broadcasted_iota(jnp.int32, (2 * HALF, ROWS), 0)
        col = lax.broadcasted_iota(jnp.int32, (2 * HALF, ROWS), 1)
        half_of_row = jnp.where(row < HALF, core, 1 - core)
        kv_of_row = half_of_row * 2 + lax.rem(row, HALF) // 8
        colslot[...] = jnp.where(lax.rem(col, KVH) == kv_of_row, col // KVH, 1 << 20)

    def norm_rope(x, gain):
        y = x * lax.rsqrt(jnp.mean(x * x, axis=-1, keepdims=True) + NORM_EPS) * gain
        y = y * cosr[...] + pltpu.roll(y, HD // 2, 1) * sinr[...]
        return y.astype(BF16).astype(F32)

    def post(n):
        for j in range(WCH // HD):
            x = proj[n % 2, :, j * HD:(j + 1) * HD].astype(BF16).astype(F32)
            if n < 4:
                qmine.at[n // 2][pl.ds(n % 2 * 4 + j, SEQS, stride=8), :] = norm_rope(x, qgain)
            else:
                rep.at[core][pl.ds(j, SEQS, stride=KVH), :] = jnp.where(core == 0, norm_rope(x, kgain), x)

    def cache_start(t):
        (v_copy if t % 2 else k_copy)(t // 2).start()

    def multiply(n):
        w_copy(n, wk).wait()
        if n + WAHEAD < NW:
            w_start(n + WAHEAD)
        else:
            cache_start(n + WAHEAD - NW)
        proj[n % 2] = jnp.dot(hid[...], w_s[n % RING], preferred_element_type=F32)

    multiply(0)
    tables()
    qgain = qn[...].astype(F32)
    kgain = kn[...].astype(F32)
    multiply(1)
    post(0)
    multiply(2)
    post(1)
    pl.semaphore_wait(barrier, 2)
    q_send(0).start()
    multiply(3)
    post(2)
    post(3)
    q_send(1).start()
    multiply(4)
    cache_start(WAHEAD)
    cache_start(WAHEAD + 1)
    post(4)
    new_send().start()
    for t in range(WAHEAD + 2, 2 * AHEAD):
        cache_start(t)
    start = me * SLOTS
    lane = lax.broadcasted_iota(jnp.int32, (HALF, HD), 1)
    lrow = lax.broadcasted_iota(jnp.int32, (HALF, HD), 0)
    lane8 = lax.broadcasted_iota(jnp.int32, (BLK, HD), 1)
    for h in range(2):
        q_send(h).wait()

    def attend(i, first=False):
        ob = opart.at[i]
        def load_q(pair, at):
            bs = [at * BLK + 2 * pair + z for z in range(2)]
            return bs, [jnp.concatenate([ref[h, pl.ds(pl.multiple_of(b * 8, 8), 8), :]
                                         for ref in (qmine, qmate) for h in range(2)], axis=0) for b in bs]

        def new_rows(z, b):
            return jnp.concatenate([jnp.broadcast_to(rep[z, pl.ds(b * KVH + h, 1), :], (8, HD))
                                    for h in (2 * core, 2 * core + 1, 2 - 2 * core, 3 - 2 * core)], axis=0)

        def scores(pair, at):
            bs, qf = load_q(pair, at)
            zero = jnp.zeros((2 * HALF, HD), BF16)
            lhs = jnp.concatenate([jnp.concatenate([qf[0].astype(BF16), zero], axis=1),
                                   jnp.concatenate([zero, qf[1].astype(BF16)], axis=1)], axis=0)
            keys = jnp.concatenate([kv[bs[0]], kv[bs[1]]], axis=1)
            sc[pair % 2] = lax.dot_general(lhs, keys, (((1,), (1,)), ((), ())), preferred_element_type=F32)

        def soft(pair):
            bs, qf = load_q(pair, i)
            out = []
            for z in range(2):
                b = bs[z]
                rel = pos_s[b] - start
                owner = jnp.logical_and(rel >= 0, rel < SLOTS)
                snew = jnp.where(owner, jnp.sum(qf[z] * new_rows(0, b), axis=-1, keepdims=True), NEG)
                sm = jnp.where(colslot[...] < rel, sc[pair % 2, z * 2 * HALF:(z + 1) * 2 * HALF], NEG)
                peak = jnp.maximum(jnp.max(sm, axis=-1, keepdims=True), snew)
                safe = jnp.where(peak == NEG, 0.0, peak)
                p = jnp.exp2((sm - safe) * EXP_SCALE)
                pn = jnp.exp2((snew - safe) * EXP_SCALE)
                pr_s[pair % 2, z * 2 * HALF:(z + 1) * 2 * HALF, :] = p.astype(BF16)
                out.append((pn.astype(BF16).astype(F32), jnp.sum(p, axis=-1, keepdims=True) + pn, peak))
            return out

        def mix(pair, st3):
            bs = [i * BLK + 2 * pair + z for z in range(2)]
            values = jnp.concatenate([vv[bs[0]], vv[bs[1]]], axis=1)
            mixed = jnp.dot(pr_s[pair % 2], values, preferred_element_type=F32)
            for z in range(2):
                extra, total, peak = st3[z]
                o = mixed[z * 2 * HALF:(z + 1) * 2 * HALF, z * HD:(z + 1) * HD] + extra * new_rows(1, bs[z])
                bb = 2 * pair + z
                for h in range(2):
                    hs = slice(h * HALF, (h + 1) * HALF)
                    ob[pl.ds(h * PIECE + bb, HALF, stride=BLK), :] = o[hs]
                    st = jnp.where(lane == lrow, peak[hs], jnp.where(lane == lrow + HALF, total[hs], 0.0))
                    ob[pl.ds(h * PIECE + HALF * BLK + bb, 1), :] = jnp.sum(st, axis=0, keepdims=True)

        if first:
            scores(0, i)
            return
        for pair in range(BLK // 2):
            if pair + 1 < BLK // 2:
                scores(pair + 1, i)
            else:
                scores(0, jnp.minimum(i + 1, NBLK - 1))
            mix(pair, soft(pair))

    def combine(i, comb, at):
        s0 = opart[i, pl.ds(HALF * BLK, BLK), :]
        s1 = drx[i, pl.ds(HALF * BLK, BLK), :]
        peak = jnp.maximum(s0, s1)
        safe = jnp.where(peak == NEG, 0.0, peak)
        f0 = jnp.exp2((s0 - safe) * EXP_SCALE)
        f1 = jnp.exp2((s1 - safe) * EXP_SCALE)
        total = f0 * pltpu.roll(s0, HD - HALF, 1) + f1 * pltpu.roll(s1, HD - HALF, 1)
        comb[at, pl.ds(HALF * BLK, BLK), :] = jnp.where(
            lane8 < HALF, peak, jnp.where(lane8 < 2 * HALF, pltpu.roll(total, HALF, 1), 0.0))
        for j in range(HALF):
            rows = pl.ds(j * BLK, BLK)
            comb[at, rows, :] = bcast_col(f0, j) * opart[i, rows, :] + bcast_col(f1, j) * drx[i, rows, :]

    def fetch(i):
        @pl.when(i + 1 < NBLK)
        def _():
            k_copy(i + 1).wait()

        v_copy(i).wait()

        @pl.when(i + AHEAD < NBLK)
        def _():
            k_copy(i + AHEAD).start()
            v_copy(i + AHEAD).start()

        @pl.when(i + AHEAD == NBLK)
        def _():
            for n in range(WSPLIT):
                wo_copy(n).start()

    def early(i, carry):
        fetch(i)
        attend(i)
        d_send(i).start()
        return carry

    def sending(i, carry):
        fetch(i)
        attend(i)
        d_send(i).start()
        d_send(i - 1).wait_recv()
        combine(i - 1, comb_a, i - 1)
        x_send(i - 1).start()
        return carry

    def keeping(i, carry):
        fetch(i)
        d_send(i - LAG).wait_recv()
        combine(i - LAG, comb_b, i - LAG - NX)
        attend(i)
        d_send(i).start()
        return carry

    def late(i, carry):
        d_send(i).wait_recv()
        combine(i, comb_b, i - NX)
        return carry

    k_copy(0).wait()
    attend(0, first=True)
    new_send().wait()
    early(0, 0)
    lax.fori_loop(1, 1 + NX, sending, 0)
    lax.fori_loop(1 + NX, LAG + NX, early, 0)
    lax.fori_loop(LAG + NX, NBLK, keeping, 0)
    lax.fori_loop(NBLK - LAG, NBLK, late, 0)

    for n in range(WSPLIT):
        wo_copy(n).wait()

    def drain(i, carry):
        d_send(i).wait_send()
        return carry

    def drain_x(i, carry):
        x_send(i).wait()
        return carry

    lax.fori_loop(0, NBLK, drain, 0)
    lax.fori_loop(0, NX, drain_x, 0)


def last_merge(chip, comb, other_ref, i, ofin, at):
    first = chip == 0

    def ordered(rows):
        mine, other = comb[i, rows, :], other_ref[i, rows, :]
        return jnp.where(first, mine, other), jnp.where(first, other, mine)

    s0, s1 = ordered(pl.ds(HALF * BLK, BLK))
    peak = jnp.maximum(s0, s1)
    f0 = jnp.exp2((s0 - peak) * EXP_SCALE)
    f1 = jnp.exp2((s1 - peak) * EXP_SCALE)
    total = f0 * pltpu.roll(s0, HD - HALF, 1) + f1 * pltpu.roll(s1, HD - HALF, 1)
    g0, g1 = f0 / total, f1 / total
    for j in range(HALF):
        a, b = ordered(pl.ds(j * BLK, BLK))
        ofin[at * BLK:(at + 1) * BLK, j * HD:(j + 1) * HD] = bcast_col(g0, j) * a + bcast_col(g1, j) * b


def block_copies(i, kv, vv, ko, vo, ksem, vsem):
    r = pl.ds(i * BLK, BLK)
    return (pltpu.make_async_copy(kv.at[r], ko.at[r], ksem.at[i]),
            pltpu.make_async_copy(vv.at[r], vo.at[r], vsem.at[i]))


def product_kernel(kv, vv, ki, vi, oa, comb_b, xrx_b, wo_v, ko, vo, part, ofin, ksem, vsem):
    for c in block_copies(NA, kv, vv, ko, vo, ksem, vsem):
        c.start()
    for i in range(NBLK - NX):
        last_merge(lax.axis_index('sp') // 2, comb_b, xrx_b, i, ofin, i)
    lhs = jnp.concatenate([oa[...].astype(BF16), ofin[...].astype(BF16)], axis=0)
    for n in range(4):
        part[:, n * WCH:(n + 1) * WCH] = jnp.dot(lhs, wo_v[n], preferred_element_type=F32)
    for c in block_copies(NA, kv, vv, ko, vo, ksem, vsem):
        c.wait()


def rest_kernel(kv, vv, ki, vi, ko, vo, ksem, vsem):
    for c in block_copies(NA + 1, kv, vv, ko, vo, ksem, vsem):
        c.start()
    for c in block_copies(NA + 1, kv, vv, ko, vo, ksem, vsem):
        c.wait()


def write_kernel(pos_h, kv, vv, rep, comb_a, xrx, wo_v, wo, ko, vo, nkv, oa, kva, vva, wo_a, pos_s, nkv_s, patch, ksem, vsem, psem, osem, wosem):
    start = lax.axis_index('sp') * SLOTS
    slot16 = lax.broadcasted_iota(jnp.int32, (4 * KVH, HD), 0) // KVH

    def copies(i):
        return block_copies(i, kv, vv, ko, vo, ksem, vsem)

    pos_copy = pltpu.make_async_copy(pos_h, pos_s, osem.at[0])
    pos_copy.start()
    for c in copies(0):
        c.start()
    for b in range(SEQS):
        nkv_s[b] = jnp.concatenate([rep[0, pl.ds(b * KVH, KVH), :], rep[1, pl.ds(b * KVH, KVH), :]], axis=0).astype(BF16)
    pos_copy.wait()

    def each(i, do):
        for bb in range(BLK):
            b = i * BLK + bb
            rel = pos_s[b] - start

            @pl.when(jnp.logical_and(rel >= 0, rel < SLOTS))
            def _():
                base = pl.multiple_of(rel // 4 * (4 * KVH), 4 * KVH)
                mask = slot16 == lax.rem(rel, 4)
                for z, (ref, out) in enumerate(((kv, ko), (vv, vo))):
                    do(b, z, base, mask, ref, out)

    def merged(b, z, base, mask, ref):
        new = jnp.concatenate([rep[z, pl.ds(b * KVH, KVH), :]] * 4, axis=0)
        old = ref[b, pl.ds(base, 4 * KVH), :].astype(F32)
        return jnp.where(mask, new, old).astype(BF16)

    def put(b, z, base, mask, ref, out):
        ref[b, pl.ds(base, 4 * KVH), :] = merged(b, z, base, mask, ref)

    def stage(b, z, base, mask, ref, out):
        patch[z, b] = merged(b, z, base, mask, ref)

    def patch_copy(b, z, base, out):
        return pltpu.make_async_copy(patch.at[z, b], out.at[b, pl.ds(base, 4 * KVH)], psem.at[z, b])

    for i in range(1, NBLK):
        each(i, put)
        if 1 < i <= NA:
            for c in copies(i - 1):
                c.start()
    core = lax.rem(lax.axis_index('sp'), 2)
    for n in range(WSPLIT, 4):
        out_weight_copy(n, core, wo, wo_v, wosem).start()
    nkv_copy = pltpu.make_async_copy(nkv_s, nkv, osem.at[1])
    nkv_copy.start()
    each(0, stage)
    for i in range(NX):
        last_merge(lax.axis_index('sp') // 2, comb_a, xrx, i, oa, i)
    for c in copies(0):
        c.wait()
    each(0, lambda b, z, base, mask, ref, out: patch_copy(b, z, base, out).start())
    nkv_copy.wait()
    each(0, lambda b, z, base, mask, ref, out: patch_copy(b, z, base, out).wait())
    for i in range(1, NA):
        for c in copies(i):
            c.wait()
    for n in range(WSPLIT, 4):
        out_weight_copy(n, core, wo, wo_v, wosem).wait()


def solution(mesh):
    cache_spec = P('dp', 'sp', None, None)
    inv_freq = (np.float64(ROPE_THETA) ** (-np.arange(HD // 2) * 2.0 / HD)).astype(np.float32)
    freq2 = np.concatenate([inv_freq, inv_freq])
    vm = pl.BlockSpec(memory_space=pltpu.VMEM)
    hbm = pl.BlockSpec(memory_space=pl.ANY)
    dma = pltpu.SemaphoreType.DMA

    def device_step(tokens, positions, k_cache, v_cache, w_q, w_k, w_v, w_o, attn_norm, q_norm, k_norm):
        in_hbm = lambda x: pltpu.with_memory_space_constraint(x, pltpu.HBM)
        in_vmem = lambda x: pltpu.with_memory_space_constraint(x, pltpu.VMEM)
        rows = (SEQS, ROWS, HD)
        piece = (PIECE, HD)
        kv, vv, rep, wo_v, comb_a, comb_b, xrx_a = pl.pallas_call(
            attend_kernel,
            out_shape=(pltpu.VMEM(rows, BF16), pltpu.VMEM(rows, BF16),
                       pltpu.VMEM((2, SEQS * KVH, HD), F32), pltpu.VMEM((4, HALF * HD, WCH), BF16),
                       pltpu.VMEM((NX,) + piece, F32), pltpu.VMEM((NBLK - NX,) + piece, F32), pltpu.VMEM((NX,) + piece, F32)),
            in_specs=[hbm] * 12,
            out_specs=(vm,) * 7,
            scratch_shapes=[
                pltpu.SMEM((SEQS,), jnp.int32), pltpu.VMEM((SEQS, DIM), BF16), pltpu.VMEM((DIM // HD, HD), BF16),
                pltpu.VMEM((1, HD), BF16), pltpu.VMEM((1, HD), BF16), pltpu.VMEM((1, HD), F32), dma((6,)),
                pltpu.VMEM((2, SEQS, WCH), F32),
                pltpu.VMEM((RING, DIM, WCH), BF16),
                pltpu.VMEM((SEQS, DIM), BF16),
                pltpu.VMEM((SEQS, HD), F32), pltpu.VMEM((SEQS, HD), F32), pltpu.VMEM((SEQS, HD), F32),
                pltpu.VMEM((2, SEQS * 8, HD), F32), pltpu.VMEM((2, SEQS * 8, HD), F32),
                pltpu.VMEM((2 * HALF, ROWS), jnp.int32),
                pltpu.VMEM((NBLK, 2 * PIECE, HD), F32),
                pltpu.VMEM((NBLK,) + piece, F32),
                pltpu.VMEM((2, 4 * HALF, ROWS), F32), pltpu.VMEM((2, 4 * HALF, ROWS), BF16),
                dma((NW,)), dma((NBLK,)), dma((NBLK,)), dma((4,)), dma((3,)), dma((3,)),
                dma((NBLK,)), dma((NBLK,)), dma((NX,)), dma((NX,)),
            ],
            compiler_params=pltpu.CompilerParams(collective_id=0, has_side_effects=True, vmem_limit_bytes=VMEM_LIMIT),
            name='attend',
        )(in_hbm(positions), in_hbm(tokens), in_hbm(attn_norm.reshape(DIM // HD, HD)), in_hbm(q_norm.reshape(1, HD)),
          in_hbm(k_norm.reshape(1, HD)), in_hbm(jnp.asarray(freq2).reshape(1, HD)), in_hbm(w_q), in_hbm(w_k), in_hbm(w_v), in_hbm(w_o),
          in_hbm(k_cache.reshape(rows)), in_hbm(v_cache.reshape(rows)))
        xrx_b = lax.ppermute(comb_b, 'sp', [(0, 2), (2, 0), (1, 3), (3, 1)])
        k_out, v_out, new_kv, oa, kv, vv, wo_v = pl.pallas_call(
            write_kernel,
            out_shape=(pltpu.HBM(rows, BF16), pltpu.HBM(rows, BF16), pltpu.HBM((SEQS, 2 * KVH, HD), BF16),
                       pltpu.VMEM((NX * BLK, HALF * HD), F32), pltpu.VMEM(rows, BF16), pltpu.VMEM(rows, BF16),
                       pltpu.VMEM((4, HALF * HD, WCH), BF16)),
            in_specs=[hbm, vm, vm, vm, vm, vm, vm, hbm],
            out_specs=(hbm, hbm, hbm, vm, vm, vm, vm),
            input_output_aliases={1: 4, 2: 5, 6: 6},
            scratch_shapes=[pltpu.SMEM((SEQS,), jnp.int32), pltpu.VMEM((SEQS, 2 * KVH, HD), BF16),
                            pltpu.VMEM((2, BLK, 4 * KVH, HD), BF16),
                            dma((NBLK,)), dma((NBLK,)), dma((2, BLK)), dma((2,)), dma((4,))],
            compiler_params=pltpu.CompilerParams(vmem_limit_bytes=VMEM_LIMIT),
            cost_estimate=pl.CostEstimate(flops=10**10, bytes_accessed=2**25, transcendentals=0),
            name='write',
        )(in_hbm(positions), in_vmem(kv), in_vmem(vv), in_vmem(rep), in_vmem(comb_a), in_vmem(xrx_a), in_vmem(wo_v), in_hbm(w_o))
        k_out, v_out, part = pl.pallas_call(
            product_kernel,
            out_shape=(pltpu.HBM(rows, BF16), pltpu.HBM(rows, BF16), pltpu.VMEM((SEQS, DIM), F32)),
            in_specs=[vm, vm, hbm, hbm, vm, vm, vm, vm],
            out_specs=(hbm, hbm, vm),
            input_output_aliases={2: 0, 3: 1},
            scratch_shapes=[pltpu.VMEM(((NBLK - NX) * BLK, HALF * HD), F32), dma((NBLK,)), dma((NBLK,))],
            compiler_params=pltpu.CompilerParams(vmem_limit_bytes=VMEM_LIMIT),
            cost_estimate=pl.CostEstimate(flops=2 * SEQS * DIM * DIM, bytes_accessed=2**22, transcendentals=0),
            name='product',
        )(in_vmem(kv), in_vmem(vv), k_out, v_out, in_vmem(oa), in_vmem(comb_b), in_vmem(xrx_b), in_vmem(wo_v))
        other = lax.ppermute(part, 'sp', [(0, 1), (1, 0), (2, 3), (3, 2)])
        k_out, v_out = pl.pallas_call(
            rest_kernel,
            out_shape=(pltpu.HBM(rows, BF16), pltpu.HBM(rows, BF16)),
            in_specs=[vm, vm, hbm, hbm],
            out_specs=(hbm, hbm),
            input_output_aliases={2: 0, 3: 1},
            scratch_shapes=[dma((NBLK,)), dma((NBLK,))],
            compiler_params=pltpu.CompilerParams(vmem_limit_bytes=VMEM_LIMIT),
            cost_estimate=pl.CostEstimate(flops=10**9, bytes_accessed=2**22, transcendentals=0),
            name='rest',
        )(in_vmem(kv), in_vmem(vv), k_out, v_out)
        block_out = (tokens.astype(F32) + (part + other)).astype(BF16)
        return block_out, k_out.reshape(k_cache.shape), v_out.reshape(v_cache.shape), new_kv.reshape(SEQS, 2, KVH, HD)

    return jax.shard_map(device_step, mesh=mesh, in_specs=(P('dp', None), P('dp'), cache_spec, cache_spec, P(), P(), P(), P(), P(), P(), P()), out_specs=(P('dp', None), cache_spec, cache_spec, P('dp', None, None, None)), check_vma=False)
```

```python
import functools

import jax
import jax.numpy as jnp
import numpy as np
from jax import lax
from jax.experimental import pallas as pl
from jax.experimental.pallas import tpu as pltpu
from jax.sharding import PartitionSpec as P

NORM_EPS = 1e-6
ROPE_THETA = 1000000.0
MESH = pl.DeviceIdType.MESH
BF16 = jnp.bfloat16
F32 = jnp.float32

SEQS = 64
DIM = 2048
HD = 128
KVH = 4
HALF = 16
SLOTS = 256
ROWS = SLOTS * KVH
BLK = 8
NBLK = SEQS // BLK
AHEAD = 4
NX = 4
NA = 6
WSPLIT = 4
NW = 5
WAHEAD = 3
RING = 4
LAG = 2
WCH = 512
PIECE = (HALF + 1) * BLK
VMEM_LIMIT = 14 * 2**20
EXP_SCALE = HD ** -0.5 * 1.4426950408889634
NEG = -jnp.inf


def bcast_col(tile, col):
    return jnp.broadcast_to(tile[:, col:col + 1], (tile.shape[0], HD))


def out_weight_copy(n, core, wo, wo_v, wosem):
    src = wo.at[pl.ds(pl.multiple_of(core * (HALF * HD), HD), HALF * HD), pl.ds(n * WCH, WCH)]
    return pltpu.make_async_copy(src, wo_v.at[n], wosem.at[n])


def attend_kernel(pos_h, tok_h, an_h, qn_h, kn_h, freq_h, wq, wk, wv, wo, kc, vc,
                  kv, vv, rep, wo_v, comb_a, comb_b, xrx,
                  pos_s, tok, an, qn, kn, freq, insem, proj, w_s, hid, ang, cosr, sinr, qmine, qmate, colslot, opart, drx, sc, pr_s,
                  wsem, ksem, vsem, wosem, qs, qr, ds_, dr, xs, xr):
    me = lax.axis_index('sp')
    core = lax.rem(me, 2)
    chip = me // 2
    mate = {'sp': me + 1 - 2 * core}
    peer = {'sp': me + 2 - 4 * chip}

    def w_copy(n, src=None):
        if n < 4:
            src = wq.at[:, pl.ds(pl.multiple_of(core * (HALF * HD) + n * WCH, WCH), WCH)]
        return pltpu.make_async_copy(src, w_s.at[n % RING], wsem.at[n])

    def w_start(n):
        if n < 4:
            w_copy(n).start()
        else:
            @pl.when(core == 0)
            def _():
                w_copy(n, wk).start()

            @pl.when(core == 1)
            def _():
                w_copy(n, wv).start()

    def wo_copy(n):
        return out_weight_copy(n, core, wo, wo_v, wosem)

    def k_copy(i):
        return pltpu.make_async_copy(kc.at[pl.ds(i * BLK, BLK)], kv.at[pl.ds(i * BLK, BLK)], ksem.at[i])

    def v_copy(i):
        return pltpu.make_async_copy(vc.at[pl.ds(i * BLK, BLK)], vv.at[pl.ds(i * BLK, BLK)], vsem.at[i])

    def q_send(h):
        return pltpu.make_async_remote_copy(qmine.at[h], qmate.at[h], qs.at[h], qr.at[h], device_id=mate, device_id_type=MESH)

    def new_send():
        return pltpu.make_async_remote_copy(rep.at[core], rep.at[core], qs.at[2], qr.at[2], device_id=mate, device_id_type=MESH)

    def d_send(i):
        return pltpu.make_async_remote_copy(opart.at[i, pl.ds(PIECE, PIECE)], drx.at[i], ds_.at[i], dr.at[i],
                                            device_id=mate, device_id_type=MESH)

    def x_send(i):
        return pltpu.make_async_remote_copy(comb_a.at[i], xrx.at[i], xs.at[i], xr.at[i],
                                            device_id=peer, device_id_type=MESH)

    small = [pltpu.make_async_copy(a, b, insem.at[z]) for z, (a, b) in enumerate(
        ((tok_h, tok), (an_h, an), (pos_h, pos_s), (qn_h, qn), (kn_h, kn), (freq_h, freq)))]
    for c in small:
        c.start()
    for n in range(WAHEAD):
        w_start(n)

    barrier = pltpu.get_barrier_semaphore()
    for other in (mate, peer):
        pl.semaphore_signal(barrier, inc=1, device_id=other, device_id_type=MESH)

    small[0].wait()
    small[1].wait()
    t = tok[...].astype(F32)
    inv = lax.rsqrt(jnp.sum(t * t, axis=-1, keepdims=True) * (1.0 / DIM) + NORM_EPS)
    gains = an[...].astype(F32)
    for j in range(DIM // HD):
        sl = slice(j * HD, (j + 1) * HD)
        hid[:, sl] = (tok[:, sl].astype(F32) * inv * gains[j:j + 1, :]).astype(BF16)

    def tables():
        for c in small[2:]:
            c.wait()
        lane1 = lax.broadcasted_iota(jnp.int32, (1, HD), 1)

        def angle(b, carry):
            ang[pl.ds(b, 1), :] = freq[...] * pos_s[b].astype(F32)
            return carry

        lax.fori_loop(0, SEQS, angle, 0, unroll=8)
        cosr[...] = jnp.cos(ang[...])
        sinr[...] = jnp.sin(ang[...]) * jnp.where(lane1 < HD // 2, -1.0, 1.0)

        row = lax.broadcasted_iota(jnp.int32, (2 * HALF, ROWS), 0)
        col = lax.broadcasted_iota(jnp.int32, (2 * HALF, ROWS), 1)
        half_of_row = jnp.where(row < HALF, core, 1 - core)
        kv_of_row = half_of_row * 2 + lax.rem(row, HALF) // 8
        colslot[...] = jnp.where(lax.rem(col, KVH) == kv_of_row, col // KVH, 1 << 20)

    def norm_rope(x, gain):
        y = x * lax.rsqrt(jnp.mean(x * x, axis=-1, keepdims=True) + NORM_EPS) * gain
        y = y * cosr[...] + pltpu.roll(y, HD // 2, 1) * sinr[...]
        return y.astype(BF16).astype(F32)

    def post(n):
        for j in range(WCH // HD):
            x = proj[n % 2, :, j * HD:(j + 1) * HD].astype(BF16).astype(F32)
            if n < 4:
                qmine.at[n // 2][pl.ds(n % 2 * 4 + j, SEQS, stride=8), :] = norm_rope(x, qgain)
            else:
                rep.at[core][pl.ds(j, SEQS, stride=KVH), :] = jnp.where(core == 0, norm_rope(x, kgain), x)

    def cache_start(t):
        (v_copy if t % 2 else k_copy)(t // 2).start()

    def multiply(n):
        w_copy(n, wk).wait()
        if n + WAHEAD < NW:
            w_start(n + WAHEAD)
        if n > 0:
            cache_start(n - 1)
        proj[n % 2] = jnp.dot(hid[...], w_s[n % RING], preferred_element_type=F32)

    multiply(0)
    tables()
    qgain = qn[...].astype(F32)
    kgain = kn[...].astype(F32)
    multiply(1)
    post(0)
    multiply(2)
    post(1)
    pl.semaphore_wait(barrier, 2)
    q_send(0).start()
    multiply(3)
    post(2)
    post(3)
    q_send(1).start()
    multiply(4)
    cache_start(NW - 1)
    cache_start(NW)
    post(4)
    new_send().start()
    for t in range(NW + 1, 2 * AHEAD):
        cache_start(t)
    start = me * SLOTS
    lane = lax.broadcasted_iota(jnp.int32, (HALF, HD), 1)
    lrow = lax.broadcasted_iota(jnp.int32, (HALF, HD), 0)
    lane8 = lax.broadcasted_iota(jnp.int32, (BLK, HD), 1)
    for h in range(2):
        q_send(h).wait()

    def attend(i, first=False):
        ob = opart.at[i]
        def load_q(pair, at):
            bs = [at * BLK + 2 * pair + z for z in range(2)]
            return bs, [jnp.concatenate([ref[h, pl.ds(pl.multiple_of(b * 8, 8), 8), :]
                                         for ref in (qmine, qmate) for h in range(2)], axis=0) for b in bs]

        def new_rows(z, b):
            return jnp.concatenate([jnp.broadcast_to(rep[z, pl.ds(b * KVH + h, 1), :], (8, HD))
                                    for h in (2 * core, 2 * core + 1, 2 - 2 * core, 3 - 2 * core)], axis=0)

        def scores(pair, at):
            bs, qf = load_q(pair, at)
            zero = jnp.zeros((2 * HALF, HD), BF16)
            lhs = jnp.concatenate([jnp.concatenate([qf[0].astype(BF16), zero], axis=1),
                                   jnp.concatenate([zero, qf[1].astype(BF16)], axis=1)], axis=0)
            keys = jnp.concatenate([kv[bs[0]], kv[bs[1]]], axis=1)
            sc[pair % 2] = lax.dot_general(lhs, keys, (((1,), (1,)), ((), ())), preferred_element_type=F32)

        def soft(pair):
            bs, qf = load_q(pair, i)
            out = []
            for z in range(2):
                b = bs[z]
                rel = pos_s[b] - start
                owner = jnp.logical_and(rel >= 0, rel < SLOTS)
                snew = jnp.where(owner, jnp.sum(qf[z] * new_rows(0, b), axis=-1, keepdims=True), NEG)
                sm = jnp.where(colslot[...] < rel, sc[pair % 2, z * 2 * HALF:(z + 1) * 2 * HALF], NEG)
                peak = jnp.maximum(jnp.max(sm, axis=-1, keepdims=True), snew)
                safe = jnp.where(peak == NEG, 0.0, peak)
                p = jnp.exp2((sm - safe) * EXP_SCALE)
                pn = jnp.exp2((snew - safe) * EXP_SCALE)
                pr_s[pair % 2, z * 2 * HALF:(z + 1) * 2 * HALF, :] = p.astype(BF16)
                out.append((pn.astype(BF16).astype(F32), jnp.sum(p, axis=-1, keepdims=True) + pn, peak))
            return out

        def mix(pair, st3):
            bs = [i * BLK + 2 * pair + z for z in range(2)]
            values = jnp.concatenate([vv[bs[0]], vv[bs[1]]], axis=1)
            mixed = jnp.dot(pr_s[pair % 2], values, preferred_element_type=F32)
            for z in range(2):
                extra, total, peak = st3[z]
                o = mixed[z * 2 * HALF:(z + 1) * 2 * HALF, z * HD:(z + 1) * HD] + extra * new_rows(1, bs[z])
                bb = 2 * pair + z
                for h in range(2):
                    hs = slice(h * HALF, (h + 1) * HALF)
                    ob[pl.ds(h * PIECE + bb, HALF, stride=BLK), :] = o[hs]
                    st = jnp.where(lane == lrow, peak[hs], jnp.where(lane == lrow + HALF, total[hs], 0.0))
                    ob[pl.ds(h * PIECE + HALF * BLK + bb, 1), :] = jnp.sum(st, axis=0, keepdims=True)

        if first:
            scores(0, i)
            return
        for pair in range(BLK // 2):
            if pair + 1 < BLK // 2:
                scores(pair + 1, i)
            else:
                scores(0, jnp.minimum(i + 1, NBLK - 1))
            mix(pair, soft(pair))

    def combine(i, comb, at):
        s0 = opart[i, pl.ds(HALF * BLK, BLK), :]
        s1 = drx[i, pl.ds(HALF * BLK, BLK), :]
        peak = jnp.maximum(s0, s1)
        safe = jnp.where(peak == NEG, 0.0, peak)
        f0 = jnp.exp2((s0 - safe) * EXP_SCALE)
        f1 = jnp.exp2((s1 - safe) * EXP_SCALE)
        total = f0 * pltpu.roll(s0, HD - HALF, 1) + f1 * pltpu.roll(s1, HD - HALF, 1)
        comb[at, pl.ds(HALF * BLK, BLK), :] = jnp.where(
            lane8 < HALF, peak, jnp.where(lane8 < 2 * HALF, pltpu.roll(total, HALF, 1), 0.0))
        for j in range(HALF):
            rows = pl.ds(j * BLK, BLK)
            comb[at, rows, :] = bcast_col(f0, j) * opart[i, rows, :] + bcast_col(f1, j) * drx[i, rows, :]

    def fetch(i):
        @pl.when(i + 1 < NBLK)
        def _():
            k_copy(i + 1).wait()

        v_copy(i).wait()

        @pl.when(i + AHEAD < NBLK)
        def _():
            k_copy(i + AHEAD).start()
            v_copy(i + AHEAD).start()

        @pl.when(i + AHEAD == NBLK)
        def _():
            for n in range(WSPLIT):
                wo_copy(n).start()

    def early(i, carry):
        fetch(i)
        attend(i)
        d_send(i).start()
        return carry

    def sending(i, carry):
        fetch(i)
        attend(i)
        d_send(i).start()
        d_send(i - 1).wait_recv()
        combine(i - 1, comb_a, i - 1)
        x_send(i - 1).start()
        return carry

    def keeping(i, carry):
        fetch(i)
        d_send(i - LAG).wait_recv()
        combine(i - LAG, comb_b, i - LAG - NX)
        attend(i)
        d_send(i).start()
        return carry

    def late(i, carry):
        d_send(i).wait_recv()
        combine(i, comb_b, i - NX)
        return carry

    k_copy(0).wait()
    attend(0, first=True)
    new_send().wait()
    early(0, 0)
    lax.fori_loop(1, 1 + NX, sending, 0)
    lax.fori_loop(1 + NX, LAG + NX, early, 0)
    lax.fori_loop(LAG + NX, NBLK, keeping, 0)
    lax.fori_loop(NBLK - LAG, NBLK, late, 0)

    for n in range(WSPLIT):
        wo_copy(n).wait()

    def drain(i, carry):
        d_send(i).wait_send()
        return carry

    def drain_x(i, carry):
        x_send(i).wait()
        return carry

    lax.fori_loop(0, NBLK, drain, 0)
    lax.fori_loop(0, NX, drain_x, 0)


def last_merge(chip, comb, other_ref, i, ofin, at):
    first = chip == 0

    def ordered(rows):
        mine, other = comb[i, rows, :], other_ref[i, rows, :]
        return jnp.where(first, mine, other), jnp.where(first, other, mine)

    s0, s1 = ordered(pl.ds(HALF * BLK, BLK))
    peak = jnp.maximum(s0, s1)
    f0 = jnp.exp2((s0 - peak) * EXP_SCALE)
    f1 = jnp.exp2((s1 - peak) * EXP_SCALE)
    total = f0 * pltpu.roll(s0, HD - HALF, 1) + f1 * pltpu.roll(s1, HD - HALF, 1)
    g0, g1 = f0 / total, f1 / total
    for j in range(HALF):
        a, b = ordered(pl.ds(j * BLK, BLK))
        ofin[at * BLK:(at + 1) * BLK, j * HD:(j + 1) * HD] = bcast_col(g0, j) * a + bcast_col(g1, j) * b


def block_copies(i, kv, vv, ko, vo, ksem, vsem):
    r = pl.ds(i * BLK, BLK)
    return (pltpu.make_async_copy(kv.at[r], ko.at[r], ksem.at[i]),
            pltpu.make_async_copy(vv.at[r], vo.at[r], vsem.at[i]))


def product_kernel(kv, vv, ki, vi, oa, comb_b, xrx_b, wo_v, ko, vo, part, ofin, ksem, vsem):
    for c in block_copies(NA, kv, vv, ko, vo, ksem, vsem):
        c.start()
    for i in range(NBLK - NX):
        last_merge(lax.axis_index('sp') // 2, comb_b, xrx_b, i, ofin, i)
    lhs = jnp.concatenate([oa[...].astype(BF16), ofin[...].astype(BF16)], axis=0)
    for n in range(4):
        part[:, n * WCH:(n + 1) * WCH] = jnp.dot(lhs, wo_v[n], preferred_element_type=F32)
    for c in block_copies(NA, kv, vv, ko, vo, ksem, vsem):
        c.wait()


def rest_kernel(kv, vv, ki, vi, ko, vo, ksem, vsem):
    for c in block_copies(NA + 1, kv, vv, ko, vo, ksem, vsem):
        c.start()
    for c in block_copies(NA + 1, kv, vv, ko, vo, ksem, vsem):
        c.wait()


def write_kernel(pos_h, kv, vv, rep, comb_a, xrx, wo_v, wo, ko, vo, nkv, oa, kva, vva, wo_a, pos_s, nkv_s, patch, ksem, vsem, psem, osem, wosem):
    start = lax.axis_index('sp') * SLOTS
    slot16 = lax.broadcasted_iota(jnp.int32, (4 * KVH, HD), 0) // KVH

    def copies(i):
        return block_copies(i, kv, vv, ko, vo, ksem, vsem)

    pos_copy = pltpu.make_async_copy(pos_h, pos_s, osem.at[0])
    pos_copy.start()
    for c in copies(0):
        c.start()
    for b in range(SEQS):
        nkv_s[b] = jnp.concatenate([rep[0, pl.ds(b * KVH, KVH), :], rep[1, pl.ds(b * KVH, KVH), :]], axis=0).astype(BF16)
    pos_copy.wait()

    def each(i, do):
        for bb in range(BLK):
            b = i * BLK + bb
            rel = pos_s[b] - start

            @pl.when(jnp.logical_and(rel >= 0, rel < SLOTS))
            def _():
                base = pl.multiple_of(rel // 4 * (4 * KVH), 4 * KVH)
                mask = slot16 == lax.rem(rel, 4)
                for z, (ref, out) in enumerate(((kv, ko), (vv, vo))):
                    do(b, z, base, mask, ref, out)

    def merged(b, z, base, mask, ref):
        new = jnp.concatenate([rep[z, pl.ds(b * KVH, KVH), :]] * 4, axis=0)
        old = ref[b, pl.ds(base, 4 * KVH), :].astype(F32)
        return jnp.where(mask, new, old).astype(BF16)

    def put(b, z, base, mask, ref, out):
        ref[b, pl.ds(base, 4 * KVH), :] = merged(b, z, base, mask, ref)

    def stage(b, z, base, mask, ref, out):
        patch[z, b] = merged(b, z, base, mask, ref)

    def patch_copy(b, z, base, out):
        return pltpu.make_async_copy(patch.at[z, b], out.at[b, pl.ds(base, 4 * KVH)], psem.at[z, b])

    for i in range(1, NBLK):
        each(i, put)
        if 1 < i <= NA:
            for c in copies(i - 1):
                c.start()
    core = lax.rem(lax.axis_index('sp'), 2)
    for n in range(WSPLIT, 4):
        out_weight_copy(n, core, wo, wo_v, wosem).start()
    nkv_copy = pltpu.make_async_copy(nkv_s, nkv, osem.at[1])
    nkv_copy.start()
    each(0, stage)
    for i in range(NX):
        last_merge(lax.axis_index('sp') // 2, comb_a, xrx, i, oa, i)
    for c in copies(0):
        c.wait()
    each(0, lambda b, z, base, mask, ref, out: patch_copy(b, z, base, out).start())
    nkv_copy.wait()
    each(0, lambda b, z, base, mask, ref, out: patch_copy(b, z, base, out).wait())
    for i in range(1, NA):
        for c in copies(i):
            c.wait()
    for n in range(WSPLIT, 4):
        out_weight_copy(n, core, wo, wo_v, wosem).wait()


def solution(mesh):
    cache_spec = P('dp', 'sp', None, None)
    inv_freq = (np.float64(ROPE_THETA) ** (-np.arange(HD // 2) * 2.0 / HD)).astype(np.float32)
    freq2 = np.concatenate([inv_freq, inv_freq])
    vm = pl.BlockSpec(memory_space=pltpu.VMEM)
    hbm = pl.BlockSpec(memory_space=pl.ANY)
    dma = pltpu.SemaphoreType.DMA

    def device_step(tokens, positions, k_cache, v_cache, w_q, w_k, w_v, w_o, attn_norm, q_norm, k_norm):
        in_hbm = lambda x: pltpu.with_memory_space_constraint(x, pltpu.HBM)
        in_vmem = lambda x: pltpu.with_memory_space_constraint(x, pltpu.VMEM)
        rows = (SEQS, ROWS, HD)
        piece = (PIECE, HD)
        kv, vv, rep, wo_v, comb_a, comb_b, xrx_a = pl.pallas_call(
            attend_kernel,
            out_shape=(pltpu.VMEM(rows, BF16), pltpu.VMEM(rows, BF16),
                       pltpu.VMEM((2, SEQS * KVH, HD), F32), pltpu.VMEM((4, HALF * HD, WCH), BF16),
                       pltpu.VMEM((NX,) + piece, F32), pltpu.VMEM((NBLK - NX,) + piece, F32), pltpu.VMEM((NX,) + piece, F32)),
            in_specs=[hbm] * 12,
            out_specs=(vm,) * 7,
            scratch_shapes=[
                pltpu.SMEM((SEQS,), jnp.int32), pltpu.VMEM((SEQS, DIM), BF16), pltpu.VMEM((DIM // HD, HD), BF16),
                pltpu.VMEM((1, HD), BF16), pltpu.VMEM((1, HD), BF16), pltpu.VMEM((1, HD), F32), dma((6,)),
                pltpu.VMEM((2, SEQS, WCH), F32),
                pltpu.VMEM((RING, DIM, WCH), BF16),
                pltpu.VMEM((SEQS, DIM), BF16),
                pltpu.VMEM((SEQS, HD), F32), pltpu.VMEM((SEQS, HD), F32), pltpu.VMEM((SEQS, HD), F32),
                pltpu.VMEM((2, SEQS * 8, HD), F32), pltpu.VMEM((2, SEQS * 8, HD), F32),
                pltpu.VMEM((2 * HALF, ROWS), jnp.int32),
                pltpu.VMEM((NBLK, 2 * PIECE, HD), F32),
                pltpu.VMEM((NBLK,) + piece, F32),
                pltpu.VMEM((2, 4 * HALF, ROWS), F32), pltpu.VMEM((2, 4 * HALF, ROWS), BF16),
                dma((NW,)), dma((NBLK,)), dma((NBLK,)), dma((4,)), dma((3,)), dma((3,)),
                dma((NBLK,)), dma((NBLK,)), dma((NX,)), dma((NX,)),
            ],
            compiler_params=pltpu.CompilerParams(collective_id=0, has_side_effects=True, vmem_limit_bytes=VMEM_LIMIT),
            name='attend',
        )(in_hbm(positions), in_hbm(tokens), in_hbm(attn_norm.reshape(DIM // HD, HD)), in_hbm(q_norm.reshape(1, HD)),
          in_hbm(k_norm.reshape(1, HD)), in_hbm(jnp.asarray(freq2).reshape(1, HD)), in_hbm(w_q), in_hbm(w_k), in_hbm(w_v), in_hbm(w_o),
          in_hbm(k_cache.reshape(rows)), in_hbm(v_cache.reshape(rows)))
        xrx_b = lax.ppermute(comb_b, 'sp', [(0, 2), (2, 0), (1, 3), (3, 1)])
        k_out, v_out, new_kv, oa, kv, vv, wo_v = pl.pallas_call(
            write_kernel,
            out_shape=(pltpu.HBM(rows, BF16), pltpu.HBM(rows, BF16), pltpu.HBM((SEQS, 2 * KVH, HD), BF16),
                       pltpu.VMEM((NX * BLK, HALF * HD), F32), pltpu.VMEM(rows, BF16), pltpu.VMEM(rows, BF16),
                       pltpu.VMEM((4, HALF * HD, WCH), BF16)),
            in_specs=[hbm, vm, vm, vm, vm, vm, vm, hbm],
            out_specs=(hbm, hbm, hbm, vm, vm, vm, vm),
            input_output_aliases={1: 4, 2: 5, 6: 6},
            scratch_shapes=[pltpu.SMEM((SEQS,), jnp.int32), pltpu.VMEM((SEQS, 2 * KVH, HD), BF16),
                            pltpu.VMEM((2, BLK, 4 * KVH, HD), BF16),
                            dma((NBLK,)), dma((NBLK,)), dma((2, BLK)), dma((2,)), dma((4,))],
            compiler_params=pltpu.CompilerParams(vmem_limit_bytes=VMEM_LIMIT),
            cost_estimate=pl.CostEstimate(flops=10**10, bytes_accessed=2**25, transcendentals=0),
            name='write',
        )(in_hbm(positions), in_vmem(kv), in_vmem(vv), in_vmem(rep), in_vmem(comb_a), in_vmem(xrx_a), in_vmem(wo_v), in_hbm(w_o))
        k_out, v_out, part = pl.pallas_call(
            product_kernel,
            out_shape=(pltpu.HBM(rows, BF16), pltpu.HBM(rows, BF16), pltpu.VMEM((SEQS, DIM), F32)),
            in_specs=[vm, vm, hbm, hbm, vm, vm, vm, vm],
            out_specs=(hbm, hbm, vm),
            input_output_aliases={2: 0, 3: 1},
            scratch_shapes=[pltpu.VMEM(((NBLK - NX) * BLK, HALF * HD), F32), dma((NBLK,)), dma((NBLK,))],
            compiler_params=pltpu.CompilerParams(vmem_limit_bytes=VMEM_LIMIT),
            cost_estimate=pl.CostEstimate(flops=2 * SEQS * DIM * DIM, bytes_accessed=2**22, transcendentals=0),
            name='product',
        )(in_vmem(kv), in_vmem(vv), k_out, v_out, in_vmem(oa), in_vmem(comb_b), in_vmem(xrx_b), in_vmem(wo_v))
        other = lax.ppermute(part, 'sp', [(0, 1), (1, 0), (2, 3), (3, 2)])
        k_out, v_out = pl.pallas_call(
            rest_kernel,
            out_shape=(pltpu.HBM(rows, BF16), pltpu.HBM(rows, BF16)),
            in_specs=[vm, vm, hbm, hbm],
            out_specs=(hbm, hbm),
            input_output_aliases={2: 0, 3: 1},
            scratch_shapes=[dma((NBLK,)), dma((NBLK,))],
            compiler_params=pltpu.CompilerParams(vmem_limit_bytes=VMEM_LIMIT),
            cost_estimate=pl.CostEstimate(flops=10**9, bytes_accessed=2**22, transcendentals=0),
            name='rest',
        )(in_vmem(kv), in_vmem(vv), k_out, v_out)
        block_out = (tokens.astype(F32) + (part + other)).astype(BF16)
        return block_out, k_out.reshape(k_cache.shape), v_out.reshape(v_cache.shape), new_kv.reshape(SEQS, 2, KVH, HD)

    return jax.shard_map(device_step, mesh=mesh, in_specs=(P('dp', None), P('dp'), cache_spec, cache_spec, P(), P(), P(), P(), P(), P(), P()), out_specs=(P('dp', None), cache_spec, cache_spec, P('dp', None, None, None)), check_vma=False)
```

```python
import functools

import jax
import jax.numpy as jnp
import numpy as np
from jax import lax
from jax.experimental import pallas as pl
from jax.experimental.pallas import tpu as pltpu
from jax.sharding import PartitionSpec as P

NORM_EPS = 1e-6
ROPE_THETA = 1000000.0
MESH = pl.DeviceIdType.MESH
BF16 = jnp.bfloat16
F32 = jnp.float32

SEQS = 64
DIM = 2048
HD = 128
KVH = 4
HALF = 16
SLOTS = 256
ROWS = SLOTS * KVH
BLK = 8
NBLK = SEQS // BLK
AHEAD = 2
NX = 4
NA = 6
WSPLIT = 4
NW = 5
WAHEAD = 3
RING = 4
LAG = 2
WCH = 512
PIECE = (HALF + 1) * BLK
VMEM_LIMIT = 14 * 2**20
EXP_SCALE = HD ** -0.5 * 1.4426950408889634
NEG = -jnp.inf


def bcast_col(tile, col):
    return jnp.broadcast_to(tile[:, col:col + 1], (tile.shape[0], HD))


def out_weight_copy(n, core, wo, wo_v, wosem):
    src = wo.at[pl.ds(pl.multiple_of(core * (HALF * HD), HD), HALF * HD), pl.ds(n * WCH, WCH)]
    return pltpu.make_async_copy(src, wo_v.at[n], wosem.at[n])


def attend_kernel(pos_h, tok_h, an_h, qn_h, kn_h, freq_h, wq, wk, wv, wo, kc, vc,
                  kv, vv, rep, wo_v, comb_a, comb_b, xrx,
                  pos_s, tok, an, qn, kn, freq, insem, proj, w_s, hid, ang, cosr, sinr, qmine, qmate, colslot, opart, drx, sc, pr_s,
                  wsem, ksem, vsem, wosem, qs, qr, ds_, dr, xs, xr):
    me = lax.axis_index('sp')
    core = lax.rem(me, 2)
    chip = me // 2
    mate = {'sp': me + 1 - 2 * core}
    peer = {'sp': me + 2 - 4 * chip}

    def w_copy(n, src=None):
        if n < 4:
            src = wq.at[:, pl.ds(pl.multiple_of(core * (HALF * HD) + n * WCH, WCH), WCH)]
        return pltpu.make_async_copy(src, w_s.at[n % RING], wsem.at[n])

    def w_start(n):
        if n < 4:
            w_copy(n).start()
        else:
            @pl.when(core == 0)
            def _():
                w_copy(n, wk).start()

            @pl.when(core == 1)
            def _():
                w_copy(n, wv).start()

    def wo_copy(n):
        return out_weight_copy(n, core, wo, wo_v, wosem)

    def k_copy(i):
        return pltpu.make_async_copy(kc.at[pl.ds(i * BLK, BLK)], kv.at[pl.ds(i * BLK, BLK)], ksem.at[i])

    def v_copy(i):
        return pltpu.make_async_copy(vc.at[pl.ds(i * BLK, BLK)], vv.at[pl.ds(i * BLK, BLK)], vsem.at[i])

    def q_send(h):
        return pltpu.make_async_remote_copy(qmine.at[h], qmate.at[h], qs.at[h], qr.at[h], device_id=mate, device_id_type=MESH)

    def new_send():
        return pltpu.make_async_remote_copy(rep.at[core], rep.at[core], qs.at[2], qr.at[2], device_id=mate, device_id_type=MESH)

    def d_send(i):
        return pltpu.make_async_remote_copy(opart.at[i, pl.ds(PIECE, PIECE)], drx.at[i], ds_.at[i], dr.at[i],
                                            device_id=mate, device_id_type=MESH)

    def x_send(i):
        return pltpu.make_async_remote_copy(comb_a.at[i], xrx.at[i], xs.at[i], xr.at[i],
                                            device_id=peer, device_id_type=MESH)

    small = [pltpu.make_async_copy(a, b, insem.at[z]) for z, (a, b) in enumerate(
        ((tok_h, tok), (an_h, an), (pos_h, pos_s), (qn_h, qn), (kn_h, kn), (freq_h, freq)))]
    for c in small:
        c.start()
    for n in range(WAHEAD):
        w_start(n)

    barrier = pltpu.get_barrier_semaphore()
    for other in (mate, peer):
        pl.semaphore_signal(barrier, inc=1, device_id=other, device_id_type=MESH)

    small[0].wait()
    small[1].wait()
    t = tok[...].astype(F32)
    inv = lax.rsqrt(jnp.sum(t * t, axis=-1, keepdims=True) * (1.0 / DIM) + NORM_EPS)
    gains = an[...].astype(F32)
    for j in range(DIM // HD):
        sl = slice(j * HD, (j + 1) * HD)
        hid[:, sl] = (tok[:, sl].astype(F32) * inv * gains[j:j + 1, :]).astype(BF16)

    def tables():
        for c in small[2:]:
            c.wait()
        lane1 = lax.broadcasted_iota(jnp.int32, (1, HD), 1)

        def angle(b, carry):
            ang[pl.ds(b, 1), :] = freq[...] * pos_s[b].astype(F32)
            return carry

        lax.fori_loop(0, SEQS, angle, 0, unroll=8)
        cosr[...] = jnp.cos(ang[...])
        sinr[...] = jnp.sin(ang[...]) * jnp.where(lane1 < HD // 2, -1.0, 1.0)

        row = lax.broadcasted_iota(jnp.int32, (2 * HALF, ROWS), 0)
        col = lax.broadcasted_iota(jnp.int32, (2 * HALF, ROWS), 1)
        half_of_row = jnp.where(row < HALF, core, 1 - core)
        kv_of_row = half_of_row * 2 + lax.rem(row, HALF) // 8
        colslot[...] = jnp.where(lax.rem(col, KVH) == kv_of_row, col // KVH, 1 << 20)

    def norm_rope(x, gain):
        y = x * lax.rsqrt(jnp.mean(x * x, axis=-1, keepdims=True) + NORM_EPS) * gain
        y = y * cosr[...] + pltpu.roll(y, HD // 2, 1) * sinr[...]
        return y.astype(BF16).astype(F32)

    def post(n):
        for j in range(WCH // HD):
            x = proj[n % 2, :, j * HD:(j + 1) * HD].astype(BF16).astype(F32)
            if n < 4:
                qmine.at[n // 2][pl.ds(n % 2 * 4 + j, SEQS, stride=8), :] = norm_rope(x, qgain)
            else:
                rep.at[core][pl.ds(j, SEQS, stride=KVH), :] = jnp.where(core == 0, norm_rope(x, kgain), x)

    def cache_start(t):
        (v_copy if t % 2 else k_copy)(t // 2).start()

    def multiply(n):
        w_copy(n, wk).wait()
        if n + WAHEAD < NW:
            w_start(n + WAHEAD)
        else:
            cache_start(n + WAHEAD - NW)
        proj[n % 2] = jnp.dot(hid[...], w_s[n % RING], preferred_element_type=F32)

    multiply(0)
    tables()
    qgain = qn[...].astype(F32)
    kgain = kn[...].astype(F32)
    multiply(1)
    post(0)
    multiply(2)
    post(1)
    pl.semaphore_wait(barrier, 2)
    q_send(0).start()
    multiply(3)
    post(2)
    post(3)
    q_send(1).start()
    multiply(4)
    cache_start(WAHEAD)
    post(4)
    new_send().start()
    for t in range(WAHEAD + 1, 2 * AHEAD):
        cache_start(t)
    start = me * SLOTS
    lane = lax.broadcasted_iota(jnp.int32, (HALF, HD), 1)
    lrow = lax.broadcasted_iota(jnp.int32, (HALF, HD), 0)
    lane8 = lax.broadcasted_iota(jnp.int32, (BLK, HD), 1)
    for h in range(2):
        q_send(h).wait()

    def attend(i, first=False):
        ob = opart.at[i]
        def load_q(pair, at):
            bs = [at * BLK + 2 * pair + z for z in range(2)]
            return bs, [jnp.concatenate([ref[h, pl.ds(pl.multiple_of(b * 8, 8), 8), :]
                                         for ref in (qmine, qmate) for h in range(2)], axis=0) for b in bs]

        def new_rows(z, b):
            return jnp.concatenate([jnp.broadcast_to(rep[z, pl.ds(b * KVH + h, 1), :], (8, HD))
                                    for h in (2 * core, 2 * core + 1, 2 - 2 * core, 3 - 2 * core)], axis=0)

        def scores(pair, at):
            bs, qf = load_q(pair, at)
            zero = jnp.zeros((2 * HALF, HD), BF16)
            lhs = jnp.concatenate([jnp.concatenate([qf[0].astype(BF16), zero], axis=1),
                                   jnp.concatenate([zero, qf[1].astype(BF16)], axis=1)], axis=0)
            keys = jnp.concatenate([kv[bs[0]], kv[bs[1]]], axis=1)
            sc[pair % 2] = lax.dot_general(lhs, keys, (((1,), (1,)), ((), ())), preferred_element_type=F32)

        def soft(pair):
            bs, qf = load_q(pair, i)
            out = []
            for z in range(2):
                b = bs[z]
                rel = pos_s[b] - start
                owner = jnp.logical_and(rel >= 0, rel < SLOTS)
                snew = jnp.where(owner, jnp.sum(qf[z] * new_rows(0, b), axis=-1, keepdims=True), NEG)
                sm = jnp.where(colslot[...] < rel, sc[pair % 2, z * 2 * HALF:(z + 1) * 2 * HALF], NEG)
                peak = jnp.maximum(jnp.max(sm, axis=-1, keepdims=True), snew)
                safe = jnp.where(peak == NEG, 0.0, peak)
                p = jnp.exp2((sm - safe) * EXP_SCALE)
                pn = jnp.exp2((snew - safe) * EXP_SCALE)
                pr_s[pair % 2, z * 2 * HALF:(z + 1) * 2 * HALF, :] = p.astype(BF16)
                out.append((pn.astype(BF16).astype(F32), jnp.sum(p, axis=-1, keepdims=True) + pn, peak))
            return out

        def mix(pair, st3):
            bs = [i * BLK + 2 * pair + z for z in range(2)]
            values = jnp.concatenate([vv[bs[0]], vv[bs[1]]], axis=1)
            mixed = jnp.dot(pr_s[pair % 2], values, preferred_element_type=F32)
            for z in range(2):
                extra, total, peak = st3[z]
                o = mixed[z * 2 * HALF:(z + 1) * 2 * HALF, z * HD:(z + 1) * HD] + extra * new_rows(1, bs[z])
                bb = 2 * pair + z
                for h in range(2):
                    hs = slice(h * HALF, (h + 1) * HALF)
                    ob[pl.ds(h * PIECE + bb, HALF, stride=BLK), :] = o[hs]
                    st = jnp.where(lane == lrow, peak[hs], jnp.where(lane == lrow + HALF, total[hs], 0.0))
                    ob[pl.ds(h * PIECE + HALF * BLK + bb, 1), :] = jnp.sum(st, axis=0, keepdims=True)

        if first:
            scores(0, i)
            return
        for pair in range(BLK // 2):
            if pair + 1 < BLK // 2:
                scores(pair + 1, i)
            else:
                scores(0, jnp.minimum(i + 1, NBLK - 1))
            mix(pair, soft(pair))

    def combine(i, comb, at):
        s0 = opart[i, pl.ds(HALF * BLK, BLK), :]
        s1 = drx[i, pl.ds(HALF * BLK, BLK), :]
        peak = jnp.maximum(s0, s1)
        safe = jnp.where(peak == NEG, 0.0, peak)
        f0 = jnp.exp2((s0 - safe) * EXP_SCALE)
        f1 = jnp.exp2((s1 - safe) * EXP_SCALE)
        total = f0 * pltpu.roll(s0, HD - HALF, 1) + f1 * pltpu.roll(s1, HD - HALF, 1)
        comb[at, pl.ds(HALF * BLK, BLK), :] = jnp.where(
            lane8 < HALF, peak, jnp.where(lane8 < 2 * HALF, pltpu.roll(total, HALF, 1), 0.0))
        for j in range(HALF):
            rows = pl.ds(j * BLK, BLK)
            comb[at, rows, :] = bcast_col(f0, j) * opart[i, rows, :] + bcast_col(f1, j) * drx[i, rows, :]

    def fetch(i):
        @pl.when(i + 1 < NBLK)
        def _():
            k_copy(i + 1).wait()

        v_copy(i).wait()

        @pl.when(i + AHEAD < NBLK)
        def _():
            k_copy(i + AHEAD).start()
            v_copy(i + AHEAD).start()

        @pl.when(i + AHEAD == NBLK)
        def _():
            for n in range(WSPLIT):
                wo_copy(n).start()

    def early(i, carry):
        fetch(i)
        attend(i)
        d_send(i).start()
        return carry

    def sending(i, carry):
        fetch(i)
        attend(i)
        d_send(i).start()
        d_send(i - 1).wait_recv()
        combine(i - 1, comb_a, i - 1)
        x_send(i - 1).start()
        return carry

    def keeping(i, carry):
        fetch(i)
        d_send(i - LAG).wait_recv()
        combine(i - LAG, comb_b, i - LAG - NX)
        attend(i)
        d_send(i).start()
        return carry

    def late(i, carry):
        d_send(i).wait_recv()
        combine(i, comb_b, i - NX)
        return carry

    k_copy(0).wait()
    attend(0, first=True)
    new_send().wait()
    early(0, 0)
    lax.fori_loop(1, 1 + NX, sending, 0)
    lax.fori_loop(1 + NX, LAG + NX, early, 0)
    lax.fori_loop(LAG + NX, NBLK, keeping, 0)
    lax.fori_loop(NBLK - LAG, NBLK, late, 0)

    for n in range(WSPLIT):
        wo_copy(n).wait()

    def drain(i, carry):
        d_send(i).wait_send()
        return carry

    def drain_x(i, carry):
        x_send(i).wait()
        return carry

    lax.fori_loop(0, NBLK, drain, 0)
    lax.fori_loop(0, NX, drain_x, 0)


def last_merge(chip, comb, other_ref, i, ofin, at):
    first = chip == 0

    def ordered(rows):
        mine, other = comb[i, rows, :], other_ref[i, rows, :]
        return jnp.where(first, mine, other), jnp.where(first, other, mine)

    s0, s1 = ordered(pl.ds(HALF * BLK, BLK))
    peak = jnp.maximum(s0, s1)
    f0 = jnp.exp2((s0 - peak) * EXP_SCALE)
    f1 = jnp.exp2((s1 - peak) * EXP_SCALE)
    total = f0 * pltpu.roll(s0, HD - HALF, 1) + f1 * pltpu.roll(s1, HD - HALF, 1)
    g0, g1 = f0 / total, f1 / total
    for j in range(HALF):
        a, b = ordered(pl.ds(j * BLK, BLK))
        ofin[at * BLK:(at + 1) * BLK, j * HD:(j + 1) * HD] = bcast_col(g0, j) * a + bcast_col(g1, j) * b


def block_copies(i, kv, vv, ko, vo, ksem, vsem):
    r = pl.ds(i * BLK, BLK)
    return (pltpu.make_async_copy(kv.at[r], ko.at[r], ksem.at[i]),
            pltpu.make_async_copy(vv.at[r], vo.at[r], vsem.at[i]))


def product_kernel(kv, vv, ki, vi, oa, comb_b, xrx_b, wo_v, ko, vo, part, ofin, ksem, vsem):
    for c in block_copies(NA, kv, vv, ko, vo, ksem, vsem):
        c.start()
    for i in range(NBLK - NX):
        last_merge(lax.axis_index('sp') // 2, comb_b, xrx_b, i, ofin, i)
    lhs = jnp.concatenate([oa[...].astype(BF16), ofin[...].astype(BF16)], axis=0)
    for n in range(4):
        part[:, n * WCH:(n + 1) * WCH] = jnp.dot(lhs, wo_v[n], preferred_element_type=F32)
    for c in block_copies(NA, kv, vv, ko, vo, ksem, vsem):
        c.wait()


def rest_kernel(kv, vv, ki, vi, ko, vo, ksem, vsem):
    for c in block_copies(NA + 1, kv, vv, ko, vo, ksem, vsem):
        c.start()
    for c in block_copies(NA + 1, kv, vv, ko, vo, ksem, vsem):
        c.wait()


def write_kernel(pos_h, kv, vv, rep, comb_a, xrx, wo_v, wo, ko, vo, nkv, oa, kva, vva, wo_a, pos_s, nkv_s, patch, ksem, vsem, psem, osem, wosem):
    start = lax.axis_index('sp') * SLOTS
    slot16 = lax.broadcasted_iota(jnp.int32, (4 * KVH, HD), 0) // KVH

    def copies(i):
        return block_copies(i, kv, vv, ko, vo, ksem, vsem)

    pos_copy = pltpu.make_async_copy(pos_h, pos_s, osem.at[0])
    pos_copy.start()
    for c in copies(0):
        c.start()
    for b in range(SEQS):
        nkv_s[b] = jnp.concatenate([rep[0, pl.ds(b * KVH, KVH), :], rep[1, pl.ds(b * KVH, KVH), :]], axis=0).astype(BF16)
    pos_copy.wait()

    def each(i, do):
        for bb in range(BLK):
            b = i * BLK + bb
            rel = pos_s[b] - start

            @pl.when(jnp.logical_and(rel >= 0, rel < SLOTS))
            def _():
                base = pl.multiple_of(rel // 4 * (4 * KVH), 4 * KVH)
                mask = slot16 == lax.rem(rel, 4)
                for z, (ref, out) in enumerate(((kv, ko), (vv, vo))):
                    do(b, z, base, mask, ref, out)

    def merged(b, z, base, mask, ref):
        new = jnp.concatenate([rep[z, pl.ds(b * KVH, KVH), :]] * 4, axis=0)
        old = ref[b, pl.ds(base, 4 * KVH), :].astype(F32)
        return jnp.where(mask, new, old).astype(BF16)

    def put(b, z, base, mask, ref, out):
        ref[b, pl.ds(base, 4 * KVH), :] = merged(b, z, base, mask, ref)

    def stage(b, z, base, mask, ref, out):
        patch[z, b] = merged(b, z, base, mask, ref)

    def patch_copy(b, z, base, out):
        return pltpu.make_async_copy(patch.at[z, b], out.at[b, pl.ds(base, 4 * KVH)], psem.at[z, b])

    for i in range(1, NBLK):
        each(i, put)
        if 1 < i <= NA:
            for c in copies(i - 1):
                c.start()
    core = lax.rem(lax.axis_index('sp'), 2)
    for n in range(WSPLIT, 4):
        out_weight_copy(n, core, wo, wo_v, wosem).start()
    nkv_copy = pltpu.make_async_copy(nkv_s, nkv, osem.at[1])
    nkv_copy.start()
    each(0, stage)
    for i in range(NX):
        last_merge(lax.axis_index('sp') // 2, comb_a, xrx, i, oa, i)
    for c in copies(0):
        c.wait()
    each(0, lambda b, z, base, mask, ref, out: patch_copy(b, z, base, out).start())
    nkv_copy.wait()
    each(0, lambda b, z, base, mask, ref, out: patch_copy(b, z, base, out).wait())
    for i in range(1, NA):
        for c in copies(i):
            c.wait()
    for n in range(WSPLIT, 4):
        out_weight_copy(n, core, wo, wo_v, wosem).wait()


def solution(mesh):
    cache_spec = P('dp', 'sp', None, None)
    inv_freq = (np.float64(ROPE_THETA) ** (-np.arange(HD // 2) * 2.0 / HD)).astype(np.float32)
    freq2 = np.concatenate([inv_freq, inv_freq])
    vm = pl.BlockSpec(memory_space=pltpu.VMEM)
    hbm = pl.BlockSpec(memory_space=pl.ANY)
    dma = pltpu.SemaphoreType.DMA

    def device_step(tokens, positions, k_cache, v_cache, w_q, w_k, w_v, w_o, attn_norm, q_norm, k_norm):
        in_hbm = lambda x: pltpu.with_memory_space_constraint(x, pltpu.HBM)
        in_vmem = lambda x: pltpu.with_memory_space_constraint(x, pltpu.VMEM)
        rows = (SEQS, ROWS, HD)
        piece = (PIECE, HD)
        kv, vv, rep, wo_v, comb_a, comb_b, xrx_a = pl.pallas_call(
            attend_kernel,
            out_shape=(pltpu.VMEM(rows, BF16), pltpu.VMEM(rows, BF16),
                       pltpu.VMEM((2, SEQS * KVH, HD), F32), pltpu.VMEM((4, HALF * HD, WCH), BF16),
                       pltpu.VMEM((NX,) + piece, F32), pltpu.VMEM((NBLK - NX,) + piece, F32), pltpu.VMEM((NX,) + piece, F32)),
            in_specs=[hbm] * 12,
            out_specs=(vm,) * 7,
            scratch_shapes=[
                pltpu.SMEM((SEQS,), jnp.int32), pltpu.VMEM((SEQS, DIM), BF16), pltpu.VMEM((DIM // HD, HD), BF16),
                pltpu.VMEM((1, HD), BF16), pltpu.VMEM((1, HD), BF16), pltpu.VMEM((1, HD), F32), dma((6,)),
                pltpu.VMEM((2, SEQS, WCH), F32),
                pltpu.VMEM((RING, DIM, WCH), BF16),
                pltpu.VMEM((SEQS, DIM), BF16),
                pltpu.VMEM((SEQS, HD), F32), pltpu.VMEM((SEQS, HD), F32), pltpu.VMEM((SEQS, HD), F32),
                pltpu.VMEM((2, SEQS * 8, HD), F32), pltpu.VMEM((2, SEQS * 8, HD), F32),
                pltpu.VMEM((2 * HALF, ROWS), jnp.int32),
                pltpu.VMEM((NBLK, 2 * PIECE, HD), F32),
                pltpu.VMEM((NBLK,) + piece, F32),
                pltpu.VMEM((2, 4 * HALF, ROWS), F32), pltpu.VMEM((2, 4 * HALF, ROWS), BF16),
                dma((NW,)), dma((NBLK,)), dma((NBLK,)), dma((4,)), dma((3,)), dma((3,)),
                dma((NBLK,)), dma((NBLK,)), dma((NX,)), dma((NX,)),
            ],
            compiler_params=pltpu.CompilerParams(collective_id=0, has_side_effects=True, vmem_limit_bytes=VMEM_LIMIT),
            name='attend',
        )(in_hbm(positions), in_hbm(tokens), in_hbm(attn_norm.reshape(DIM // HD, HD)), in_hbm(q_norm.reshape(1, HD)),
          in_hbm(k_norm.reshape(1, HD)), in_hbm(jnp.asarray(freq2).reshape(1, HD)), in_hbm(w_q), in_hbm(w_k), in_hbm(w_v), in_hbm(w_o),
          in_hbm(k_cache.reshape(rows)), in_hbm(v_cache.reshape(rows)))
        xrx_b = lax.ppermute(comb_b, 'sp', [(0, 2), (2, 0), (1, 3), (3, 1)])
        k_out, v_out, new_kv, oa, kv, vv, wo_v = pl.pallas_call(
            write_kernel,
            out_shape=(pltpu.HBM(rows, BF16), pltpu.HBM(rows, BF16), pltpu.HBM((SEQS, 2 * KVH, HD), BF16),
                       pltpu.VMEM((NX * BLK, HALF * HD), F32), pltpu.VMEM(rows, BF16), pltpu.VMEM(rows, BF16),
                       pltpu.VMEM((4, HALF * HD, WCH), BF16)),
            in_specs=[hbm, vm, vm, vm, vm, vm, vm, hbm],
            out_specs=(hbm, hbm, hbm, vm, vm, vm, vm),
            input_output_aliases={1: 4, 2: 5, 6: 6},
            scratch_shapes=[pltpu.SMEM((SEQS,), jnp.int32), pltpu.VMEM((SEQS, 2 * KVH, HD), BF16),
                            pltpu.VMEM((2, BLK, 4 * KVH, HD), BF16),
                            dma((NBLK,)), dma((NBLK,)), dma((2, BLK)), dma((2,)), dma((4,))],
            compiler_params=pltpu.CompilerParams(vmem_limit_bytes=VMEM_LIMIT),
            cost_estimate=pl.CostEstimate(flops=10**10, bytes_accessed=2**25, transcendentals=0),
            name='write',
        )(in_hbm(positions), in_vmem(kv), in_vmem(vv), in_vmem(rep), in_vmem(comb_a), in_vmem(xrx_a), in_vmem(wo_v), in_hbm(w_o))
        k_out, v_out, part = pl.pallas_call(
            product_kernel,
            out_shape=(pltpu.HBM(rows, BF16), pltpu.HBM(rows, BF16), pltpu.VMEM((SEQS, DIM), F32)),
            in_specs=[vm, vm, hbm, hbm, vm, vm, vm, vm],
            out_specs=(hbm, hbm, vm),
            input_output_aliases={2: 0, 3: 1},
            scratch_shapes=[pltpu.VMEM(((NBLK - NX) * BLK, HALF * HD), F32), dma((NBLK,)), dma((NBLK,))],
            compiler_params=pltpu.CompilerParams(vmem_limit_bytes=VMEM_LIMIT),
            cost_estimate=pl.CostEstimate(flops=2 * SEQS * DIM * DIM, bytes_accessed=2**22, transcendentals=0),
            name='product',
        )(in_vmem(kv), in_vmem(vv), k_out, v_out, in_vmem(oa), in_vmem(comb_b), in_vmem(xrx_b), in_vmem(wo_v))
        other = lax.ppermute(part, 'sp', [(0, 1), (1, 0), (2, 3), (3, 2)])
        k_out, v_out = pl.pallas_call(
            rest_kernel,
            out_shape=(pltpu.HBM(rows, BF16), pltpu.HBM(rows, BF16)),
            in_specs=[vm, vm, hbm, hbm],
            out_specs=(hbm, hbm),
            input_output_aliases={2: 0, 3: 1},
            scratch_shapes=[dma((NBLK,)), dma((NBLK,))],
            compiler_params=pltpu.CompilerParams(vmem_limit_bytes=VMEM_LIMIT),
            cost_estimate=pl.CostEstimate(flops=10**9, bytes_accessed=2**22, transcendentals=0),
            name='rest',
        )(in_vmem(kv), in_vmem(vv), k_out, v_out)
        block_out = (tokens.astype(F32) + (part + other)).astype(BF16)
        return block_out, k_out.reshape(k_cache.shape), v_out.reshape(v_cache.shape), new_kv.reshape(SEQS, 2, KVH, HD)

    return jax.shard_map(device_step, mesh=mesh, in_specs=(P('dp', None), P('dp'), cache_spec, cache_spec, P(), P(), P(), P(), P(), P(), P()), out_specs=(P('dp', None), cache_spec, cache_spec, P('dp', None, None, None)), check_vma=False)
```

```python
import functools

import jax
import jax.numpy as jnp
import numpy as np
from jax import lax
from jax.experimental import pallas as pl
from jax.experimental.pallas import tpu as pltpu
from jax.sharding import PartitionSpec as P

NORM_EPS = 1e-6
ROPE_THETA = 1000000.0
MESH = pl.DeviceIdType.MESH
BF16 = jnp.bfloat16
F32 = jnp.float32

SEQS = 64
DIM = 2048
HD = 128
KVH = 4
HALF = 16
SLOTS = 256
ROWS = SLOTS * KVH
BLK = 8
NBLK = SEQS // BLK
AHEAD = 6
NX = 4
NA = 6
WSPLIT = 4
NW = 5
WAHEAD = 3
RING = 4
LAG = 2
WCH = 512
PIECE = (HALF + 1) * BLK
VMEM_LIMIT = 14 * 2**20
EXP_SCALE = HD ** -0.5 * 1.4426950408889634
NEG = -jnp.inf


def bcast_col(tile, col):
    return jnp.broadcast_to(tile[:, col:col + 1], (tile.shape[0], HD))


def out_weight_copy(n, core, wo, wo_v, wosem):
    src = wo.at[pl.ds(pl.multiple_of(core * (HALF * HD), HD), HALF * HD), pl.ds(n * WCH, WCH)]
    return pltpu.make_async_copy(src, wo_v.at[n], wosem.at[n])


def attend_kernel(pos_h, tok_h, an_h, qn_h, kn_h, freq_h, wq, wk, wv, wo, kc, vc,
                  kv, vv, rep, wo_v, comb_a, comb_b, xrx,
                  pos_s, tok, an, qn, kn, freq, insem, proj, w_s, hid, ang, cosr, sinr, qmine, qmate, colslot, opart, drx, sc, pr_s,
                  wsem, ksem, vsem, wosem, qs, qr, ds_, dr, xs, xr):
    me = lax.axis_index('sp')
    core = lax.rem(me, 2)
    chip = me // 2
    mate = {'sp': me + 1 - 2 * core}
    peer = {'sp': me + 2 - 4 * chip}

    def w_copy(n, src=None):
        if n < 4:
            src = wq.at[:, pl.ds(pl.multiple_of(core * (HALF * HD) + n * WCH, WCH), WCH)]
        return pltpu.make_async_copy(src, w_s.at[n % RING], wsem.at[n])

    def w_start(n):
        if n < 4:
            w_copy(n).start()
        else:
            @pl.when(core == 0)
            def _():
                w_copy(n, wk).start()

            @pl.when(core == 1)
            def _():
                w_copy(n, wv).start()

    def wo_copy(n):
        return out_weight_copy(n, core, wo, wo_v, wosem)

    def k_copy(i):
        return pltpu.make_async_copy(kc.at[pl.ds(i * BLK, BLK)], kv.at[pl.ds(i * BLK, BLK)], ksem.at[i])

    def v_copy(i):
        return pltpu.make_async_copy(vc.at[pl.ds(i * BLK, BLK)], vv.at[pl.ds(i * BLK, BLK)], vsem.at[i])

    def q_send(h):
        return pltpu.make_async_remote_copy(qmine.at[h], qmate.at[h], qs.at[h], qr.at[h], device_id=mate, device_id_type=MESH)

    def new_send():
        return pltpu.make_async_remote_copy(rep.at[core], rep.at[core], qs.at[2], qr.at[2], device_id=mate, device_id_type=MESH)

    def d_send(i):
        return pltpu.make_async_remote_copy(opart.at[i, pl.ds(PIECE, PIECE)], drx.at[i], ds_.at[i], dr.at[i],
                                            device_id=mate, device_id_type=MESH)

    def x_send(i):
        return pltpu.make_async_remote_copy(comb_a.at[i], xrx.at[i], xs.at[i], xr.at[i],
                                            device_id=peer, device_id_type=MESH)

    small = [pltpu.make_async_copy(a, b, insem.at[z]) for z, (a, b) in enumerate(
        ((tok_h, tok), (an_h, an), (pos_h, pos_s), (qn_h, qn), (kn_h, kn), (freq_h, freq)))]
    for c in small:
        c.start()
    for n in range(WAHEAD):
        w_start(n)

    barrier = pltpu.get_barrier_semaphore()
    for other in (mate, peer):
        pl.semaphore_signal(barrier, inc=1, device_id=other, device_id_type=MESH)

    small[0].wait()
    small[1].wait()
    t = tok[...].astype(F32)
    inv = lax.rsqrt(jnp.sum(t * t, axis=-1, keepdims=True) * (1.0 / DIM) + NORM_EPS)
    gains = an[...].astype(F32)
    for j in range(DIM // HD):
        sl = slice(j * HD, (j + 1) * HD)
        hid[:, sl] = (tok[:, sl].astype(F32) * inv * gains[j:j + 1, :]).astype(BF16)

    def tables():
        for c in small[2:]:
            c.wait()
        lane1 = lax.broadcasted_iota(jnp.int32, (1, HD), 1)

        def angle(b, carry):
            ang[pl.ds(b, 1), :] = freq[...] * pos_s[b].astype(F32)
            return carry

        lax.fori_loop(0, SEQS, angle, 0, unroll=8)
        cosr[...] = jnp.cos(ang[...])
        sinr[...] = jnp.sin(ang[...]) * jnp.where(lane1 < HD // 2, -1.0, 1.0)

        row = lax.broadcasted_iota(jnp.int32, (2 * HALF, ROWS), 0)
        col = lax.broadcasted_iota(jnp.int32, (2 * HALF, ROWS), 1)
        half_of_row = jnp.where(row < HALF, core, 1 - core)
        kv_of_row = half_of_row * 2 + lax.rem(row, HALF) // 8
        colslot[...] = jnp.where(lax.rem(col, KVH) == kv_of_row, col // KVH, 1 << 20)

    def norm_rope(x, gain):
        y = x * lax.rsqrt(jnp.mean(x * x, axis=-1, keepdims=True) + NORM_EPS) * gain
        y = y * cosr[...] + pltpu.roll(y, HD // 2, 1) * sinr[...]
        return y.astype(BF16).astype(F32)

    def post(n):
        for j in range(WCH // HD):
            x = proj[n % 2, :, j * HD:(j + 1) * HD].astype(BF16).astype(F32)
            if n < 4:
                qmine.at[n // 2][pl.ds(n % 2 * 4 + j, SEQS, stride=8), :] = norm_rope(x, qgain)
            else:
                rep.at[core][pl.ds(j, SEQS, stride=KVH), :] = jnp.where(core == 0, norm_rope(x, kgain), x)

    def cache_start(t):
        (v_copy if t % 2 else k_copy)(t // 2).start()

    def multiply(n):
        w_copy(n, wk).wait()
        if n + WAHEAD < NW:
            w_start(n + WAHEAD)
        else:
            cache_start(n + WAHEAD - NW)
        proj[n % 2] = jnp.dot(hid[...], w_s[n % RING], preferred_element_type=F32)

    multiply(0)
    tables()
    qgain = qn[...].astype(F32)
    kgain = kn[...].astype(F32)
    multiply(1)
    post(0)
    multiply(2)
    post(1)
    pl.semaphore_wait(barrier, 2)
    q_send(0).start()
    multiply(3)
    post(2)
    post(3)
    q_send(1).start()
    multiply(4)
    cache_start(WAHEAD)
    cache_start(WAHEAD + 1)
    post(4)
    new_send().start()
    for t in range(WAHEAD + 2, 2 * 4):
        cache_start(t)
    start = me * SLOTS
    lane = lax.broadcasted_iota(jnp.int32, (HALF, HD), 1)
    lrow = lax.broadcasted_iota(jnp.int32, (HALF, HD), 0)
    lane8 = lax.broadcasted_iota(jnp.int32, (BLK, HD), 1)
    for h in range(2):
        q_send(h).wait()

    def attend(i, first=False):
        ob = opart.at[i]
        def load_q(pair, at):
            bs = [at * BLK + 2 * pair + z for z in range(2)]
            return bs, [jnp.concatenate([ref[h, pl.ds(pl.multiple_of(b * 8, 8), 8), :]
                                         for ref in (qmine, qmate) for h in range(2)], axis=0) for b in bs]

        def new_rows(z, b):
            return jnp.concatenate([jnp.broadcast_to(rep[z, pl.ds(b * KVH + h, 1), :], (8, HD))
                                    for h in (2 * core, 2 * core + 1, 2 - 2 * core, 3 - 2 * core)], axis=0)

        def scores(pair, at):
            bs, qf = load_q(pair, at)
            zero = jnp.zeros((2 * HALF, HD), BF16)
            lhs = jnp.concatenate([jnp.concatenate([qf[0].astype(BF16), zero], axis=1),
                                   jnp.concatenate([zero, qf[1].astype(BF16)], axis=1)], axis=0)
            keys = jnp.concatenate([kv[bs[0]], kv[bs[1]]], axis=1)
            sc[pair % 2] = lax.dot_general(lhs, keys, (((1,), (1,)), ((), ())), preferred_element_type=F32)

        def soft(pair):
            bs, qf = load_q(pair, i)
            out = []
            for z in range(2):
                b = bs[z]
                rel = pos_s[b] - start
                owner = jnp.logical_and(rel >= 0, rel < SLOTS)
                snew = jnp.where(owner, jnp.sum(qf[z] * new_rows(0, b), axis=-1, keepdims=True), NEG)
                sm = jnp.where(colslot[...] < rel, sc[pair % 2, z * 2 * HALF:(z + 1) * 2 * HALF], NEG)
                peak = jnp.maximum(jnp.max(sm, axis=-1, keepdims=True), snew)
                safe = jnp.where(peak == NEG, 0.0, peak)
                p = jnp.exp2((sm - safe) * EXP_SCALE)
                pn = jnp.exp2((snew - safe) * EXP_SCALE)
                pr_s[pair % 2, z * 2 * HALF:(z + 1) * 2 * HALF, :] = p.astype(BF16)
                out.append((pn.astype(BF16).astype(F32), jnp.sum(p, axis=-1, keepdims=True) + pn, peak))
            return out

        def mix(pair, st3):
            bs = [i * BLK + 2 * pair + z for z in range(2)]
            values = jnp.concatenate([vv[bs[0]], vv[bs[1]]], axis=1)
            mixed = jnp.dot(pr_s[pair % 2], values, preferred_element_type=F32)
            for z in range(2):
                extra, total, peak = st3[z]
                o = mixed[z * 2 * HALF:(z + 1) * 2 * HALF, z * HD:(z + 1) * HD] + extra * new_rows(1, bs[z])
                bb = 2 * pair + z
                for h in range(2):
                    hs = slice(h * HALF, (h + 1) * HALF)
                    ob[pl.ds(h * PIECE + bb, HALF, stride=BLK), :] = o[hs]
                    st = jnp.where(lane == lrow, peak[hs], jnp.where(lane == lrow + HALF, total[hs], 0.0))
                    ob[pl.ds(h * PIECE + HALF * BLK + bb, 1), :] = jnp.sum(st, axis=0, keepdims=True)

        if first:
            scores(0, i)
            return
        for pair in range(BLK // 2):
            if pair + 1 < BLK // 2:
                scores(pair + 1, i)
            else:
                scores(0, jnp.minimum(i + 1, NBLK - 1))
            mix(pair, soft(pair))

    def combine(i, comb, at):
        s0 = opart[i, pl.ds(HALF * BLK, BLK), :]
        s1 = drx[i, pl.ds(HALF * BLK, BLK), :]
        peak = jnp.maximum(s0, s1)
        safe = jnp.where(peak == NEG, 0.0, peak)
        f0 = jnp.exp2((s0 - safe) * EXP_SCALE)
        f1 = jnp.exp2((s1 - safe) * EXP_SCALE)
        total = f0 * pltpu.roll(s0, HD - HALF, 1) + f1 * pltpu.roll(s1, HD - HALF, 1)
        comb[at, pl.ds(HALF * BLK, BLK), :] = jnp.where(
            lane8 < HALF, peak, jnp.where(lane8 < 2 * HALF, pltpu.roll(total, HALF, 1), 0.0))
        for j in range(HALF):
            rows = pl.ds(j * BLK, BLK)
            comb[at, rows, :] = bcast_col(f0, j) * opart[i, rows, :] + bcast_col(f1, j) * drx[i, rows, :]

    def fetch(i):
        @pl.when(i + 1 < NBLK)
        def _():
            k_copy(i + 1).wait()

        v_copy(i).wait()

        @pl.when(i + AHEAD < NBLK)
        def _():
            k_copy(i + AHEAD).start()
            v_copy(i + AHEAD).start()

        @pl.when(i == NBLK - 4)
        def _():
            for n in range(WSPLIT):
                wo_copy(n).start()

    def early(i, carry):
        fetch(i)
        attend(i)
        d_send(i).start()
        return carry

    def sending(i, carry):
        fetch(i)
        attend(i)
        d_send(i).start()
        d_send(i - 1).wait_recv()
        combine(i - 1, comb_a, i - 1)
        x_send(i - 1).start()
        return carry

    def keeping(i, carry):
        fetch(i)
        d_send(i - LAG).wait_recv()
        combine(i - LAG, comb_b, i - LAG - NX)
        attend(i)
        d_send(i).start()
        return carry

    def late(i, carry):
        d_send(i).wait_recv()
        combine(i, comb_b, i - NX)
        return carry

    k_copy(0).wait()
    attend(0, first=True)
    new_send().wait()
    for t in range(2 * 4, 2 * AHEAD):
        cache_start(t)
    early(0, 0)
    lax.fori_loop(1, 1 + NX, sending, 0)
    lax.fori_loop(1 + NX, LAG + NX, early, 0)
    lax.fori_loop(LAG + NX, NBLK, keeping, 0)
    lax.fori_loop(NBLK - LAG, NBLK, late, 0)

    for n in range(WSPLIT):
        wo_copy(n).wait()

    def drain(i, carry):
        d_send(i).wait_send()
        return carry

    def drain_x(i, carry):
        x_send(i).wait()
        return carry

    lax.fori_loop(0, NBLK, drain, 0)
    lax.fori_loop(0, NX, drain_x, 0)


def last_merge(chip, comb, other_ref, i, ofin, at):
    first = chip == 0

    def ordered(rows):
        mine, other = comb[i, rows, :], other_ref[i, rows, :]
        return jnp.where(first, mine, other), jnp.where(first, other, mine)

    s0, s1 = ordered(pl.ds(HALF * BLK, BLK))
    peak = jnp.maximum(s0, s1)
    f0 = jnp.exp2((s0 - peak) * EXP_SCALE)
    f1 = jnp.exp2((s1 - peak) * EXP_SCALE)
    total = f0 * pltpu.roll(s0, HD - HALF, 1) + f1 * pltpu.roll(s1, HD - HALF, 1)
    g0, g1 = f0 / total, f1 / total
    for j in range(HALF):
        a, b = ordered(pl.ds(j * BLK, BLK))
        ofin[at * BLK:(at + 1) * BLK, j * HD:(j + 1) * HD] = bcast_col(g0, j) * a + bcast_col(g1, j) * b


def block_copies(i, kv, vv, ko, vo, ksem, vsem):
    r = pl.ds(i * BLK, BLK)
    return (pltpu.make_async_copy(kv.at[r], ko.at[r], ksem.at[i]),
            pltpu.make_async_copy(vv.at[r], vo.at[r], vsem.at[i]))


def product_kernel(kv, vv, ki, vi, oa, comb_b, xrx_b, wo_v, ko, vo, part, ofin, ksem, vsem):
    for c in block_copies(NA, kv, vv, ko, vo, ksem, vsem):
        c.start()
    for i in range(NBLK - NX):
        last_merge(lax.axis_index('sp') // 2, comb_b, xrx_b, i, ofin, i)
    lhs = jnp.concatenate([oa[...].astype(BF16), ofin[...].astype(BF16)], axis=0)
    for n in range(4):
        part[:, n * WCH:(n + 1) * WCH] = jnp.dot(lhs, wo_v[n], preferred_element_type=F32)
    for c in block_copies(NA, kv, vv, ko, vo, ksem, vsem):
        c.wait()


def rest_kernel(kv, vv, ki, vi, ko, vo, ksem, vsem):
    for c in block_copies(NA + 1, kv, vv, ko, vo, ksem, vsem):
        c.start()
    for c in block_copies(NA + 1, kv, vv, ko, vo, ksem, vsem):
        c.wait()


def write_kernel(pos_h, kv, vv, rep, comb_a, xrx, wo_v, wo, ko, vo, nkv, oa, kva, vva, wo_a, pos_s, nkv_s, patch, ksem, vsem, psem, osem, wosem):
    start = lax.axis_index('sp') * SLOTS
    slot16 = lax.broadcasted_iota(jnp.int32, (4 * KVH, HD), 0) // KVH

    def copies(i):
        return block_copies(i, kv, vv, ko, vo, ksem, vsem)

    pos_copy = pltpu.make_async_copy(pos_h, pos_s, osem.at[0])
    pos_copy.start()
    for c in copies(0):
        c.start()
    for b in range(SEQS):
        nkv_s[b] = jnp.concatenate([rep[0, pl.ds(b * KVH, KVH), :], rep[1, pl.ds(b * KVH, KVH), :]], axis=0).astype(BF16)
    pos_copy.wait()

    def each(i, do):
        for bb in range(BLK):
            b = i * BLK + bb
            rel = pos_s[b] - start

            @pl.when(jnp.logical_and(rel >= 0, rel < SLOTS))
            def _():
                base = pl.multiple_of(rel // 4 * (4 * KVH), 4 * KVH)
                mask = slot16 == lax.rem(rel, 4)
                for z, (ref, out) in enumerate(((kv, ko), (vv, vo))):
                    do(b, z, base, mask, ref, out)

    def merged(b, z, base, mask, ref):
        new = jnp.concatenate([rep[z, pl.ds(b * KVH, KVH), :]] * 4, axis=0)
        old = ref[b, pl.ds(base, 4 * KVH), :].astype(F32)
        return jnp.where(mask, new, old).astype(BF16)

    def put(b, z, base, mask, ref, out):
        ref[b, pl.ds(base, 4 * KVH), :] = merged(b, z, base, mask, ref)

    def stage(b, z, base, mask, ref, out):
        patch[z, b] = merged(b, z, base, mask, ref)

    def patch_copy(b, z, base, out):
        return pltpu.make_async_copy(patch.at[z, b], out.at[b, pl.ds(base, 4 * KVH)], psem.at[z, b])

    for i in range(1, NBLK):
        each(i, put)
        if 1 < i <= NA:
            for c in copies(i - 1):
                c.start()
    core = lax.rem(lax.axis_index('sp'), 2)
    for n in range(WSPLIT, 4):
        out_weight_copy(n, core, wo, wo_v, wosem).start()
    nkv_copy = pltpu.make_async_copy(nkv_s, nkv, osem.at[1])
    nkv_copy.start()
    each(0, stage)
    for i in range(NX):
        last_merge(lax.axis_index('sp') // 2, comb_a, xrx, i, oa, i)
    for c in copies(0):
        c.wait()
    each(0, lambda b, z, base, mask, ref, out: patch_copy(b, z, base, out).start())
    nkv_copy.wait()
    each(0, lambda b, z, base, mask, ref, out: patch_copy(b, z, base, out).wait())
    for i in range(1, NA):
        for c in copies(i):
            c.wait()
    for n in range(WSPLIT, 4):
        out_weight_copy(n, core, wo, wo_v, wosem).wait()


def solution(mesh):
    cache_spec = P('dp', 'sp', None, None)
    inv_freq = (np.float64(ROPE_THETA) ** (-np.arange(HD // 2) * 2.0 / HD)).astype(np.float32)
    freq2 = np.concatenate([inv_freq, inv_freq])
    vm = pl.BlockSpec(memory_space=pltpu.VMEM)
    hbm = pl.BlockSpec(memory_space=pl.ANY)
    dma = pltpu.SemaphoreType.DMA

    def device_step(tokens, positions, k_cache, v_cache, w_q, w_k, w_v, w_o, attn_norm, q_norm, k_norm):
        in_hbm = lambda x: pltpu.with_memory_space_constraint(x, pltpu.HBM)
        in_vmem = lambda x: pltpu.with_memory_space_constraint(x, pltpu.VMEM)
        rows = (SEQS, ROWS, HD)
        piece = (PIECE, HD)
        kv, vv, rep, wo_v, comb_a, comb_b, xrx_a = pl.pallas_call(
            attend_kernel,
            out_shape=(pltpu.VMEM(rows, BF16), pltpu.VMEM(rows, BF16),
                       pltpu.VMEM((2, SEQS * KVH, HD), F32), pltpu.VMEM((4, HALF * HD, WCH), BF16),
                       pltpu.VMEM((NX,) + piece, F32), pltpu.VMEM((NBLK - NX,) + piece, F32), pltpu.VMEM((NX,) + piece, F32)),
            in_specs=[hbm] * 12,
            out_specs=(vm,) * 7,
            scratch_shapes=[
                pltpu.SMEM((SEQS,), jnp.int32), pltpu.VMEM((SEQS, DIM), BF16), pltpu.VMEM((DIM // HD, HD), BF16),
                pltpu.VMEM((1, HD), BF16), pltpu.VMEM((1, HD), BF16), pltpu.VMEM((1, HD), F32), dma((6,)),
                pltpu.VMEM((2, SEQS, WCH), F32),
                pltpu.VMEM((RING, DIM, WCH), BF16),
                pltpu.VMEM((SEQS, DIM), BF16),
                pltpu.VMEM((SEQS, HD), F32), pltpu.VMEM((SEQS, HD), F32), pltpu.VMEM((SEQS, HD), F32),
                pltpu.VMEM((2, SEQS * 8, HD), F32), pltpu.VMEM((2, SEQS * 8, HD), F32),
                pltpu.VMEM((2 * HALF, ROWS), jnp.int32),
                pltpu.VMEM((NBLK, 2 * PIECE, HD), F32),
                pltpu.VMEM((NBLK,) + piece, F32),
                pltpu.VMEM((2, 4 * HALF, ROWS), F32), pltpu.VMEM((2, 4 * HALF, ROWS), BF16),
                dma((NW,)), dma((NBLK,)), dma((NBLK,)), dma((4,)), dma((3,)), dma((3,)),
                dma((NBLK,)), dma((NBLK,)), dma((NX,)), dma((NX,)),
            ],
            compiler_params=pltpu.CompilerParams(collective_id=0, has_side_effects=True, vmem_limit_bytes=VMEM_LIMIT),
            name='attend',
        )(in_hbm(positions), in_hbm(tokens), in_hbm(attn_norm.reshape(DIM // HD, HD)), in_hbm(q_norm.reshape(1, HD)),
          in_hbm(k_norm.reshape(1, HD)), in_hbm(jnp.asarray(freq2).reshape(1, HD)), in_hbm(w_q), in_hbm(w_k), in_hbm(w_v), in_hbm(w_o),
          in_hbm(k_cache.reshape(rows)), in_hbm(v_cache.reshape(rows)))
        xrx_b = lax.ppermute(comb_b, 'sp', [(0, 2), (2, 0), (1, 3), (3, 1)])
        k_out, v_out, new_kv, oa, kv, vv, wo_v = pl.pallas_call(
            write_kernel,
            out_shape=(pltpu.HBM(rows, BF16), pltpu.HBM(rows, BF16), pltpu.HBM((SEQS, 2 * KVH, HD), BF16),
                       pltpu.VMEM((NX * BLK, HALF * HD), F32), pltpu.VMEM(rows, BF16), pltpu.VMEM(rows, BF16),
                       pltpu.VMEM((4, HALF * HD, WCH), BF16)),
            in_specs=[hbm, vm, vm, vm, vm, vm, vm, hbm],
            out_specs=(hbm, hbm, hbm, vm, vm, vm, vm),
            input_output_aliases={1: 4, 2: 5, 6: 6},
            scratch_shapes=[pltpu.SMEM((SEQS,), jnp.int32), pltpu.VMEM((SEQS, 2 * KVH, HD), BF16),
                            pltpu.VMEM((2, BLK, 4 * KVH, HD), BF16),
                            dma((NBLK,)), dma((NBLK,)), dma((2, BLK)), dma((2,)), dma((4,))],
            compiler_params=pltpu.CompilerParams(vmem_limit_bytes=VMEM_LIMIT),
            cost_estimate=pl.CostEstimate(flops=10**10, bytes_accessed=2**25, transcendentals=0),
            name='write',
        )(in_hbm(positions), in_vmem(kv), in_vmem(vv), in_vmem(rep), in_vmem(comb_a), in_vmem(xrx_a), in_vmem(wo_v), in_hbm(w_o))
        k_out, v_out, part = pl.pallas_call(
            product_kernel,
            out_shape=(pltpu.HBM(rows, BF16), pltpu.HBM(rows, BF16), pltpu.VMEM((SEQS, DIM), F32)),
            in_specs=[vm, vm, hbm, hbm, vm, vm, vm, vm],
            out_specs=(hbm, hbm, vm),
            input_output_aliases={2: 0, 3: 1},
            scratch_shapes=[pltpu.VMEM(((NBLK - NX) * BLK, HALF * HD), F32), dma((NBLK,)), dma((NBLK,))],
            compiler_params=pltpu.CompilerParams(vmem_limit_bytes=VMEM_LIMIT),
            cost_estimate=pl.CostEstimate(flops=2 * SEQS * DIM * DIM, bytes_accessed=2**22, transcendentals=0),
            name='product',
        )(in_vmem(kv), in_vmem(vv), k_out, v_out, in_vmem(oa), in_vmem(comb_b), in_vmem(xrx_b), in_vmem(wo_v))
        other = lax.ppermute(part, 'sp', [(0, 1), (1, 0), (2, 3), (3, 2)])
        k_out, v_out = pl.pallas_call(
            rest_kernel,
            out_shape=(pltpu.HBM(rows, BF16), pltpu.HBM(rows, BF16)),
            in_specs=[vm, vm, hbm, hbm],
            out_specs=(hbm, hbm),
            input_output_aliases={2: 0, 3: 1},
            scratch_shapes=[dma((NBLK,)), dma((NBLK,))],
            compiler_params=pltpu.CompilerParams(vmem_limit_bytes=VMEM_LIMIT),
            cost_estimate=pl.CostEstimate(flops=10**9, bytes_accessed=2**22, transcendentals=0),
            name='rest',
        )(in_vmem(kv), in_vmem(vv), k_out, v_out)
        block_out = (tokens.astype(F32) + (part + other)).astype(BF16)
        return block_out, k_out.reshape(k_cache.shape), v_out.reshape(v_cache.shape), new_kv.reshape(SEQS, 2, KVH, HD)

    return jax.shard_map(device_step, mesh=mesh, in_specs=(P('dp', None), P('dp'), cache_spec, cache_spec, P(), P(), P(), P(), P(), P(), P()), out_specs=(P('dp', None), cache_spec, cache_spec, P('dp', None, None, None)), check_vma=False)
```
